32 devices in a mesh: part: 1 (over z), row: 4 (over y), col: 4 (over x), dep: 2 (over core).
Axes of the slice: x: 4, y: 4, z: 1, core: 2. Of those that a mesh axis runs over, the one named last changes fastest.
The devices are a block of a 4x4x8 slice.
Arguments:
- x_in: bfloat16 [16384, 768], P(('part', 'row', 'col'), 'dep')
- ln_scale: float32 [768], P('dep')
- ln_shift: float32 [768], P('dep')
- w_up: bfloat16 [768, 3072], P(('dep', 'row'), 'col')
- b_up: bfloat16 [3072], P('col')
- w_down: bfloat16 [3072, 768], P(('col', 'row'), 'dep')
- b_down: bfloat16 [768], P('dep')
- y_grad: bfloat16 [16384, 768], P(('part', 'row', 'col'), 'dep')
Outputs:
- output 1: bfloat16 [16384, 768], P(('part', 'row', 'col'), 'dep')
- output 2: bfloat16 [16384, 768], P(('part', 'row', 'col'), 'dep')
- output 3: bfloat16 [768, 3072], P(('part', 'dep', 'row'), 'col')
- output 4: float32 [3072], P(('part', 'col'))
- output 5: bfloat16 [3072, 768], P(('part', 'col', 'row'), 'dep')
- output 6: float32 [768], P(('part', 'dep'))
- output 7: float32 [768], P(('part', 'dep'))
- output 8: float32 [768], P(('part', 'dep'))
All inputs are finite; a program needn't handle non-finite values.
Results may differ from the reference program's by a relative error of at most 0.00141.
Values are sent between devices in bfloat16 or wider.
A program may use at most 768 MiB of HBM per device.

```python
import jax
import jax.numpy as jnp
from jax import lax

TOKENS = 16384
D_MODEL = 768
D_FF = 3072

BLOCK_ROWS = min(TOKENS, 512)
N_BLOCKS = TOKENS // BLOCK_ROWS
LN_EPS = 1e-5
GELU_K = 0.7978845608028654
GELU_C = 0.044715
TWO_PI = 6.283185307179586


def setup_inputs(seed: int = 0, part: int = 0) -> dict:
    shared_root, part_root = jax.random.split(jax.random.key(seed))
    part_keys = jax.random.split(jax.random.fold_in(part_root, part), 4)
    shared_keys = jax.random.split(shared_root, 6)
    col_pos = jnp.arange(D_MODEL, dtype=jnp.float32) / D_MODEL
    col_phase = jax.random.uniform(part_keys[0], (), jnp.float32, 0.0, TWO_PI)
    col_mean = 1.5 * jnp.sin(TWO_PI * col_pos + col_phase) + 0.5 * jax.random.normal(part_keys[1], (D_MODEL,), jnp.float32)
    x_vals = jax.random.normal(part_keys[2], (TOKENS, D_MODEL), jnp.float32) + col_mean
    g_vals = jax.random.normal(part_keys[3], (TOKENS, D_MODEL), jnp.float32)
    return {
        "x_in": x_vals.astype(jnp.bfloat16),
        "ln_scale": 1.0 + 0.3 * jax.random.normal(shared_keys[0], (D_MODEL,), jnp.float32),
        "ln_shift": 0.5 * jax.random.normal(shared_keys[1], (D_MODEL,), jnp.float32),
        "w_up": (jax.random.normal(shared_keys[2], (D_MODEL, D_FF), jnp.float32) * D_MODEL ** -0.5).astype(jnp.bfloat16),
        "b_up": (0.5 * jax.random.normal(shared_keys[3], (D_FF,), jnp.float32)).astype(jnp.bfloat16),
        "w_down": (jax.random.normal(shared_keys[4], (D_FF, D_MODEL), jnp.float32) * D_FF ** -0.5).astype(jnp.bfloat16),
        "b_down": (0.5 * jax.random.normal(shared_keys[5], (D_MODEL,), jnp.float32)).astype(jnp.bfloat16),
        "y_grad": g_vals.astype(jnp.bfloat16),
    }


def gelu_tanh(pre_act):
    inner_arg = GELU_K * (pre_act + GELU_C * pre_act * (pre_act * pre_act))
    return 0.5 * pre_act * (1.0 + jnp.tanh(inner_arg))


def gelu_slope(pre_act):
    squared = pre_act * pre_act
    tanh_val = jnp.tanh(GELU_K * (pre_act + GELU_C * pre_act * squared))
    return 0.5 * (1.0 + tanh_val) + 0.5 * pre_act * (1.0 - tanh_val * tanh_val) * GELU_K * (1.0 + 3.0 * GELU_C * squared)


def block_pass(x_blk, g_blk, ln_scale, ln_shift, w_up, b_up, w_down, b_down):
    x_float = x_blk.astype(jnp.float32)
    mean_row = jnp.sum(x_float, axis=1, keepdims=True) / D_MODEL
    var_row = jnp.sum(x_float * x_float, axis=1, keepdims=True) / D_MODEL - mean_row * mean_row
    inv_std = lax.rsqrt(var_row + LN_EPS)
    x_hat = (x_float - mean_row) * inv_std
    normed = (x_hat * ln_scale + ln_shift).astype(jnp.bfloat16)
    pre_act = jnp.dot(normed, w_up, preferred_element_type=jnp.float32) + b_up.astype(jnp.float32)
    hidden = gelu_tanh(pre_act).astype(jnp.bfloat16)
    out_sum = jnp.dot(hidden, w_down, preferred_element_type=jnp.float32)
    y_blk = (x_float + out_sum + b_down.astype(jnp.float32)).astype(jnp.bfloat16)
    g_float = g_blk.astype(jnp.float32)
    w_down_part = jnp.dot(hidden.T, g_blk, preferred_element_type=jnp.float32)
    hid_grad = jnp.dot(g_blk, w_down.T, preferred_element_type=jnp.float32)
    pre_grad = hid_grad * gelu_slope(pre_act)
    pre_lowp = pre_grad.astype(jnp.bfloat16)
    w_up_part = jnp.dot(normed.T, pre_lowp, preferred_element_type=jnp.float32)
    norm_grad = jnp.dot(pre_lowp, w_up.T, preferred_element_type=jnp.float32)
    xhat_grad = norm_grad * ln_scale
    mean_one = jnp.sum(xhat_grad, axis=1, keepdims=True) / D_MODEL
    mean_two = jnp.sum(xhat_grad * x_hat, axis=1, keepdims=True) / D_MODEL
    dx_blk = (g_float + inv_std * (xhat_grad - mean_one - x_hat * mean_two)).astype(jnp.bfloat16)
    part_sums = (w_up_part, jnp.sum(pre_grad, axis=0), w_down_part, jnp.sum(g_float, axis=0), jnp.sum(norm_grad * x_hat, axis=0), jnp.sum(norm_grad, axis=0))
    return y_blk, dx_blk, part_sums


def reference(x_in, ln_scale, ln_shift, w_up, b_up, w_down, b_down, y_grad):
    x_blocks = x_in.reshape(N_BLOCKS, BLOCK_ROWS, D_MODEL)
    g_blocks = y_grad.reshape(N_BLOCKS, BLOCK_ROWS, D_MODEL)

    def scan_step(acc_sums, blk_pair):
        y_blk, dx_blk, part_sums = block_pass(blk_pair[0], blk_pair[1], ln_scale, ln_shift, w_up, b_up, w_down, b_down)
        new_sums = tuple(acc_val + add_val for acc_val, add_val in zip(acc_sums, part_sums))
        return new_sums, (y_blk, dx_blk)

    zero_sums = (jnp.zeros((D_MODEL, D_FF), jnp.float32), jnp.zeros((D_FF,), jnp.float32), jnp.zeros((D_FF, D_MODEL), jnp.float32), jnp.zeros((D_MODEL,), jnp.float32), jnp.zeros((D_MODEL,), jnp.float32), jnp.zeros((D_MODEL,), jnp.float32))
    total_sums, out_blocks = lax.scan(scan_step, zero_sums, (x_blocks, g_blocks))
    return (out_blocks[0].reshape(TOKENS, D_MODEL), out_blocks[1].reshape(TOKENS, D_MODEL), total_sums[0].astype(jnp.bfloat16), total_sums[1], total_sums[2].astype(jnp.bfloat16), total_sums[3], total_sums[4], total_sums[5])
```

```python
import functools

import jax
import jax.numpy as jnp
from jax import lax
from jax.experimental import pallas as pl
from jax.experimental.pallas import tpu as pltpu
from jax.sharding import PartitionSpec as P

LN_EPS = 1e-5
GELU_K = 0.7978845608028654
GELU_C = 0.044715
MESH = pl.DeviceIdType.MESH
F32 = jnp.float32
BF16 = jnp.bfloat16
RING = 4
PAD = 16

_next = [0]


def _ids(count=1):
    base = _next[0]
    _next[0] += count
    return base


IN_SEM = _ids(8)
ST = _ids(2)
DX, DG, DLN = _ids(), _ids(), _ids()
S1, S2, S3, S4, S5, S6 = (_ids() for _ in range(6))
M1, M2, M3, M4 = (_ids(RING) for _ in range(4))
M5, M6, MB1, MB2, MB3 = (_ids() for _ in range(5))
R1, R2, R5, R6 = (_ids(RING) for _ in range(4))
R3, R4 = _ids(), _ids()
Q1, Q2, Q3, Q4, Q5, Q6 = (_ids() for _ in range(6))
VM, VS = _ids(RING), _ids(RING)
VP = _ids()
EY, ED, ES = _ids(), _ids(), _ids()
FO = _ids(2)
N_SEM = _next[0]


def gray(t):
    return t + (t // 2) * (5 - 2 * t)


def split_halves(v, unit):
    lo = [v[:, 2 * k * unit:(2 * k + 1) * unit] for k in range(RING)]
    hi = [v[:, (2 * k + 1) * unit:(2 * k + 2) * unit] for k in range(RING)]
    return jnp.concatenate(lo, axis=1), jnp.concatenate(hi, axis=1)


def join_halves(lo, hi, unit):
    parts = []
    for k in range(RING):
        parts += [lo[:, k * unit:(k + 1) * unit], hi[:, k * unit:(k + 1) * unit]]
    return jnp.concatenate(parts, axis=1)


def dot(a, b, dims=((1,), (0,))):
    return lax.dot_general(a, b, (dims, ((), ())), preferred_element_type=F32)


def kernel(tile, x_hbm, sc_ref, sh_ref, w1_hbm, bu_ref, w2_hbm, bd_ref, g_hbm,
           y_hbm, dx_hbm, dw1_ref, dbu_ref, dw2_ref, dbd_ref, dsc_ref, dsh_ref,
           w1v, w2v, st, land, xf, gf, lnv, w1g, w2g, biasg, ab, gb, mean_s, inv_s,
           y_acc, da_acc, yr, dar, stat, statr, hs, dcs, gw1, gw2,
           opp1, opp2, dir1, dir2, rel1, rel2, s_opp1, s_opp2, s_dir1, s_dir2, s_rel1, s_rel2,
           vv, vm, vs, vp, fo, fland, yo, dxo, send, recv):
    r, c, e = lax.axis_index("row"), lax.axis_index("col"), lax.axis_index("dep")
    p = c + e * (r - c)
    q = r + e * (c - r)
    tokens, half = xf.shape[1], xf.shape[2]
    width = 2 * half
    unit = w2v.shape[0] // 2
    fb = RING * unit
    n_tiles = tokens // tile
    diag = r == c

    def wrap(v):
        return lax.rem(v + 2 * RING, RING)

    def dev(pp, qq):
        return {"row": qq + e * (pp - qq), "col": pp + e * (qq - pp), "dep": e}

    m_right, m_left, m_opp = dev(wrap(p + 1), q), dev(wrap(p - 1), q), dev(wrap(p + 2), q)
    s_right, s_left, s_opp = dev(p, wrap(q + 1)), dev(p, wrap(q - 1)), dev(p, wrap(q + 2))
    partner = {"row": r, "col": c, "dep": 1 - e}
    turned0 = {"row": c, "col": r, "dep": 0}
    turned1 = {"row": c, "col": r, "dep": 1}
    pr, pl_, po = wrap(p + 1), wrap(p - 1), wrap(p + 2)
    qr, ql, qo = wrap(q + 1), wrap(q - 1), wrap(q + 2)

    def rc(src, dst, ssem, device, rsem=None):
        return pltpu.make_async_remote_copy(
            src_ref=src, dst_ref=dst, send_sem=send.at[ssem], recv_sem=recv.at[ssem if rsem is None else rsem],
            device_id=device, device_id_type=MESH)

    def arrive(dst, rsem):
        rc(dst, dst, rsem, partner).wait_recv()

    def sent(src, ssem):
        rc(src, src, ssem, partner).wait_send()

    load_w1 = pltpu.make_async_copy(w1_hbm, w1v, recv.at[IN_SEM])
    load_w2 = pltpu.make_async_copy(w2_hbm, w2v, recv.at[IN_SEM + 1])
    load_x = pltpu.make_async_copy(x_hbm, xf.at[e], recv.at[IN_SEM + 2])
    load_g = pltpu.make_async_copy(g_hbm, gf.at[e], recv.at[IN_SEM + 3])
    load_w1.start()
    load_w2.start()
    load_x.start()
    load_g.start()

    barrier = pltpu.get_barrier_semaphore()
    for d in (m_right, m_left, s_right, s_left, m_opp, s_opp, partner, turned1):
        pl.semaphore_signal(barrier, inc=1, device_id=d, device_id_type=MESH)

    @pl.when(e == 1)
    def _():
        pl.semaphore_signal(barrier, inc=1, device_id=turned0, device_id_type=MESH)

    lnv[e, 0:1] = sc_ref[...]
    lnv[e, 1:2] = sh_ref[...]
    bias_lo, bias_hi = split_halves(bu_ref[...].astype(F32), unit)
    load_w1.wait()
    load_w2.wait()
    w_lo, w_hi = split_halves(w1v[...].astype(F32), unit)
    for h, (w_half, b_half) in enumerate(((w_lo, bias_lo), (w_hi, bias_hi))):
        st[h, 0:unit] = w_half.astype(BF16)
        st[h, unit:2 * unit] = w2v[h * unit:(h + 1) * unit]
        st[h, 2 * unit:2 * unit + PAD] = jnp.broadcast_to(b_half, (PAD, fb)).astype(BF16)

    pl.semaphore_wait(barrier, 8 + e)

    @pl.when(e == 0)
    def _():
        land[0] = st[0]
        rc(st.at[1], land.at[0], ST + 1, turned1, ST).start()

    @pl.when(e == 1)
    def _():
        rc(st.at[0], land.at[1], ST, partner, ST + 1).start()

        @pl.when(diag)
        def _():
            land[1] = st[1]

        @pl.when(jnp.logical_not(diag))
        def _():
            rc(st.at[1], land.at[1], ST + 1, turned1, ST + 1).start()

    rc(lnv.at[e], lnv.at[e], DLN, partner).start()
    rc(x_hbm, xf.at[e], DX, partner).start()
    rc(g_hbm, gf.at[e], DG, partner).start()

    @pl.when(e == 1)
    def _():
        arrive(land.at[0], ST)

        @pl.when(jnp.logical_not(diag))
        def _():
            arrive(land.at[1], ST + 1)

    @pl.when(e == 0)
    def _():
        arrive(land.at[1], ST + 1)

    w1g[p, 0, q] = land[0, 0:unit]
    w1g[p, 1, q] = land[1, 0:unit]
    w2g[p, q, :, 0:half] = land[0, unit:2 * unit]
    w2g[p, q, :, half:width] = land[1, unit:2 * unit]
    biasg[p] = land[0, 2 * unit:2 * unit + PAD]

    def w1u(b, s):
        return w1g.at[b, :, s]

    def w2u(b, s):
        return w2g.at[b, s]

    def go(ref, sem, device):
        rc(ref, ref, sem, device).start()

    go(w1u(p, q), M1, m_right)
    go(w2u(p, q), M2, m_left)
    go(w1u(p, q), S1, s_right)
    go(w2u(p, q), S4, s_left)
    go(w2u(p, q), S2, s_right)
    go(w1u(p, q), S3, s_left)
    go(biasg.at[p], MB1, m_right)
    go(biasg.at[p], MB2, m_left)

    arrive(lnv.at[1 - e], DLN)
    load_x.wait()
    arrive(xf.at[1 - e], DX)
    load_g.wait()
    arrive(gf.at[1 - e], DG)
    vv[...] = jnp.zeros_like(vv)

    def norm_tile(t, carry):
        rows = pl.ds(pl.multiple_of(t * tile, tile), tile)
        x0, x1 = xf[0, rows].astype(F32), xf[1, rows].astype(F32)
        total = jnp.sum(x0, axis=1, keepdims=True) + jnp.sum(x1, axis=1, keepdims=True)
        squares = jnp.sum(x0 * x0, axis=1, keepdims=True) + jnp.sum(x1 * x1, axis=1, keepdims=True)
        mean = total / width
        inv = lax.rsqrt(squares / width - mean * mean + LN_EPS)
        mean_s[rows] = mean
        inv_s[rows] = inv
        ab[rows, 0:half] = ((x0 - mean) * inv * lnv[0, 0:1] + lnv[0, 1:2]).astype(BF16)
        ab[rows, half:width] = ((x1 - mean) * inv * lnv[1, 0:1] + lnv[1, 1:2]).astype(BF16)
        gb[rows, 0:half] = gf[0, rows]
        gb[rows, half:width] = gf[1, rows]
        vv[RING:RING + 1] += jnp.sum(gf[e, rows].astype(F32), axis=0, keepdims=True)
        return carry

    lax.fori_loop(0, n_tiles, norm_tile, 0)

    arrive(w1u(p, ql), S1)
    go(w1u(p, ql), S5, s_right)
    go(w1u(p, ql), M1 + 1, m_right)
    arrive(w2u(p, qr), S4)
    go(w2u(p, qr), S6, s_left)
    go(w2u(p, qr), M2 + 1, m_left)
    arrive(w1u(p, qr), S3)
    go(w1u(p, qr), M1 + 2, m_right)
    arrive(w2u(p, ql), S2)
    go(w2u(p, ql), M2 + 2, m_left)
    arrive(w1u(p, qo), S5)
    go(w1u(p, qo), M1 + 3, m_right)
    arrive(w2u(p, qo), S6)
    go(w2u(p, qo), M2 + 3, m_left)

    def unit1(t):
        return wrap(q - gray(t))

    def unit2(t):
        return wrap(q + gray(t))

    def block(b, first, hook=None):
        bias = biasg[b, 0:1].astype(F32)

        def block_tile(t, carry):
            rows = pl.ds(pl.multiple_of(t * tile, tile), tile)
            w1 = w1g[b].reshape(width, fb)
            w2 = w2g[b].reshape(fb, width)
            pre = dot(ab[rows, :], w1) + bias
            squared = pre * pre
            tanh_val = jnp.tanh(GELU_K * (pre + GELU_C * pre * squared))
            hidden = (0.5 * pre * (1.0 + tanh_val)).astype(BF16)
            hs[rows, :] = hidden
            slope = 0.5 * (1.0 + tanh_val) + 0.5 * pre * (1.0 - tanh_val * tanh_val) * GELU_K * (1.0 + 3.0 * GELU_C * squared)
            pre_grad = dot(gb[rows, :], w2, ((1,), (1,))) * slope
            vv[pl.ds(b, 1)] += jnp.sum(pre_grad, axis=0, keepdims=True)
            lowp = pre_grad.astype(BF16)
            dcs[rows, :] = lowp
            out = dot(hidden, w2)
            back = dot(lowp, w1, ((1,), (1,)))
            if first:
                y_acc[0, rows] = out[:, 0:half]
                y_acc[1, rows] = out[:, half:width]
                da_acc[0, rows] = back[:, 0:half]
                da_acc[1, rows] = back[:, half:width]
            else:
                y_acc[0, rows] += out[:, 0:half]
                y_acc[1, rows] += out[:, half:width]
                da_acc[0, rows] += back[:, 0:half]
                da_acc[1, rows] += back[:, half:width]
            if hook is not None:
                hook(t)
            return carry

        lax.fori_loop(0, n_tiles, block_tile, 0)
        gw1[b] = dot(ab[...], dcs[...], ((0,), (0,))).reshape(2, RING, unit, fb)
        gw2[b] = dot(hs[...], gb[...], ((0,), (0,))).reshape(RING, unit, width)

    def relay_gather(t):
        u1, u2 = unit1(t), unit2(t)
        arrive(w1u(pl_, u1), M1 + t)
        go(w1u(pl_, u1), M3 + t, m_right)
        arrive(w2u(pr, u2), M2 + t)
        go(w2u(pr, u2), M4 + t, m_left)

    assert n_tiles == RING
    block(p, True, relay_gather)
    go(w2g.at[p], M5, m_right)
    go(w1g.at[p], M6, m_left)
    arrive(biasg.at[pl_], MB1)
    go(biasg.at[pl_], MB3, m_right)
    arrive(biasg.at[pr], MB2)

    arrive(biasg.at[po], MB3)
    for t in range(RING):
        arrive(w1u(po, unit1(t)), M3 + t)
        arrive(w2u(po, unit2(t)), M4 + t)
    block(po, False)

    def back1(t):
        return wrap(q + gray(RING - 1 - t))

    def back2(t):
        return wrap(q - gray(RING - 1 - t))

    for t in range(RING):
        u1, u2 = back1(t), back2(t)
        rc(gw1.at[po, :, u1], opp1.at[:, u1], R1 + t, m_right).start()
        rc(gw2.at[po, u2], opp2.at[u2], R2 + t, m_left).start()

    arrive(w1g.at[pr], M6)
    block(pr, False)
    rc(gw2.at[pr], dir2, R3, m_right).start()
    arrive(w2g.at[pl_], M5)
    block(pl_, False)
    rc(gw1.at[pl_], dir1, R4, m_left).start()

    lane = lax.broadcasted_iota(jnp.int32, (tile, 128), 1)

    def stat_tile(t, carry):
        rows = pl.ds(pl.multiple_of(t * tile, tile), tile)
        mean, inv = mean_s[rows], inv_s[rows]
        v0 = da_acc[0, rows] * lnv[0, 0:1]
        v1 = da_acc[1, rows] * lnv[1, 0:1]
        h0 = (xf[0, rows].astype(F32) - mean) * inv
        h1 = (xf[1, rows].astype(F32) - mean) * inv
        one = jnp.sum(v0, axis=1, keepdims=True) + jnp.sum(v1, axis=1, keepdims=True)
        two = jnp.sum(v0 * h0, axis=1, keepdims=True) + jnp.sum(v1 * h1, axis=1, keepdims=True)
        stat[rows] = jnp.where(lane < 64, one, two)
        return carry

    rc(y_acc.at[1 - e], yr, EY, partner).start()
    rc(da_acc.at[1 - e], dar, ED, partner).start()
    lax.fori_loop(0, n_tiles, stat_tile, 0)
    rc(stat, statr, ES, partner).start()

    for t in range(RING):
        u1, u2 = back1(t), back2(t)
        arrive(opp1.at[:, u1], R1 + t)
        gw1[pr, :, u1] += opp1[:, u1]
        rc(gw1.at[pr, :, u1], rel1.at[:, u1], R5 + t, m_right).start()
        arrive(opp2.at[u2], R2 + t)
        gw2[pl_, u2] += opp2[u2]
        rc(gw2.at[pl_, u2], rel2.at[u2], R6 + t, m_left).start()

    arrive(yr, EY)
    arrive(dar, ED)
    arrive(statr, ES)
    b_down = bd_ref[...].astype(F32)

    def out_tile(t, carry):
        rows = pl.ds(pl.multiple_of(t * tile, tile), tile)
        x_own = xf[e, rows].astype(F32)
        yo[rows] = (x_own + (y_acc[e, rows] + yr[rows]) + b_down).astype(BF16)
        norm_grad = da_acc[e, rows] + dar[rows]
        sums = (stat[rows] + statr[rows]) / width
        inv = inv_s[rows]
        x_hat = (x_own - mean_s[rows]) * inv
        value = norm_grad * lnv[e, 0:1]
        dxo[rows] = (gf[e, rows].astype(F32) + inv * (value - sums[:, 0:1] - x_hat * sums[:, 64:65])).astype(BF16)
        vv[RING + 1:RING + 2] += jnp.sum(norm_grad * x_hat, axis=0, keepdims=True)
        vv[RING + 2:RING + 3] += jnp.sum(norm_grad, axis=0, keepdims=True)
        return carry

    lax.fori_loop(0, n_tiles, out_tile, 0)
    store_y = pltpu.make_async_copy(yo, y_hbm, recv.at[IN_SEM + 4])
    store_dx = pltpu.make_async_copy(dxo, dx_hbm, recv.at[IN_SEM + 5])
    store_y.start()
    store_dx.start()

    vm[p] = vv[...]
    for k, d in ((1, m_right), (2, m_opp), (3, m_left)):
        rc(vm.at[p], vm.at[p], VM + k, d).start()
    for k in range(1, RING):
        arrive(vm.at[wrap(p - k)], VM + k)
    vs[q] = ((vm[0] + vm[1]) + vm[2]) + vm[3]
    for k, d in ((1, s_right), (2, s_opp), (3, s_left)):
        rc(vs.at[q], vs.at[q], VS + k, d).start()
    for k in range(1, RING):
        arrive(vs.at[wrap(q - k)], VS + k)
    vp[e] = ((vs[0] + vs[1]) + vs[2]) + vs[3]
    rc(vp.at[e], vp.at[e], VP, partner).start()

    arrive(dir1, R4)
    arrive(dir2, R3)
    for t in range(RING):
        u1, u2 = back1(t), back2(t)
        arrive(rel1.at[:, u1], R5 + t)
        gw1[p, :, u1] += dir1[:, u1] + rel1[:, u1]
        if t == 0:
            rc(gw1.at[p, :, u1], s_opp1, Q1, s_right).start()
        if t == 1:
            rc(gw1.at[p, :, u1], s_dir1, Q4, s_left).start()
        if t == 2:
            arrive(s_opp1, Q1)
            gw1[p, :, u1] += s_opp1[...]
            rc(gw1.at[p, :, u1], s_rel1, Q5, s_right).start()
        arrive(rel2.at[u2], R6 + t)
        gw2[p, u2] += dir2[u2] + rel2[u2]
        if t == 0:
            rc(gw2.at[p, u2], s_opp2, Q2, s_left).start()
        if t == 1:
            rc(gw2.at[p, u2], s_dir2, Q3, s_right).start()
        if t == 2:
            arrive(s_opp2, Q2)
            gw2[p, u2] += s_opp2[...]
            rc(gw2.at[p, u2], s_rel2, Q6, s_left).start()

    arrive(vp.at[1 - e], VP)
    dbu_ref[...] = join_halves(vp[0, pl.ds(c, 1)], vp[1, pl.ds(c, 1)], unit)
    dbd_ref[...] = vp[e, RING:RING + 1]
    dsc_ref[...] = vp[e, RING + 1:RING + 2]
    dsh_ref[...] = vp[e, RING + 2:RING + 3]

    arrive(s_dir1, Q4)
    arrive(s_dir2, Q3)
    arrive(s_rel1, Q5)
    done1 = (gw1[p, :, q] + s_dir1[...] + s_rel1[...]).astype(BF16)
    fo[0, 0:unit] = done1[0]
    fo[1, 0:unit] = done1[1]
    arrive(s_rel2, Q6)
    done2 = (gw2[p, q] + s_dir2[...] + s_rel2[...]).astype(BF16)
    fo[0, unit:2 * unit] = done2[:, 0:half]
    fo[1, unit:2 * unit] = done2[:, half:width]

    @pl.when(e == 0)
    def _():
        fland[0] = fo[0]
        rc(fo.at[1], fland.at[0], FO, partner, FO).start()

    @pl.when(e == 1)
    def _():
        rc(fo.at[0], fland.at[1], FO, turned0, FO + 1).start()

        @pl.when(diag)
        def _():
            fland[1] = fo[1]

        @pl.when(jnp.logical_not(diag))
        def _():
            rc(fo.at[1], fland.at[1], FO + 1, turned1, FO + 1).start()

    @pl.when(e == 0)
    def _():
        arrive(fland.at[1], FO + 1)

    @pl.when(e == 1)
    def _():
        arrive(fland.at[0], FO)

        @pl.when(jnp.logical_not(diag))
        def _():
            arrive(fland.at[1], FO + 1)

    dw1_ref[...] = join_halves(fland[0, 0:unit].astype(F32), fland[1, 0:unit].astype(F32), unit).astype(BF16)
    dw2_ref[0:unit] = fland[0, unit:2 * unit]
    dw2_ref[unit:2 * unit] = fland[1, unit:2 * unit]

    @pl.when(e == 0)
    def _():
        sent(st.at[1], ST + 1)
        sent(fo.at[1], FO)

    @pl.when(e == 1)
    def _():
        sent(st.at[0], ST)
        sent(fo.at[0], FO)

        @pl.when(jnp.logical_not(diag))
        def _():
            sent(st.at[1], ST + 1)
            sent(fo.at[1], FO + 1)

    sent(lnv.at[0], DLN)
    sent(x_hbm, DX)
    sent(g_hbm, DG)
    for sem in (S1, S3, S5):
        sent(w1u(p, q), sem)
    for sem in (S2, S4, S6):
        sent(w2u(p, q), sem)
    for t in range(RING):
        for sem in (M1, M3):
            sent(w1u(p, q), sem + t)
        for sem in (M2, M4):
            sent(w2u(p, q), sem + t)
        for sem in (R1, R5):
            sent(gw1.at[p, :, q], sem + t)
        for sem in (R2, R6):
            sent(gw2.at[p, q], sem + t)
    sent(w2g.at[p], M5)
    sent(w1g.at[p], M6)
    for sem in (MB1, MB2, MB3):
        sent(biasg.at[p], sem)
    sent(gw2.at[p], R3)
    sent(gw1.at[p], R4)
    for sem in (Q1, Q4, Q5):
        sent(gw1.at[p, :, q], sem)
    for sem in (Q2, Q3, Q6):
        sent(gw2.at[p, q], sem)
    for k in range(1, RING):
        sent(vm.at[p], VM + k)
        sent(vs.at[q], VS + k)
    sent(vp.at[e], VP)
    sent(yr, EY)
    sent(dar, ED)
    sent(stat, ES)
    store_y.wait()
    store_dx.wait()


def solution(mesh):
    assert mesh.shape["row"] == RING and mesh.shape["col"] == RING and mesh.shape["dep"] == 2
    tok_spec = P(("part", "row", "col"), "dep")
    vec_dep = P("dep")
    part_dep = P(("part", "dep"))
    in_specs = (tok_spec, vec_dep, vec_dep, P(("dep", "row"), "col"), P("col"), P(("col", "row"), "dep"), vec_dep, tok_spec)
    out_specs = (tok_spec, tok_spec, P(("part", "dep", "row"), "col"), P(("part", "col")), P(("part", "col", "row"), "dep"), part_dep, part_dep, part_dep)

    def local_step(x_in, ln_scale, ln_shift, w_up, b_up, w_down, b_down, y_grad):
        tokens, half = x_in.shape
        width = 2 * half
        unit = w_down.shape[0] // 2
        fb = RING * unit
        assert w_up.shape == (unit, 2 * fb) and half == RING * unit and fb == half
        tile = tokens // RING
        any_spec = pl.BlockSpec(memory_space=pl.ANY)
        vmem_spec = pl.BlockSpec(memory_space=pltpu.VMEM)
        vmem = pltpu.VMEM
        scratch = [
            vmem((unit, 2 * fb), BF16), vmem((2 * unit, half), BF16),
            vmem((2, 2 * unit + PAD, fb), BF16), vmem((2, 2 * unit + PAD, fb), BF16),
            vmem((2, tokens, half), BF16), vmem((2, tokens, half), BF16),
            vmem((2, 8, half), F32),
            vmem((RING, 2, RING, unit, fb), BF16), vmem((RING, RING, unit, width), BF16),
            vmem((RING, PAD, fb), BF16),
            vmem((tokens, width), BF16), vmem((tokens, width), BF16),
            vmem((tokens, 1), F32), vmem((tokens, 1), F32),
            vmem((2, tokens, half), F32), vmem((2, tokens, half), F32),
            vmem((tokens, half), F32), vmem((tokens, half), F32),
            vmem((tokens, 128), F32), vmem((tokens, 128), F32),
            vmem((tokens, fb), BF16), vmem((tokens, fb), BF16),
            vmem((RING, 2, RING, unit, fb), F32), vmem((RING, RING, unit, width), F32),
            vmem((2, RING, unit, fb), F32), vmem((RING, unit, width), F32),
            vmem((2, RING, unit, fb), F32), vmem((RING, unit, width), F32),
            vmem((2, RING, unit, fb), F32), vmem((RING, unit, width), F32),
            vmem((2, unit, fb), F32), vmem((unit, width), F32),
            vmem((2, unit, fb), F32), vmem((unit, width), F32),
            vmem((2, unit, fb), F32), vmem((unit, width), F32),
            vmem((8, half), F32), vmem((RING, 8, half), F32), vmem((RING, 8, half), F32), vmem((2, 8, half), F32),
            vmem((2, 2 * unit, fb), BF16), vmem((2, 2 * unit, fb), BF16),
            vmem((tokens, half), BF16), vmem((tokens, half), BF16),
            pltpu.SemaphoreType.DMA((N_SEM,)), pltpu.SemaphoreType.DMA((N_SEM,)),
        ]
        row = lambda v: v.reshape(1, v.shape[0])
        outs = pl.pallas_call(
            functools.partial(kernel, tile),
            out_shape=(
                jax.ShapeDtypeStruct((tokens, half), BF16), jax.ShapeDtypeStruct((tokens, half), BF16),
                jax.ShapeDtypeStruct(w_up.shape, BF16), jax.ShapeDtypeStruct((1, 2 * fb), F32),
                jax.ShapeDtypeStruct(w_down.shape, BF16), jax.ShapeDtypeStruct((1, half), F32),
                jax.ShapeDtypeStruct((1, half), F32), jax.ShapeDtypeStruct((1, half), F32)),
            in_specs=[any_spec, vmem_spec, vmem_spec, any_spec, vmem_spec, any_spec, vmem_spec, any_spec],
            out_specs=(any_spec, any_spec) + (vmem_spec,) * 6,
            scratch_shapes=scratch,
            compiler_params=pltpu.CompilerParams(collective_id=0, has_side_effects=True, vmem_limit_bytes=66 * 1024 * 1024 - 2 * 1024 * 1024 - 128 * 1024),
        )(x_in, row(ln_scale), row(ln_shift), w_up, row(b_up), w_down, row(b_down), y_grad)
        y_out, x_grad, w_up_grad, b_up_grad, w_down_grad, b_down_grad, scale_grad, shift_grad = outs
        return (y_out, x_grad, w_up_grad, b_up_grad.reshape(-1), w_down_grad, b_down_grad.reshape(-1), scale_grad.reshape(-1), shift_grad.reshape(-1))

    return jax.shard_map(local_step, mesh=mesh, in_specs=in_specs, out_specs=out_specs, check_vma=False)
```

```python
import functools

import jax
import jax.numpy as jnp
from jax import lax
from jax.experimental import pallas as pl
from jax.experimental.pallas import tpu as pltpu
from jax.sharding import PartitionSpec as P

LN_EPS = 1e-5
GELU_K = 0.7978845608028654
GELU_C = 0.044715
MESH = pl.DeviceIdType.MESH
F32 = jnp.float32
BF16 = jnp.bfloat16
RING = 4
LANES = 128

_next = [0]


def _ids(count=1):
    base = _next[0]
    _next[0] += count
    return base


IN_SEM = _ids(8)
P1 = _ids(2 * RING)
P2, DX, DG, DLN = _ids(), _ids(), _ids(), _ids()
BI = _ids(RING)
S1, S2, S3, S4, S5, S6 = (_ids() for _ in range(6))
M1, M2, M3, M4 = (_ids(RING) for _ in range(4))
M5, M6 = _ids(), _ids()
R1, R2, R5, R6 = (_ids(RING) for _ in range(4))
R3, R4 = _ids(), _ids()
Q1, Q2, Q3, Q4, Q5, Q6 = (_ids() for _ in range(6))
VM, VS = _ids(RING), _ids(RING)
VP = _ids()
EY, ED, ES = _ids(), _ids(), _ids()
F1 = _ids(2 * RING)
F2 = _ids()
N_SEM = _next[0]


def gray(t):
    return t + (t // 2) * (5 - 2 * t)


def dot(a, b, dims=((1,), (0,))):
    return lax.dot_general(a, b, (dims, ((), ())), preferred_element_type=F32)


def kernel(tile, x_hbm, sc_ref, sh_ref, w1_hbm, bu_ref, w2_hbm, bd_ref, g_hbm,
           y_hbm, dx_hbm, dw1_ref, dbu_ref, dw2_ref, dbd_ref, dsc_ref, dsh_ref,
           w1v, st1, l1, l2, xf, gf, lnv, wg, bi, bias_s, ab, gb, mean_s, inv_s,
           y_acc, da_acc, yr, dar, stat, statr, hs, dcs, gw, opp, dirs, rel, s_opp, s_dir, s_rel,
           vv, vm, vs, vp, f1, f1l, f2, f2l, yo, dxo, send, recv):
    r, c, e = lax.axis_index("row"), lax.axis_index("col"), lax.axis_index("dep")
    p = c + e * (r - c)
    q = r + e * (c - r)
    tokens, half = xf.shape[1], xf.shape[2]
    width = 2 * half
    unit = l2.shape[1]
    fb = RING * unit
    n_tiles = tokens // tile
    other = 1 - e

    def wrap(v):
        return lax.rem(v + 2 * RING, RING)

    def dev(pp, qq):
        return {"row": qq + e * (pp - qq), "col": pp + e * (qq - pp), "dep": e}

    m_right, m_left, m_opp = dev(wrap(p + 1), q), dev(wrap(p - 1), q), dev(wrap(p + 2), q)
    s_right, s_left, s_opp_dev = dev(p, wrap(q + 1)), dev(p, wrap(q - 1)), dev(p, wrap(q + 2))
    partner = {"row": r, "col": c, "dep": other}
    pr, pl_, po = wrap(p + 1), wrap(p - 1), wrap(p + 2)
    qr, ql, qo = wrap(q + 1), wrap(q - 1), wrap(q + 2)

    def rc(src, dst, ssem, device, rsem=None):
        return pltpu.make_async_remote_copy(
            src_ref=src, dst_ref=dst, send_sem=send.at[ssem], recv_sem=recv.at[ssem if rsem is None else rsem],
            device_id=device, device_id_type=MESH)

    def arrive(dst, rsem):
        rc(dst, dst, rsem, partner).wait_recv()

    def sent(src, ssem):
        rc(src, src, ssem, partner).wait_send()

    def go(ref, sem, device):
        rc(ref, ref, sem, device).start()

    load_w1 = pltpu.make_async_copy(w1_hbm, w1v, recv.at[IN_SEM])
    load_w2 = pltpu.make_async_copy(w2_hbm.at[pl.ds(pl.multiple_of(e * unit, 16), unit)], l2.at[e], recv.at[IN_SEM + 1])
    load_x = pltpu.make_async_copy(x_hbm, xf.at[e], recv.at[IN_SEM + 2])
    load_g = pltpu.make_async_copy(g_hbm, gf.at[e], recv.at[IN_SEM + 3])
    load_w1.start()
    load_w2.start()
    load_x.start()
    load_g.start()

    barrier = pltpu.get_barrier_semaphore()
    peers = [m_right, m_left, s_right, s_left, m_opp, s_opp_dev, partner]
    peers += [{"row": wrap(r + k), "col": c, "dep": other} for k in range(1, RING)]
    for d in peers:
        pl.semaphore_signal(barrier, inc=1, device_id=d, device_id_type=MESH)

    lnv[e, 0:1] = sc_ref[...].reshape(1, half)
    lnv[e, 1:2] = sh_ref[...].reshape(1, half)
    bi[c] = jnp.broadcast_to(bu_ref[...].astype(F32).reshape(1, 2 * fb), (8, 2 * fb))
    load_w1.wait()
    turned = w1v[...].astype(F32)
    turned = jnp.concatenate([turned, jnp.zeros((LANES - unit, 2 * fb), F32)], axis=0).T.astype(BF16)
    for k in range(RING):
        for h in range(2):
            st1[k, h] = turned[(2 * k + h) * unit:(2 * k + h + 1) * unit]

    pl.semaphore_wait(barrier, len(peers))

    rc(w2_hbm.at[pl.ds(pl.multiple_of(other * unit, 16), unit)], l2.at[e], P2, partner).start()
    rc(st1.at[r, other], l1.at[r, e], P1 + other, partner, P1 + e).start()
    for k in (2, 1, 3):
        for h in range(2):
            rc(st1.at[wrap(r + k), h], l1.at[r, e], P1 + 2 * k + h,
               {"row": wrap(r + k), "col": c, "dep": h}, P1 + 2 * k + e).start()
    rc(lnv.at[e], lnv.at[e], DLN, partner).start()
    rc(x_hbm, xf.at[e], DX, partner).start()
    rc(g_hbm, gf.at[e], DG, partner).start()
    for k in range(1, RING):
        rc(bi.at[c], bi.at[c], BI + k, {"row": r, "col": wrap(c + k), "dep": e}).start()
    l1[r, e] = st1[r, e]

    def w1u(b, s):
        return wg.at[0, b, s]

    def w2u(b, s):
        return wg.at[1, b, s]

    load_w2.wait()
    arrive(l2.at[other], P2)
    wg[1, p, q, :, 0:half] = l2[0]
    wg[1, p, q, :, half:width] = l2[1]
    go(w2u(p, q), M2, m_right)
    go(w2u(p, q), S2, s_right)
    go(w2u(p, q), S4, s_left)

    arrive(l1.at[r, other], P1 + other)
    for k in range(1, RING):
        for h in range(2):
            arrive(l1.at[wrap(r - k), h], P1 + 2 * k + h)
    wg[0, p, q] = jnp.concatenate([l1[k, h][:, 0:unit].astype(F32) for h in range(2) for k in range(RING)], axis=1).astype(BF16)
    go(w1u(p, q), M1, m_left)
    go(w1u(p, q), S1, s_right)
    go(w1u(p, q), S3, s_left)

    arrive(w2u(p, ql), S2)
    go(w2u(p, ql), S6, s_right)
    go(w2u(p, ql), M2 + 1, m_right)
    arrive(w2u(p, qr), S4)
    go(w2u(p, qr), M2 + 2, m_right)

    arrive(lnv.at[other], DLN)
    load_x.wait()
    arrive(xf.at[other], DX)
    load_g.wait()
    arrive(gf.at[other], DG)
    vv[...] = jnp.zeros_like(vv)
    def norm_tile(t, carry):
        rows = pl.ds(pl.multiple_of(t * tile, tile), tile)
        x0, x1 = xf[0, rows].astype(F32), xf[1, rows].astype(F32)
        total = jnp.sum(x0, axis=1, keepdims=True) + jnp.sum(x1, axis=1, keepdims=True)
        squares = jnp.sum(x0 * x0, axis=1, keepdims=True) + jnp.sum(x1 * x1, axis=1, keepdims=True)
        mean = total / width
        inv = lax.rsqrt(squares / width - mean * mean + LN_EPS)
        mean_s[rows] = mean
        inv_s[rows] = inv
        ab[rows, 0:half] = ((x0 - mean) * inv * lnv[0, 0:1] + lnv[0, 1:2]).astype(BF16)
        ab[rows, half:width] = ((x1 - mean) * inv * lnv[1, 0:1] + lnv[1, 1:2]).astype(BF16)
        gb[rows, 0:half] = gf[0, rows]
        gb[rows, half:width] = gf[1, rows]
        vv[RING:RING + 1] += jnp.sum(gf[e, rows].astype(F32), axis=0, keepdims=True)
        return carry

    lax.fori_loop(0, n_tiles, norm_tile, 0)

    arrive(w1u(p, qr), S3)
    go(w1u(p, qr), S5, s_left)
    go(w1u(p, qr), M1 + 1, m_left)
    arrive(w1u(p, ql), S1)
    go(w1u(p, ql), M1 + 2, m_left)
    arrive(w2u(p, qo), S6)
    go(w2u(p, qo), M2 + 3, m_right)
    for k in range(1, RING):
        arrive(bi.at[wrap(c - k)], BI + k)
    for b in range(RING):
        flat = jnp.concatenate([bi[b, 0:1, 2 * k * unit:(2 * k + 1) * unit] for k in range(RING)], axis=1)
        across = jnp.concatenate([bi[k, 0:1, (2 * b + 1) * unit:(2 * b + 2) * unit] for k in range(RING)], axis=1)
        bias_s[b, 0:1] = jnp.where(e == 0, flat, across)
    arrive(w1u(p, qo), S5)
    go(w1u(p, qo), M1 + 3, m_left)

    def unit1(t):
        return wrap(q + gray(t))

    def unit2(t):
        return wrap(q - gray(t))

    def block(b, first, hook=None):
        bias = bias_s[b, 0:1]

        def block_tile(t, carry):
            rows = pl.ds(pl.multiple_of(t * tile, tile), tile)
            w1 = wg[0, b].reshape(fb, width)
            w2 = wg[1, b].reshape(fb, width)
            pre = dot(ab[rows, :], w1, ((1,), (1,))) + bias
            squared = pre * pre
            tanh_val = jnp.tanh(GELU_K * (pre + GELU_C * pre * squared))
            hidden = (0.5 * pre * (1.0 + tanh_val)).astype(BF16)
            hs[rows, :] = hidden
            slope = 0.5 * (1.0 + tanh_val) + 0.5 * pre * (1.0 - tanh_val * tanh_val) * GELU_K * (1.0 + 3.0 * GELU_C * squared)
            pre_grad = dot(gb[rows, :], w2, ((1,), (1,))) * slope
            vv[pl.ds(b, 1)] += jnp.sum(pre_grad, axis=0, keepdims=True)
            lowp = pre_grad.astype(BF16)
            dcs[rows, :] = lowp
            out = dot(hidden, w2)
            back = dot(lowp, w1)
            if first:
                y_acc[0, rows] = out[:, 0:half]
                y_acc[1, rows] = out[:, half:width]
                da_acc[0, rows] = back[:, 0:half]
                da_acc[1, rows] = back[:, half:width]
            else:
                y_acc[0, rows] += out[:, 0:half]
                y_acc[1, rows] += out[:, half:width]
                da_acc[0, rows] += back[:, 0:half]
                da_acc[1, rows] += back[:, half:width]
            if hook is not None:
                hook(t)
            return carry

        lax.fori_loop(0, n_tiles, block_tile, 0)
        gw[0, b] = dot(dcs[...], ab[...], ((0,), (0,))).reshape(RING, unit, width)
        gw[1, b] = dot(hs[...], gb[...], ((0,), (0,))).reshape(RING, unit, width)

    def relay_gather(t):
        u1, u2 = unit1(t), unit2(t)
        arrive(w2u(pl_, u2), M2 + t)
        go(w2u(pl_, u2), M4 + t, m_right)
        arrive(w1u(pr, u1), M1 + t)
        go(w1u(pr, u1), M3 + t, m_left)

    assert n_tiles == RING
    block(p, True, relay_gather)
    go(wg.at[0, p], M5, m_right)
    go(wg.at[1, p], M6, m_left)

    for t in range(RING):
        arrive(w2u(po, unit2(t)), M4 + t)
        arrive(w1u(po, unit1(t)), M3 + t)
    block(po, False)

    def back1(t):
        return wrap(q - gray(RING - 1 - t))

    def back2(t):
        return wrap(q + gray(RING - 1 - t))

    for t in range(RING):
        u1, u2 = back1(t), back2(t)
        rc(gw.at[1, po, u2], opp.at[1, u2], R2 + t, m_right).start()
        rc(gw.at[0, po, u1], opp.at[0, u1], R1 + t, m_left).start()

    arrive(wg.at[1, pr], M6)
    block(pr, False)
    rc(gw.at[0, pr], dirs.at[0], R3, m_right).start()
    arrive(wg.at[0, pl_], M5)
    block(pl_, False)
    rc(gw.at[1, pl_], dirs.at[1], R4, m_left).start()

    lane = lax.broadcasted_iota(jnp.int32, (tile, 128), 1)

    def stat_tile(t, carry):
        rows = pl.ds(pl.multiple_of(t * tile, tile), tile)
        mean, inv = mean_s[rows], inv_s[rows]
        v0 = da_acc[0, rows] * lnv[0, 0:1]
        v1 = da_acc[1, rows] * lnv[1, 0:1]
        h0 = (xf[0, rows].astype(F32) - mean) * inv
        h1 = (xf[1, rows].astype(F32) - mean) * inv
        one = jnp.sum(v0, axis=1, keepdims=True) + jnp.sum(v1, axis=1, keepdims=True)
        two = jnp.sum(v0 * h0, axis=1, keepdims=True) + jnp.sum(v1 * h1, axis=1, keepdims=True)
        stat[rows] = jnp.where(lane < 64, one, two)
        return carry

    rc(y_acc.at[other], yr, EY, partner).start()
    rc(da_acc.at[other], dar, ED, partner).start()
    lax.fori_loop(0, n_tiles, stat_tile, 0)
    rc(stat, statr, ES, partner).start()

    for t in range(RING):
        u1, u2 = back1(t), back2(t)
        arrive(opp.at[1, u2], R2 + t)
        gw[1, pr, u2] += opp[1, u2]
        rc(gw.at[1, pr, u2], rel.at[1, u2], R6 + t, m_right).start()
        arrive(opp.at[0, u1], R1 + t)
        gw[0, pl_, u1] += opp[0, u1]
        rc(gw.at[0, pl_, u1], rel.at[0, u1], R5 + t, m_left).start()

    arrive(yr, EY)
    arrive(dar, ED)
    arrive(statr, ES)
    b_down = bd_ref[...].astype(F32).reshape(1, half)

    def out_tile(t, carry):
        rows = pl.ds(pl.multiple_of(t * tile, tile), tile)
        x_own = xf[e, rows].astype(F32)
        yo[rows] = (x_own + (y_acc[e, rows] + yr[rows]) + b_down).astype(BF16)
        norm_grad = da_acc[e, rows] + dar[rows]
        sums = (stat[rows] + statr[rows]) / width
        inv = inv_s[rows]
        x_hat = (x_own - mean_s[rows]) * inv
        value = norm_grad * lnv[e, 0:1]
        dxo[rows] = (gf[e, rows].astype(F32) + inv * (value - sums[:, 0:1] - x_hat * sums[:, 64:65])).astype(BF16)
        vv[RING + 1:RING + 2] += jnp.sum(norm_grad * x_hat, axis=0, keepdims=True)
        vv[RING + 2:RING + 3] += jnp.sum(norm_grad, axis=0, keepdims=True)
        return carry

    lax.fori_loop(0, n_tiles, out_tile, 0)
    store_y = pltpu.make_async_copy(yo, y_hbm, recv.at[IN_SEM + 4])
    store_dx = pltpu.make_async_copy(dxo, dx_hbm, recv.at[IN_SEM + 5])
    store_y.start()
    store_dx.start()

    vs[q] = vv[...]
    for k, d in ((1, s_right), (2, s_opp_dev), (3, s_left)):
        go(vs.at[q], VS + k, d)
    for k in range(1, RING):
        arrive(vs.at[wrap(q - k)], VS + k)
    vm[p] = ((vs[0] + vs[1]) + vs[2]) + vs[3]
    for k, d in ((1, m_right), (2, m_opp), (3, m_left)):
        go(vm.at[p], VM + k, d)

    arrive(dirs.at[0], R3)
    arrive(dirs.at[1], R4)
    for t in range(RING):
        u1, u2 = back1(t), back2(t)
        arrive(rel.at[1, u2], R6 + t)
        gw[1, p, u2] += dirs[1, u2] + rel[1, u2]
        if t == 0:
            rc(gw.at[1, p, u2], s_opp.at[1], Q2, s_right).start()
        if t == 1:
            rc(gw.at[1, p, u2], s_dir.at[1], Q4, s_left).start()
        if t == 2:
            arrive(s_opp.at[1], Q2)
            gw[1, p, u2] += s_opp[1]
            rc(gw.at[1, p, u2], s_rel.at[1], Q6, s_right).start()
        arrive(rel.at[0, u1], R5 + t)
        gw[0, p, u1] += dirs[0, u1] + rel[0, u1]
        if t == 0:
            rc(gw.at[0, p, u1], s_opp.at[0], Q1, s_left).start()
        if t == 1:
            rc(gw.at[0, p, u1], s_dir.at[0], Q3, s_right).start()
        if t == 2:
            arrive(s_opp.at[0], Q1)
            gw[0, p, u1] += s_opp[0]
            rc(gw.at[0, p, u1], s_rel.at[0], Q5, s_left).start()

    for k in range(1, RING):
        arrive(vm.at[wrap(p - k)], VM + k)
    vp[e] = ((vm[0] + vm[1]) + vm[2]) + vm[3]
    go(vp.at[e], VP, partner)

    arrive(s_dir.at[0], Q3)
    arrive(s_rel.at[0], Q5)
    done1 = gw[0, p, q] + s_dir[0] + s_rel[0]
    for k in range(RING):
        for h in range(2):
            start = (h * RING + k) * unit
            piece = jnp.concatenate([done1[:, start:start + unit], jnp.zeros((unit, LANES - unit), F32)], axis=1)
            f1[k, h] = piece.astype(BF16)
    for k in (2, 1, 3):
        for h in range(2):
            rc(f1.at[wrap(r + k), h], f1l.at[r, e], F1 + 2 * k + h,
               {"row": wrap(r + k), "col": c, "dep": h}, F1 + 2 * k + e).start()
    rc(f1.at[r, other], f1l.at[r, e], F1 + other, partner, F1 + e).start()
    f1l[r, e] = f1[r, e]
    arrive(s_dir.at[1], Q4)
    arrive(s_rel.at[1], Q6)
    done2 = (gw[1, p, q] + s_dir[1] + s_rel[1]).astype(BF16)
    f2[0] = done2[:, 0:half]
    f2[1] = done2[:, half:width]
    rc(f2.at[other], f2l.at[e], F2, partner).start()
    f2l[e] = f2[e]

    arrive(vp.at[other], VP)
    pieces = []
    for k in range(RING):
        pieces.append(vp[0, pl.ds(c, 1)][:, k * unit:(k + 1) * unit])
        row = vp[1, k:k + 1]
        piece = row[:, 0:unit]
        for j in range(1, RING):
            piece = jnp.where(c == j, row[:, j * unit:(j + 1) * unit], piece)
        pieces.append(piece)
    dbu_ref[...] = jnp.concatenate(pieces, axis=1).reshape(dbu_ref.shape)
    dbd_ref[...] = vp[e, RING:RING + 1].reshape(dbd_ref.shape)
    dsc_ref[...] = vp[e, RING + 1:RING + 2].reshape(dsc_ref.shape)
    dsh_ref[...] = vp[e, RING + 2:RING + 3].reshape(dsh_ref.shape)

    sent(l2.at[0], P2)
    sent(l1.at[0, 0], P1 + other)
    sent(l1.at[0, 0], F1 + other)
    for k in range(1, RING):
        for h in range(2):
            sent(l1.at[0, 0], P1 + 2 * k + h)
            sent(l1.at[0, 0], F1 + 2 * k + h)
        sent(bi.at[c], BI + k)
        sent(vm.at[p], VM + k)
        sent(vs.at[q], VS + k)
    sent(f2.at[0], F2)
    sent(lnv.at[0], DLN)
    sent(x_hbm, DX)
    sent(g_hbm, DG)
    for sem in (S1, S2, S3, S4, S5, S6):
        sent(w1u(p, q), sem)
    for t in range(RING):
        for sem in (M1, M2, M3, M4):
            sent(w1u(p, q), sem + t)
        for sem in (R1, R2, R5, R6):
            sent(gw.at[0, p, q], sem + t)
    sent(wg.at[0, p], M5)
    sent(wg.at[0, p], M6)
    sent(gw.at[0, p], R3)
    sent(gw.at[0, p], R4)
    for sem in (Q1, Q2, Q3, Q4, Q5, Q6):
        sent(gw.at[0, p, q], sem)
    sent(vp.at[e], VP)
    sent(yr, EY)
    sent(dar, ED)
    sent(stat, ES)
    store_y.wait()
    store_dx.wait()

    arrive(f2l.at[other], F2)
    dw2_ref[0:unit] = f2l[0]
    dw2_ref[unit:2 * unit] = f2l[1]
    arrive(f1l.at[r, other], F1 + other)
    for k in range(1, RING):
        for h in range(2):
            arrive(f1l.at[wrap(r - k), h], F1 + 2 * k + h)
    dw1_ref[...] = f1l[...].astype(F32).reshape(2 * fb, LANES).T[0:unit].astype(BF16)


def copy_out(*refs):
    n = (len(refs) - 1) // 3
    srcs, dsts, bufs, sems = refs[:n], refs[n:2 * n], refs[2 * n:3 * n], refs[3 * n]
    order = sorted(range(n), key=lambda i: -srcs[i].size)
    pieces = []
    for i in order:
        rows = srcs[i].shape[0]
        step = rows // RING if len(srcs[i].shape) > 1 and rows >= 1024 else rows
        for start in range(0, rows, step):
            pieces.append((i, pl.ds(start, step)))
    loads = []
    for j, (i, ds) in enumerate(pieces):
        copy = pltpu.make_async_copy(srcs[i].at[ds], bufs[i].at[ds], sems.at[0, j])
        copy.start()
        loads.append(copy)
    stores = []
    for j, (i, ds) in enumerate(pieces):
        loads[j].wait()
        copy = pltpu.make_async_copy(bufs[i].at[ds], dsts[i].at[ds], sems.at[1, j])
        copy.start()
        stores.append(copy)
    for copy in stores:
        copy.wait()


def solution(mesh):
    assert mesh.shape["row"] == RING and mesh.shape["col"] == RING and mesh.shape["dep"] == 2
    tok_spec = P(("part", "row", "col"), "dep")
    vec_dep = P("dep")
    part_dep = P(("part", "dep"))
    in_specs = (tok_spec, vec_dep, vec_dep, P(("dep", "row"), "col"), P("col"), P(("col", "row"), "dep"), vec_dep, tok_spec)
    out_specs = (tok_spec, tok_spec, P(("part", "dep", "row"), "col"), P(("part", "col")), P(("part", "col", "row"), "dep"), part_dep, part_dep, part_dep)

    def local_step(x_in, ln_scale, ln_shift, w_up, b_up, w_down, b_down, y_grad):
        tokens, half = x_in.shape
        width = 2 * half
        unit = w_down.shape[0] // 2
        fb = RING * unit
        assert w_up.shape == (unit, 2 * fb) and half == RING * unit and fb == half
        tile = tokens // RING
        any_spec = pl.BlockSpec(memory_space=pl.ANY)
        vmem_spec = pl.BlockSpec(memory_space=pltpu.VMEM)
        vmem = pltpu.VMEM
        scratch = [
            vmem((unit, 2 * fb), BF16),
            vmem((RING, 2, unit, LANES), BF16), vmem((RING, 2, unit, LANES), BF16), vmem((2, unit, half), BF16),
            vmem((2, tokens, half), BF16), vmem((2, tokens, half), BF16),
            vmem((2, 8, half), F32),
            vmem((2, RING, RING, unit, width), BF16),
            vmem((RING, 8, 2 * fb), F32), vmem((RING, 8, fb), F32),
            vmem((tokens, width), BF16), vmem((tokens, width), BF16),
            vmem((tokens, 1), F32), vmem((tokens, 1), F32),
            vmem((2, tokens, half), F32), vmem((2, tokens, half), F32),
            vmem((tokens, half), F32), vmem((tokens, half), F32),
            vmem((tokens, 128), F32), vmem((tokens, 128), F32),
            vmem((tokens, fb), BF16), vmem((tokens, fb), BF16),
            vmem((2, RING, RING, unit, width), F32),
            vmem((2, RING, unit, width), F32), vmem((2, RING, unit, width), F32), vmem((2, RING, unit, width), F32),
            vmem((2, unit, width), F32), vmem((2, unit, width), F32), vmem((2, unit, width), F32),
            vmem((8, half), F32), vmem((RING, 8, half), F32), vmem((RING, 8, half), F32), vmem((2, 8, half), F32),
            vmem((RING, 2, unit, LANES), BF16), vmem((RING, 2, unit, LANES), BF16),
            vmem((2, unit, half), BF16), vmem((2, unit, half), BF16),
            vmem((tokens, half), BF16), vmem((tokens, half), BF16),
            pltpu.SemaphoreType.DMA((N_SEM,)), pltpu.SemaphoreType.DMA((N_SEM,)),
        ]
        shapes = (
            jax.ShapeDtypeStruct((tokens, half), BF16), jax.ShapeDtypeStruct((tokens, half), BF16),
            jax.ShapeDtypeStruct(w_up.shape, BF16), jax.ShapeDtypeStruct(b_up.shape, F32),
            jax.ShapeDtypeStruct(w_down.shape, BF16), jax.ShapeDtypeStruct((half,), F32),
            jax.ShapeDtypeStruct((half,), F32), jax.ShapeDtypeStruct((half,), F32))
        outs = pl.pallas_call(
            functools.partial(kernel, tile),
            out_shape=shapes,
            in_specs=[any_spec, vmem_spec, vmem_spec, any_spec, vmem_spec, any_spec, vmem_spec, any_spec],
            out_specs=(any_spec, any_spec) + (vmem_spec,) * 6,
            scratch_shapes=scratch,
            compiler_params=pltpu.CompilerParams(collective_id=0, has_side_effects=True, vmem_limit_bytes=64 * 1024 * 1024 - 128 * 1024),
        )(x_in, ln_scale, ln_shift, w_up, b_up, w_down, b_down, y_grad)
        return pl.pallas_call(
            copy_out,
            out_shape=shapes,
            in_specs=[any_spec] * len(shapes),
            out_specs=(any_spec,) * len(shapes),
            scratch_shapes=[vmem(s.shape, s.dtype) for s in shapes] + [pltpu.SemaphoreType.DMA((2, 16))],
            compiler_params=pltpu.CompilerParams(vmem_limit_bytes=64 * 1024 * 1024 - 128 * 1024),
        )(*outs)

    return jax.shard_map(local_step, mesh=mesh, in_specs=in_specs, out_specs=out_specs, check_vma=False)
```

```python
import functools

import jax
import jax.numpy as jnp
from jax import lax
from jax.experimental import pallas as pl
from jax.experimental.pallas import tpu as pltpu
from jax.sharding import PartitionSpec as P

LN_EPS = 1e-5
GELU_K = 0.7978845608028654
GELU_C = 0.044715
MESH = pl.DeviceIdType.MESH
F32 = jnp.float32
BF16 = jnp.bfloat16
RING = 4
LANES = 128

_next = [0]


def _ids(count=1):
    base = _next[0]
    _next[0] += count
    return base


IN_SEM = _ids(8)
P1 = _ids(2 * RING)
P2, DX, DG, DLN = _ids(), _ids(), _ids(), _ids()
BI = _ids(RING)
S1, S2, S3, S4, S5, S6 = (_ids() for _ in range(6))
M1, M2, M3, M4 = (_ids(RING) for _ in range(4))
M5, M6 = _ids(), _ids()
R1, R2, R5, R6 = (_ids(RING) for _ in range(4))
R3, R4 = _ids(), _ids(RING)
Q1, Q2, Q3, Q4, Q5, Q6 = (_ids() for _ in range(6))
VM, VS = _ids(RING), _ids(RING)
VP = _ids()
EY, ED, ES = _ids(), _ids(), _ids()
F1 = _ids(2 * RING)
F2 = _ids()
N_SEM = _next[0]


def gray(t):
    return t + (t // 2) * (5 - 2 * t)


def dot(a, b, dims=((1,), (0,))):
    return lax.dot_general(a, b, (dims, ((), ())), preferred_element_type=F32)


def kernel(tile, x_hbm, sc_hbm, sh_hbm, w1_hbm, bu_hbm, w2_hbm, bd_hbm, g_hbm,
           y_ref, dx_ref, dw1_ref, dbu_ref, dw2_ref, dbd_ref, dsc_ref, dsh_ref,
           w1v, st1, l1, l2, xf, gf, lnv, wg, bi, bias_s, ab, gb, mean_s, inv_s,
           y_acc, da_acc, yr, dar, stat, statr, hs, dcs, gw, opp, dirs, rel, s_opp, s_dir, s_rel,
           vv, vm, vs, vp, f1, f1l, f2, f2l, sc_ref, sh_ref, bu_ref, bd_ref, send, recv):
    r, c, e = lax.axis_index("row"), lax.axis_index("col"), lax.axis_index("dep")
    p = c + e * (r - c)
    q = r + e * (c - r)
    tokens, half = xf.shape[1], xf.shape[2]
    width = 2 * half
    unit = l2.shape[1]
    fb = RING * unit
    n_tiles = tokens // tile
    other = 1 - e

    def wrap(v):
        return lax.rem(v + 2 * RING, RING)

    def dev(pp, qq):
        return {"row": qq + e * (pp - qq), "col": pp + e * (qq - pp), "dep": e}

    m_right, m_left, m_opp = dev(wrap(p + 1), q), dev(wrap(p - 1), q), dev(wrap(p + 2), q)
    s_right, s_left, s_opp_dev = dev(p, wrap(q + 1)), dev(p, wrap(q - 1)), dev(p, wrap(q + 2))
    partner = {"row": r, "col": c, "dep": other}
    pr, pl_, po = wrap(p + 1), wrap(p - 1), wrap(p + 2)
    qr, ql, qo = wrap(q + 1), wrap(q - 1), wrap(q + 2)

    def rc(src, dst, ssem, device, rsem=None):
        return pltpu.make_async_remote_copy(
            src_ref=src, dst_ref=dst, send_sem=send.at[ssem], recv_sem=recv.at[ssem if rsem is None else rsem],
            device_id=device, device_id_type=MESH)

    def arrive(dst, rsem):
        rc(dst, dst, rsem, partner).wait_recv()

    def sent(src, ssem):
        rc(src, src, ssem, partner).wait_send()

    def go(ref, sem, device):
        rc(ref, ref, sem, device).start()

    load_w1 = pltpu.make_async_copy(w1_hbm, w1v, recv.at[IN_SEM])
    load_w2 = pltpu.make_async_copy(w2_hbm.at[pl.ds(pl.multiple_of(e * unit, 16), unit)], l2.at[e], recv.at[IN_SEM + 1])
    load_x = pltpu.make_async_copy(x_hbm, xf.at[e], recv.at[IN_SEM + 2])
    load_g = pltpu.make_async_copy(g_hbm, gf.at[e], recv.at[IN_SEM + 3])
    load_vectors = [pltpu.make_async_copy(src, dst, recv.at[IN_SEM + 4 + i]) for i, (src, dst) in enumerate(
        ((sc_hbm, sc_ref), (sh_hbm, sh_ref), (bu_hbm, bu_ref), (bd_hbm, bd_ref)))]
    load_w1.start()
    load_w2.start()
    for load in load_vectors:
        load.start()
    load_x.start()
    load_g.start()

    barrier = pltpu.get_barrier_semaphore()
    peers = [m_right, m_left, s_right, s_left, m_opp, s_opp_dev, partner]
    peers += [{"row": wrap(r + k), "col": c, "dep": other} for k in range(1, RING)]
    for d in peers:
        pl.semaphore_signal(barrier, inc=1, device_id=d, device_id_type=MESH)

    load_w1.wait()
    turned = w1v[...].astype(F32)
    turned = jnp.concatenate([turned, jnp.zeros((LANES - unit, 2 * fb), F32)], axis=0).T.astype(BF16)
    for k in range(RING):
        for h in range(2):
            st1[k, h] = turned[(2 * k + h) * unit:(2 * k + h + 1) * unit]

    for load in load_vectors:
        load.wait()
    lnv[e, 0:1] = sc_ref[...].reshape(1, half)
    lnv[e, 1:2] = sh_ref[...].reshape(1, half)
    bi[c] = jnp.broadcast_to(bu_ref[...].astype(F32).reshape(1, 2 * fb), (8, 2 * fb))

    pl.semaphore_wait(barrier, len(peers))

    rc(w2_hbm.at[pl.ds(pl.multiple_of(other * unit, 16), unit)], l2.at[e], P2, partner).start()
    rc(st1.at[r, other], l1.at[r, e], P1 + other, partner, P1 + e).start()
    for k in (2, 1, 3):
        for h in range(2):
            rc(st1.at[wrap(r + k), h], l1.at[r, e], P1 + 2 * k + h,
               {"row": wrap(r + k), "col": c, "dep": h}, P1 + 2 * k + e).start()
    rc(lnv.at[e], lnv.at[e], DLN, partner).start()
    rc(x_hbm, xf.at[e], DX, partner).start()
    rc(g_hbm, gf.at[e], DG, partner).start()
    for k in range(1, RING):
        rc(bi.at[c], bi.at[c], BI + k, {"row": r, "col": wrap(c + k), "dep": e}).start()
    l1[r, e] = st1[r, e]

    def w1u(b, s):
        return wg.at[0, b, s]

    def w2u(b, s):
        return wg.at[1, b, s]

    load_w2.wait()
    arrive(l2.at[other], P2)
    wg[1, p, q, :, 0:half] = l2[0]
    wg[1, p, q, :, half:width] = l2[1]
    go(w2u(p, q), M2, m_right)
    go(w2u(p, q), S2, s_right)
    go(w2u(p, q), S4, s_left)

    arrive(l1.at[r, other], P1 + other)
    for k in range(1, RING):
        for h in range(2):
            arrive(l1.at[wrap(r - k), h], P1 + 2 * k + h)
    wg[0, p, q] = jnp.concatenate([l1[k, h][:, 0:unit].astype(F32) for h in range(2) for k in range(RING)], axis=1).astype(BF16)
    go(w1u(p, q), M1, m_left)
    go(w1u(p, q), S1, s_right)
    go(w1u(p, q), S3, s_left)

    arrive(w2u(p, ql), S2)
    go(w2u(p, ql), S6, s_right)
    go(w2u(p, ql), M2 + 1, m_right)
    arrive(w2u(p, qr), S4)
    go(w2u(p, qr), M2 + 2, m_right)

    def unit1(t):
        return wrap(q + gray(t))

    def unit2(t):
        return wrap(q - gray(t))

    arrive(lnv.at[other], DLN)
    load_x.wait()
    arrive(xf.at[other], DX)
    load_g.wait()
    arrive(gf.at[other], DG)
    vv[...] = jnp.zeros_like(vv)
    def norm_tile(t, carry):
        rows = pl.ds(pl.multiple_of(t * tile, tile), tile)
        x0, x1 = xf[0, rows].astype(F32), xf[1, rows].astype(F32)
        total = jnp.sum(x0, axis=1, keepdims=True) + jnp.sum(x1, axis=1, keepdims=True)
        squares = jnp.sum(x0 * x0, axis=1, keepdims=True) + jnp.sum(x1 * x1, axis=1, keepdims=True)
        mean = total / width
        inv = lax.rsqrt(squares / width - mean * mean + LN_EPS)
        mean_s[rows] = mean
        inv_s[rows] = inv
        ab[rows, 0:half] = ((x0 - mean) * inv * lnv[0, 0:1] + lnv[0, 1:2]).astype(BF16)
        ab[rows, half:width] = ((x1 - mean) * inv * lnv[1, 0:1] + lnv[1, 1:2]).astype(BF16)
        gb[rows, 0:half] = gf[0, rows]
        gb[rows, half:width] = gf[1, rows]
        vv[RING:RING + 1] += jnp.sum(gf[e, rows].astype(F32), axis=0, keepdims=True)
        return carry

    lax.fori_loop(0, n_tiles // 2, norm_tile, 0)
    arrive(w1u(p, qr), S3)
    go(w1u(p, qr), S5, s_left)
    go(w1u(p, qr), M1 + 1, m_left)
    lax.fori_loop(n_tiles // 2, n_tiles, norm_tile, 0)

    def relay1(t):
        arrive(w1u(pr, unit1(t)), M1 + t)
        go(w1u(pr, unit1(t)), M3 + t, m_left)

    def relay2(t):
        arrive(w2u(pl_, unit2(t)), M2 + t)
        go(w2u(pl_, unit2(t)), M4 + t, m_right)

    arrive(w1u(p, ql), S1)
    go(w1u(p, ql), M1 + 2, m_left)
    relay2(0)
    for k in range(1, RING):
        arrive(bi.at[wrap(c - k)], BI + k)
    for b in range(RING):
        flat = jnp.concatenate([bi[b, 0:1, 2 * k * unit:(2 * k + 1) * unit] for k in range(RING)], axis=1)
        across = jnp.concatenate([bi[k, 0:1, (2 * b + 1) * unit:(2 * b + 2) * unit] for k in range(RING)], axis=1)
        bias_s[b, 0:1] = jnp.where(e == 0, flat, across)
    arrive(w2u(p, qo), S6)
    go(w2u(p, qo), M2 + 3, m_right)
    relay1(0)
    arrive(w1u(p, qo), S5)
    go(w1u(p, qo), M1 + 3, m_left)
    relay2(1)
    relay2(2)

    def block(b, first, hook=None, send_part=None):
        bias = bias_s[b, 0:1]

        def block_tile(t, carry):
            rows = pl.ds(pl.multiple_of(t * tile, tile), tile)
            w1 = wg[0, b].reshape(fb, width)
            w2 = wg[1, b].reshape(fb, width)
            pre = dot(ab[rows, :], w1, ((1,), (1,))) + bias
            squared = pre * pre
            tanh_val = jnp.tanh(GELU_K * (pre + GELU_C * pre * squared))
            hidden = (0.5 * pre * (1.0 + tanh_val)).astype(BF16)
            hs[rows, :] = hidden
            slope = 0.5 * (1.0 + tanh_val) + 0.5 * pre * (1.0 - tanh_val * tanh_val) * GELU_K * (1.0 + 3.0 * GELU_C * squared)
            pre_grad = dot(gb[rows, :], w2, ((1,), (1,))) * slope
            vv[pl.ds(b, 1)] += jnp.sum(pre_grad, axis=0, keepdims=True)
            lowp = pre_grad.astype(BF16)
            dcs[rows, :] = lowp
            out = dot(hidden, w2)
            back = dot(lowp, w1)
            if first:
                y_acc[0, rows] = out[:, 0:half]
                y_acc[1, rows] = out[:, half:width]
                da_acc[0, rows] = back[:, 0:half]
                da_acc[1, rows] = back[:, half:width]
            else:
                y_acc[0, rows] += out[:, 0:half]
                y_acc[1, rows] += out[:, half:width]
                da_acc[0, rows] += back[:, 0:half]
                da_acc[1, rows] += back[:, half:width]
            if hook is not None:
                hook(t)
            return carry

        lax.fori_loop(0, n_tiles, block_tile, 0)
        for i, (rows_of, columns_of) in enumerate(((dcs, ab), (hs, gb))):
            gw[i, b] = dot(rows_of[...], columns_of[...], ((0,), (0,))).reshape(RING, unit, width)
            if send_part is not None:
                send_part(i)

    def relay_gather(t):
        @pl.when(t == 0)
        def _():
            relay1(1)

        @pl.when(t == 1)
        def _():
            relay1(2)
            relay2(3)

    assert n_tiles == RING
    block(p, True, relay_gather)
    relay1(3)
    go(wg.at[0, p], M5, m_right)
    go(wg.at[1, p], M6, m_left)

    for t in range(RING):
        arrive(w2u(po, unit2(t)), M4 + t)
        arrive(w1u(po, unit1(t)), M3 + t)
    def back1(t):
        return wrap(q - gray(RING - 1 - t))

    def back2(t):
        return wrap(q + gray(RING - 1 - t))

    def send_opposite(i):
        for t in range(RING):
            u = back2(t) if i else back1(t)
            rc(gw.at[i, po, u], opp.at[i, u], (R2 if i else R1) + t, m_right if i else m_left).start()

    block(po, False, send_part=send_opposite)

    arrive(wg.at[1, pr], M6)
    def send_right(i):
        if i == 0:
            rc(gw.at[0, pr], dirs.at[0], R3, m_right).start()

    block(pr, False, send_part=send_right)
    arrive(wg.at[0, pl_], M5)
    block(pl_, False)

    def direct2(t):
        u = back2(t)
        rc(gw.at[1, pl_, u], dirs.at[1, u], R4 + t, m_left).start()

    direct2(0)
    direct2(1)

    lane = lax.broadcasted_iota(jnp.int32, (tile, 128), 1)

    def stat_tile(t, carry):
        rows = pl.ds(pl.multiple_of(t * tile, tile), tile)
        mean, inv = mean_s[rows], inv_s[rows]
        v0 = da_acc[0, rows] * lnv[0, 0:1]
        v1 = da_acc[1, rows] * lnv[1, 0:1]
        h0 = (xf[0, rows].astype(F32) - mean) * inv
        h1 = (xf[1, rows].astype(F32) - mean) * inv
        one = jnp.sum(v0, axis=1, keepdims=True) + jnp.sum(v1, axis=1, keepdims=True)
        two = jnp.sum(v0 * h0, axis=1, keepdims=True) + jnp.sum(v1 * h1, axis=1, keepdims=True)
        stat[rows] = jnp.where(lane < 64, one, two)
        return carry

    rc(y_acc.at[other], yr, EY, partner).start()
    rc(da_acc.at[other], dar, ED, partner).start()
    lax.fori_loop(0, n_tiles, stat_tile, 0)
    rc(stat, statr, ES, partner).start()

    for t in range(RING):
        u1, u2 = back1(t), back2(t)
        arrive(opp.at[1, u2], R2 + t)
        gw[1, pr, u2] += opp[1, u2]
        rc(gw.at[1, pr, u2], rel.at[1, u2], R6 + t, m_right).start()
        arrive(opp.at[0, u1], R1 + t)
        gw[0, pl_, u1] += opp[0, u1]
        rc(gw.at[0, pl_, u1], rel.at[0, u1], R5 + t, m_left).start()
    direct2(2)
    direct2(3)

    arrive(yr, EY)
    arrive(dar, ED)
    arrive(statr, ES)
    b_down = bd_ref[...].astype(F32).reshape(1, half)

    def out_tile(t, carry):
        rows = pl.ds(pl.multiple_of(t * tile, tile), tile)
        x_own = xf[e, rows].astype(F32)
        y_ref[rows] = (x_own + (y_acc[e, rows] + yr[rows]) + b_down).astype(BF16)
        norm_grad = da_acc[e, rows] + dar[rows]
        sums = (stat[rows] + statr[rows]) / width
        inv = inv_s[rows]
        x_hat = (x_own - mean_s[rows]) * inv
        value = norm_grad * lnv[e, 0:1]
        dx_ref[rows] = (gf[e, rows].astype(F32) + inv * (value - sums[:, 0:1] - x_hat * sums[:, 64:65])).astype(BF16)
        vv[RING + 1:RING + 2] += jnp.sum(norm_grad * x_hat, axis=0, keepdims=True)
        vv[RING + 2:RING + 3] += jnp.sum(norm_grad, axis=0, keepdims=True)
        return carry

    lax.fori_loop(0, n_tiles, out_tile, 0)

    vs[q] = vv[...]
    for k, d in ((1, s_right), (2, s_opp_dev), (3, s_left)):
        go(vs.at[q], VS + k, d)
    for k in range(1, RING):
        arrive(vs.at[wrap(q - k)], VS + k)
    vm[p] = ((vs[0] + vs[1]) + vs[2]) + vs[3]
    for k, d in ((1, m_right), (2, m_opp), (3, m_left)):
        go(vm.at[p], VM + k, d)

    arrive(dirs.at[0], R3)

    def reduce1(t):
        u = back1(t)
        arrive(rel.at[0, u], R5 + t)
        gw[0, p, u] += dirs[0, u] + rel[0, u]
        if t == 0:
            rc(gw.at[0, p, u], s_opp.at[0], Q1, s_left).start()
        if t == 1:
            rc(gw.at[0, p, u], s_dir.at[0], Q3, s_right).start()
        if t == 2:
            arrive(s_opp.at[0], Q1)
            gw[0, p, u] += s_opp[0]
            rc(gw.at[0, p, u], s_rel.at[0], Q5, s_left).start()

    def reduce2(t):
        u = back2(t)
        arrive(dirs.at[1, u], R4 + t)
        arrive(rel.at[1, u], R6 + t)
        gw[1, p, u] += dirs[1, u] + rel[1, u]
        if t == 0:
            rc(gw.at[1, p, u], s_opp.at[1], Q2, s_right).start()
        if t == 1:
            rc(gw.at[1, p, u], s_dir.at[1], Q4, s_left).start()
        if t == 2:
            arrive(s_opp.at[1], Q2)
            gw[1, p, u] += s_opp[1]
            rc(gw.at[1, p, u], s_rel.at[1], Q6, s_right).start()

    reduce1(0)
    reduce1(1)
    reduce2(0)
    reduce1(2)
    reduce2(1)
    reduce1(3)
    reduce2(2)

    arrive(s_dir.at[0], Q3)
    arrive(s_rel.at[0], Q5)
    done1 = gw[0, p, q] + s_dir[0] + s_rel[0]
    for k in range(RING):
        for h in range(2):
            start = (h * RING + k) * unit
            piece = jnp.concatenate([done1[:, start:start + unit], jnp.zeros((unit, LANES - unit), F32)], axis=1)
            f1[k, h] = piece.astype(BF16)
    for k in (2, 1, 3):
        for h in range(2):
            rc(f1.at[wrap(r + k), h], f1l.at[r, e], F1 + 2 * k + h,
               {"row": wrap(r + k), "col": c, "dep": h}, F1 + 2 * k + e).start()
    rc(f1.at[r, other], f1l.at[r, e], F1 + other, partner, F1 + e).start()
    f1l[r, e] = f1[r, e]
    reduce2(3)
    for k in range(1, RING):
        arrive(vm.at[wrap(p - k)], VM + k)
    vp[e] = ((vm[0] + vm[1]) + vm[2]) + vm[3]
    go(vp.at[e], VP, partner)
    arrive(s_dir.at[1], Q4)
    arrive(s_rel.at[1], Q6)
    done2 = (gw[1, p, q] + s_dir[1] + s_rel[1]).astype(BF16)
    f2[0] = done2[:, 0:half]
    f2[1] = done2[:, half:width]
    rc(f2.at[other], f2l.at[e], F2, partner).start()
    f2l[e] = f2[e]

    arrive(vp.at[other], VP)
    pieces = []
    for k in range(RING):
        pieces.append(vp[0, pl.ds(c, 1)][:, k * unit:(k + 1) * unit])
        row = vp[1, k:k + 1]
        piece = row[:, 0:unit]
        for j in range(1, RING):
            piece = jnp.where(c == j, row[:, j * unit:(j + 1) * unit], piece)
        pieces.append(piece)
    dbu_ref[...] = jnp.concatenate(pieces, axis=1).reshape(dbu_ref.shape)
    dbd_ref[...] = vp[e, RING:RING + 1].reshape(dbd_ref.shape)
    dsc_ref[...] = vp[e, RING + 1:RING + 2].reshape(dsc_ref.shape)
    dsh_ref[...] = vp[e, RING + 2:RING + 3].reshape(dsh_ref.shape)

    sent(l2.at[0], P2)
    sent(l1.at[0, 0], P1 + other)
    sent(l1.at[0, 0], F1 + other)
    for k in range(1, RING):
        for h in range(2):
            sent(l1.at[0, 0], P1 + 2 * k + h)
            sent(l1.at[0, 0], F1 + 2 * k + h)
        sent(bi.at[c], BI + k)
        sent(vm.at[p], VM + k)
        sent(vs.at[q], VS + k)
    sent(f2.at[0], F2)
    sent(lnv.at[0], DLN)
    sent(x_hbm, DX)
    sent(g_hbm, DG)
    for sem in (S1, S2, S3, S4, S5, S6):
        sent(w1u(p, q), sem)
    for t in range(RING):
        for sem in (M1, M2, M3, M4):
            sent(w1u(p, q), sem + t)
        for sem in (R1, R2, R4, R5, R6):
            sent(gw.at[0, p, q], sem + t)
    sent(wg.at[0, p], M5)
    sent(wg.at[0, p], M6)
    sent(gw.at[0, p], R3)
    for sem in (Q1, Q2, Q3, Q4, Q5, Q6):
        sent(gw.at[0, p, q], sem)
    sent(vp.at[e], VP)
    sent(yr, EY)
    sent(dar, ED)
    sent(stat, ES)

    arrive(f2l.at[other], F2)
    dw2_ref[0:unit] = f2l[0]
    dw2_ref[unit:2 * unit] = f2l[1]
    arrive(f1l.at[r, other], F1 + other)
    for k in range(1, RING):
        for h in range(2):
            arrive(f1l.at[wrap(r - k), h], F1 + 2 * k + h)
    dw1_ref[...] = f1l[...].astype(F32).reshape(2 * fb, LANES).T[0:unit].astype(BF16)


def copy_out(*refs):
    n = len(refs) // 2
    copies = [pltpu.make_async_copy(refs[i], refs[n + i], refs[2 * n].at[i]) for i in range(n)]
    for copy in copies:
        copy.start()
    for copy in copies:
        copy.wait()


def solution(mesh):
    assert mesh.shape["row"] == RING and mesh.shape["col"] == RING and mesh.shape["dep"] == 2
    tok_spec = P(("part", "row", "col"), "dep")
    vec_dep = P("dep")
    part_dep = P(("part", "dep"))
    in_specs = (tok_spec, vec_dep, vec_dep, P(("dep", "row"), "col"), P("col"), P(("col", "row"), "dep"), vec_dep, tok_spec)
    out_specs = (tok_spec, tok_spec, P(("part", "dep", "row"), "col"), P(("part", "col")), P(("part", "col", "row"), "dep"), part_dep, part_dep, part_dep)

    def local_step(x_in, ln_scale, ln_shift, w_up, b_up, w_down, b_down, y_grad):
        tokens, half = x_in.shape
        width = 2 * half
        unit = w_down.shape[0] // 2
        fb = RING * unit
        assert w_up.shape == (unit, 2 * fb) and half == RING * unit and fb == half
        tile = tokens // RING
        hbm_spec = pl.BlockSpec(memory_space=pltpu.HBM)
        vmem_spec = pl.BlockSpec(memory_space=pltpu.VMEM)
        vmem = pltpu.VMEM
        scratch = [
            vmem((unit, 2 * fb), BF16),
            vmem((RING, 2, unit, LANES), BF16), vmem((RING, 2, unit, LANES), BF16), vmem((2, unit, half), BF16),
            vmem((2, tokens, half), BF16), vmem((2, tokens, half), BF16),
            vmem((2, 8, half), F32),
            vmem((2, RING, RING, unit, width), BF16),
            vmem((RING, 8, 2 * fb), F32), vmem((RING, 8, fb), F32),
            vmem((tokens, width), BF16), vmem((tokens, width), BF16),
            vmem((tokens, 1), F32), vmem((tokens, 1), F32),
            vmem((2, tokens, half), F32), vmem((2, tokens, half), F32),
            vmem((tokens, half), F32), vmem((tokens, half), F32),
            vmem((tokens, 128), F32), vmem((tokens, 128), F32),
            vmem((tokens, fb), BF16), vmem((tokens, fb), BF16),
            vmem((2, RING, RING, unit, width), F32),
            vmem((2, RING, unit, width), F32), vmem((2, RING, unit, width), F32), vmem((2, RING, unit, width), F32),
            vmem((2, unit, width), F32), vmem((2, unit, width), F32), vmem((2, unit, width), F32),
            vmem((8, half), F32), vmem((RING, 8, half), F32), vmem((RING, 8, half), F32), vmem((2, 8, half), F32),
            vmem((RING, 2, unit, LANES), BF16), vmem((RING, 2, unit, LANES), BF16),
            vmem((2, unit, half), BF16), vmem((2, unit, half), BF16),
            vmem((half,), F32), vmem((half,), F32), vmem((2 * fb,), BF16), vmem((half,), BF16),
            pltpu.SemaphoreType.DMA((N_SEM,)), pltpu.SemaphoreType.DMA((N_SEM,)),
        ]
        shapes = (
            jax.ShapeDtypeStruct((tokens, half), BF16), jax.ShapeDtypeStruct((tokens, half), BF16),
            jax.ShapeDtypeStruct(w_up.shape, BF16), jax.ShapeDtypeStruct(b_up.shape, F32),
            jax.ShapeDtypeStruct(w_down.shape, BF16), jax.ShapeDtypeStruct((half,), F32),
            jax.ShapeDtypeStruct((half,), F32), jax.ShapeDtypeStruct((half,), F32))
        outs = pl.pallas_call(
            functools.partial(kernel, tile),
            out_shape=shapes,
            in_specs=[hbm_spec] * 8,
            out_specs=(vmem_spec,) * 8,
            scratch_shapes=scratch,
            compiler_params=pltpu.CompilerParams(collective_id=0, has_side_effects=True, vmem_limit_bytes=46 * 1024 * 1024),
        )(*(pltpu.with_memory_space_constraint(v, pltpu.HBM) for v in (x_in, ln_scale, ln_shift, w_up, b_up, w_down, b_down, y_grad)))
        return pl.pallas_call(
            copy_out,
            out_shape=shapes,
            in_specs=[vmem_spec] * len(shapes),
            out_specs=(hbm_spec,) * len(shapes),
            scratch_shapes=[pltpu.SemaphoreType.DMA((len(shapes),))],
            compiler_params=pltpu.CompilerParams(vmem_limit_bytes=4 * 1024 * 1024),
        )(*outs)

    return jax.shard_map(local_step, mesh=mesh, in_specs=in_specs, out_specs=out_specs, check_vma=False)
```

```python
import functools

import jax
import jax.numpy as jnp
from jax import lax
from jax.experimental import pallas as pl
from jax.experimental.pallas import tpu as pltpu
from jax.sharding import PartitionSpec as P

LN_EPS = 1e-5
GELU_K = 0.7978845608028654
GELU_C = 0.044715
MESH = pl.DeviceIdType.MESH
F32 = jnp.float32
BF16 = jnp.bfloat16
RING = 4
LANES = 128

_next = [0]


def _ids(count=1):
    base = _next[0]
    _next[0] += count
    return base


IN_SEM = _ids(8)
P1 = _ids(2 * RING)
P2, DX, DG, DLN = _ids(), _ids(), _ids(), _ids()
BI = _ids(RING)
S1, S2, S3, S4, S5, S6 = (_ids() for _ in range(6))
M1, M2, M3, M4 = (_ids(RING) for _ in range(4))
M5, M6 = _ids(RING), _ids(RING)
R1, R2, R5, R6 = (_ids(RING) for _ in range(4))
R3, R4 = _ids(), _ids(RING)
Q1, Q2, Q3, Q4, Q5, Q6 = (_ids() for _ in range(6))
VM, VS = _ids(RING), _ids(RING)
VP = _ids()
EY, ED, ES = _ids(), _ids(), _ids()
F1 = _ids(2 * RING)
F2 = _ids()
N_SEM = _next[0]


def gray(t):
    return t + (t // 2) * (5 - 2 * t)


def dot(a, b, dims=((1,), (0,))):
    return lax.dot_general(a, b, (dims, ((), ())), preferred_element_type=F32)


def kernel(tile, x_hbm, sc_hbm, sh_hbm, w1_hbm, bu_hbm, w2_hbm, bd_hbm, g_hbm,
           y_ref, dx_ref, dw1_ref, dbu_ref, dw2_ref, dbd_ref, dsc_ref, dsh_ref,
           w1v, st1, l1, l2, xf, gf, lnv, wg, bi, bias_u, ab, gb, mean_s, inv_s,
           y_acc, da_acc, yr, dar, stat, statr, hs, dcs, hs2, dcs2, db_u, gw, opp, dirs, rel, s_opp, s_dir, s_rel,
           vv, vm, vs, vp, f1, f1l, f2, f2l, sc_ref, sh_ref, bu_ref, bd_ref, send, recv):
    r, c, e = lax.axis_index("row"), lax.axis_index("col"), lax.axis_index("dep")
    p = c + e * (r - c)
    q = r + e * (c - r)
    tokens, half = xf.shape[1], xf.shape[2]
    width = 2 * half
    unit = l2.shape[1]
    fb = RING * unit
    n_tiles = tokens // tile
    other = 1 - e

    def wrap(v):
        return lax.rem(v + 2 * RING, RING)

    def dev(pp, qq):
        return {"row": qq + e * (pp - qq), "col": pp + e * (qq - pp), "dep": e}

    m_right, m_left, m_opp = dev(wrap(p + 1), q), dev(wrap(p - 1), q), dev(wrap(p + 2), q)
    s_right, s_left, s_opp_dev = dev(p, wrap(q + 1)), dev(p, wrap(q - 1)), dev(p, wrap(q + 2))
    partner = {"row": r, "col": c, "dep": other}
    pr, pl_, po = wrap(p + 1), wrap(p - 1), wrap(p + 2)
    qr, ql, qo = wrap(q + 1), wrap(q - 1), wrap(q + 2)

    def rc(src, dst, ssem, device, rsem=None):
        return pltpu.make_async_remote_copy(
            src_ref=src, dst_ref=dst, send_sem=send.at[ssem], recv_sem=recv.at[ssem if rsem is None else rsem],
            device_id=device, device_id_type=MESH)

    def arrive(dst, rsem):
        rc(dst, dst, rsem, partner).wait_recv()

    def sent(src, ssem):
        rc(src, src, ssem, partner).wait_send()

    def go(ref, sem, device):
        rc(ref, ref, sem, device).start()

    load_w1 = pltpu.make_async_copy(w1_hbm, w1v, recv.at[IN_SEM])
    load_w2 = pltpu.make_async_copy(w2_hbm.at[pl.ds(pl.multiple_of(e * unit, 16), unit)], l2.at[e], recv.at[IN_SEM + 1])
    load_x = pltpu.make_async_copy(x_hbm, xf.at[e], recv.at[IN_SEM + 2])
    load_g = pltpu.make_async_copy(g_hbm, gf.at[e], recv.at[IN_SEM + 3])
    load_vectors = [pltpu.make_async_copy(src, dst, recv.at[IN_SEM + 4 + i]) for i, (src, dst) in enumerate(
        ((sc_hbm, sc_ref), (sh_hbm, sh_ref), (bu_hbm, bu_ref), (bd_hbm, bd_ref)))]
    load_w1.start()
    load_w2.start()
    for load in load_vectors:
        load.start()
    load_x.start()
    load_g.start()

    barrier = pltpu.get_barrier_semaphore()
    peers = [m_right, m_left, s_right, s_left, m_opp, s_opp_dev, partner]
    peers += [{"row": wrap(r + k), "col": c, "dep": other} for k in range(1, RING)]
    for d in peers:
        pl.semaphore_signal(barrier, inc=1, device_id=d, device_id_type=MESH)

    load_w1.wait()
    turned = w1v[...].astype(F32)
    turned = jnp.concatenate([turned, jnp.zeros((LANES - unit, 2 * fb), F32)], axis=0).T.astype(BF16)
    for k in range(RING):
        for h in range(2):
            st1[k, h] = turned[(2 * k + h) * unit:(2 * k + h + 1) * unit]

    for load in load_vectors:
        load.wait()
    lnv[e, 0:1] = sc_ref[...].reshape(1, half)
    lnv[e, 1:2] = sh_ref[...].reshape(1, half)
    bi[c] = jnp.broadcast_to(bu_ref[...].astype(F32).reshape(1, 2 * fb), (8, 2 * fb))

    pl.semaphore_wait(barrier, len(peers))

    rc(w2_hbm.at[pl.ds(pl.multiple_of(other * unit, 16), unit)], l2.at[e], P2, partner).start()
    rc(st1.at[r, other], l1.at[r, e], P1 + other, partner, P1 + e).start()
    for k in (2, 1, 3):
        for h in range(2):
            rc(st1.at[wrap(r + k), h], l1.at[r, e], P1 + 2 * k + h,
               {"row": wrap(r + k), "col": c, "dep": h}, P1 + 2 * k + e).start()
    rc(lnv.at[e], lnv.at[e], DLN, partner).start()
    rc(x_hbm, xf.at[e], DX, partner).start()
    rc(g_hbm, gf.at[e], DG, partner).start()
    for k in range(1, RING):
        rc(bi.at[c], bi.at[c], BI + k, {"row": r, "col": wrap(c + k), "dep": e}).start()
    l1[r, e] = st1[r, e]

    def w1u(b, s):
        return wg.at[0, b, s]

    def w2u(b, s):
        return wg.at[1, b, s]

    load_w2.wait()
    arrive(l2.at[other], P2)
    wg[1, p, q, :, 0:half] = l2[0]
    wg[1, p, q, :, half:width] = l2[1]
    go(w2u(p, q), M2, m_right)
    go(w2u(p, q), S2, s_right)
    go(w2u(p, q), S4, s_left)
    go(w2u(p, q), M6, m_left)

    arrive(l1.at[r, other], P1 + other)
    for k in range(1, RING):
        for h in range(2):
            arrive(l1.at[wrap(r - k), h], P1 + 2 * k + h)
    wg[0, p, q] = jnp.concatenate([l1[k, h][:, 0:unit].astype(F32) for h in range(2) for k in range(RING)], axis=1).astype(BF16)
    go(w1u(p, q), M1, m_left)
    go(w1u(p, q), S1, s_right)
    go(w1u(p, q), S3, s_left)
    go(w1u(p, q), M5, m_right)

    arrive(w2u(p, ql), S2)
    go(w2u(p, ql), S6, s_right)
    arrive(w2u(p, qr), S4)
    go(w2u(p, qr), M2 + 1, m_right)
    go(w2u(p, ql), M2 + 2, m_right)
    go(w2u(p, qr), M6 + 1, m_left)
    go(w2u(p, ql), M6 + 2, m_left)

    def nth(t):
        return wrap(q + gray(t))

    arrive(lnv.at[other], DLN)
    load_x.wait()
    arrive(xf.at[other], DX)
    load_g.wait()
    arrive(gf.at[other], DG)
    vv[...] = jnp.zeros_like(vv)
    def norm_tile(t, carry):
        rows = pl.ds(pl.multiple_of(t * tile, tile), tile)
        x0, x1 = xf[0, rows].astype(F32), xf[1, rows].astype(F32)
        total = jnp.sum(x0, axis=1, keepdims=True) + jnp.sum(x1, axis=1, keepdims=True)
        squares = jnp.sum(x0 * x0, axis=1, keepdims=True) + jnp.sum(x1 * x1, axis=1, keepdims=True)
        mean = total / width
        inv = lax.rsqrt(squares / width - mean * mean + LN_EPS)
        mean_s[rows] = mean
        inv_s[rows] = inv
        ab[rows, 0:half] = ((x0 - mean) * inv * lnv[0, 0:1] + lnv[0, 1:2]).astype(BF16)
        ab[rows, half:width] = ((x1 - mean) * inv * lnv[1, 0:1] + lnv[1, 1:2]).astype(BF16)
        gb[rows, 0:half] = gf[0, rows]
        gb[rows, half:width] = gf[1, rows]
        vv[RING:RING + 1] += jnp.sum(gf[e, rows].astype(F32), axis=0, keepdims=True)
        return carry

    lax.fori_loop(0, n_tiles // 2, norm_tile, 0)
    arrive(w1u(p, qr), S3)
    go(w1u(p, qr), S5, s_left)
    go(w1u(p, qr), M1 + 1, m_left)
    lax.fori_loop(n_tiles // 2, n_tiles, norm_tile, 0)

    def relay1(t):
        arrive(w1u(pr, nth(t)), M1 + t)
        go(w1u(pr, nth(t)), M3 + t, m_left)

    def relay2(t):
        arrive(w2u(pl_, nth(t)), M2 + t)
        go(w2u(pl_, nth(t)), M4 + t, m_right)

    arrive(w1u(p, ql), S1)
    go(w1u(p, ql), M1 + 2, m_left)
    relay2(0)
    for k in range(1, RING):
        arrive(bi.at[wrap(c - k)], BI + k)
    for b in range(RING):
        for k in range(RING):
            flat = bi[b, 0:1, 2 * k * unit:(2 * k + 1) * unit]
            across = bi[k, 0:1, (2 * b + 1) * unit:(2 * b + 2) * unit]
            bias_u[b, k, 0:1, 0:unit] = jnp.where(e == 0, flat, across)
    arrive(w2u(p, qo), S6)
    go(w2u(p, qo), M2 + 3, m_right)
    relay1(0)
    relay2(1)
    arrive(w1u(p, qo), S5)
    go(w1u(p, qo), M1 + 3, m_left)
    relay2(2)

    def block(b, first=False, units=None, hook=None, send_part=None):
        bias = jnp.concatenate([bias_u[b, u, 0:1, 0:unit] for u in (range(RING) if units is None else units)], axis=1)
        hid, low = (hs, dcs) if units is None else (hs2, dcs2)

        def weight(i):
            if units is None:
                return wg[i, b].reshape(fb, width)
            return jnp.concatenate([wg[i, b, u] for u in units], axis=0)

        def block_tile(t, carry):
            rows = pl.ds(pl.multiple_of(t * tile, tile), tile)
            w1, w2 = weight(0), weight(1)
            pre = dot(ab[rows, :], w1, ((1,), (1,))) + bias
            squared = pre * pre
            tanh_val = jnp.tanh(GELU_K * (pre + GELU_C * pre * squared))
            hidden = (0.5 * pre * (1.0 + tanh_val)).astype(BF16)
            hid[rows, :] = hidden
            slope = 0.5 * (1.0 + tanh_val) + 0.5 * pre * (1.0 - tanh_val * tanh_val) * GELU_K * (1.0 + 3.0 * GELU_C * squared)
            pre_grad = dot(gb[rows, :], w2, ((1,), (1,))) * slope
            sums = jnp.sum(pre_grad, axis=0, keepdims=True)
            if units is None:
                vv[pl.ds(b, 1)] += sums
            else:
                for i, u in enumerate(units):
                    db_u[u, 0:1, 0:unit] += sums[:, i * unit:(i + 1) * unit]
            lowp = pre_grad.astype(BF16)
            low[rows, :] = lowp
            out = dot(hidden, w2)
            back = dot(lowp, w1)
            if first:
                y_acc[0, rows] = out[:, 0:half]
                y_acc[1, rows] = out[:, half:width]
                da_acc[0, rows] = back[:, 0:half]
                da_acc[1, rows] = back[:, half:width]
            else:
                y_acc[0, rows] += out[:, 0:half]
                y_acc[1, rows] += out[:, half:width]
                da_acc[0, rows] += back[:, 0:half]
                da_acc[1, rows] += back[:, half:width]
            if hook is not None:
                hook(t)
            return carry

        lax.fori_loop(0, n_tiles, block_tile, 0)
        for i, (rows_of, columns_of) in enumerate(((low, ab), (hid, gb))):
            part = dot(rows_of[...], columns_of[...], ((0,), (0,)))
            if units is None:
                gw[i, b] = part.reshape(RING, unit, width)
            else:
                for j, u in enumerate(units):
                    gw[i, b, u] = part[j * unit:(j + 1) * unit]
            if send_part is not None:
                send_part(i)

    def relay_gather(t):
        @pl.when(t == 0)
        def _():
            relay1(1)

        @pl.when(t == 1)
        def _():
            relay1(2)
            relay2(3)

    assert n_tiles == RING
    block(p, first=True, hook=relay_gather)
    relay1(3)
    for t in range(1, RING):
        go(w1u(p, nth(t)), M5 + t, m_right)
    go(w2u(p, qo), M6 + 3, m_left)

    def back1(t):
        return wrap(q - gray(RING - 1 - t))

    def back2(t):
        return wrap(q + gray(RING - 1 - t))

    db_u[...] = jnp.zeros_like(db_u)
    for first in (0, 2):
        for t in (first, first + 1):
            arrive(w2u(po, nth(t)), M4 + t)
            arrive(w1u(po, nth(t)), M3 + t)

        def send_opposite(i):
            for t in (first, first + 1):
                u = nth(t)
                rc(gw.at[i, po, u], opp.at[i, u], (R2 if i else R1) + t, m_right if i else m_left).start()

        block(po, units=(nth(first), nth(first + 1)), send_part=send_opposite)
    vv[pl.ds(po, 1)] = jnp.concatenate([db_u[u, 0:1, 0:unit] for u in range(RING)], axis=1)

    for t in range(RING):
        arrive(w2u(pr, nth(t)), M6 + t)
    def send_right(i):
        if i == 0:
            rc(gw.at[0, pr], dirs.at[0], R3, m_right).start()

    block(pr, send_part=send_right)
    for t in range(RING):
        arrive(w1u(pl_, nth(t)), M5 + t)
    block(pl_)

    def direct2(t):
        u = back2(t)
        rc(gw.at[1, pl_, u], dirs.at[1, u], R4 + t, m_left).start()

    direct2(0)
    direct2(1)

    lane = lax.broadcasted_iota(jnp.int32, (tile, 128), 1)

    def stat_tile(t, carry):
        rows = pl.ds(pl.multiple_of(t * tile, tile), tile)
        mean, inv = mean_s[rows], inv_s[rows]
        v0 = da_acc[0, rows] * lnv[0, 0:1]
        v1 = da_acc[1, rows] * lnv[1, 0:1]
        h0 = (xf[0, rows].astype(F32) - mean) * inv
        h1 = (xf[1, rows].astype(F32) - mean) * inv
        one = jnp.sum(v0, axis=1, keepdims=True) + jnp.sum(v1, axis=1, keepdims=True)
        two = jnp.sum(v0 * h0, axis=1, keepdims=True) + jnp.sum(v1 * h1, axis=1, keepdims=True)
        stat[rows] = jnp.where(lane < 64, one, two)
        return carry

    rc(y_acc.at[other], yr, EY, partner).start()
    rc(da_acc.at[other], dar, ED, partner).start()
    lax.fori_loop(0, n_tiles, stat_tile, 0)
    rc(stat, statr, ES, partner).start()

    for t in range(RING):
        arrive(opp.at[1, nth(t)], R2 + t)
        arrive(opp.at[0, nth(t)], R1 + t)
    for t in range(RING):
        u1, u2 = back1(t), back2(t)
        gw[1, pr, u2] += opp[1, u2]
        rc(gw.at[1, pr, u2], rel.at[1, u2], R6 + t, m_right).start()
        gw[0, pl_, u1] += opp[0, u1]
        rc(gw.at[0, pl_, u1], rel.at[0, u1], R5 + t, m_left).start()
    direct2(2)
    direct2(3)

    arrive(yr, EY)
    arrive(dar, ED)
    arrive(statr, ES)
    b_down = bd_ref[...].astype(F32).reshape(1, half)

    def out_tile(t, carry):
        rows = pl.ds(pl.multiple_of(t * tile, tile), tile)
        x_own = xf[e, rows].astype(F32)
        y_ref[rows] = (x_own + (y_acc[e, rows] + yr[rows]) + b_down).astype(BF16)
        norm_grad = da_acc[e, rows] + dar[rows]
        sums = (stat[rows] + statr[rows]) / width
        inv = inv_s[rows]
        x_hat = (x_own - mean_s[rows]) * inv
        value = norm_grad * lnv[e, 0:1]
        dx_ref[rows] = (gf[e, rows].astype(F32) + inv * (value - sums[:, 0:1] - x_hat * sums[:, 64:65])).astype(BF16)
        vv[RING + 1:RING + 2] += jnp.sum(norm_grad * x_hat, axis=0, keepdims=True)
        vv[RING + 2:RING + 3] += jnp.sum(norm_grad, axis=0, keepdims=True)
        return carry

    lax.fori_loop(0, n_tiles, out_tile, 0)

    vs[q] = vv[...]
    for k, d in ((1, s_right), (2, s_opp_dev), (3, s_left)):
        go(vs.at[q], VS + k, d)
    for k in range(1, RING):
        arrive(vs.at[wrap(q - k)], VS + k)
    vm[p] = ((vs[0] + vs[1]) + vs[2]) + vs[3]
    for k, d in ((1, m_right), (2, m_opp), (3, m_left)):
        go(vm.at[p], VM + k, d)

    arrive(dirs.at[0], R3)

    def reduce1(t):
        u = back1(t)
        arrive(rel.at[0, u], R5 + t)
        gw[0, p, u] += dirs[0, u] + rel[0, u]
        if t == 0:
            rc(gw.at[0, p, u], s_opp.at[0], Q1, s_left).start()
        if t == 1:
            rc(gw.at[0, p, u], s_dir.at[0], Q3, s_right).start()
        if t == 2:
            arrive(s_opp.at[0], Q1)
            gw[0, p, u] += s_opp[0]
            rc(gw.at[0, p, u], s_rel.at[0], Q5, s_left).start()

    def reduce2(t):
        u = back2(t)
        arrive(dirs.at[1, u], R4 + t)
        arrive(rel.at[1, u], R6 + t)
        gw[1, p, u] += dirs[1, u] + rel[1, u]
        if t == 0:
            rc(gw.at[1, p, u], s_opp.at[1], Q2, s_right).start()
        if t == 1:
            rc(gw.at[1, p, u], s_dir.at[1], Q4, s_left).start()
        if t == 2:
            arrive(s_opp.at[1], Q2)
            gw[1, p, u] += s_opp[1]
            rc(gw.at[1, p, u], s_rel.at[1], Q6, s_right).start()

    reduce1(0)
    reduce1(1)
    reduce2(0)
    reduce1(2)
    reduce2(1)
    reduce1(3)
    reduce2(2)

    arrive(s_dir.at[0], Q3)
    arrive(s_rel.at[0], Q5)
    done1 = gw[0, p, q] + s_dir[0] + s_rel[0]
    for k in range(RING):
        for h in range(2):
            start = (h * RING + k) * unit
            piece = jnp.concatenate([done1[:, start:start + unit], jnp.zeros((unit, LANES - unit), F32)], axis=1)
            f1[k, h] = piece.astype(BF16)
    for k in (2, 1, 3):
        for h in range(2):
            rc(f1.at[wrap(r + k), h], f1l.at[r, e], F1 + 2 * k + h,
               {"row": wrap(r + k), "col": c, "dep": h}, F1 + 2 * k + e).start()
    rc(f1.at[r, other], f1l.at[r, e], F1 + other, partner, F1 + e).start()
    f1l[r, e] = f1[r, e]
    reduce2(3)
    for k in range(1, RING):
        arrive(vm.at[wrap(p - k)], VM + k)
    vp[e] = ((vm[0] + vm[1]) + vm[2]) + vm[3]
    go(vp.at[e], VP, partner)
    arrive(s_dir.at[1], Q4)
    arrive(s_rel.at[1], Q6)
    done2 = (gw[1, p, q] + s_dir[1] + s_rel[1]).astype(BF16)
    f2[0] = done2[:, 0:half]
    f2[1] = done2[:, half:width]
    rc(f2.at[other], f2l.at[e], F2, partner).start()
    f2l[e] = f2[e]

    arrive(vp.at[other], VP)
    pieces = []
    for k in range(RING):
        pieces.append(vp[0, pl.ds(c, 1)][:, k * unit:(k + 1) * unit])
        row = vp[1, k:k + 1]
        piece = row[:, 0:unit]
        for j in range(1, RING):
            piece = jnp.where(c == j, row[:, j * unit:(j + 1) * unit], piece)
        pieces.append(piece)
    dbu_ref[...] = jnp.concatenate(pieces, axis=1).reshape(dbu_ref.shape)
    dbd_ref[...] = vp[e, RING:RING + 1].reshape(dbd_ref.shape)
    dsc_ref[...] = vp[e, RING + 1:RING + 2].reshape(dsc_ref.shape)
    dsh_ref[...] = vp[e, RING + 2:RING + 3].reshape(dsh_ref.shape)

    sent(l2.at[0], P2)
    sent(l1.at[0, 0], P1 + other)
    sent(l1.at[0, 0], F1 + other)
    for k in range(1, RING):
        for h in range(2):
            sent(l1.at[0, 0], P1 + 2 * k + h)
            sent(l1.at[0, 0], F1 + 2 * k + h)
        sent(bi.at[c], BI + k)
        sent(vm.at[p], VM + k)
        sent(vs.at[q], VS + k)
    sent(f2.at[0], F2)
    sent(lnv.at[0], DLN)
    sent(x_hbm, DX)
    sent(g_hbm, DG)
    for sem in (S1, S2, S3, S4, S5, S6):
        sent(w1u(p, q), sem)
    for t in range(RING):
        for sem in (M1, M2, M3, M4, M5, M6):
            sent(w1u(p, q), sem + t)
        for sem in (R1, R2, R4, R5, R6):
            sent(gw.at[0, p, q], sem + t)
    sent(gw.at[0, p], R3)
    for sem in (Q1, Q2, Q3, Q4, Q5, Q6):
        sent(gw.at[0, p, q], sem)
    sent(vp.at[e], VP)
    sent(yr, EY)
    sent(dar, ED)
    sent(stat, ES)

    arrive(f2l.at[other], F2)
    dw2_ref[0:unit] = f2l[0]
    dw2_ref[unit:2 * unit] = f2l[1]
    arrive(f1l.at[r, other], F1 + other)
    for k in range(1, RING):
        for h in range(2):
            arrive(f1l.at[wrap(r - k), h], F1 + 2 * k + h)
    dw1_ref[...] = f1l[...].astype(F32).reshape(2 * fb, LANES).T[0:unit].astype(BF16)


def copy_out(*refs):
    n = len(refs) // 2
    copies = [pltpu.make_async_copy(refs[i], refs[n + i], refs[2 * n].at[i]) for i in range(n)]
    for copy in copies:
        copy.start()
    for copy in copies:
        copy.wait()


def solution(mesh):
    assert mesh.shape["row"] == RING and mesh.shape["col"] == RING and mesh.shape["dep"] == 2
    tok_spec = P(("part", "row", "col"), "dep")
    vec_dep = P("dep")
    part_dep = P(("part", "dep"))
    in_specs = (tok_spec, vec_dep, vec_dep, P(("dep", "row"), "col"), P("col"), P(("col", "row"), "dep"), vec_dep, tok_spec)
    out_specs = (tok_spec, tok_spec, P(("part", "dep", "row"), "col"), P(("part", "col")), P(("part", "col", "row"), "dep"), part_dep, part_dep, part_dep)

    def local_step(x_in, ln_scale, ln_shift, w_up, b_up, w_down, b_down, y_grad):
        tokens, half = x_in.shape
        width = 2 * half
        unit = w_down.shape[0] // 2
        fb = RING * unit
        assert w_up.shape == (unit, 2 * fb) and half == RING * unit and fb == half
        tile = tokens // RING
        hbm_spec = pl.BlockSpec(memory_space=pltpu.HBM)
        vmem_spec = pl.BlockSpec(memory_space=pltpu.VMEM)
        vmem = pltpu.VMEM
        scratch = [
            vmem((unit, 2 * fb), BF16),
            vmem((RING, 2, unit, LANES), BF16), vmem((RING, 2, unit, LANES), BF16), vmem((2, unit, half), BF16),
            vmem((2, tokens, half), BF16), vmem((2, tokens, half), BF16),
            vmem((2, 8, half), F32),
            vmem((2, RING, RING, unit, width), BF16),
            vmem((RING, 8, 2 * fb), F32), vmem((RING, RING, 8, LANES), F32),
            vmem((tokens, width), BF16), vmem((tokens, width), BF16),
            vmem((tokens, 1), F32), vmem((tokens, 1), F32),
            vmem((2, tokens, half), F32), vmem((2, tokens, half), F32),
            vmem((tokens, half), F32), vmem((tokens, half), F32),
            vmem((tokens, 128), F32), vmem((tokens, 128), F32),
            vmem((tokens, fb), BF16), vmem((tokens, fb), BF16),
            vmem((tokens, 2 * unit), BF16), vmem((tokens, 2 * unit), BF16), vmem((RING, 8, LANES), F32),
            vmem((2, RING, RING, unit, width), F32),
            vmem((2, RING, unit, width), F32), vmem((2, RING, unit, width), F32), vmem((2, RING, unit, width), F32),
            vmem((2, unit, width), F32), vmem((2, unit, width), F32), vmem((2, unit, width), F32),
            vmem((8, half), F32), vmem((RING, 8, half), F32), vmem((RING, 8, half), F32), vmem((2, 8, half), F32),
            vmem((RING, 2, unit, LANES), BF16), vmem((RING, 2, unit, LANES), BF16),
            vmem((2, unit, half), BF16), vmem((2, unit, half), BF16),
            vmem((half,), F32), vmem((half,), F32), vmem((2 * fb,), BF16), vmem((half,), BF16),
            pltpu.SemaphoreType.DMA((N_SEM,)), pltpu.SemaphoreType.DMA((N_SEM,)),
        ]
        shapes = (
            jax.ShapeDtypeStruct((tokens, half), BF16), jax.ShapeDtypeStruct((tokens, half), BF16),
            jax.ShapeDtypeStruct(w_up.shape, BF16), jax.ShapeDtypeStruct(b_up.shape, F32),
            jax.ShapeDtypeStruct(w_down.shape, BF16), jax.ShapeDtypeStruct((half,), F32),
            jax.ShapeDtypeStruct((half,), F32), jax.ShapeDtypeStruct((half,), F32))
        outs = pl.pallas_call(
            functools.partial(kernel, tile),
            out_shape=shapes,
            in_specs=[hbm_spec] * 8,
            out_specs=(vmem_spec,) * 8,
            scratch_shapes=scratch,
            compiler_params=pltpu.CompilerParams(collective_id=0, has_side_effects=True, vmem_limit_bytes=50 * 1024 * 1024),
        )(*(pltpu.with_memory_space_constraint(v, pltpu.HBM) for v in (x_in, ln_scale, ln_shift, w_up, b_up, w_down, b_down, y_grad)))
        return pl.pallas_call(
            copy_out,
            out_shape=shapes,
            in_specs=[vmem_spec] * len(shapes),
            out_specs=(hbm_spec,) * len(shapes),
            scratch_shapes=[pltpu.SemaphoreType.DMA((len(shapes),))],
            compiler_params=pltpu.CompilerParams(vmem_limit_bytes=4 * 1024 * 1024),
        )(*outs)

    return jax.shard_map(local_step, mesh=mesh, in_specs=in_specs, out_specs=out_specs, check_vma=False)
```

```python
import functools

import jax
import jax.numpy as jnp
from jax import lax
from jax.experimental import pallas as pl
from jax.experimental.pallas import tpu as pltpu
from jax.sharding import PartitionSpec as P

LN_EPS = 1e-5
GELU_K = 0.7978845608028654
GELU_C = 0.044715
MESH = pl.DeviceIdType.MESH
F32 = jnp.float32
BF16 = jnp.bfloat16
RING = 4
LANES = 128

_next = [0]


def _ids(count=1):
    base = _next[0]
    _next[0] += count
    return base


IN_SEM = _ids(8)
P1 = _ids(2 * RING)
P2, DX, DG, DLN = _ids(), _ids(), _ids(), _ids()
BI = _ids(RING)
S1, S2, S3, S4, S5, S6 = (_ids() for _ in range(6))
M1, M2, M3, M4 = (_ids(RING) for _ in range(4))
M5, M6 = _ids(RING), _ids(RING)
R1, R2, R5, R6 = (_ids(RING) for _ in range(4))
R3, R4 = _ids(), _ids(RING)
Q1, Q2, Q3, Q4, Q5, Q6 = (_ids() for _ in range(6))
VM, VS = _ids(RING), _ids(RING)
VP = _ids()
EY, ED, ES = _ids(), _ids(), _ids()
F1 = _ids(2 * RING)
F2 = _ids()
N_SEM = _next[0]


def gray(t):
    return t + (t // 2) * (5 - 2 * t)


def dot(a, b, dims=((1,), (0,))):
    return lax.dot_general(a, b, (dims, ((), ())), preferred_element_type=F32)


def kernel(tile, x_hbm, sc_hbm, sh_hbm, w1_hbm, bu_hbm, w2_hbm, bd_hbm, g_hbm,
           y_ref, dx_ref, dw1_ref, dbu_ref, dw2_ref, dbd_ref, dsc_ref, dsh_ref,
           w1v, st1, l1, l2, xf, gf, lnv, wg, bi, bias_u, ab, gb, mean_s, inv_s,
           y_acc, da_acc, yr, dar, stat, statr, hs, dcs, hs2, dcs2, db_u, gw, opp, dirs, rel, s_opp, s_dir, s_rel,
           vv, vm, vs, vp, f1, f1l, f2, f2l, sc_ref, sh_ref, bu_ref, bd_ref, send, recv):
    r, c, e = lax.axis_index("row"), lax.axis_index("col"), lax.axis_index("dep")
    p = c + e * (r - c)
    q = r + e * (c - r)
    tokens, half = xf.shape[1], xf.shape[2]
    width = 2 * half
    unit = l2.shape[1]
    fb = RING * unit
    n_tiles = tokens // tile
    other = 1 - e

    def wrap(v):
        return lax.rem(v + 2 * RING, RING)

    def dev(pp, qq):
        return {"row": qq + e * (pp - qq), "col": pp + e * (qq - pp), "dep": e}

    m_right, m_left, m_opp = dev(wrap(p + 1), q), dev(wrap(p - 1), q), dev(wrap(p + 2), q)
    s_right, s_left, s_opp_dev = dev(p, wrap(q + 1)), dev(p, wrap(q - 1)), dev(p, wrap(q + 2))
    partner = {"row": r, "col": c, "dep": other}
    pr, pl_, po = wrap(p + 1), wrap(p - 1), wrap(p + 2)
    qr, ql, qo = wrap(q + 1), wrap(q - 1), wrap(q + 2)

    def rc(src, dst, ssem, device, rsem=None):
        return pltpu.make_async_remote_copy(
            src_ref=src, dst_ref=dst, send_sem=send.at[ssem], recv_sem=recv.at[ssem if rsem is None else rsem],
            device_id=device, device_id_type=MESH)

    def arrive(dst, rsem):
        rc(dst, dst, rsem, partner).wait_recv()

    def sent(src, ssem):
        rc(src, src, ssem, partner).wait_send()

    def go(ref, sem, device):
        rc(ref, ref, sem, device).start()

    load_w1 = pltpu.make_async_copy(w1_hbm, w1v, recv.at[IN_SEM])
    load_w2 = pltpu.make_async_copy(w2_hbm.at[pl.ds(pl.multiple_of(e * unit, 16), unit)], l2.at[e], recv.at[IN_SEM + 1])
    load_x = pltpu.make_async_copy(x_hbm, xf.at[e], recv.at[IN_SEM + 2])
    load_g = pltpu.make_async_copy(g_hbm, gf.at[e], recv.at[IN_SEM + 3])
    load_vectors = [pltpu.make_async_copy(src, dst, recv.at[IN_SEM + 4 + i]) for i, (src, dst) in enumerate(
        ((sc_hbm, sc_ref), (sh_hbm, sh_ref), (bu_hbm, bu_ref), (bd_hbm, bd_ref)))]
    load_w1.start()
    load_w2.start()
    for load in load_vectors:
        load.start()
    load_x.start()
    load_g.start()

    barrier = pltpu.get_barrier_semaphore()
    peers = [m_right, m_left, s_right, s_left, m_opp, s_opp_dev, partner]
    peers += [{"row": wrap(r + k), "col": c, "dep": other} for k in range(1, RING)]
    for d in peers:
        pl.semaphore_signal(barrier, inc=1, device_id=d, device_id_type=MESH)

    load_w1.wait()
    turned = w1v[...].astype(F32)
    turned = jnp.concatenate([turned, jnp.zeros((LANES - unit, 2 * fb), F32)], axis=0).T.astype(BF16)
    for k in range(RING):
        for h in range(2):
            st1[k, h] = turned[(2 * k + h) * unit:(2 * k + h + 1) * unit]

    for load in load_vectors:
        load.wait()
    lnv[e, 0:1] = sc_ref[...].reshape(1, half)
    lnv[e, 1:2] = sh_ref[...].reshape(1, half)
    bi[c] = jnp.broadcast_to(bu_ref[...].astype(F32).reshape(1, 2 * fb), (8, 2 * fb))

    pl.semaphore_wait(barrier, len(peers))

    rc(w2_hbm.at[pl.ds(pl.multiple_of(other * unit, 16), unit)], l2.at[e], P2, partner).start()
    rc(st1.at[r, other], l1.at[r, e], P1 + other, partner, P1 + e).start()
    for k in (2, 1, 3):
        for h in range(2):
            rc(st1.at[wrap(r + k), h], l1.at[r, e], P1 + 2 * k + h,
               {"row": wrap(r + k), "col": c, "dep": h}, P1 + 2 * k + e).start()
    rc(lnv.at[e], lnv.at[e], DLN, partner).start()
    rc(x_hbm, xf.at[e], DX, partner).start()
    rc(g_hbm, gf.at[e], DG, partner).start()
    for k in range(1, RING):
        rc(bi.at[c], bi.at[c], BI + k, {"row": r, "col": wrap(c + k), "dep": e}).start()
    l1[r, e] = st1[r, e]

    def w1u(b, s):
        return wg.at[0, b, s]

    def w2u(b, s):
        return wg.at[1, b, s]

    load_w2.wait()
    arrive(l2.at[other], P2)
    wg[1, p, q, :, 0:half] = l2[0]
    wg[1, p, q, :, half:width] = l2[1]
    go(w2u(p, q), M2, m_right)
    go(w2u(p, q), S2, s_right)
    go(w2u(p, q), S4, s_left)

    arrive(l1.at[r, other], P1 + other)
    for k in range(1, RING):
        for h in range(2):
            arrive(l1.at[wrap(r - k), h], P1 + 2 * k + h)
    wg[0, p, q] = jnp.concatenate([l1[k, h][:, 0:unit].astype(F32) for h in range(2) for k in range(RING)], axis=1).astype(BF16)
    go(w1u(p, q), M1, m_left)
    go(w1u(p, q), S1, s_right)
    go(w1u(p, q), S3, s_left)

    arrive(w2u(p, ql), S2)
    go(w2u(p, ql), S6, s_right)
    arrive(w2u(p, qr), S4)
    go(w2u(p, qr), M2 + 1, m_right)
    go(w2u(p, ql), M2 + 2, m_right)

    def nth(t):
        return wrap(q + gray(t))

    arrive(lnv.at[other], DLN)
    load_x.wait()
    arrive(xf.at[other], DX)
    load_g.wait()
    arrive(gf.at[other], DG)
    vv[...] = jnp.zeros_like(vv)
    def norm_tile(t, carry):
        rows = pl.ds(pl.multiple_of(t * tile, tile), tile)
        x0, x1 = xf[0, rows].astype(F32), xf[1, rows].astype(F32)
        total = jnp.sum(x0, axis=1, keepdims=True) + jnp.sum(x1, axis=1, keepdims=True)
        squares = jnp.sum(x0 * x0, axis=1, keepdims=True) + jnp.sum(x1 * x1, axis=1, keepdims=True)
        mean = total / width
        inv = lax.rsqrt(squares / width - mean * mean + LN_EPS)
        mean_s[rows] = mean
        inv_s[rows] = inv
        ab[rows, 0:half] = ((x0 - mean) * inv * lnv[0, 0:1] + lnv[0, 1:2]).astype(BF16)
        ab[rows, half:width] = ((x1 - mean) * inv * lnv[1, 0:1] + lnv[1, 1:2]).astype(BF16)
        gb[rows, 0:half] = gf[0, rows]
        gb[rows, half:width] = gf[1, rows]
        vv[RING:RING + 1] += jnp.sum(gf[e, rows].astype(F32), axis=0, keepdims=True)
        return carry

    lax.fori_loop(0, n_tiles // 2, norm_tile, 0)
    arrive(w1u(p, qr), S3)
    go(w1u(p, qr), S5, s_left)
    go(w1u(p, qr), M1 + 1, m_left)
    lax.fori_loop(n_tiles // 2, n_tiles, norm_tile, 0)

    def relay1(t):
        arrive(w1u(pr, nth(t)), M1 + t)
        go(w1u(pr, nth(t)), M3 + t, m_left)

    def relay2(t):
        arrive(w2u(pl_, nth(t)), M2 + t)
        go(w2u(pl_, nth(t)), M4 + t, m_right)

    arrive(w1u(p, ql), S1)
    go(w1u(p, ql), M1 + 2, m_left)
    relay2(0)
    for k in range(1, RING):
        arrive(bi.at[wrap(c - k)], BI + k)
    for b in range(RING):
        for k in range(RING):
            flat = bi[b, 0:1, 2 * k * unit:(2 * k + 1) * unit]
            across = bi[k, 0:1, (2 * b + 1) * unit:(2 * b + 2) * unit]
            bias_u[b, k, 0:1, 0:unit] = jnp.where(e == 0, flat, across)
    arrive(w2u(p, qo), S6)
    go(w2u(p, qo), M2 + 3, m_right)
    relay1(0)
    relay2(1)
    arrive(w1u(p, qo), S5)
    go(w1u(p, qo), M1 + 3, m_left)
    relay2(2)

    def block(b, first=False, units=None, hook=None, send_part=None):
        bias = jnp.concatenate([bias_u[b, u, 0:1, 0:unit] for u in (range(RING) if units is None else units)], axis=1)
        hid, low = (hs, dcs) if units is None else (hs2, dcs2)

        def weight(i):
            if units is None:
                return wg[i, b].reshape(fb, width)
            return jnp.concatenate([wg[i, b, u] for u in units], axis=0)

        def block_tile(t, carry):
            rows = pl.ds(pl.multiple_of(t * tile, tile), tile)
            w1, w2 = weight(0), weight(1)
            pre = dot(ab[rows, :], w1, ((1,), (1,))) + bias
            squared = pre * pre
            tanh_val = jnp.tanh(GELU_K * (pre + GELU_C * pre * squared))
            hidden = (0.5 * pre * (1.0 + tanh_val)).astype(BF16)
            hid[rows, :] = hidden
            slope = 0.5 * (1.0 + tanh_val) + 0.5 * pre * (1.0 - tanh_val * tanh_val) * GELU_K * (1.0 + 3.0 * GELU_C * squared)
            pre_grad = dot(gb[rows, :], w2, ((1,), (1,))) * slope
            sums = jnp.sum(pre_grad, axis=0, keepdims=True)
            if units is None:
                vv[pl.ds(b, 1)] += sums
            else:
                for i, u in enumerate(units):
                    db_u[u, 0:1, 0:unit] += sums[:, i * unit:(i + 1) * unit]
            lowp = pre_grad.astype(BF16)
            low[rows, :] = lowp
            out = dot(hidden, w2)
            back = dot(lowp, w1)
            if first:
                y_acc[0, rows] = out[:, 0:half]
                y_acc[1, rows] = out[:, half:width]
                da_acc[0, rows] = back[:, 0:half]
                da_acc[1, rows] = back[:, half:width]
            else:
                y_acc[0, rows] += out[:, 0:half]
                y_acc[1, rows] += out[:, half:width]
                da_acc[0, rows] += back[:, 0:half]
                da_acc[1, rows] += back[:, half:width]
            if hook is not None:
                hook(t)
            return carry

        lax.fori_loop(0, n_tiles, block_tile, 0)
        for i, (rows_of, columns_of) in enumerate(((low, ab), (hid, gb))):
            part = dot(rows_of[...], columns_of[...], ((0,), (0,)))
            if units is None:
                gw[i, b] = part.reshape(RING, unit, width)
            else:
                for j, u in enumerate(units):
                    gw[i, b, u] = part[j * unit:(j + 1) * unit]
            if send_part is not None:
                send_part(i)

    def relay_gather(t):
        @pl.when(t == 0)
        def _():
            relay1(1)

        @pl.when(t == 1)
        def _():
            relay1(2)
            relay2(3)

    assert n_tiles == RING
    block(p, first=True, hook=relay_gather)
    relay1(3)
    for t in range(RING):
        go(w1u(p, nth(t)), M5 + t, m_right)
        go(w2u(p, nth(t)), M6 + t, m_left)

    def back1(t):
        return wrap(q - gray(RING - 1 - t))

    def back2(t):
        return wrap(q + gray(RING - 1 - t))

    db_u[...] = jnp.zeros_like(db_u)
    for first in (0, 2):
        for t in (first, first + 1):
            arrive(w2u(po, nth(t)), M4 + t)
            arrive(w1u(po, nth(t)), M3 + t)

        def send_opposite(i):
            for t in (first, first + 1):
                u = nth(t)
                rc(gw.at[i, po, u], opp.at[i, u], (R2 if i else R1) + t, m_right if i else m_left).start()

        block(po, units=(nth(first), nth(first + 1)), send_part=send_opposite)
    vv[pl.ds(po, 1)] = jnp.concatenate([db_u[u, 0:1, 0:unit] for u in range(RING)], axis=1)

    for t in range(RING):
        arrive(w2u(pr, nth(t)), M6 + t)
    def send_right(i):
        if i == 0:
            rc(gw.at[0, pr], dirs.at[0], R3, m_right).start()

    block(pr, send_part=send_right)
    for t in range(RING):
        arrive(w1u(pl_, nth(t)), M5 + t)
    block(pl_)

    def direct2(t):
        u = back2(t)
        rc(gw.at[1, pl_, u], dirs.at[1, u], R4 + t, m_left).start()

    direct2(0)
    direct2(1)

    lane = lax.broadcasted_iota(jnp.int32, (tile, 128), 1)

    def stat_tile(t, carry):
        rows = pl.ds(pl.multiple_of(t * tile, tile), tile)
        mean, inv = mean_s[rows], inv_s[rows]
        v0 = da_acc[0, rows] * lnv[0, 0:1]
        v1 = da_acc[1, rows] * lnv[1, 0:1]
        h0 = (xf[0, rows].astype(F32) - mean) * inv
        h1 = (xf[1, rows].astype(F32) - mean) * inv
        one = jnp.sum(v0, axis=1, keepdims=True) + jnp.sum(v1, axis=1, keepdims=True)
        two = jnp.sum(v0 * h0, axis=1, keepdims=True) + jnp.sum(v1 * h1, axis=1, keepdims=True)
        stat[rows] = jnp.where(lane < 64, one, two)
        return carry

    rc(y_acc.at[other], yr, EY, partner).start()
    rc(da_acc.at[other], dar, ED, partner).start()
    lax.fori_loop(0, n_tiles, stat_tile, 0)
    rc(stat, statr, ES, partner).start()

    for t in range(RING):
        arrive(opp.at[1, nth(t)], R2 + t)
        arrive(opp.at[0, nth(t)], R1 + t)
    for t in range(RING):
        u1, u2 = back1(t), back2(t)
        gw[1, pr, u2] += opp[1, u2]
        rc(gw.at[1, pr, u2], rel.at[1, u2], R6 + t, m_right).start()
        gw[0, pl_, u1] += opp[0, u1]
        rc(gw.at[0, pl_, u1], rel.at[0, u1], R5 + t, m_left).start()
    direct2(2)
    direct2(3)

    arrive(yr, EY)
    arrive(dar, ED)
    arrive(statr, ES)
    b_down = bd_ref[...].astype(F32).reshape(1, half)

    def out_tile(t, carry):
        rows = pl.ds(pl.multiple_of(t * tile, tile), tile)
        x_own = xf[e, rows].astype(F32)
        y_ref[rows] = (x_own + (y_acc[e, rows] + yr[rows]) + b_down).astype(BF16)
        norm_grad = da_acc[e, rows] + dar[rows]
        sums = (stat[rows] + statr[rows]) / width
        inv = inv_s[rows]
        x_hat = (x_own - mean_s[rows]) * inv
        value = norm_grad * lnv[e, 0:1]
        dx_ref[rows] = (gf[e, rows].astype(F32) + inv * (value - sums[:, 0:1] - x_hat * sums[:, 64:65])).astype(BF16)
        vv[RING + 1:RING + 2] += jnp.sum(norm_grad * x_hat, axis=0, keepdims=True)
        vv[RING + 2:RING + 3] += jnp.sum(norm_grad, axis=0, keepdims=True)
        return carry

    lax.fori_loop(0, n_tiles, out_tile, 0)

    vs[q] = vv[...]
    for k, d in ((1, s_right), (2, s_opp_dev), (3, s_left)):
        go(vs.at[q], VS + k, d)
    for k in range(1, RING):
        arrive(vs.at[wrap(q - k)], VS + k)
    vm[p] = ((vs[0] + vs[1]) + vs[2]) + vs[3]
    for k, d in ((1, m_right), (2, m_opp), (3, m_left)):
        go(vm.at[p], VM + k, d)

    arrive(dirs.at[0], R3)

    def reduce1(t):
        u = back1(t)
        arrive(rel.at[0, u], R5 + t)
        gw[0, p, u] += dirs[0, u] + rel[0, u]
        if t == 0:
            rc(gw.at[0, p, u], s_opp.at[0], Q1, s_left).start()
        if t == 1:
            rc(gw.at[0, p, u], s_dir.at[0], Q3, s_right).start()
        if t == 2:
            arrive(s_opp.at[0], Q1)
            gw[0, p, u] += s_opp[0]
            rc(gw.at[0, p, u], s_rel.at[0], Q5, s_left).start()

    def reduce2(t):
        u = back2(t)
        arrive(dirs.at[1, u], R4 + t)
        arrive(rel.at[1, u], R6 + t)
        gw[1, p, u] += dirs[1, u] + rel[1, u]
        if t == 0:
            rc(gw.at[1, p, u], s_opp.at[1], Q2, s_right).start()
        if t == 1:
            rc(gw.at[1, p, u], s_dir.at[1], Q4, s_left).start()
        if t == 2:
            arrive(s_opp.at[1], Q2)
            gw[1, p, u] += s_opp[1]
            rc(gw.at[1, p, u], s_rel.at[1], Q6, s_right).start()

    reduce1(0)
    reduce1(1)
    reduce2(0)
    reduce1(2)
    reduce2(1)
    reduce1(3)
    reduce2(2)

    arrive(s_dir.at[0], Q3)
    arrive(s_rel.at[0], Q5)
    done1 = gw[0, p, q] + s_dir[0] + s_rel[0]
    for k in range(RING):
        for h in range(2):
            start = (h * RING + k) * unit
            piece = jnp.concatenate([done1[:, start:start + unit], jnp.zeros((unit, LANES - unit), F32)], axis=1)
            f1[k, h] = piece.astype(BF16)
    for k in (2, 1, 3):
        for h in range(2):
            rc(f1.at[wrap(r + k), h], f1l.at[r, e], F1 + 2 * k + h,
               {"row": wrap(r + k), "col": c, "dep": h}, F1 + 2 * k + e).start()
    rc(f1.at[r, other], f1l.at[r, e], F1 + other, partner, F1 + e).start()
    f1l[r, e] = f1[r, e]
    reduce2(3)
    for k in range(1, RING):
        arrive(vm.at[wrap(p - k)], VM + k)
    vp[e] = ((vm[0] + vm[1]) + vm[2]) + vm[3]
    go(vp.at[e], VP, partner)
    arrive(s_dir.at[1], Q4)
    arrive(s_rel.at[1], Q6)
    done2 = (gw[1, p, q] + s_dir[1] + s_rel[1]).astype(BF16)
    f2[0] = done2[:, 0:half]
    f2[1] = done2[:, half:width]
    rc(f2.at[other], f2l.at[e], F2, partner).start()
    f2l[e] = f2[e]

    arrive(vp.at[other], VP)
    pieces = []
    for k in range(RING):
        pieces.append(vp[0, pl.ds(c, 1)][:, k * unit:(k + 1) * unit])
        row = vp[1, k:k + 1]
        piece = row[:, 0:unit]
        for j in range(1, RING):
            piece = jnp.where(c == j, row[:, j * unit:(j + 1) * unit], piece)
        pieces.append(piece)
    dbu_ref[...] = jnp.concatenate(pieces, axis=1).reshape(dbu_ref.shape)
    dbd_ref[...] = vp[e, RING:RING + 1].reshape(dbd_ref.shape)
    dsc_ref[...] = vp[e, RING + 1:RING + 2].reshape(dsc_ref.shape)
    dsh_ref[...] = vp[e, RING + 2:RING + 3].reshape(dsh_ref.shape)

    sent(l2.at[0], P2)
    sent(l1.at[0, 0], P1 + other)
    sent(l1.at[0, 0], F1 + other)
    for k in range(1, RING):
        for h in range(2):
            sent(l1.at[0, 0], P1 + 2 * k + h)
            sent(l1.at[0, 0], F1 + 2 * k + h)
        sent(bi.at[c], BI + k)
        sent(vm.at[p], VM + k)
        sent(vs.at[q], VS + k)
    sent(f2.at[0], F2)
    sent(lnv.at[0], DLN)
    sent(x_hbm, DX)
    sent(g_hbm, DG)
    for sem in (S1, S2, S3, S4, S5, S6):
        sent(w1u(p, q), sem)
    for t in range(RING):
        for sem in (M1, M2, M3, M4, M5, M6):
            sent(w1u(p, q), sem + t)
        for sem in (R1, R2, R4, R5, R6):
            sent(gw.at[0, p, q], sem + t)
    sent(gw.at[0, p], R3)
    for sem in (Q1, Q2, Q3, Q4, Q5, Q6):
        sent(gw.at[0, p, q], sem)
    sent(vp.at[e], VP)
    sent(yr, EY)
    sent(dar, ED)
    sent(stat, ES)

    arrive(f2l.at[other], F2)
    dw2_ref[0:unit] = f2l[0]
    dw2_ref[unit:2 * unit] = f2l[1]
    arrive(f1l.at[r, other], F1 + other)
    for k in range(1, RING):
        for h in range(2):
            arrive(f1l.at[wrap(r - k), h], F1 + 2 * k + h)
    dw1_ref[...] = f1l[...].astype(F32).reshape(2 * fb, LANES).T[0:unit].astype(BF16)


def copy_out(*refs):
    n = len(refs) // 2
    copies = [pltpu.make_async_copy(refs[i], refs[n + i], refs[2 * n].at[i]) for i in range(n)]
    for copy in copies:
        copy.start()
    for copy in copies:
        copy.wait()


def solution(mesh):
    assert mesh.shape["row"] == RING and mesh.shape["col"] == RING and mesh.shape["dep"] == 2
    tok_spec = P(("part", "row", "col"), "dep")
    vec_dep = P("dep")
    part_dep = P(("part", "dep"))
    in_specs = (tok_spec, vec_dep, vec_dep, P(("dep", "row"), "col"), P("col"), P(("col", "row"), "dep"), vec_dep, tok_spec)
    out_specs = (tok_spec, tok_spec, P(("part", "dep", "row"), "col"), P(("part", "col")), P(("part", "col", "row"), "dep"), part_dep, part_dep, part_dep)

    def local_step(x_in, ln_scale, ln_shift, w_up, b_up, w_down, b_down, y_grad):
        tokens, half = x_in.shape
        width = 2 * half
        unit = w_down.shape[0] // 2
        fb = RING * unit
        assert w_up.shape == (unit, 2 * fb) and half == RING * unit and fb == half
        tile = tokens // RING
        hbm_spec = pl.BlockSpec(memory_space=pltpu.HBM)
        vmem_spec = pl.BlockSpec(memory_space=pltpu.VMEM)
        vmem = pltpu.VMEM
        scratch = [
            vmem((unit, 2 * fb), BF16),
            vmem((RING, 2, unit, LANES), BF16), vmem((RING, 2, unit, LANES), BF16), vmem((2, unit, half), BF16),
            vmem((2, tokens, half), BF16), vmem((2, tokens, half), BF16),
            vmem((2, 8, half), F32),
            vmem((2, RING, RING, unit, width), BF16),
            vmem((RING, 8, 2 * fb), F32), vmem((RING, RING, 8, LANES), F32),
            vmem((tokens, width), BF16), vmem((tokens, width), BF16),
            vmem((tokens, 1), F32), vmem((tokens, 1), F32),
            vmem((2, tokens, half), F32), vmem((2, tokens, half), F32),
            vmem((tokens, half), F32), vmem((tokens, half), F32),
            vmem((tokens, 128), F32), vmem((tokens, 128), F32),
            vmem((tokens, fb), BF16), vmem((tokens, fb), BF16),
            vmem((tokens, 2 * unit), BF16), vmem((tokens, 2 * unit), BF16), vmem((RING, 8, LANES), F32),
            vmem((2, RING, RING, unit, width), F32),
            vmem((2, RING, unit, width), F32), vmem((2, RING, unit, width), F32), vmem((2, RING, unit, width), F32),
            vmem((2, unit, width), F32), vmem((2, unit, width), F32), vmem((2, unit, width), F32),
            vmem((8, half), F32), vmem((RING, 8, half), F32), vmem((RING, 8, half), F32), vmem((2, 8, half), F32),
            vmem((RING, 2, unit, LANES), BF16), vmem((RING, 2, unit, LANES), BF16),
            vmem((2, unit, half), BF16), vmem((2, unit, half), BF16),
            vmem((half,), F32), vmem((half,), F32), vmem((2 * fb,), BF16), vmem((half,), BF16),
            pltpu.SemaphoreType.DMA((N_SEM,)), pltpu.SemaphoreType.DMA((N_SEM,)),
        ]
        shapes = (
            jax.ShapeDtypeStruct((tokens, half), BF16), jax.ShapeDtypeStruct((tokens, half), BF16),
            jax.ShapeDtypeStruct(w_up.shape, BF16), jax.ShapeDtypeStruct(b_up.shape, F32),
            jax.ShapeDtypeStruct(w_down.shape, BF16), jax.ShapeDtypeStruct((half,), F32),
            jax.ShapeDtypeStruct((half,), F32), jax.ShapeDtypeStruct((half,), F32))
        outs = pl.pallas_call(
            functools.partial(kernel, tile),
            out_shape=shapes,
            in_specs=[hbm_spec] * 8,
            out_specs=(vmem_spec,) * 8,
            scratch_shapes=scratch,
            compiler_params=pltpu.CompilerParams(collective_id=0, has_side_effects=True, vmem_limit_bytes=50 * 1024 * 1024),
        )(*(pltpu.with_memory_space_constraint(v, pltpu.HBM) for v in (x_in, ln_scale, ln_shift, w_up, b_up, w_down, b_down, y_grad)))
        return pl.pallas_call(
            copy_out,
            out_shape=shapes,
            in_specs=[vmem_spec] * len(shapes),
            out_specs=(hbm_spec,) * len(shapes),
            scratch_shapes=[pltpu.SemaphoreType.DMA((len(shapes),))],
            compiler_params=pltpu.CompilerParams(vmem_limit_bytes=4 * 1024 * 1024),
        )(*outs)

    return jax.shard_map(local_step, mesh=mesh, in_specs=in_specs, out_specs=out_specs, check_vma=False)
```

```python
import functools

import jax
import jax.numpy as jnp
from jax import lax
from jax.experimental import pallas as pl
from jax.experimental.pallas import tpu as pltpu
from jax.sharding import PartitionSpec as P

LN_EPS = 1e-5
GELU_K = 0.7978845608028654
GELU_C = 0.044715
MESH = pl.DeviceIdType.MESH
F32 = jnp.float32
BF16 = jnp.bfloat16
RING = 4
LANES = 128

_next = [0]


def _ids(count=1):
    base = _next[0]
    _next[0] += count
    return base


IN_SEM = _ids(8)
P1 = _ids(2 * RING)
P2, DX, DG, DLN = _ids(), _ids(), _ids(), _ids()
BI = _ids(RING)
S1, S2, S3, S4, S5, S6 = (_ids() for _ in range(6))
M1, M2, M3, M4 = (_ids(RING) for _ in range(4))
M5, M6 = _ids(RING), _ids(RING)
R1, R2, R5, R6 = (_ids(RING) for _ in range(4))
R3, R4 = _ids(), _ids(RING)
Q1, Q2, Q3, Q4, Q5, Q6 = (_ids() for _ in range(6))
VM, VS = _ids(RING), _ids(RING)
VP = _ids()
EY, ED, ES = _ids(), _ids(), _ids()
F1 = _ids(2 * RING)
F2 = _ids()
N_SEM = _next[0]


def gray(t):
    return t + (t // 2) * (5 - 2 * t)


def dot(a, b, dims=((1,), (0,))):
    return lax.dot_general(a, b, (dims, ((), ())), preferred_element_type=F32)


def kernel(tile, x_hbm, sc_hbm, sh_hbm, w1_hbm, bu_hbm, w2_hbm, bd_hbm, g_hbm,
           y_ref, dx_ref, dw1_ref, dbu_ref, dw2_ref, dbd_ref, dsc_ref, dsh_ref,
           w1v, st1, l1, l2, xf, gf, lnv, wg, bi, bias_u, ab, gb, mean_s, inv_s,
           y_acc, da_acc, yr, dar, stat, statr, hs, dcs, gw, opp, dirs, rel, s_opp, s_dir, s_rel,
           vv, vm, vs, vp, f1, f1l, f2, f2l, sc_ref, sh_ref, bu_ref, bd_ref, send, recv):
    r, c, e = lax.axis_index("row"), lax.axis_index("col"), lax.axis_index("dep")
    p = c + e * (r - c)
    q = r + e * (c - r)
    tokens, half = xf.shape[1], xf.shape[2]
    width = 2 * half
    unit = l2.shape[1]
    fb = RING * unit
    n_tiles = tokens // tile
    other = 1 - e

    def wrap(v):
        return lax.rem(v + 2 * RING, RING)

    def dev(pp, qq):
        return {"row": qq + e * (pp - qq), "col": pp + e * (qq - pp), "dep": e}

    m_right, m_left, m_opp = dev(wrap(p + 1), q), dev(wrap(p - 1), q), dev(wrap(p + 2), q)
    s_right, s_left, s_opp_dev = dev(p, wrap(q + 1)), dev(p, wrap(q - 1)), dev(p, wrap(q + 2))
    partner = {"row": r, "col": c, "dep": other}
    pr, pl_, po = wrap(p + 1), wrap(p - 1), wrap(p + 2)
    qr, ql, qo = wrap(q + 1), wrap(q - 1), wrap(q + 2)

    def rc(src, dst, ssem, device, rsem=None):
        return pltpu.make_async_remote_copy(
            src_ref=src, dst_ref=dst, send_sem=send.at[ssem], recv_sem=recv.at[ssem if rsem is None else rsem],
            device_id=device, device_id_type=MESH)

    def arrive(dst, rsem):
        rc(dst, dst, rsem, partner).wait_recv()

    def sent(src, ssem):
        rc(src, src, ssem, partner).wait_send()

    def go(ref, sem, device):
        rc(ref, ref, sem, device).start()

    load_w1 = pltpu.make_async_copy(w1_hbm, w1v, recv.at[IN_SEM])
    load_w2 = pltpu.make_async_copy(w2_hbm.at[pl.ds(pl.multiple_of(e * unit, 16), unit)], l2.at[e], recv.at[IN_SEM + 1])
    load_x = pltpu.make_async_copy(x_hbm, xf.at[e], recv.at[IN_SEM + 2])
    load_g = pltpu.make_async_copy(g_hbm, gf.at[e], recv.at[IN_SEM + 3])
    load_vectors = [pltpu.make_async_copy(src, dst, recv.at[IN_SEM + 4 + i]) for i, (src, dst) in enumerate(
        ((sc_hbm, sc_ref), (sh_hbm, sh_ref), (bu_hbm, bu_ref), (bd_hbm, bd_ref)))]
    load_w1.start()
    load_w2.start()
    for load in load_vectors:
        load.start()
    load_x.start()
    load_g.start()

    barrier = pltpu.get_barrier_semaphore()
    peers = [m_right, m_left, s_right, s_left, m_opp, s_opp_dev, partner]
    peers += [{"row": wrap(r + k), "col": c, "dep": other} for k in range(1, RING)]
    for d in peers:
        pl.semaphore_signal(barrier, inc=1, device_id=d, device_id_type=MESH)

    load_w1.wait()
    turned = w1v[...].astype(F32)
    turned = jnp.concatenate([turned, jnp.zeros((LANES - unit, 2 * fb), F32)], axis=0).T.astype(BF16)
    for k in range(RING):
        for h in range(2):
            st1[k, h] = turned[(2 * k + h) * unit:(2 * k + h + 1) * unit]

    for load in load_vectors:
        load.wait()
    lnv[e, 0:1] = sc_ref[...].reshape(1, half)
    lnv[e, 1:2] = sh_ref[...].reshape(1, half)
    bi[c] = jnp.broadcast_to(bu_ref[...].astype(F32).reshape(1, 2 * fb), (8, 2 * fb))

    pl.semaphore_wait(barrier, len(peers))

    rc(w2_hbm.at[pl.ds(pl.multiple_of(other * unit, 16), unit)], l2.at[e], P2, partner).start()
    rc(st1.at[r, other], l1.at[r, e], P1 + other, partner, P1 + e).start()
    for k in (2, 1, 3):
        for h in range(2):
            rc(st1.at[wrap(r + k), h], l1.at[r, e], P1 + 2 * k + h,
               {"row": wrap(r + k), "col": c, "dep": h}, P1 + 2 * k + e).start()
    rc(lnv.at[e], lnv.at[e], DLN, partner).start()
    rc(x_hbm, xf.at[e], DX, partner).start()
    rc(g_hbm, gf.at[e], DG, partner).start()
    for k in range(1, RING):
        rc(bi.at[c], bi.at[c], BI + k, {"row": r, "col": wrap(c + k), "dep": e}).start()
    l1[r, e] = st1[r, e]

    def w1u(b, s):
        return wg.at[0, b, s]

    def w2u(b, s):
        return wg.at[1, b, s]

    load_w2.wait()
    arrive(l2.at[other], P2)
    wg[1, p, q, :, 0:half] = l2[0]
    wg[1, p, q, :, half:width] = l2[1]
    go(w2u(p, q), M2, m_right)
    go(w2u(p, q), S2, s_right)
    go(w2u(p, q), S4, s_left)
    go(w2u(p, q), M6, m_left)

    arrive(l1.at[r, other], P1 + other)
    for k in range(1, RING):
        for h in range(2):
            arrive(l1.at[wrap(r - k), h], P1 + 2 * k + h)
    wg[0, p, q] = jnp.concatenate([l1[k, h][:, 0:unit].astype(F32) for h in range(2) for k in range(RING)], axis=1).astype(BF16)
    go(w1u(p, q), M1, m_left)
    go(w1u(p, q), S1, s_right)
    go(w1u(p, q), S3, s_left)
    go(w1u(p, q), M5, m_right)

    arrive(w2u(p, ql), S2)
    go(w2u(p, ql), S6, s_right)
    arrive(w2u(p, qr), S4)
    go(w2u(p, qr), M2 + 1, m_right)
    go(w2u(p, ql), M2 + 2, m_right)
    go(w2u(p, qr), M6 + 1, m_left)
    go(w2u(p, ql), M6 + 2, m_left)

    def nth(t):
        return wrap(q + gray(t))

    arrive(lnv.at[other], DLN)
    load_x.wait()
    arrive(xf.at[other], DX)
    load_g.wait()
    arrive(gf.at[other], DG)
    vv[...] = jnp.zeros_like(vv)
    def norm_tile(t, carry):
        rows = pl.ds(pl.multiple_of(t * tile, tile), tile)
        x0, x1 = xf[0, rows].astype(F32), xf[1, rows].astype(F32)
        total = jnp.sum(x0, axis=1, keepdims=True) + jnp.sum(x1, axis=1, keepdims=True)
        squares = jnp.sum(x0 * x0, axis=1, keepdims=True) + jnp.sum(x1 * x1, axis=1, keepdims=True)
        mean = total / width
        inv = lax.rsqrt(squares / width - mean * mean + LN_EPS)
        mean_s[rows] = mean
        inv_s[rows] = inv
        ab[rows, 0:half] = ((x0 - mean) * inv * lnv[0, 0:1] + lnv[0, 1:2]).astype(BF16)
        ab[rows, half:width] = ((x1 - mean) * inv * lnv[1, 0:1] + lnv[1, 1:2]).astype(BF16)
        gb[rows, 0:half] = gf[0, rows]
        gb[rows, half:width] = gf[1, rows]
        vv[RING:RING + 1] += jnp.sum(gf[e, rows].astype(F32), axis=0, keepdims=True)
        return carry

    lax.fori_loop(0, n_tiles // 2, norm_tile, 0)
    arrive(w1u(p, qr), S3)
    go(w1u(p, qr), S5, s_left)
    go(w1u(p, qr), M1 + 1, m_left)
    lax.fori_loop(n_tiles // 2, n_tiles, norm_tile, 0)

    def relay1(t):
        arrive(w1u(pr, nth(t)), M1 + t)
        go(w1u(pr, nth(t)), M3 + t, m_left)

    def relay2(t):
        arrive(w2u(pl_, nth(t)), M2 + t)
        go(w2u(pl_, nth(t)), M4 + t, m_right)

    arrive(w1u(p, ql), S1)
    go(w1u(p, ql), M1 + 2, m_left)
    relay2(0)
    for k in range(1, RING):
        arrive(bi.at[wrap(c - k)], BI + k)
    for b in range(RING):
        for k in range(RING):
            flat = bi[b, 0:1, 2 * k * unit:(2 * k + 1) * unit]
            across = bi[k, 0:1, (2 * b + 1) * unit:(2 * b + 2) * unit]
            bias_u[b, k, 0:1, 0:unit] = jnp.where(e == 0, flat, across)
    arrive(w2u(p, qo), S6)
    go(w2u(p, qo), M2 + 3, m_right)
    relay1(0)
    relay2(1)
    arrive(w1u(p, qo), S5)
    go(w1u(p, qo), M1 + 3, m_left)
    relay2(2)

    def block(slot, b, hook=None, send_part=None):
        bias = jnp.concatenate([bias_u[b, u, 0:1, 0:unit] for u in range(RING)], axis=1)

        def block_tile(t, carry):
            rows = pl.ds(pl.multiple_of(t * tile, tile), tile)
            pre = dot(ab[rows, :], wg[0, b].reshape(fb, width), ((1,), (1,))) + bias
            squared = pre * pre
            tanh_val = jnp.tanh(GELU_K * (pre + GELU_C * pre * squared))
            hs[slot, rows] = (0.5 * pre * (1.0 + tanh_val)).astype(BF16)
            slope = 0.5 * (1.0 + tanh_val) + 0.5 * pre * (1.0 - tanh_val * tanh_val) * GELU_K * (1.0 + 3.0 * GELU_C * squared)
            pre_grad = dot(gb[rows, :], wg[1, b].reshape(fb, width), ((1,), (1,))) * slope
            vv[pl.ds(b, 1)] += jnp.sum(pre_grad, axis=0, keepdims=True)
            dcs[slot, rows] = pre_grad.astype(BF16)
            if hook is not None:
                hook(t)
            return carry

        lax.fori_loop(0, n_tiles, block_tile, 0)
        for i, (rows_of, columns_of) in enumerate(((dcs, ab), (hs, gb))):
            gw[i, b] = dot(rows_of[slot], columns_of[...], ((0,), (0,))).reshape(RING, unit, width)
            if send_part is not None:
                send_part(i)

    def relay_gather(t):
        @pl.when(t == 0)
        def _():
            relay1(1)

        @pl.when(t == 1)
        def _():
            relay1(2)
            relay2(3)

    assert n_tiles == RING
    block(0, p, hook=relay_gather)
    relay1(3)
    for t in range(1, RING):
        go(w1u(p, nth(t)), M5 + t, m_right)
    go(w2u(p, qo), M6 + 3, m_left)

    def back1(t):
        return wrap(q - gray(RING - 1 - t))

    def back2(t):
        return wrap(q + gray(RING - 1 - t))

    for t in range(RING):
        arrive(w2u(po, nth(t)), M4 + t)
        arrive(w1u(po, nth(t)), M3 + t)

    def send_opposite(i):
        for t in range(RING):
            u = back2(t) if i else back1(t)
            rc(gw.at[i, po, u], opp.at[i, u], (R2 if i else R1) + t, m_right if i else m_left).start()

    block(1, po, send_part=send_opposite)

    for t in range(RING):
        arrive(w2u(pr, nth(t)), M6 + t)
    def send_right(i):
        if i == 0:
            rc(gw.at[0, pr], dirs.at[0], R3, m_right).start()

    block(2, pr, send_part=send_right)
    for t in range(RING):
        arrive(w1u(pl_, nth(t)), M5 + t)
    block(3, pl_)

    def direct2(t):
        u = back2(t)
        rc(gw.at[1, pl_, u], dirs.at[1, u], R4 + t, m_left).start()

    direct2(0)
    direct2(1)

    def product_tile(t, carry):
        rows = pl.ds(pl.multiple_of(t * tile, tile), tile)
        for i, (left, acc) in enumerate(((dcs, da_acc), (hs, y_acc))):
            weights = jnp.concatenate([wg[i, b].reshape(fb, width) for b in (p, po, pr, pl_)], axis=0)
            out = dot(jnp.concatenate([left[slot, rows] for slot in range(RING)], axis=1), weights)
            acc[0, rows] = out[:, 0:half]
            acc[1, rows] = out[:, half:width]
        return carry

    lax.fori_loop(0, n_tiles, product_tile, 0)

    lane = lax.broadcasted_iota(jnp.int32, (tile, 128), 1)

    def stat_tile(t, carry):
        rows = pl.ds(pl.multiple_of(t * tile, tile), tile)
        mean, inv = mean_s[rows], inv_s[rows]
        v0 = da_acc[0, rows] * lnv[0, 0:1]
        v1 = da_acc[1, rows] * lnv[1, 0:1]
        h0 = (xf[0, rows].astype(F32) - mean) * inv
        h1 = (xf[1, rows].astype(F32) - mean) * inv
        one = jnp.sum(v0, axis=1, keepdims=True) + jnp.sum(v1, axis=1, keepdims=True)
        two = jnp.sum(v0 * h0, axis=1, keepdims=True) + jnp.sum(v1 * h1, axis=1, keepdims=True)
        stat[rows] = jnp.where(lane < 64, one, two)
        return carry

    rc(y_acc.at[other], yr, EY, partner).start()
    rc(da_acc.at[other], dar, ED, partner).start()
    lax.fori_loop(0, n_tiles, stat_tile, 0)
    rc(stat, statr, ES, partner).start()

    for t in range(RING):
        u1, u2 = back1(t), back2(t)
        arrive(opp.at[1, u2], R2 + t)
        gw[1, pr, u2] += opp[1, u2]
        rc(gw.at[1, pr, u2], rel.at[1, u2], R6 + t, m_right).start()
        arrive(opp.at[0, u1], R1 + t)
        gw[0, pl_, u1] += opp[0, u1]
        rc(gw.at[0, pl_, u1], rel.at[0, u1], R5 + t, m_left).start()
    direct2(2)
    direct2(3)

    arrive(yr, EY)
    arrive(dar, ED)
    arrive(statr, ES)
    b_down = bd_ref[...].astype(F32).reshape(1, half)

    def out_tile(t, carry):
        rows = pl.ds(pl.multiple_of(t * tile, tile), tile)
        x_own = xf[e, rows].astype(F32)
        y_ref[rows] = (x_own + (y_acc[e, rows] + yr[rows]) + b_down).astype(BF16)
        norm_grad = da_acc[e, rows] + dar[rows]
        sums = (stat[rows] + statr[rows]) / width
        inv = inv_s[rows]
        x_hat = (x_own - mean_s[rows]) * inv
        value = norm_grad * lnv[e, 0:1]
        dx_ref[rows] = (gf[e, rows].astype(F32) + inv * (value - sums[:, 0:1] - x_hat * sums[:, 64:65])).astype(BF16)
        vv[RING + 1:RING + 2] += jnp.sum(norm_grad * x_hat, axis=0, keepdims=True)
        vv[RING + 2:RING + 3] += jnp.sum(norm_grad, axis=0, keepdims=True)
        return carry

    lax.fori_loop(0, n_tiles, out_tile, 0)

    vs[q] = vv[...]
    for k, d in ((1, s_right), (2, s_opp_dev), (3, s_left)):
        go(vs.at[q], VS + k, d)
    for k in range(1, RING):
        arrive(vs.at[wrap(q - k)], VS + k)
    vm[p] = ((vs[0] + vs[1]) + vs[2]) + vs[3]
    for k, d in ((1, m_right), (2, m_opp), (3, m_left)):
        go(vm.at[p], VM + k, d)

    arrive(dirs.at[0], R3)

    def reduce1(t):
        u = back1(t)
        arrive(rel.at[0, u], R5 + t)
        gw[0, p, u] += dirs[0, u] + rel[0, u]
        if t == 0:
            rc(gw.at[0, p, u], s_opp.at[0], Q1, s_left).start()
        if t == 1:
            rc(gw.at[0, p, u], s_dir.at[0], Q3, s_right).start()
        if t == 2:
            arrive(s_opp.at[0], Q1)
            gw[0, p, u] += s_opp[0]
            rc(gw.at[0, p, u], s_rel.at[0], Q5, s_left).start()

    def reduce2(t):
        u = back2(t)
        arrive(dirs.at[1, u], R4 + t)
        arrive(rel.at[1, u], R6 + t)
        gw[1, p, u] += dirs[1, u] + rel[1, u]
        if t == 0:
            rc(gw.at[1, p, u], s_opp.at[1], Q2, s_right).start()
        if t == 1:
            rc(gw.at[1, p, u], s_dir.at[1], Q4, s_left).start()
        if t == 2:
            arrive(s_opp.at[1], Q2)
            gw[1, p, u] += s_opp[1]
            rc(gw.at[1, p, u], s_rel.at[1], Q6, s_right).start()

    reduce1(0)
    reduce1(1)
    reduce2(0)
    reduce1(2)
    reduce2(1)
    reduce1(3)
    reduce2(2)

    arrive(s_dir.at[0], Q3)
    arrive(s_rel.at[0], Q5)
    done1 = gw[0, p, q] + s_dir[0] + s_rel[0]
    for k in range(RING):
        for h in range(2):
            start = (h * RING + k) * unit
            piece = jnp.concatenate([done1[:, start:start + unit], jnp.zeros((unit, LANES - unit), F32)], axis=1)
            f1[k, h] = piece.astype(BF16)
    for k in (2, 1, 3):
        for h in range(2):
            rc(f1.at[wrap(r + k), h], f1l.at[r, e], F1 + 2 * k + h,
               {"row": wrap(r + k), "col": c, "dep": h}, F1 + 2 * k + e).start()
    rc(f1.at[r, other], f1l.at[r, e], F1 + other, partner, F1 + e).start()
    f1l[r, e] = f1[r, e]
    reduce2(3)
    for k in range(1, RING):
        arrive(vm.at[wrap(p - k)], VM + k)
    vp[e] = ((vm[0] + vm[1]) + vm[2]) + vm[3]
    go(vp.at[e], VP, partner)
    arrive(s_dir.at[1], Q4)
    arrive(s_rel.at[1], Q6)
    done2 = (gw[1, p, q] + s_dir[1] + s_rel[1]).astype(BF16)
    f2[0] = done2[:, 0:half]
    f2[1] = done2[:, half:width]
    rc(f2.at[other], f2l.at[e], F2, partner).start()
    f2l[e] = f2[e]

    arrive(vp.at[other], VP)
    pieces = []
    for k in range(RING):
        pieces.append(vp[0, pl.ds(c, 1)][:, k * unit:(k + 1) * unit])
        row = vp[1, k:k + 1]
        piece = row[:, 0:unit]
        for j in range(1, RING):
            piece = jnp.where(c == j, row[:, j * unit:(j + 1) * unit], piece)
        pieces.append(piece)
    dbu_ref[...] = jnp.concatenate(pieces, axis=1).reshape(dbu_ref.shape)
    dbd_ref[...] = vp[e, RING:RING + 1].reshape(dbd_ref.shape)
    dsc_ref[...] = vp[e, RING + 1:RING + 2].reshape(dsc_ref.shape)
    dsh_ref[...] = vp[e, RING + 2:RING + 3].reshape(dsh_ref.shape)

    sent(l2.at[0], P2)
    sent(l1.at[0, 0], P1 + other)
    sent(l1.at[0, 0], F1 + other)
    for k in range(1, RING):
        for h in range(2):
            sent(l1.at[0, 0], P1 + 2 * k + h)
            sent(l1.at[0, 0], F1 + 2 * k + h)
        sent(bi.at[c], BI + k)
        sent(vm.at[p], VM + k)
        sent(vs.at[q], VS + k)
    sent(f2.at[0], F2)
    sent(lnv.at[0], DLN)
    sent(x_hbm, DX)
    sent(g_hbm, DG)
    for sem in (S1, S2, S3, S4, S5, S6):
        sent(w1u(p, q), sem)
    for t in range(RING):
        for sem in (M1, M2, M3, M4, M5, M6):
            sent(w1u(p, q), sem + t)
        for sem in (R1, R2, R4, R5, R6):
            sent(gw.at[0, p, q], sem + t)
    sent(gw.at[0, p], R3)
    for sem in (Q1, Q2, Q3, Q4, Q5, Q6):
        sent(gw.at[0, p, q], sem)
    sent(vp.at[e], VP)
    sent(yr, EY)
    sent(dar, ED)
    sent(stat, ES)

    arrive(f2l.at[other], F2)
    dw2_ref[0:unit] = f2l[0]
    dw2_ref[unit:2 * unit] = f2l[1]
    arrive(f1l.at[r, other], F1 + other)
    for k in range(1, RING):
        for h in range(2):
            arrive(f1l.at[wrap(r - k), h], F1 + 2 * k + h)
    dw1_ref[...] = f1l[...].astype(F32).reshape(2 * fb, LANES).T[0:unit].astype(BF16)


def copy_out(*refs):
    n = len(refs) // 2
    copies = [pltpu.make_async_copy(refs[i], refs[n + i], refs[2 * n].at[i]) for i in range(n)]
    for copy in copies:
        copy.start()
    for copy in copies:
        copy.wait()


def solution(mesh):
    assert mesh.shape["row"] == RING and mesh.shape["col"] == RING and mesh.shape["dep"] == 2
    tok_spec = P(("part", "row", "col"), "dep")
    vec_dep = P("dep")
    part_dep = P(("part", "dep"))
    in_specs = (tok_spec, vec_dep, vec_dep, P(("dep", "row"), "col"), P("col"), P(("col", "row"), "dep"), vec_dep, tok_spec)
    out_specs = (tok_spec, tok_spec, P(("part", "dep", "row"), "col"), P(("part", "col")), P(("part", "col", "row"), "dep"), part_dep, part_dep, part_dep)

    def local_step(x_in, ln_scale, ln_shift, w_up, b_up, w_down, b_down, y_grad):
        tokens, half = x_in.shape
        width = 2 * half
        unit = w_down.shape[0] // 2
        fb = RING * unit
        assert w_up.shape == (unit, 2 * fb) and half == RING * unit and fb == half
        tile = tokens // RING
        hbm_spec = pl.BlockSpec(memory_space=pltpu.HBM)
        vmem_spec = pl.BlockSpec(memory_space=pltpu.VMEM)
        vmem = pltpu.VMEM
        scratch = [
            vmem((unit, 2 * fb), BF16),
            vmem((RING, 2, unit, LANES), BF16), vmem((RING, 2, unit, LANES), BF16), vmem((2, unit, half), BF16),
            vmem((2, tokens, half), BF16), vmem((2, tokens, half), BF16),
            vmem((2, 8, half), F32),
            vmem((2, RING, RING, unit, width), BF16),
            vmem((RING, 8, 2 * fb), F32), vmem((RING, RING, 8, LANES), F32),
            vmem((tokens, width), BF16), vmem((tokens, width), BF16),
            vmem((tokens, 1), F32), vmem((tokens, 1), F32),
            vmem((2, tokens, half), F32), vmem((2, tokens, half), F32),
            vmem((tokens, half), F32), vmem((tokens, half), F32),
            vmem((tokens, 128), F32), vmem((tokens, 128), F32),
            vmem((RING, tokens, fb), BF16), vmem((RING, tokens, fb), BF16),
            vmem((2, RING, RING, unit, width), F32),
            vmem((2, RING, unit, width), F32), vmem((2, RING, unit, width), F32), vmem((2, RING, unit, width), F32),
            vmem((2, unit, width), F32), vmem((2, unit, width), F32), vmem((2, unit, width), F32),
            vmem((8, half), F32), vmem((RING, 8, half), F32), vmem((RING, 8, half), F32), vmem((2, 8, half), F32),
            vmem((RING, 2, unit, LANES), BF16), vmem((RING, 2, unit, LANES), BF16),
            vmem((2, unit, half), BF16), vmem((2, unit, half), BF16),
            vmem((half,), F32), vmem((half,), F32), vmem((2 * fb,), BF16), vmem((half,), BF16),
            pltpu.SemaphoreType.DMA((N_SEM,)), pltpu.SemaphoreType.DMA((N_SEM,)),
        ]
        shapes = (
            jax.ShapeDtypeStruct((tokens, half), BF16), jax.ShapeDtypeStruct((tokens, half), BF16),
            jax.ShapeDtypeStruct(w_up.shape, BF16), jax.ShapeDtypeStruct(b_up.shape, F32),
            jax.ShapeDtypeStruct(w_down.shape, BF16), jax.ShapeDtypeStruct((half,), F32),
            jax.ShapeDtypeStruct((half,), F32), jax.ShapeDtypeStruct((half,), F32))
        outs = pl.pallas_call(
            functools.partial(kernel, tile),
            out_shape=shapes,
            in_specs=[hbm_spec] * 8,
            out_specs=(vmem_spec,) * 8,
            scratch_shapes=scratch,
            compiler_params=pltpu.CompilerParams(collective_id=0, has_side_effects=True, vmem_limit_bytes=51 * 1024 * 1024),
        )(*(pltpu.with_memory_space_constraint(v, pltpu.HBM) for v in (x_in, ln_scale, ln_shift, w_up, b_up, w_down, b_down, y_grad)))
        return pl.pallas_call(
            copy_out,
            out_shape=shapes,
            in_specs=[vmem_spec] * len(shapes),
            out_specs=(hbm_spec,) * len(shapes),
            scratch_shapes=[pltpu.SemaphoreType.DMA((len(shapes),))],
            compiler_params=pltpu.CompilerParams(vmem_limit_bytes=4 * 1024 * 1024),
        )(*outs)

    return jax.shard_map(local_step, mesh=mesh, in_specs=in_specs, out_specs=out_specs, check_vma=False)
```

```python
import functools

import jax
import jax.numpy as jnp
from jax import lax
from jax.experimental import pallas as pl
from jax.experimental.pallas import tpu as pltpu
from jax.sharding import PartitionSpec as P

LN_EPS = 1e-5
GELU_K = 0.7978845608028654
GELU_C = 0.044715
MESH = pl.DeviceIdType.MESH
F32 = jnp.float32
BF16 = jnp.bfloat16
RING = 4
LANES = 128

_next = [0]


def _ids(count=1):
    base = _next[0]
    _next[0] += count
    return base


IN_SEM = _ids(8)
P1 = _ids(2 * RING)
P2, DX, DG, DLN = _ids(), _ids(), _ids(), _ids()
BI = _ids(RING)
S1, S2, S3, S4, S5, S6 = (_ids() for _ in range(6))
M1, M2, M3, M4 = (_ids(RING) for _ in range(4))
M5, M6 = _ids(RING), _ids(RING)
R1, R2, R5, R6 = (_ids(RING) for _ in range(4))
R3, R4 = _ids(), _ids(RING)
Q1, Q2, Q3, Q4, Q5, Q6 = (_ids() for _ in range(6))
VM, VS = _ids(RING), _ids(RING)
VP = _ids()
EY, ED, ES = _ids(), _ids(), _ids()
F1 = _ids(2 * RING)
F2 = _ids()
N_SEM = _next[0]


def gray(t):
    return t + (t // 2) * (5 - 2 * t)


def dot(a, b, dims=((1,), (0,))):
    return lax.dot_general(a, b, (dims, ((), ())), preferred_element_type=F32)


def kernel(tile, x_hbm, sc_hbm, sh_hbm, w1_hbm, bu_hbm, w2_hbm, bd_hbm, g_hbm,
           y_ref, dx_ref, dw1_ref, dbu_ref, dw2_ref, dbd_ref, dsc_ref, dsh_ref,
           w1v, st1, l1, l2, xf, gf, lnv, wg, bi, bias_u, ab, gb, mean_s, inv_s,
           y_acc, da_acc, yr, dar, stat, statr, hs, dcs, hs2, dcs2, db_u, gw, opp, dirs, rel, s_opp, s_dir, s_rel,
           vv, vm, vs, vp, f1, f1l, f2, f2l, sc_ref, sh_ref, bu_ref, bd_ref, send, recv):
    r, c, e = lax.axis_index("row"), lax.axis_index("col"), lax.axis_index("dep")
    p = c + e * (r - c)
    q = r + e * (c - r)
    tokens, half = xf.shape[1], xf.shape[2]
    width = 2 * half
    unit = l2.shape[1]
    fb = RING * unit
    n_tiles = tokens // tile
    other = 1 - e

    def wrap(v):
        return lax.rem(v + 2 * RING, RING)

    def dev(pp, qq):
        return {"row": qq + e * (pp - qq), "col": pp + e * (qq - pp), "dep": e}

    m_right, m_left, m_opp = dev(wrap(p + 1), q), dev(wrap(p - 1), q), dev(wrap(p + 2), q)
    s_right, s_left, s_opp_dev = dev(p, wrap(q + 1)), dev(p, wrap(q - 1)), dev(p, wrap(q + 2))
    partner = {"row": r, "col": c, "dep": other}
    pr, pl_, po = wrap(p + 1), wrap(p - 1), wrap(p + 2)
    qr, ql, qo = wrap(q + 1), wrap(q - 1), wrap(q + 2)

    def rc(src, dst, ssem, device, rsem=None):
        return pltpu.make_async_remote_copy(
            src_ref=src, dst_ref=dst, send_sem=send.at[ssem], recv_sem=recv.at[ssem if rsem is None else rsem],
            device_id=device, device_id_type=MESH)

    def arrive(dst, rsem):
        rc(dst, dst, rsem, partner).wait_recv()

    def sent(src, ssem):
        rc(src, src, ssem, partner).wait_send()

    def go(ref, sem, device):
        rc(ref, ref, sem, device).start()

    load_w1 = pltpu.make_async_copy(w1_hbm, w1v, recv.at[IN_SEM])
    load_w2 = pltpu.make_async_copy(w2_hbm.at[pl.ds(pl.multiple_of(e * unit, 16), unit)], l2.at[e], recv.at[IN_SEM + 1])
    load_x = pltpu.make_async_copy(x_hbm, xf.at[e], recv.at[IN_SEM + 2])
    load_g = pltpu.make_async_copy(g_hbm, gf.at[e], recv.at[IN_SEM + 3])
    load_vectors = [pltpu.make_async_copy(src, dst, recv.at[IN_SEM + 4 + i]) for i, (src, dst) in enumerate(
        ((sc_hbm, sc_ref), (sh_hbm, sh_ref), (bu_hbm, bu_ref), (bd_hbm, bd_ref)))]
    load_w1.start()
    load_w2.start()
    for load in load_vectors:
        load.start()
    load_x.start()
    load_g.start()

    barrier = pltpu.get_barrier_semaphore()
    peers = [m_right, m_left, s_right, s_left, m_opp, s_opp_dev, partner]
    peers += [{"row": wrap(r + k), "col": c, "dep": other} for k in range(1, RING)]
    for d in peers:
        pl.semaphore_signal(barrier, inc=1, device_id=d, device_id_type=MESH)

    load_w1.wait()
    turned = w1v[...].astype(F32)
    turned = jnp.concatenate([turned, jnp.zeros((LANES - unit, 2 * fb), F32)], axis=0).T.astype(BF16)
    for k in range(RING):
        for h in range(2):
            st1[k, h] = turned[(2 * k + h) * unit:(2 * k + h + 1) * unit]

    for load in load_vectors:
        load.wait()
    lnv[e, 0:1] = sc_ref[...].reshape(1, half)
    lnv[e, 1:2] = sh_ref[...].reshape(1, half)
    bi[c] = jnp.broadcast_to(bu_ref[...].astype(F32).reshape(1, 2 * fb), (8, 2 * fb))

    pl.semaphore_wait(barrier, len(peers))

    rc(w2_hbm.at[pl.ds(pl.multiple_of(other * unit, 16), unit)], l2.at[e], P2, partner).start()
    rc(st1.at[r, other], l1.at[r, e], P1 + other, partner, P1 + e).start()
    for k in (2, 1, 3):
        for h in range(2):
            rc(st1.at[wrap(r + k), h], l1.at[r, e], P1 + 2 * k + h,
               {"row": wrap(r + k), "col": c, "dep": h}, P1 + 2 * k + e).start()
    rc(lnv.at[e], lnv.at[e], DLN, partner).start()
    rc(x_hbm, xf.at[e], DX, partner).start()
    rc(g_hbm, gf.at[e], DG, partner).start()
    for k in range(1, RING):
        rc(bi.at[c], bi.at[c], BI + k, {"row": r, "col": wrap(c + k), "dep": e}).start()
    l1[r, e] = st1[r, e]

    def w1u(b, s):
        return wg.at[0, b, s]

    def w2u(b, s):
        return wg.at[1, b, s]

    load_w2.wait()
    arrive(l2.at[other], P2)
    wg[1, p, q, :, 0:half] = l2[0]
    wg[1, p, q, :, half:width] = l2[1]
    go(w2u(p, q), M2, m_right)
    go(w2u(p, q), S2, s_right)
    go(w2u(p, q), S4, s_left)
    go(w2u(p, q), M6, m_left)

    arrive(l1.at[r, other], P1 + other)
    for k in range(1, RING):
        for h in range(2):
            arrive(l1.at[wrap(r - k), h], P1 + 2 * k + h)
    wg[0, p, q] = jnp.concatenate([l1[k, h][:, 0:unit].astype(F32) for h in range(2) for k in range(RING)], axis=1).astype(BF16)
    go(w1u(p, q), M1, m_left)
    go(w1u(p, q), S1, s_right)
    go(w1u(p, q), S3, s_left)
    go(w1u(p, q), M5, m_right)

    arrive(w2u(p, ql), S2)
    go(w2u(p, ql), S6, s_right)
    arrive(w2u(p, qr), S4)
    go(w2u(p, qr), M2 + 1, m_right)
    go(w2u(p, ql), M2 + 2, m_right)
    go(w2u(p, qr), M6 + 1, m_left)
    go(w2u(p, ql), M6 + 2, m_left)

    def nth(t):
        return wrap(q + gray(t))

    arrive(lnv.at[other], DLN)
    load_x.wait()
    arrive(xf.at[other], DX)
    load_g.wait()
    arrive(gf.at[other], DG)
    vv[...] = jnp.zeros_like(vv)
    def norm_tile(t, carry):
        rows = pl.ds(pl.multiple_of(t * tile, tile), tile)
        x0, x1 = xf[0, rows].astype(F32), xf[1, rows].astype(F32)
        total = jnp.sum(x0, axis=1, keepdims=True) + jnp.sum(x1, axis=1, keepdims=True)
        squares = jnp.sum(x0 * x0, axis=1, keepdims=True) + jnp.sum(x1 * x1, axis=1, keepdims=True)
        mean = total / width
        inv = lax.rsqrt(squares / width - mean * mean + LN_EPS)
        mean_s[rows] = mean
        inv_s[rows] = inv
        ab[rows, 0:half] = ((x0 - mean) * inv * lnv[0, 0:1] + lnv[0, 1:2]).astype(BF16)
        ab[rows, half:width] = ((x1 - mean) * inv * lnv[1, 0:1] + lnv[1, 1:2]).astype(BF16)
        gb[rows, 0:half] = gf[0, rows]
        gb[rows, half:width] = gf[1, rows]
        vv[RING:RING + 1] += jnp.sum(gf[e, rows].astype(F32), axis=0, keepdims=True)
        return carry

    lax.fori_loop(0, n_tiles // 2, norm_tile, 0)
    arrive(w1u(p, qr), S3)
    go(w1u(p, qr), S5, s_left)
    go(w1u(p, qr), M1 + 1, m_left)
    lax.fori_loop(n_tiles // 2, n_tiles, norm_tile, 0)

    def relay1(t):
        arrive(w1u(pr, nth(t)), M1 + t)
        go(w1u(pr, nth(t)), M3 + t, m_left)

    def relay2(t):
        arrive(w2u(pl_, nth(t)), M2 + t)
        go(w2u(pl_, nth(t)), M4 + t, m_right)

    arrive(w1u(p, ql), S1)
    go(w1u(p, ql), M1 + 2, m_left)
    relay2(0)
    for k in range(1, RING):
        arrive(bi.at[wrap(c - k)], BI + k)
    for b in range(RING):
        for k in range(RING):
            flat = bi[b, 0:1, 2 * k * unit:(2 * k + 1) * unit]
            across = bi[k, 0:1, (2 * b + 1) * unit:(2 * b + 2) * unit]
            bias_u[b, k, 0:1, 0:unit] = jnp.where(e == 0, flat, across)
    arrive(w2u(p, qo), S6)
    go(w2u(p, qo), M2 + 3, m_right)
    relay1(0)
    relay2(1)
    arrive(w1u(p, qo), S5)
    go(w1u(p, qo), M1 + 3, m_left)
    relay2(2)

    def block(slot, b, hook=None, send_part=None):
        bias = jnp.concatenate([bias_u[b, u, 0:1, 0:unit] for u in range(RING)], axis=1)

        def block_tile(t, carry):
            rows = pl.ds(pl.multiple_of(t * tile, tile), tile)
            pre = dot(ab[rows, :], wg[0, b].reshape(fb, width), ((1,), (1,))) + bias
            squared = pre * pre
            tanh_val = jnp.tanh(GELU_K * (pre + GELU_C * pre * squared))
            hs[slot, rows] = (0.5 * pre * (1.0 + tanh_val)).astype(BF16)
            slope = 0.5 * (1.0 + tanh_val) + 0.5 * pre * (1.0 - tanh_val * tanh_val) * GELU_K * (1.0 + 3.0 * GELU_C * squared)
            pre_grad = dot(gb[rows, :], wg[1, b].reshape(fb, width), ((1,), (1,))) * slope
            vv[pl.ds(b, 1)] += jnp.sum(pre_grad, axis=0, keepdims=True)
            dcs[slot, rows] = pre_grad.astype(BF16)
            if hook is not None:
                hook(t)
            return carry

        lax.fori_loop(0, n_tiles, block_tile, 0)
        for i, (rows_of, columns_of) in enumerate(((dcs, ab), (hs, gb))):
            gw[i, b] = dot(rows_of[slot], columns_of[...], ((0,), (0,))).reshape(RING, unit, width)
            if send_part is not None:
                send_part(i)

    def half_block(slot, b, part, units, send_part):
        bias = jnp.concatenate([bias_u[b, u, 0:1, 0:unit] for u in units], axis=1)
        columns = slice(2 * part * unit, 2 * (part + 1) * unit)

        def half_tile(t, carry):
            rows = pl.ds(pl.multiple_of(t * tile, tile), tile)
            w1, w2 = (jnp.concatenate([wg[i, b, u] for u in units], axis=0) for i in range(2))
            pre = dot(ab[rows, :], w1, ((1,), (1,))) + bias
            squared = pre * pre
            tanh_val = jnp.tanh(GELU_K * (pre + GELU_C * pre * squared))
            hidden = (0.5 * pre * (1.0 + tanh_val)).astype(BF16)
            hs2[rows, :] = hidden
            hs[slot, rows, columns] = hidden
            slope = 0.5 * (1.0 + tanh_val) + 0.5 * pre * (1.0 - tanh_val * tanh_val) * GELU_K * (1.0 + 3.0 * GELU_C * squared)
            pre_grad = dot(gb[rows, :], w2, ((1,), (1,))) * slope
            sums = jnp.sum(pre_grad, axis=0, keepdims=True)
            for j, u in enumerate(units):
                db_u[u, 0:1, 0:unit] += sums[:, j * unit:(j + 1) * unit]
            lowp = pre_grad.astype(BF16)
            dcs2[rows, :] = lowp
            dcs[slot, rows, columns] = lowp
            return carry

        lax.fori_loop(0, n_tiles, half_tile, 0)
        for i, (rows_of, columns_of) in enumerate(((dcs2, ab), (hs2, gb))):
            out = dot(rows_of[...], columns_of[...], ((0,), (0,)))
            for j, u in enumerate(units):
                gw[i, b, u] = out[j * unit:(j + 1) * unit]
            send_part(i)

    def relay_gather(t):
        @pl.when(t == 0)
        def _():
            relay1(1)

        @pl.when(t == 1)
        def _():
            relay1(2)
            relay2(3)

    assert n_tiles == RING
    block(0, p, hook=relay_gather)
    relay1(3)
    for t in range(1, RING):
        go(w1u(p, nth(t)), M5 + t, m_right)
    go(w2u(p, qo), M6 + 3, m_left)

    def back1(t):
        return wrap(q - gray(RING - 1 - t))

    def back2(t):
        return wrap(q + gray(RING - 1 - t))

    db_u[...] = jnp.zeros_like(db_u)
    for part in range(2):
        mine = (2 * part, 2 * part + 1)
        for t in mine:
            arrive(w2u(po, nth(t)), M4 + t)
            arrive(w1u(po, nth(t)), M3 + t)

        def send_opposite(i):
            for t in mine:
                u = nth(t)
                rc(gw.at[i, po, u], opp.at[i, u], (R2 if i else R1) + t, m_right if i else m_left).start()

        half_block(1, po, part, tuple(nth(t) for t in mine), send_opposite)
    vv[pl.ds(po, 1)] = jnp.concatenate([db_u[u, 0:1, 0:unit] for u in range(RING)], axis=1)

    for t in range(RING):
        arrive(w2u(pr, nth(t)), M6 + t)
    def send_right(i):
        if i == 0:
            rc(gw.at[0, pr], dirs.at[0], R3, m_right).start()

    block(2, pr, send_part=send_right)
    for t in range(RING):
        arrive(w1u(pl_, nth(t)), M5 + t)
    block(3, pl_)

    def direct2(t):
        u = back2(t)
        rc(gw.at[1, pl_, u], dirs.at[1, u], R4 + t, m_left).start()

    direct2(0)
    direct2(1)

    def product_tile(t, carry):
        rows = pl.ds(pl.multiple_of(t * tile, tile), tile)
        for i, (left, acc) in enumerate(((dcs, da_acc), (hs, y_acc))):
            weights = jnp.concatenate([wg[i, p].reshape(fb, width)] + [wg[i, po, nth(k)] for k in range(RING)]
                                      + [wg[i, b].reshape(fb, width) for b in (pr, pl_)], axis=0)
            out = dot(jnp.concatenate([left[slot, rows] for slot in range(RING)], axis=1), weights)
            acc[0, rows] = out[:, 0:half]
            acc[1, rows] = out[:, half:width]
        return carry

    lax.fori_loop(0, n_tiles, product_tile, 0)

    lane = lax.broadcasted_iota(jnp.int32, (tile, 128), 1)

    def stat_tile(t, carry):
        rows = pl.ds(pl.multiple_of(t * tile, tile), tile)
        mean, inv = mean_s[rows], inv_s[rows]
        v0 = da_acc[0, rows] * lnv[0, 0:1]
        v1 = da_acc[1, rows] * lnv[1, 0:1]
        h0 = (xf[0, rows].astype(F32) - mean) * inv
        h1 = (xf[1, rows].astype(F32) - mean) * inv
        one = jnp.sum(v0, axis=1, keepdims=True) + jnp.sum(v1, axis=1, keepdims=True)
        two = jnp.sum(v0 * h0, axis=1, keepdims=True) + jnp.sum(v1 * h1, axis=1, keepdims=True)
        stat[rows] = jnp.where(lane < 64, one, two)
        return carry

    rc(y_acc.at[other], yr, EY, partner).start()
    rc(da_acc.at[other], dar, ED, partner).start()
    lax.fori_loop(0, n_tiles, stat_tile, 0)
    rc(stat, statr, ES, partner).start()

    for t in range(RING):
        u1, u2 = back1(t), back2(t)
        arrive(opp.at[1, u2], R2 + (3, 2, 1, 0)[t])
        gw[1, pr, u2] += opp[1, u2]
        rc(gw.at[1, pr, u2], rel.at[1, u2], R6 + t, m_right).start()
        arrive(opp.at[0, u1], R1 + (3, 1, 2, 0)[t])
        gw[0, pl_, u1] += opp[0, u1]
        rc(gw.at[0, pl_, u1], rel.at[0, u1], R5 + t, m_left).start()
    direct2(2)
    direct2(3)

    arrive(yr, EY)
    arrive(dar, ED)
    arrive(statr, ES)
    b_down = bd_ref[...].astype(F32).reshape(1, half)

    def out_tile(t, carry):
        rows = pl.ds(pl.multiple_of(t * tile, tile), tile)
        x_own = xf[e, rows].astype(F32)
        y_ref[rows] = (x_own + (y_acc[e, rows] + yr[rows]) + b_down).astype(BF16)
        norm_grad = da_acc[e, rows] + dar[rows]
        sums = (stat[rows] + statr[rows]) / width
        inv = inv_s[rows]
        x_hat = (x_own - mean_s[rows]) * inv
        value = norm_grad * lnv[e, 0:1]
        dx_ref[rows] = (gf[e, rows].astype(F32) + inv * (value - sums[:, 0:1] - x_hat * sums[:, 64:65])).astype(BF16)
        vv[RING + 1:RING + 2] += jnp.sum(norm_grad * x_hat, axis=0, keepdims=True)
        vv[RING + 2:RING + 3] += jnp.sum(norm_grad, axis=0, keepdims=True)
        return carry

    lax.fori_loop(0, n_tiles, out_tile, 0)

    vs[q] = vv[...]
    for k, d in ((1, s_right), (2, s_opp_dev), (3, s_left)):
        go(vs.at[q], VS + k, d)
    for k in range(1, RING):
        arrive(vs.at[wrap(q - k)], VS + k)
    vm[p] = ((vs[0] + vs[1]) + vs[2]) + vs[3]
    for k, d in ((1, m_right), (2, m_opp), (3, m_left)):
        go(vm.at[p], VM + k, d)

    arrive(dirs.at[0], R3)

    def reduce1(t):
        u = back1(t)
        arrive(rel.at[0, u], R5 + t)
        gw[0, p, u] += dirs[0, u] + rel[0, u]
        if t == 0:
            rc(gw.at[0, p, u], s_opp.at[0], Q1, s_left).start()
        if t == 1:
            rc(gw.at[0, p, u], s_dir.at[0], Q3, s_right).start()
        if t == 2:
            arrive(s_opp.at[0], Q1)
            gw[0, p, u] += s_opp[0]
            rc(gw.at[0, p, u], s_rel.at[0], Q5, s_left).start()

    def reduce2(t):
        u = back2(t)
        arrive(dirs.at[1, u], R4 + t)
        arrive(rel.at[1, u], R6 + t)
        gw[1, p, u] += dirs[1, u] + rel[1, u]
        if t == 0:
            rc(gw.at[1, p, u], s_opp.at[1], Q2, s_right).start()
        if t == 1:
            rc(gw.at[1, p, u], s_dir.at[1], Q4, s_left).start()
        if t == 2:
            arrive(s_opp.at[1], Q2)
            gw[1, p, u] += s_opp[1]
            rc(gw.at[1, p, u], s_rel.at[1], Q6, s_right).start()

    reduce1(0)
    reduce1(1)
    reduce2(0)
    reduce1(2)
    reduce2(1)
    reduce1(3)
    reduce2(2)

    arrive(s_dir.at[0], Q3)
    arrive(s_rel.at[0], Q5)
    done1 = gw[0, p, q] + s_dir[0] + s_rel[0]
    for k in range(RING):
        for h in range(2):
            start = (h * RING + k) * unit
            piece = jnp.concatenate([done1[:, start:start + unit], jnp.zeros((unit, LANES - unit), F32)], axis=1)
            f1[k, h] = piece.astype(BF16)
    for k in (2, 1, 3):
        for h in range(2):
            rc(f1.at[wrap(r + k), h], f1l.at[r, e], F1 + 2 * k + h,
               {"row": wrap(r + k), "col": c, "dep": h}, F1 + 2 * k + e).start()
    rc(f1.at[r, other], f1l.at[r, e], F1 + other, partner, F1 + e).start()
    f1l[r, e] = f1[r, e]
    reduce2(3)
    for k in range(1, RING):
        arrive(vm.at[wrap(p - k)], VM + k)
    vp[e] = ((vm[0] + vm[1]) + vm[2]) + vm[3]
    go(vp.at[e], VP, partner)
    arrive(s_dir.at[1], Q4)
    arrive(s_rel.at[1], Q6)
    done2 = (gw[1, p, q] + s_dir[1] + s_rel[1]).astype(BF16)
    f2[0] = done2[:, 0:half]
    f2[1] = done2[:, half:width]
    rc(f2.at[other], f2l.at[e], F2, partner).start()
    f2l[e] = f2[e]

    arrive(vp.at[other], VP)
    pieces = []
    for k in range(RING):
        pieces.append(vp[0, pl.ds(c, 1)][:, k * unit:(k + 1) * unit])
        row = vp[1, k:k + 1]
        piece = row[:, 0:unit]
        for j in range(1, RING):
            piece = jnp.where(c == j, row[:, j * unit:(j + 1) * unit], piece)
        pieces.append(piece)
    dbu_ref[...] = jnp.concatenate(pieces, axis=1).reshape(dbu_ref.shape)
    dbd_ref[...] = vp[e, RING:RING + 1].reshape(dbd_ref.shape)
    dsc_ref[...] = vp[e, RING + 1:RING + 2].reshape(dsc_ref.shape)
    dsh_ref[...] = vp[e, RING + 2:RING + 3].reshape(dsh_ref.shape)

    sent(l2.at[0], P2)
    sent(l1.at[0, 0], P1 + other)
    sent(l1.at[0, 0], F1 + other)
    for k in range(1, RING):
        for h in range(2):
            sent(l1.at[0, 0], P1 + 2 * k + h)
            sent(l1.at[0, 0], F1 + 2 * k + h)
        sent(bi.at[c], BI + k)
        sent(vm.at[p], VM + k)
        sent(vs.at[q], VS + k)
    sent(f2.at[0], F2)
    sent(lnv.at[0], DLN)
    sent(x_hbm, DX)
    sent(g_hbm, DG)
    for sem in (S1, S2, S3, S4, S5, S6):
        sent(w1u(p, q), sem)
    for t in range(RING):
        for sem in (M1, M2, M3, M4, M5, M6):
            sent(w1u(p, q), sem + t)
        for sem in (R1, R2, R4, R5, R6):
            sent(gw.at[0, p, q], sem + t)
    sent(gw.at[0, p], R3)
    for sem in (Q1, Q2, Q3, Q4, Q5, Q6):
        sent(gw.at[0, p, q], sem)
    sent(vp.at[e], VP)
    sent(yr, EY)
    sent(dar, ED)
    sent(stat, ES)

    arrive(f2l.at[other], F2)
    dw2_ref[0:unit] = f2l[0]
    dw2_ref[unit:2 * unit] = f2l[1]
    arrive(f1l.at[r, other], F1 + other)
    for k in range(1, RING):
        for h in range(2):
            arrive(f1l.at[wrap(r - k), h], F1 + 2 * k + h)
    dw1_ref[...] = f1l[...].astype(F32).reshape(2 * fb, LANES).T[0:unit].astype(BF16)


def copy_out(*refs):
    n = len(refs) // 2
    copies = [pltpu.make_async_copy(refs[i], refs[n + i], refs[2 * n].at[i]) for i in range(n)]
    for copy in copies:
        copy.start()
    for copy in copies:
        copy.wait()


def solution(mesh):
    assert mesh.shape["row"] == RING and mesh.shape["col"] == RING and mesh.shape["dep"] == 2
    tok_spec = P(("part", "row", "col"), "dep")
    vec_dep = P("dep")
    part_dep = P(("part", "dep"))
    in_specs = (tok_spec, vec_dep, vec_dep, P(("dep", "row"), "col"), P("col"), P(("col", "row"), "dep"), vec_dep, tok_spec)
    out_specs = (tok_spec, tok_spec, P(("part", "dep", "row"), "col"), P(("part", "col")), P(("part", "col", "row"), "dep"), part_dep, part_dep, part_dep)

    def local_step(x_in, ln_scale, ln_shift, w_up, b_up, w_down, b_down, y_grad):
        tokens, half = x_in.shape
        width = 2 * half
        unit = w_down.shape[0] // 2
        fb = RING * unit
        assert w_up.shape == (unit, 2 * fb) and half == RING * unit and fb == half
        tile = tokens // RING
        hbm_spec = pl.BlockSpec(memory_space=pltpu.HBM)
        vmem_spec = pl.BlockSpec(memory_space=pltpu.VMEM)
        vmem = pltpu.VMEM
        scratch = [
            vmem((unit, 2 * fb), BF16),
            vmem((RING, 2, unit, LANES), BF16), vmem((RING, 2, unit, LANES), BF16), vmem((2, unit, half), BF16),
            vmem((2, tokens, half), BF16), vmem((2, tokens, half), BF16),
            vmem((2, 8, half), F32),
            vmem((2, RING, RING, unit, width), BF16),
            vmem((RING, 8, 2 * fb), F32), vmem((RING, RING, 8, LANES), F32),
            vmem((tokens, width), BF16), vmem((tokens, width), BF16),
            vmem((tokens, 1), F32), vmem((tokens, 1), F32),
            vmem((2, tokens, half), F32), vmem((2, tokens, half), F32),
            vmem((tokens, half), F32), vmem((tokens, half), F32),
            vmem((tokens, 128), F32), vmem((tokens, 128), F32),
            vmem((RING, tokens, fb), BF16), vmem((RING, tokens, fb), BF16),
            vmem((tokens, 2 * unit), BF16), vmem((tokens, 2 * unit), BF16), vmem((RING, 8, LANES), F32),
            vmem((2, RING, RING, unit, width), F32),
            vmem((2, RING, unit, width), F32), vmem((2, RING, unit, width), F32), vmem((2, RING, unit, width), F32),
            vmem((2, unit, width), F32), vmem((2, unit, width), F32), vmem((2, unit, width), F32),
            vmem((8, half), F32), vmem((RING, 8, half), F32), vmem((RING, 8, half), F32), vmem((2, 8, half), F32),
            vmem((RING, 2, unit, LANES), BF16), vmem((RING, 2, unit, LANES), BF16),
            vmem((2, unit, half), BF16), vmem((2, unit, half), BF16),
            vmem((half,), F32), vmem((half,), F32), vmem((2 * fb,), BF16), vmem((half,), BF16),
            pltpu.SemaphoreType.DMA((N_SEM,)), pltpu.SemaphoreType.DMA((N_SEM,)),
        ]
        shapes = (
            jax.ShapeDtypeStruct((tokens, half), BF16), jax.ShapeDtypeStruct((tokens, half), BF16),
            jax.ShapeDtypeStruct(w_up.shape, BF16), jax.ShapeDtypeStruct(b_up.shape, F32),
            jax.ShapeDtypeStruct(w_down.shape, BF16), jax.ShapeDtypeStruct((half,), F32),
            jax.ShapeDtypeStruct((half,), F32), jax.ShapeDtypeStruct((half,), F32))
        outs = pl.pallas_call(
            functools.partial(kernel, tile),
            out_shape=shapes,
            in_specs=[hbm_spec] * 8,
            out_specs=(vmem_spec,) * 8,
            scratch_shapes=scratch,
            compiler_params=pltpu.CompilerParams(collective_id=0, has_side_effects=True, vmem_limit_bytes=51 * 1024 * 1024),
        )(*(pltpu.with_memory_space_constraint(v, pltpu.HBM) for v in (x_in, ln_scale, ln_shift, w_up, b_up, w_down, b_down, y_grad)))
        return pl.pallas_call(
            copy_out,
            out_shape=shapes,
            in_specs=[vmem_spec] * len(shapes),
            out_specs=(hbm_spec,) * len(shapes),
            scratch_shapes=[pltpu.SemaphoreType.DMA((len(shapes),))],
            compiler_params=pltpu.CompilerParams(vmem_limit_bytes=4 * 1024 * 1024),
        )(*outs)

    return jax.shard_map(local_step, mesh=mesh, in_specs=in_specs, out_specs=out_specs, check_vma=False)
```

```python
import functools

import jax
import jax.numpy as jnp
from jax import lax
from jax.experimental import pallas as pl
from jax.experimental.pallas import tpu as pltpu
from jax.sharding import PartitionSpec as P

LN_EPS = 1e-5
GELU_K = 0.7978845608028654
GELU_C = 0.044715
MESH = pl.DeviceIdType.MESH
F32 = jnp.float32
BF16 = jnp.bfloat16
RING = 4
LANES = 128

_next = [0]


def _ids(count=1):
    base = _next[0]
    _next[0] += count
    return base


IN_SEM = _ids(8)
P1 = _ids(2 * RING)
P2, DX, DG, DLN = _ids(), _ids(), _ids(), _ids()
BI = _ids(RING)
S1, S2, S3, S4, S5, S6 = (_ids() for _ in range(6))
M1, M2, M3, M4 = (_ids(RING) for _ in range(4))
M5, M6 = _ids(RING), _ids(RING)
R1, R2, R5, R6 = (_ids(RING) for _ in range(4))
R3, R4 = _ids(), _ids(RING)
Q1, Q2, Q3, Q4, Q5, Q6 = (_ids() for _ in range(6))
VM, VS = _ids(RING), _ids(RING)
VP = _ids()
EY, ED, ES = _ids(), _ids(), _ids()
F1 = _ids(2 * RING)
F2 = _ids()
N_SEM = _next[0]


def gray(t):
    return t + (t // 2) * (5 - 2 * t)


def dot(a, b, dims=((1,), (0,))):
    return lax.dot_general(a, b, (dims, ((), ())), preferred_element_type=F32)


def pack(piece):
    u = piece.shape[0]
    cut, third = 3 * u // 4, u // 3
    beside = jnp.concatenate([piece[cut:, k * third:(k + 1) * third] for k in range(3)], axis=0)
    return jnp.concatenate([piece[:cut], beside], axis=1)


def unpack(packed):
    cut = packed.shape[0]
    u = 4 * cut // 3
    quarter = u - cut
    below = jnp.concatenate([packed[k * quarter:(k + 1) * quarter, u:] for k in range(3)], axis=1)
    return jnp.concatenate([packed[:, :u], below], axis=0)


def kernel(tile, x_hbm, sc_hbm, sh_hbm, w1_hbm, bu_hbm, w2_hbm, bd_hbm, g_hbm,
           y_ref, dx_ref, dw1_ref, dbu_ref, dw2_ref, dbd_ref, dsc_ref, dsh_ref,
           w1v, st1, l1, l2, xf, gf, lnv, wg, bi, bias_u, ab, gb, mean_s, inv_s,
           y_acc, da_acc, yr, dar, stat, statr, hs, dcs, hs2, dcs2, db_u, gw, opp, dirs, rel, s_opp, s_dir, s_rel,
           vv, vm, vs, vp, f1, f1l, f2, f2l, sc_ref, sh_ref, bu_ref, bd_ref, send, recv):
    r, c, e = lax.axis_index("row"), lax.axis_index("col"), lax.axis_index("dep")
    p = c + e * (r - c)
    q = r + e * (c - r)
    tokens, half = xf.shape[1], xf.shape[2]
    width = 2 * half
    unit = l2.shape[1]
    fb = RING * unit
    n_tiles = tokens // tile
    other = 1 - e

    def wrap(v):
        return lax.rem(v + 2 * RING, RING)

    def dev(pp, qq):
        return {"row": qq + e * (pp - qq), "col": pp + e * (qq - pp), "dep": e}

    m_right, m_left, m_opp = dev(wrap(p + 1), q), dev(wrap(p - 1), q), dev(wrap(p + 2), q)
    s_right, s_left, s_opp_dev = dev(p, wrap(q + 1)), dev(p, wrap(q - 1)), dev(p, wrap(q + 2))
    partner = {"row": r, "col": c, "dep": other}
    pr, pl_, po = wrap(p + 1), wrap(p - 1), wrap(p + 2)
    qr, ql, qo = wrap(q + 1), wrap(q - 1), wrap(q + 2)

    def rc(src, dst, ssem, device, rsem=None):
        return pltpu.make_async_remote_copy(
            src_ref=src, dst_ref=dst, send_sem=send.at[ssem], recv_sem=recv.at[ssem if rsem is None else rsem],
            device_id=device, device_id_type=MESH)

    def arrive(dst, rsem):
        rc(dst, dst, rsem, partner).wait_recv()

    def sent(src, ssem):
        rc(src, src, ssem, partner).wait_send()

    def go(ref, sem, device):
        rc(ref, ref, sem, device).start()

    load_w1 = pltpu.make_async_copy(w1_hbm, w1v, recv.at[IN_SEM])
    load_w2 = pltpu.make_async_copy(w2_hbm.at[pl.ds(pl.multiple_of(e * unit, 16), unit)], l2.at[e], recv.at[IN_SEM + 1])
    load_x = pltpu.make_async_copy(x_hbm, xf.at[e], recv.at[IN_SEM + 2])
    load_g = pltpu.make_async_copy(g_hbm, gf.at[e], recv.at[IN_SEM + 3])
    load_vectors = [pltpu.make_async_copy(src, dst, recv.at[IN_SEM + 4 + i]) for i, (src, dst) in enumerate(
        ((sc_hbm, sc_ref), (sh_hbm, sh_ref), (bu_hbm, bu_ref), (bd_hbm, bd_ref)))]
    load_w1.start()
    load_w2.start()
    for load in load_vectors:
        load.start()
    load_x.start()
    load_g.start()

    barrier = pltpu.get_barrier_semaphore()
    peers = [m_right, m_left, s_right, s_left, m_opp, s_opp_dev, partner]
    peers += [{"row": wrap(r + k), "col": c, "dep": other} for k in range(1, RING)]
    for d in peers:
        pl.semaphore_signal(barrier, inc=1, device_id=d, device_id_type=MESH)

    load_w1.wait()
    turned = w1v[...].astype(F32)
    turned = jnp.concatenate([turned, jnp.zeros((LANES - unit, 2 * fb), F32)], axis=0).T
    for k in range(RING):
        for h in range(2):
            st1[k, h] = pack(turned[(2 * k + h) * unit:(2 * k + h + 1) * unit, 0:unit]).astype(BF16)

    for load in load_vectors:
        load.wait()
    lnv[e, 0:1] = sc_ref[...].reshape(1, half)
    lnv[e, 1:2] = sh_ref[...].reshape(1, half)
    bi[c] = jnp.broadcast_to(bu_ref[...].astype(F32).reshape(1, 2 * fb), (8, 2 * fb))

    pl.semaphore_wait(barrier, len(peers))

    rc(w2_hbm.at[pl.ds(pl.multiple_of(other * unit, 16), unit)], l2.at[e], P2, partner).start()
    rc(st1.at[r, other], l1.at[r, e], P1 + other, partner, P1 + e).start()
    for k in (2, 1, 3):
        for h in range(2):
            rc(st1.at[wrap(r + k), h], l1.at[r, e], P1 + 2 * k + h,
               {"row": wrap(r + k), "col": c, "dep": h}, P1 + 2 * k + e).start()
    rc(lnv.at[e], lnv.at[e], DLN, partner).start()
    rc(x_hbm, xf.at[e], DX, partner).start()
    rc(g_hbm, gf.at[e], DG, partner).start()
    for k in range(1, RING):
        rc(bi.at[c], bi.at[c], BI + k, {"row": r, "col": wrap(c + k), "dep": e}).start()
    l1[r, e] = st1[r, e]

    def w1u(b, s):
        return wg.at[0, b, s]

    def w2u(b, s):
        return wg.at[1, b, s]

    load_w2.wait()
    arrive(l2.at[other], P2)
    wg[1, p, q, :, 0:half] = l2[0]
    wg[1, p, q, :, half:width] = l2[1]
    go(w2u(p, q), M2, m_right)
    go(w2u(p, q), S2, s_right)
    go(w2u(p, q), S4, s_left)
    go(w2u(p, q), M6, m_left)

    arrive(l1.at[r, other], P1 + other)
    for k in range(1, RING):
        for h in range(2):
            arrive(l1.at[wrap(r - k), h], P1 + 2 * k + h)
    wg[0, p, q] = jnp.concatenate([unpack(l1[k, h].astype(F32)) for h in range(2) for k in range(RING)], axis=1).astype(BF16)
    go(w1u(p, q), M1, m_left)
    go(w1u(p, q), S1, s_right)
    go(w1u(p, q), S3, s_left)
    go(w1u(p, q), M5, m_right)

    arrive(w2u(p, ql), S2)
    go(w2u(p, ql), S6, s_right)
    arrive(w2u(p, qr), S4)
    go(w2u(p, qr), M2 + 1, m_right)
    go(w2u(p, ql), M2 + 2, m_right)
    go(w2u(p, qr), M6 + 1, m_left)
    go(w2u(p, ql), M6 + 2, m_left)

    def nth(t):
        return wrap(q + gray(t))

    arrive(lnv.at[other], DLN)
    load_x.wait()
    arrive(xf.at[other], DX)
    load_g.wait()
    arrive(gf.at[other], DG)
    vv[...] = jnp.zeros_like(vv)
    def norm_tile(t, carry):
        rows = pl.ds(pl.multiple_of(t * tile, tile), tile)
        x0, x1 = xf[0, rows].astype(F32), xf[1, rows].astype(F32)
        total = jnp.sum(x0, axis=1, keepdims=True) + jnp.sum(x1, axis=1, keepdims=True)
        squares = jnp.sum(x0 * x0, axis=1, keepdims=True) + jnp.sum(x1 * x1, axis=1, keepdims=True)
        mean = total / width
        inv = lax.rsqrt(squares / width - mean * mean + LN_EPS)
        mean_s[rows] = mean
        inv_s[rows] = inv
        ab[rows, 0:half] = ((x0 - mean) * inv * lnv[0, 0:1] + lnv[0, 1:2]).astype(BF16)
        ab[rows, half:width] = ((x1 - mean) * inv * lnv[1, 0:1] + lnv[1, 1:2]).astype(BF16)
        gb[rows, 0:half] = gf[0, rows]
        gb[rows, half:width] = gf[1, rows]
        vv[RING:RING + 1] += jnp.sum(gf[e, rows].astype(F32), axis=0, keepdims=True)
        return carry

    lax.fori_loop(0, n_tiles // 2, norm_tile, 0)
    arrive(w1u(p, qr), S3)
    go(w1u(p, qr), S5, s_left)
    go(w1u(p, qr), M1 + 1, m_left)
    lax.fori_loop(n_tiles // 2, n_tiles, norm_tile, 0)

    def relay1(t):
        arrive(w1u(pr, nth(t)), M1 + t)
        go(w1u(pr, nth(t)), M3 + t, m_left)

    def relay2(t):
        arrive(w2u(pl_, nth(t)), M2 + t)
        go(w2u(pl_, nth(t)), M4 + t, m_right)

    arrive(w1u(p, ql), S1)
    go(w1u(p, ql), M1 + 2, m_left)
    relay2(0)
    for k in range(1, RING):
        arrive(bi.at[wrap(c - k)], BI + k)
    for b in range(RING):
        for k in range(RING):
            flat = bi[b, 0:1, 2 * k * unit:(2 * k + 1) * unit]
            across = bi[k, 0:1, (2 * b + 1) * unit:(2 * b + 2) * unit]
            bias_u[b, k, 0:1, 0:unit] = jnp.where(e == 0, flat, across)
    arrive(w2u(p, qo), S6)
    go(w2u(p, qo), M2 + 3, m_right)
    relay1(0)
    relay2(1)
    arrive(w1u(p, qo), S5)
    go(w1u(p, qo), M1 + 3, m_left)
    relay2(2)

    def block(slot, b, hook=None, send_part=None):
        bias = jnp.concatenate([bias_u[b, u, 0:1, 0:unit] for u in range(RING)], axis=1)

        def block_tile(t, carry):
            rows = pl.ds(pl.multiple_of(t * tile, tile), tile)
            pre = dot(ab[rows, :], wg[0, b].reshape(fb, width), ((1,), (1,))) + bias
            squared = pre * pre
            tanh_val = jnp.tanh(GELU_K * (pre + GELU_C * pre * squared))
            hs[slot, rows] = (0.5 * pre * (1.0 + tanh_val)).astype(BF16)
            slope = 0.5 * (1.0 + tanh_val) + 0.5 * pre * (1.0 - tanh_val * tanh_val) * GELU_K * (1.0 + 3.0 * GELU_C * squared)
            pre_grad = dot(gb[rows, :], wg[1, b].reshape(fb, width), ((1,), (1,))) * slope
            vv[pl.ds(b, 1)] += jnp.sum(pre_grad, axis=0, keepdims=True)
            dcs[slot, rows] = pre_grad.astype(BF16)
            if hook is not None:
                hook(t)
            return carry

        lax.fori_loop(0, n_tiles, block_tile, 0)
        for i, (rows_of, columns_of) in enumerate(((dcs, ab), (hs, gb))):
            gw[i, b] = dot(rows_of[slot], columns_of[...], ((0,), (0,))).reshape(RING, unit, width)
            if send_part is not None:
                send_part(i)

    def half_block(slot, b, part, units, send_part):
        bias = jnp.concatenate([bias_u[b, u, 0:1, 0:unit] for u in units], axis=1)
        columns = slice(2 * part * unit, 2 * (part + 1) * unit)

        def half_tile(t, carry):
            rows = pl.ds(pl.multiple_of(t * tile, tile), tile)
            w1, w2 = (jnp.concatenate([wg[i, b, u] for u in units], axis=0) for i in range(2))
            pre = dot(ab[rows, :], w1, ((1,), (1,))) + bias
            squared = pre * pre
            tanh_val = jnp.tanh(GELU_K * (pre + GELU_C * pre * squared))
            hidden = (0.5 * pre * (1.0 + tanh_val)).astype(BF16)
            hs2[rows, :] = hidden
            hs[slot, rows, columns] = hidden
            slope = 0.5 * (1.0 + tanh_val) + 0.5 * pre * (1.0 - tanh_val * tanh_val) * GELU_K * (1.0 + 3.0 * GELU_C * squared)
            pre_grad = dot(gb[rows, :], w2, ((1,), (1,))) * slope
            sums = jnp.sum(pre_grad, axis=0, keepdims=True)
            for j, u in enumerate(units):
                db_u[u, 0:1, 0:unit] += sums[:, j * unit:(j + 1) * unit]
            lowp = pre_grad.astype(BF16)
            dcs2[rows, :] = lowp
            dcs[slot, rows, columns] = lowp
            return carry

        lax.fori_loop(0, n_tiles, half_tile, 0)
        for i, (rows_of, columns_of) in enumerate(((dcs2, ab), (hs2, gb))):
            out = dot(rows_of[...], columns_of[...], ((0,), (0,)))
            for j, u in enumerate(units):
                gw[i, b, u] = out[j * unit:(j + 1) * unit]
            send_part(i)

    def relay_gather(t):
        @pl.when(t == 0)
        def _():
            relay1(1)

        @pl.when(t == 1)
        def _():
            relay1(2)
            relay2(3)

    assert n_tiles == RING
    block(0, p, hook=relay_gather)
    relay1(3)
    for t in range(1, RING):
        go(w1u(p, nth(t)), M5 + t, m_right)
    go(w2u(p, qo), M6 + 3, m_left)

    def back1(t):
        return wrap(q - gray(RING - 1 - t))

    def back2(t):
        return wrap(q + gray(RING - 1 - t))

    db_u[...] = jnp.zeros_like(db_u)
    for part in range(2):
        mine = (2 * part, 2 * part + 1)
        for t in mine:
            arrive(w2u(po, nth(t)), M4 + t)
            arrive(w1u(po, nth(t)), M3 + t)

        def send_opposite(i):
            for t in mine:
                u = nth(t)
                rc(gw.at[i, po, u], opp.at[i, u], (R2 if i else R1) + t, m_right if i else m_left).start()

        half_block(1, po, part, tuple(nth(t) for t in mine), send_opposite)
    vv[pl.ds(po, 1)] = jnp.concatenate([db_u[u, 0:1, 0:unit] for u in range(RING)], axis=1)

    for t in range(RING):
        arrive(w2u(pr, nth(t)), M6 + t)
    def send_right(i):
        if i == 0:
            rc(gw.at[0, pr], dirs.at[0], R3, m_right).start()

    block(2, pr, send_part=send_right)
    for t in range(RING):
        arrive(w1u(pl_, nth(t)), M5 + t)
    block(3, pl_)

    def direct2(t):
        u = back2(t)
        rc(gw.at[1, pl_, u], dirs.at[1, u], R4 + t, m_left).start()

    direct2(0)
    direct2(1)

    def product_tile(t, carry):
        rows = pl.ds(pl.multiple_of(t * tile, tile), tile)
        for i, (left, acc) in enumerate(((dcs, da_acc), (hs, y_acc))):
            weights = jnp.concatenate([wg[i, p].reshape(fb, width)] + [wg[i, po, nth(k)] for k in range(RING)]
                                      + [wg[i, b].reshape(fb, width) for b in (pr, pl_)], axis=0)
            out = dot(jnp.concatenate([left[slot, rows] for slot in range(RING)], axis=1), weights)
            acc[0, rows] = out[:, 0:half]
            acc[1, rows] = out[:, half:width]
        return carry

    lax.fori_loop(0, n_tiles, product_tile, 0)

    lane = lax.broadcasted_iota(jnp.int32, (tile, 128), 1)

    def stat_tile(t, carry):
        rows = pl.ds(pl.multiple_of(t * tile, tile), tile)
        mean, inv = mean_s[rows], inv_s[rows]
        v0 = da_acc[0, rows] * lnv[0, 0:1]
        v1 = da_acc[1, rows] * lnv[1, 0:1]
        h0 = (xf[0, rows].astype(F32) - mean) * inv
        h1 = (xf[1, rows].astype(F32) - mean) * inv
        one = jnp.sum(v0, axis=1, keepdims=True) + jnp.sum(v1, axis=1, keepdims=True)
        two = jnp.sum(v0 * h0, axis=1, keepdims=True) + jnp.sum(v1 * h1, axis=1, keepdims=True)
        stat[rows] = jnp.where(lane < 64, one, two)
        return carry

    rc(y_acc.at[other], yr, EY, partner).start()
    rc(da_acc.at[other], dar, ED, partner).start()
    lax.fori_loop(0, n_tiles, stat_tile, 0)
    rc(stat, statr, ES, partner).start()

    for t in range(RING):
        u1, u2 = back1(t), back2(t)
        arrive(opp.at[1, u2], R2 + (3, 2, 1, 0)[t])
        gw[1, pr, u2] += opp[1, u2]
        rc(gw.at[1, pr, u2], rel.at[1, u2], R6 + t, m_right).start()
        arrive(opp.at[0, u1], R1 + (3, 1, 2, 0)[t])
        gw[0, pl_, u1] += opp[0, u1]
        rc(gw.at[0, pl_, u1], rel.at[0, u1], R5 + t, m_left).start()
    direct2(2)
    direct2(3)

    arrive(yr, EY)
    arrive(dar, ED)
    arrive(statr, ES)
    b_down = bd_ref[...].astype(F32).reshape(1, half)

    def out_tile(t, carry):
        rows = pl.ds(pl.multiple_of(t * tile, tile), tile)
        x_own = xf[e, rows].astype(F32)
        y_ref[rows] = (x_own + (y_acc[e, rows] + yr[rows]) + b_down).astype(BF16)
        norm_grad = da_acc[e, rows] + dar[rows]
        sums = (stat[rows] + statr[rows]) / width
        inv = inv_s[rows]
        x_hat = (x_own - mean_s[rows]) * inv
        value = norm_grad * lnv[e, 0:1]
        dx_ref[rows] = (gf[e, rows].astype(F32) + inv * (value - sums[:, 0:1] - x_hat * sums[:, 64:65])).astype(BF16)
        vv[RING + 1:RING + 2] += jnp.sum(norm_grad * x_hat, axis=0, keepdims=True)
        vv[RING + 2:RING + 3] += jnp.sum(norm_grad, axis=0, keepdims=True)
        return carry

    lax.fori_loop(0, n_tiles, out_tile, 0)

    vs[q] = vv[...]
    for k, d in ((1, s_right), (2, s_opp_dev), (3, s_left)):
        go(vs.at[q], VS + k, d)
    for k in range(1, RING):
        arrive(vs.at[wrap(q - k)], VS + k)
    vm[p] = ((vs[0] + vs[1]) + vs[2]) + vs[3]
    for k, d in ((1, m_right), (2, m_opp), (3, m_left)):
        go(vm.at[p], VM + k, d)

    arrive(dirs.at[0], R3)

    def reduce1(t):
        u = back1(t)
        arrive(rel.at[0, u], R5 + t)
        gw[0, p, u] += dirs[0, u] + rel[0, u]
        if t == 0:
            rc(gw.at[0, p, u], s_opp.at[0], Q1, s_left).start()
        if t == 1:
            rc(gw.at[0, p, u], s_dir.at[0], Q3, s_right).start()
        if t == 2:
            arrive(s_opp.at[0], Q1)
            gw[0, p, u] += s_opp[0]
            rc(gw.at[0, p, u], s_rel.at[0], Q5, s_left).start()

    def reduce2(t):
        u = back2(t)
        arrive(dirs.at[1, u], R4 + t)
        arrive(rel.at[1, u], R6 + t)
        gw[1, p, u] += dirs[1, u] + rel[1, u]
        if t == 0:
            rc(gw.at[1, p, u], s_opp.at[1], Q2, s_right).start()
        if t == 1:
            rc(gw.at[1, p, u], s_dir.at[1], Q4, s_left).start()
        if t == 2:
            arrive(s_opp.at[1], Q2)
            gw[1, p, u] += s_opp[1]
            rc(gw.at[1, p, u], s_rel.at[1], Q6, s_right).start()

    reduce1(0)
    reduce1(1)
    reduce2(0)
    reduce1(2)
    reduce2(1)
    reduce1(3)
    reduce2(2)

    arrive(s_dir.at[0], Q3)
    arrive(s_rel.at[0], Q5)
    done1 = gw[0, p, q] + s_dir[0] + s_rel[0]
    for k in range(RING):
        for h in range(2):
            start = (h * RING + k) * unit
            f1[k, h] = pack(done1[:, start:start + unit]).astype(BF16)
    for k in (2, 1, 3):
        for h in range(2):
            rc(f1.at[wrap(r + k), h], f1l.at[r, e], F1 + 2 * k + h,
               {"row": wrap(r + k), "col": c, "dep": h}, F1 + 2 * k + e).start()
    rc(f1.at[r, other], f1l.at[r, e], F1 + other, partner, F1 + e).start()
    f1l[r, e] = f1[r, e]
    reduce2(3)
    for k in range(1, RING):
        arrive(vm.at[wrap(p - k)], VM + k)
    vp[e] = ((vm[0] + vm[1]) + vm[2]) + vm[3]
    go(vp.at[e], VP, partner)
    arrive(s_dir.at[1], Q4)
    arrive(s_rel.at[1], Q6)
    done2 = (gw[1, p, q] + s_dir[1] + s_rel[1]).astype(BF16)
    f2[0] = done2[:, 0:half]
    f2[1] = done2[:, half:width]
    rc(f2.at[other], f2l.at[e], F2, partner).start()
    f2l[e] = f2[e]

    arrive(vp.at[other], VP)
    pieces = []
    for k in range(RING):
        pieces.append(vp[0, pl.ds(c, 1)][:, k * unit:(k + 1) * unit])
        row = vp[1, k:k + 1]
        piece = row[:, 0:unit]
        for j in range(1, RING):
            piece = jnp.where(c == j, row[:, j * unit:(j + 1) * unit], piece)
        pieces.append(piece)
    dbu_ref[...] = jnp.concatenate(pieces, axis=1).reshape(dbu_ref.shape)
    dbd_ref[...] = vp[e, RING:RING + 1].reshape(dbd_ref.shape)
    dsc_ref[...] = vp[e, RING + 1:RING + 2].reshape(dsc_ref.shape)
    dsh_ref[...] = vp[e, RING + 2:RING + 3].reshape(dsh_ref.shape)

    sent(l2.at[0], P2)
    sent(l1.at[0, 0], P1 + other)
    sent(l1.at[0, 0], F1 + other)
    for k in range(1, RING):
        for h in range(2):
            sent(l1.at[0, 0], P1 + 2 * k + h)
            sent(l1.at[0, 0], F1 + 2 * k + h)
        sent(bi.at[c], BI + k)
        sent(vm.at[p], VM + k)
        sent(vs.at[q], VS + k)
    sent(f2.at[0], F2)
    sent(lnv.at[0], DLN)
    sent(x_hbm, DX)
    sent(g_hbm, DG)
    for sem in (S1, S2, S3, S4, S5, S6):
        sent(w1u(p, q), sem)
    for t in range(RING):
        for sem in (M1, M2, M3, M4, M5, M6):
            sent(w1u(p, q), sem + t)
        for sem in (R1, R2, R4, R5, R6):
            sent(gw.at[0, p, q], sem + t)
    sent(gw.at[0, p], R3)
    for sem in (Q1, Q2, Q3, Q4, Q5, Q6):
        sent(gw.at[0, p, q], sem)
    sent(vp.at[e], VP)
    sent(yr, EY)
    sent(dar, ED)
    sent(stat, ES)

    arrive(f2l.at[other], F2)
    dw2_ref[0:unit] = f2l[0]
    dw2_ref[unit:2 * unit] = f2l[1]
    arrive(f1l.at[r, other], F1 + other)
    for k in range(1, RING):
        for h in range(2):
            arrive(f1l.at[wrap(r - k), h], F1 + 2 * k + h)
    turned = jnp.concatenate([unpack(f1l[k, h].astype(F32)) for k in range(RING) for h in range(2)], axis=0)
    turned = jnp.concatenate([turned, jnp.zeros((2 * fb, LANES - unit), F32)], axis=1)
    dw1_ref[...] = turned.T[0:unit].astype(BF16)


def copy_out(*refs):
    n = len(refs) // 2
    copies = [pltpu.make_async_copy(refs[i], refs[n + i], refs[2 * n].at[i]) for i in range(n)]
    for copy in copies:
        copy.start()
    for copy in copies:
        copy.wait()


def solution(mesh):
    assert mesh.shape["row"] == RING and mesh.shape["col"] == RING and mesh.shape["dep"] == 2
    tok_spec = P(("part", "row", "col"), "dep")
    vec_dep = P("dep")
    part_dep = P(("part", "dep"))
    in_specs = (tok_spec, vec_dep, vec_dep, P(("dep", "row"), "col"), P("col"), P(("col", "row"), "dep"), vec_dep, tok_spec)
    out_specs = (tok_spec, tok_spec, P(("part", "dep", "row"), "col"), P(("part", "col")), P(("part", "col", "row"), "dep"), part_dep, part_dep, part_dep)

    def local_step(x_in, ln_scale, ln_shift, w_up, b_up, w_down, b_down, y_grad):
        tokens, half = x_in.shape
        width = 2 * half
        unit = w_down.shape[0] // 2
        fb = RING * unit
        assert w_up.shape == (unit, 2 * fb) and half == RING * unit and fb == half
        tile = tokens // RING
        packed = (RING, 2, 3 * unit // 4, LANES)
        assert 3 * LANES == 4 * unit
        hbm_spec = pl.BlockSpec(memory_space=pltpu.HBM)
        vmem_spec = pl.BlockSpec(memory_space=pltpu.VMEM)
        vmem = pltpu.VMEM
        scratch = [
            vmem((unit, 2 * fb), BF16),
            vmem(packed, BF16), vmem(packed, BF16), vmem((2, unit, half), BF16),
            vmem((2, tokens, half), BF16), vmem((2, tokens, half), BF16),
            vmem((2, 8, half), F32),
            vmem((2, RING, RING, unit, width), BF16),
            vmem((RING, 8, 2 * fb), F32), vmem((RING, RING, 8, LANES), F32),
            vmem((tokens, width), BF16), vmem((tokens, width), BF16),
            vmem((tokens, 1), F32), vmem((tokens, 1), F32),
            vmem((2, tokens, half), F32), vmem((2, tokens, half), F32),
            vmem((tokens, half), F32), vmem((tokens, half), F32),
            vmem((tokens, 128), F32), vmem((tokens, 128), F32),
            vmem((RING, tokens, fb), BF16), vmem((RING, tokens, fb), BF16),
            vmem((tokens, 2 * unit), BF16), vmem((tokens, 2 * unit), BF16), vmem((RING, 8, LANES), F32),
            vmem((2, RING, RING, unit, width), F32),
            vmem((2, RING, unit, width), F32), vmem((2, RING, unit, width), F32), vmem((2, RING, unit, width), F32),
            vmem((2, unit, width), F32), vmem((2, unit, width), F32), vmem((2, unit, width), F32),
            vmem((8, half), F32), vmem((RING, 8, half), F32), vmem((RING, 8, half), F32), vmem((2, 8, half), F32),
            vmem(packed, BF16), vmem(packed, BF16),
            vmem((2, unit, half), BF16), vmem((2, unit, half), BF16),
            vmem((half,), F32), vmem((half,), F32), vmem((2 * fb,), BF16), vmem((half,), BF16),
            pltpu.SemaphoreType.DMA((N_SEM,)), pltpu.SemaphoreType.DMA((N_SEM,)),
        ]
        shapes = (
            jax.ShapeDtypeStruct((tokens, half), BF16), jax.ShapeDtypeStruct((tokens, half), BF16),
            jax.ShapeDtypeStruct(w_up.shape, BF16), jax.ShapeDtypeStruct(b_up.shape, F32),
            jax.ShapeDtypeStruct(w_down.shape, BF16), jax.ShapeDtypeStruct((half,), F32),
            jax.ShapeDtypeStruct((half,), F32), jax.ShapeDtypeStruct((half,), F32))
        outs = pl.pallas_call(
            functools.partial(kernel, tile),
            out_shape=shapes,
            in_specs=[hbm_spec] * 8,
            out_specs=(vmem_spec,) * 8,
            scratch_shapes=scratch,
            compiler_params=pltpu.CompilerParams(collective_id=0, has_side_effects=True, vmem_limit_bytes=51 * 1024 * 1024),
        )(*(pltpu.with_memory_space_constraint(v, pltpu.HBM) for v in (x_in, ln_scale, ln_shift, w_up, b_up, w_down, b_down, y_grad)))
        return pl.pallas_call(
            copy_out,
            out_shape=shapes,
            in_specs=[vmem_spec] * len(shapes),
            out_specs=(hbm_spec,) * len(shapes),
            scratch_shapes=[pltpu.SemaphoreType.DMA((len(shapes),))],
            compiler_params=pltpu.CompilerParams(vmem_limit_bytes=4 * 1024 * 1024),
        )(*outs)

    return jax.shard_map(local_step, mesh=mesh, in_specs=in_specs, out_specs=out_specs, check_vma=False)
```

```python
import functools

import jax
import jax.numpy as jnp
from jax import lax
from jax.experimental import pallas as pl
from jax.experimental.pallas import tpu as pltpu
from jax.sharding import PartitionSpec as P

LN_EPS = 1e-5
GELU_K = 0.7978845608028654
GELU_C = 0.044715
MESH = pl.DeviceIdType.MESH
F32 = jnp.float32
BF16 = jnp.bfloat16
RING = 4
LANES = 128

_next = [0]


def _ids(count=1):
    base = _next[0]
    _next[0] += count
    return base


IN_SEM = _ids(8)
P1 = _ids(2 * RING)
P2, DX, DG, DLN = _ids(), _ids(), _ids(), _ids()
BI = _ids(RING)
S1, S2, S3, S4, S5, S6 = (_ids() for _ in range(6))
M1, M2, M3, M4 = (_ids(RING) for _ in range(4))
M5, M6 = _ids(RING), _ids(RING)
R1, R2, R5, R6 = (_ids(RING) for _ in range(4))
R3, R4 = _ids(), _ids(RING)
Q1, Q2, Q3, Q4, Q5, Q6, Q2B, Q4B, Q6B = (_ids() for _ in range(9))
VM, VS = _ids(RING), _ids(RING)
VP = _ids()
EY, ED, ES = _ids(), _ids(), _ids()
F1 = _ids(2 * RING)
F2 = _ids()
N_SEM = _next[0]


def gray(t):
    return t + (t // 2) * (5 - 2 * t)


def dot(a, b, dims=((1,), (0,))):
    return lax.dot_general(a, b, (dims, ((), ())), preferred_element_type=F32)


def pack(piece):
    u = piece.shape[0]
    cut, third = 3 * u // 4, u // 3
    beside = jnp.concatenate([piece[cut:, k * third:(k + 1) * third] for k in range(3)], axis=0)
    return jnp.concatenate([piece[:cut], beside], axis=1)


def unpack(packed):
    cut = packed.shape[0]
    u = 4 * cut // 3
    quarter = u - cut
    below = jnp.concatenate([packed[k * quarter:(k + 1) * quarter, u:] for k in range(3)], axis=1)
    return jnp.concatenate([packed[:, :u], below], axis=0)


def kernel(tile, x_hbm, sc_hbm, sh_hbm, w1_hbm, bu_hbm, w2_hbm, bd_hbm, g_hbm,
           y_ref, dx_ref, dw1_ref, dbu_ref, dw2_ref, dbd_ref, dsc_ref, dsh_ref,
           w1v, st1, l1, l2, xf, gf, lnv, wg, bi, bias_u, ab, gb, mean_s, inv_s,
           y_acc, da_acc, yr, dar, stat, statr, hs, dcs, hs2, dcs2, db_u, gw, opp, dirs, rel, s_opp, s_dir, s_rel,
           vv, vm, vs, vp, f1, f1l, f2, f2l, sc_ref, sh_ref, bu_ref, bd_ref, send, recv):
    r, c, e = lax.axis_index("row"), lax.axis_index("col"), lax.axis_index("dep")
    p = c + e * (r - c)
    q = r + e * (c - r)
    tokens, half = xf.shape[1], xf.shape[2]
    width = 2 * half
    unit = l2.shape[1]
    fb = RING * unit
    n_tiles = tokens // tile
    other = 1 - e

    def wrap(v):
        return lax.rem(v + 2 * RING, RING)

    def dev(pp, qq):
        return {"row": qq + e * (pp - qq), "col": pp + e * (qq - pp), "dep": e}

    m_right, m_left, m_opp = dev(wrap(p + 1), q), dev(wrap(p - 1), q), dev(wrap(p + 2), q)
    s_right, s_left, s_opp_dev = dev(p, wrap(q + 1)), dev(p, wrap(q - 1)), dev(p, wrap(q + 2))
    partner = {"row": r, "col": c, "dep": other}
    pr, pl_, po = wrap(p + 1), wrap(p - 1), wrap(p + 2)
    qr, ql, qo = wrap(q + 1), wrap(q - 1), wrap(q + 2)

    def rc(src, dst, ssem, device, rsem=None):
        return pltpu.make_async_remote_copy(
            src_ref=src, dst_ref=dst, send_sem=send.at[ssem], recv_sem=recv.at[ssem if rsem is None else rsem],
            device_id=device, device_id_type=MESH)

    def arrive(dst, rsem):
        rc(dst, dst, rsem, partner).wait_recv()

    def sent(src, ssem):
        rc(src, src, ssem, partner).wait_send()

    def go(ref, sem, device):
        rc(ref, ref, sem, device).start()

    load_w1 = pltpu.make_async_copy(w1_hbm, w1v, recv.at[IN_SEM])
    load_w2 = pltpu.make_async_copy(w2_hbm.at[pl.ds(pl.multiple_of(e * unit, 16), unit)], l2.at[e], recv.at[IN_SEM + 1])
    load_x = pltpu.make_async_copy(x_hbm, xf.at[e], recv.at[IN_SEM + 2])
    load_g = pltpu.make_async_copy(g_hbm, gf.at[e], recv.at[IN_SEM + 3])
    load_vectors = [pltpu.make_async_copy(src, dst, recv.at[IN_SEM + 4 + i]) for i, (src, dst) in enumerate(
        ((sc_hbm, sc_ref), (sh_hbm, sh_ref), (bu_hbm, bu_ref), (bd_hbm, bd_ref)))]
    load_w1.start()
    load_w2.start()
    for load in load_vectors:
        load.start()
    load_x.start()
    load_g.start()

    barrier = pltpu.get_barrier_semaphore()
    peers = [m_right, m_left, s_right, s_left, m_opp, s_opp_dev, partner]
    peers += [{"row": wrap(r + k), "col": c, "dep": other} for k in range(1, RING)]
    for d in peers:
        pl.semaphore_signal(barrier, inc=1, device_id=d, device_id_type=MESH)

    pl.semaphore_wait(barrier, len(peers))
    rc(w2_hbm.at[pl.ds(pl.multiple_of(other * unit, 16), unit)], l2.at[e], P2, partner).start()
    load_w1.wait()
    turned = w1v[...].astype(F32)
    turned = jnp.concatenate([turned, jnp.zeros((LANES - unit, 2 * fb), F32)], axis=0).T
    for k in range(RING):
        for h in range(2):
            st1[k, h] = pack(turned[(2 * k + h) * unit:(2 * k + h + 1) * unit, 0:unit]).astype(BF16)

    rc(st1.at[r, other], l1.at[r, e], P1 + other, partner, P1 + e).start()
    for k in (2, 1, 3):
        for h in range(2):
            rc(st1.at[wrap(r + k), h], l1.at[r, e], P1 + 2 * k + h,
               {"row": wrap(r + k), "col": c, "dep": h}, P1 + 2 * k + e).start()
    l1[r, e] = st1[r, e]
    rc(x_hbm, xf.at[e], DX, partner).start()
    rc(g_hbm, gf.at[e], DG, partner).start()

    def w1u(b, s):
        return wg.at[0, b, s]

    def w2u(b, s):
        return wg.at[1, b, s]

    load_w2.wait()
    arrive(l2.at[other], P2)
    wg[1, p, q, :, 0:half] = l2[0]
    wg[1, p, q, :, half:width] = l2[1]
    go(w2u(p, q), M2, m_right)
    go(w2u(p, q), S2, s_right)
    go(w2u(p, q), S4, s_left)
    go(w2u(p, q), M6, m_left)
    for load in load_vectors:
        load.wait()
    lnv[e, 0:1] = sc_ref[...].reshape(1, half)
    lnv[e, 1:2] = sh_ref[...].reshape(1, half)
    bi[c] = jnp.broadcast_to(bu_ref[...].astype(F32).reshape(1, 2 * fb), (8, 2 * fb))
    rc(lnv.at[e], lnv.at[e], DLN, partner).start()
    for k in range(1, RING):
        rc(bi.at[c], bi.at[c], BI + k, {"row": r, "col": wrap(c + k), "dep": e}).start()

    arrive(l1.at[r, other], P1 + other)
    for k in range(1, RING):
        for h in range(2):
            arrive(l1.at[wrap(r - k), h], P1 + 2 * k + h)
    wg[0, p, q] = jnp.concatenate([unpack(l1[k, h].astype(F32)) for h in range(2) for k in range(RING)], axis=1).astype(BF16)
    go(w1u(p, q), M1, m_left)
    go(w1u(p, q), S1, s_right)
    go(w1u(p, q), S3, s_left)
    go(w1u(p, q), M5, m_right)

    arrive(w2u(p, ql), S2)
    go(w2u(p, ql), S6, s_right)
    arrive(w2u(p, qr), S4)
    go(w2u(p, qr), M2 + 1, m_right)
    go(w2u(p, ql), M2 + 2, m_right)
    go(w2u(p, qr), M6 + 1, m_left)
    go(w2u(p, ql), M6 + 2, m_left)

    def nth(t):
        return wrap(q + gray(t))

    arrive(lnv.at[other], DLN)
    load_x.wait()
    arrive(xf.at[other], DX)
    load_g.wait()
    arrive(gf.at[other], DG)
    vv[...] = jnp.zeros_like(vv)
    def norm_tile(t, carry):
        rows = pl.ds(pl.multiple_of(t * tile, tile), tile)
        x0, x1 = xf[0, rows].astype(F32), xf[1, rows].astype(F32)
        total = jnp.sum(x0, axis=1, keepdims=True) + jnp.sum(x1, axis=1, keepdims=True)
        squares = jnp.sum(x0 * x0, axis=1, keepdims=True) + jnp.sum(x1 * x1, axis=1, keepdims=True)
        mean = total / width
        inv = lax.rsqrt(squares / width - mean * mean + LN_EPS)
        mean_s[rows] = mean
        inv_s[rows] = inv
        ab[rows, 0:half] = ((x0 - mean) * inv * lnv[0, 0:1] + lnv[0, 1:2]).astype(BF16)
        ab[rows, half:width] = ((x1 - mean) * inv * lnv[1, 0:1] + lnv[1, 1:2]).astype(BF16)
        gb[rows, 0:half] = gf[0, rows]
        gb[rows, half:width] = gf[1, rows]
        vv[RING:RING + 1] += jnp.sum(gf[e, rows].astype(F32), axis=0, keepdims=True)
        return carry

    lax.fori_loop(0, n_tiles // 2, norm_tile, 0)
    arrive(w1u(p, qr), S3)
    go(w1u(p, qr), S5, s_left)
    go(w1u(p, qr), M1 + 1, m_left)
    lax.fori_loop(n_tiles // 2, n_tiles, norm_tile, 0)

    def relay1(t):
        arrive(w1u(pr, nth(t)), M1 + t)
        go(w1u(pr, nth(t)), M3 + t, m_left)

    def relay2(t):
        arrive(w2u(pl_, nth(t)), M2 + t)
        go(w2u(pl_, nth(t)), M4 + t, m_right)

    arrive(w1u(p, ql), S1)
    go(w1u(p, ql), M1 + 2, m_left)
    relay2(0)
    for k in range(1, RING):
        arrive(bi.at[wrap(c - k)], BI + k)
    for b in range(RING):
        for k in range(RING):
            flat = bi[b, 0:1, 2 * k * unit:(2 * k + 1) * unit]
            across = bi[k, 0:1, (2 * b + 1) * unit:(2 * b + 2) * unit]
            bias_u[b, k, 0:1, 0:unit] = jnp.where(e == 0, flat, across)
    arrive(w2u(p, qo), S6)
    go(w2u(p, qo), M2 + 3, m_right)
    relay1(0)
    relay2(1)
    arrive(w1u(p, qo), S5)
    go(w1u(p, qo), M1 + 3, m_left)
    relay2(2)

    def block(slot, b, hook=None, send_part=None):
        bias = jnp.concatenate([bias_u[b, u, 0:1, 0:unit] for u in range(RING)], axis=1)

        def block_tile(t, carry):
            rows = pl.ds(pl.multiple_of(t * tile, tile), tile)
            pre = dot(ab[rows, :], wg[0, b].reshape(fb, width), ((1,), (1,))) + bias
            squared = pre * pre
            tanh_val = jnp.tanh(GELU_K * (pre + GELU_C * pre * squared))
            hs[slot, rows] = (0.5 * pre * (1.0 + tanh_val)).astype(BF16)
            slope = 0.5 * (1.0 + tanh_val) + 0.5 * pre * (1.0 - tanh_val * tanh_val) * GELU_K * (1.0 + 3.0 * GELU_C * squared)
            pre_grad = dot(gb[rows, :], wg[1, b].reshape(fb, width), ((1,), (1,))) * slope
            vv[pl.ds(b, 1)] += jnp.sum(pre_grad, axis=0, keepdims=True)
            dcs[slot, rows] = pre_grad.astype(BF16)
            if hook is not None:
                hook(t)
            return carry

        lax.fori_loop(0, n_tiles, block_tile, 0)
        for i, (rows_of, columns_of) in enumerate(((dcs, ab), (hs, gb))):
            gw[i, b] = dot(rows_of[slot], columns_of[...], ((0,), (0,))).reshape(RING, unit, width)
            if send_part is not None:
                send_part(i)

    def half_block(slot, b, part, units, send_part):
        bias = jnp.concatenate([bias_u[b, u, 0:1, 0:unit] for u in units], axis=1)
        columns = slice(2 * part * unit, 2 * (part + 1) * unit)

        def half_tile(t, carry):
            rows = pl.ds(pl.multiple_of(t * tile, tile), tile)
            w1, w2 = (jnp.concatenate([wg[i, b, u] for u in units], axis=0) for i in range(2))
            pre = dot(ab[rows, :], w1, ((1,), (1,))) + bias
            squared = pre * pre
            tanh_val = jnp.tanh(GELU_K * (pre + GELU_C * pre * squared))
            hidden = (0.5 * pre * (1.0 + tanh_val)).astype(BF16)
            hs2[rows, :] = hidden
            hs[slot, rows, columns] = hidden
            slope = 0.5 * (1.0 + tanh_val) + 0.5 * pre * (1.0 - tanh_val * tanh_val) * GELU_K * (1.0 + 3.0 * GELU_C * squared)
            pre_grad = dot(gb[rows, :], w2, ((1,), (1,))) * slope
            sums = jnp.sum(pre_grad, axis=0, keepdims=True)
            for j, u in enumerate(units):
                db_u[u, 0:1, 0:unit] += sums[:, j * unit:(j + 1) * unit]
            lowp = pre_grad.astype(BF16)
            dcs2[rows, :] = lowp
            dcs[slot, rows, columns] = lowp
            return carry

        lax.fori_loop(0, n_tiles, half_tile, 0)
        for i, (rows_of, columns_of) in enumerate(((dcs2, ab), (hs2, gb))):
            out = dot(rows_of[...], columns_of[...], ((0,), (0,)))
            for j, u in enumerate(units):
                gw[i, b, u] = out[j * unit:(j + 1) * unit]
            send_part(i)

    def relay_gather(t):
        @pl.when(t == 0)
        def _():
            relay1(1)

        @pl.when(t == 1)
        def _():
            relay1(2)
            relay2(3)

    assert n_tiles == RING
    block(0, p, hook=relay_gather)
    relay1(3)
    for t in range(1, RING):
        go(w1u(p, nth(t)), M5 + t, m_right)
    go(w2u(p, qo), M6 + 3, m_left)

    def back1(t):
        return wrap(q - gray(RING - 1 - t))

    def back2(t):
        return wrap(q + gray(RING - 1 - t))

    db_u[...] = jnp.zeros_like(db_u)
    for part in range(2):
        mine = (2 * part, 2 * part + 1)
        for t in mine:
            arrive(w2u(po, nth(t)), M4 + t)
            arrive(w1u(po, nth(t)), M3 + t)

        def send_opposite(i):
            for t in mine:
                u = nth(t)
                rc(gw.at[i, po, u], opp.at[i, u], (R2 if i else R1) + t, m_right if i else m_left).start()

        half_block(1, po, part, tuple(nth(t) for t in mine), send_opposite)
    vv[pl.ds(po, 1)] = jnp.concatenate([db_u[u, 0:1, 0:unit] for u in range(RING)], axis=1)

    for t in range(RING):
        arrive(w2u(pr, nth(t)), M6 + t)
    def send_right(i):
        if i == 0:
            rc(gw.at[0, pr], dirs.at[0], R3, m_right).start()

    block(2, pr, send_part=send_right)
    for t in range(RING):
        arrive(w1u(pl_, nth(t)), M5 + t)
    block(3, pl_)

    def direct2(t):
        u = back2(t)
        rc(gw.at[1, pl_, u], dirs.at[1, u], R4 + t, m_left).start()

    direct2(0)
    direct2(1)

    def product_tile(t, carry):
        rows = pl.ds(pl.multiple_of(t * tile, tile), tile)
        for i, (left, acc) in enumerate(((dcs, da_acc), (hs, y_acc))):
            weights = jnp.concatenate([wg[i, p].reshape(fb, width)] + [wg[i, po, nth(k)] for k in range(RING)]
                                      + [wg[i, b].reshape(fb, width) for b in (pr, pl_)], axis=0)
            out = dot(jnp.concatenate([left[slot, rows] for slot in range(RING)], axis=1), weights)
            acc[0, rows] = out[:, 0:half]
            acc[1, rows] = out[:, half:width]
        return carry

    lax.fori_loop(0, n_tiles, product_tile, 0)

    lane = lax.broadcasted_iota(jnp.int32, (tile, 128), 1)

    def stat_tile(t, carry):
        rows = pl.ds(pl.multiple_of(t * tile, tile), tile)
        mean, inv = mean_s[rows], inv_s[rows]
        v0 = da_acc[0, rows] * lnv[0, 0:1]
        v1 = da_acc[1, rows] * lnv[1, 0:1]
        h0 = (xf[0, rows].astype(F32) - mean) * inv
        h1 = (xf[1, rows].astype(F32) - mean) * inv
        one = jnp.sum(v0, axis=1, keepdims=True) + jnp.sum(v1, axis=1, keepdims=True)
        two = jnp.sum(v0 * h0, axis=1, keepdims=True) + jnp.sum(v1 * h1, axis=1, keepdims=True)
        stat[rows] = jnp.where(lane < 64, one, two)
        return carry

    rc(y_acc.at[other], yr, EY, partner).start()
    rc(da_acc.at[other], dar, ED, partner).start()
    lax.fori_loop(0, n_tiles, stat_tile, 0)
    rc(stat, statr, ES, partner).start()

    for t in range(RING):
        u1, u2 = back1(t), back2(t)
        arrive(opp.at[1, u2], R2 + (3, 2, 1, 0)[t])
        gw[1, pr, u2] += opp[1, u2]
        rc(gw.at[1, pr, u2], rel.at[1, u2], R6 + t, m_right).start()
        arrive(opp.at[0, u1], R1 + (3, 1, 2, 0)[t])
        gw[0, pl_, u1] += opp[0, u1]
        rc(gw.at[0, pl_, u1], rel.at[0, u1], R5 + t, m_left).start()
    direct2(2)
    direct2(3)

    arrive(yr, EY)
    arrive(dar, ED)
    arrive(statr, ES)
    b_down = bd_ref[...].astype(F32).reshape(1, half)

    def out_tile(t, carry):
        rows = pl.ds(pl.multiple_of(t * tile, tile), tile)
        x_own = xf[e, rows].astype(F32)
        y_ref[rows] = (x_own + (y_acc[e, rows] + yr[rows]) + b_down).astype(BF16)
        norm_grad = da_acc[e, rows] + dar[rows]
        sums = (stat[rows] + statr[rows]) / width
        inv = inv_s[rows]
        x_hat = (x_own - mean_s[rows]) * inv
        value = norm_grad * lnv[e, 0:1]
        dx_ref[rows] = (gf[e, rows].astype(F32) + inv * (value - sums[:, 0:1] - x_hat * sums[:, 64:65])).astype(BF16)
        vv[RING + 1:RING + 2] += jnp.sum(norm_grad * x_hat, axis=0, keepdims=True)
        vv[RING + 2:RING + 3] += jnp.sum(norm_grad, axis=0, keepdims=True)
        return carry

    lax.fori_loop(0, n_tiles, out_tile, 0)

    vs[q] = vv[...]
    for k, d in ((1, s_right), (2, s_opp_dev), (3, s_left)):
        go(vs.at[q], VS + k, d)
    for k in range(1, RING):
        arrive(vs.at[wrap(q - k)], VS + k)
    vm[p] = ((vs[0] + vs[1]) + vs[2]) + vs[3]
    for k, d in ((1, m_right), (2, m_opp), (3, m_left)):
        go(vm.at[p], VM + k, d)

    arrive(dirs.at[0], R3)

    def reduce1(t):
        u = back1(t)
        arrive(rel.at[0, u], R5 + t)
        gw[0, p, u] += dirs[0, u] + rel[0, u]
        if t == 0:
            rc(gw.at[0, p, u], s_opp.at[0], Q1, s_left).start()
        if t == 1:
            rc(gw.at[0, p, u], s_dir.at[0], Q3, s_right).start()
        if t == 2:
            arrive(s_opp.at[0], Q1)
            gw[0, p, u] += s_opp[0]
            rc(gw.at[0, p, u], s_rel.at[0], Q5, s_left).start()

    most, rest = pl.ds(0, 3 * unit // 4), pl.ds(3 * unit // 4, unit // 4)

    def reduce2(t):
        u = back2(t)
        arrive(dirs.at[1, u], R4 + t)
        arrive(rel.at[1, u], R6 + t)
        gw[1, p, u] += dirs[1, u] + rel[1, u]
        if t == 0:
            rc(gw.at[1, p, u, most], s_opp.at[1, most], Q2, s_right).start()
            rc(gw.at[1, p, u, rest], s_opp.at[1, rest], Q2B, s_left).start()
        if t == 1:
            rc(gw.at[1, p, u, most], s_dir.at[1, most], Q4, s_left).start()
        if t == 2:
            rc(gw.at[1, p, u, rest], s_dir.at[1, rest], Q4B, s_right).start()
            before = back2(1)
            arrive(s_opp.at[1, rest], Q2B)
            gw[1, p, before, rest] += s_opp[1, rest]
            rc(gw.at[1, p, before, rest], s_rel.at[1, rest], Q6B, s_left).start()
            arrive(s_opp.at[1, most], Q2)
            gw[1, p, u, most] += s_opp[1, most]
            rc(gw.at[1, p, u, most], s_rel.at[1, most], Q6, s_right).start()

    reduce1(0)
    reduce1(1)
    reduce2(0)
    reduce1(2)
    reduce2(1)
    reduce1(3)
    reduce2(2)

    arrive(s_dir.at[0], Q3)
    arrive(s_rel.at[0], Q5)
    done1 = gw[0, p, q] + s_dir[0] + s_rel[0]
    for k in range(RING):
        for h in range(2):
            start = (h * RING + k) * unit
            f1[k, h] = pack(done1[:, start:start + unit]).astype(BF16)
    for k in (2, 1, 3):
        for h in range(2):
            rc(f1.at[wrap(r + k), h], f1l.at[r, e], F1 + 2 * k + h,
               {"row": wrap(r + k), "col": c, "dep": h}, F1 + 2 * k + e).start()
    rc(f1.at[r, other], f1l.at[r, e], F1 + other, partner, F1 + e).start()
    f1l[r, e] = f1[r, e]
    reduce2(3)
    for k in range(1, RING):
        arrive(vm.at[wrap(p - k)], VM + k)
    vp[e] = ((vm[0] + vm[1]) + vm[2]) + vm[3]
    go(vp.at[e], VP, partner)
    arrive(s_dir.at[1, most], Q4)
    arrive(s_dir.at[1, rest], Q4B)
    arrive(s_rel.at[1, rest], Q6B)
    arrive(s_rel.at[1, most], Q6)
    done2 = (gw[1, p, q] + s_dir[1] + s_rel[1]).astype(BF16)
    f2[0] = done2[:, 0:half]
    f2[1] = done2[:, half:width]
    rc(f2.at[other], f2l.at[e], F2, partner).start()
    f2l[e] = f2[e]

    arrive(vp.at[other], VP)
    pieces = []
    for k in range(RING):
        pieces.append(vp[0, pl.ds(c, 1)][:, k * unit:(k + 1) * unit])
        row = vp[1, k:k + 1]
        piece = row[:, 0:unit]
        for j in range(1, RING):
            piece = jnp.where(c == j, row[:, j * unit:(j + 1) * unit], piece)
        pieces.append(piece)
    dbu_ref[...] = jnp.concatenate(pieces, axis=1).reshape(dbu_ref.shape)
    dbd_ref[...] = vp[e, RING:RING + 1].reshape(dbd_ref.shape)
    dsc_ref[...] = vp[e, RING + 1:RING + 2].reshape(dsc_ref.shape)
    dsh_ref[...] = vp[e, RING + 2:RING + 3].reshape(dsh_ref.shape)

    sent(l2.at[0], P2)
    sent(l1.at[0, 0], P1 + other)
    sent(l1.at[0, 0], F1 + other)
    for k in range(1, RING):
        for h in range(2):
            sent(l1.at[0, 0], P1 + 2 * k + h)
            sent(l1.at[0, 0], F1 + 2 * k + h)
        sent(bi.at[c], BI + k)
        sent(vm.at[p], VM + k)
        sent(vs.at[q], VS + k)
    sent(f2.at[0], F2)
    sent(lnv.at[0], DLN)
    sent(x_hbm, DX)
    sent(g_hbm, DG)
    for sem in (S1, S2, S3, S4, S5, S6):
        sent(w1u(p, q), sem)
    for t in range(RING):
        for sem in (M1, M2, M3, M4, M5, M6):
            sent(w1u(p, q), sem + t)
        for sem in (R1, R2, R4, R5, R6):
            sent(gw.at[0, p, q], sem + t)
    sent(gw.at[0, p], R3)
    for sem in (Q1, Q3, Q5):
        sent(gw.at[0, p, q], sem)
    for sem in (Q2, Q4, Q6):
        sent(gw.at[1, p, q, most], sem)
    for sem in (Q2B, Q4B, Q6B):
        sent(gw.at[1, p, q, rest], sem)
    sent(vp.at[e], VP)
    sent(yr, EY)
    sent(dar, ED)
    sent(stat, ES)

    arrive(f2l.at[other], F2)
    dw2_ref[0:unit] = f2l[0]
    dw2_ref[unit:2 * unit] = f2l[1]
    arrive(f1l.at[r, other], F1 + other)
    for k in range(1, RING):
        for h in range(2):
            arrive(f1l.at[wrap(r - k), h], F1 + 2 * k + h)
    turned = jnp.concatenate([unpack(f1l[k, h].astype(F32)) for k in range(RING) for h in range(2)], axis=0)
    turned = jnp.concatenate([turned, jnp.zeros((2 * fb, LANES - unit), F32)], axis=1)
    dw1_ref[...] = turned.T[0:unit].astype(BF16)


def copy_out(*refs):
    n = len(refs) // 2
    copies = [pltpu.make_async_copy(refs[i], refs[n + i], refs[2 * n].at[i]) for i in range(n)]
    for copy in copies:
        copy.start()
    for copy in copies:
        copy.wait()


def solution(mesh):
    assert mesh.shape["row"] == RING and mesh.shape["col"] == RING and mesh.shape["dep"] == 2
    tok_spec = P(("part", "row", "col"), "dep")
    vec_dep = P("dep")
    part_dep = P(("part", "dep"))
    in_specs = (tok_spec, vec_dep, vec_dep, P(("dep", "row"), "col"), P("col"), P(("col", "row"), "dep"), vec_dep, tok_spec)
    out_specs = (tok_spec, tok_spec, P(("part", "dep", "row"), "col"), P(("part", "col")), P(("part", "col", "row"), "dep"), part_dep, part_dep, part_dep)

    def local_step(x_in, ln_scale, ln_shift, w_up, b_up, w_down, b_down, y_grad):
        tokens, half = x_in.shape
        width = 2 * half
        unit = w_down.shape[0] // 2
        fb = RING * unit
        assert w_up.shape == (unit, 2 * fb) and half == RING * unit and fb == half
        tile = tokens // RING
        packed = (RING, 2, 3 * unit // 4, LANES)
        assert 3 * LANES == 4 * unit
        hbm_spec = pl.BlockSpec(memory_space=pltpu.HBM)
        vmem_spec = pl.BlockSpec(memory_space=pltpu.VMEM)
        vmem = pltpu.VMEM
        scratch = [
            vmem((unit, 2 * fb), BF16),
            vmem(packed, BF16), vmem(packed, BF16), vmem((2, unit, half), BF16),
            vmem((2, tokens, half), BF16), vmem((2, tokens, half), BF16),
            vmem((2, 8, half), F32),
            vmem((2, RING, RING, unit, width), BF16),
            vmem((RING, 8, 2 * fb), F32), vmem((RING, RING, 8, LANES), F32),
            vmem((tokens, width), BF16), vmem((tokens, width), BF16),
            vmem((tokens, 1), F32), vmem((tokens, 1), F32),
            vmem((2, tokens, half), F32), vmem((2, tokens, half), F32),
            vmem((tokens, half), F32), vmem((tokens, half), F32),
            vmem((tokens, 128), F32), vmem((tokens, 128), F32),
            vmem((RING, tokens, fb), BF16), vmem((RING, tokens, fb), BF16),
            vmem((tokens, 2 * unit), BF16), vmem((tokens, 2 * unit), BF16), vmem((RING, 8, LANES), F32),
            vmem((2, RING, RING, unit, width), F32),
            vmem((2, RING, unit, width), F32), vmem((2, RING, unit, width), F32), vmem((2, RING, unit, width), F32),
            vmem((2, unit, width), F32), vmem((2, unit, width), F32), vmem((2, unit, width), F32),
            vmem((8, half), F32), vmem((RING, 8, half), F32), vmem((RING, 8, half), F32), vmem((2, 8, half), F32),
            vmem(packed, BF16), vmem(packed, BF16),
            vmem((2, unit, half), BF16), vmem((2, unit, half), BF16),
            vmem((half,), F32), vmem((half,), F32), vmem((2 * fb,), BF16), vmem((half,), BF16),
            pltpu.SemaphoreType.DMA((N_SEM,)), pltpu.SemaphoreType.DMA((N_SEM,)),
        ]
        shapes = (
            jax.ShapeDtypeStruct((tokens, half), BF16), jax.ShapeDtypeStruct((tokens, half), BF16),
            jax.ShapeDtypeStruct(w_up.shape, BF16), jax.ShapeDtypeStruct(b_up.shape, F32),
            jax.ShapeDtypeStruct(w_down.shape, BF16), jax.ShapeDtypeStruct((half,), F32),
            jax.ShapeDtypeStruct((half,), F32), jax.ShapeDtypeStruct((half,), F32))
        outs = pl.pallas_call(
            functools.partial(kernel, tile),
            out_shape=shapes,
            in_specs=[hbm_spec] * 8,
            out_specs=(vmem_spec,) * 8,
            scratch_shapes=scratch,
            compiler_params=pltpu.CompilerParams(collective_id=0, has_side_effects=True, vmem_limit_bytes=51 * 1024 * 1024),
        )(*(pltpu.with_memory_space_constraint(v, pltpu.HBM) for v in (x_in, ln_scale, ln_shift, w_up, b_up, w_down, b_down, y_grad)))
        return pl.pallas_call(
            copy_out,
            out_shape=shapes,
            in_specs=[vmem_spec] * len(shapes),
            out_specs=(hbm_spec,) * len(shapes),
            scratch_shapes=[pltpu.SemaphoreType.DMA((len(shapes),))],
            compiler_params=pltpu.CompilerParams(vmem_limit_bytes=4 * 1024 * 1024),
        )(*outs)

    return jax.shard_map(local_step, mesh=mesh, in_specs=in_specs, out_specs=out_specs, check_vma=False)
```

```python
import functools

import jax
import jax.numpy as jnp
from jax import lax
from jax.experimental import pallas as pl
from jax.experimental.pallas import tpu as pltpu
from jax.sharding import PartitionSpec as P

LN_EPS = 1e-5
GELU_K = 0.7978845608028654
GELU_C = 0.044715
MESH = pl.DeviceIdType.MESH
F32 = jnp.float32
BF16 = jnp.bfloat16
RING = 4
LANES = 128

_next = [0]


def _ids(count=1):
    base = _next[0]
    _next[0] += count
    return base


IN_SEM = _ids(8)
P1 = _ids(2 * RING)
P2, DX, DG, DLN = _ids(), _ids(), _ids(), _ids()
BI = _ids(RING)
S1, S2, S3, S4, S5, S6 = (_ids() for _ in range(6))
M1, M2, M3, M4 = (_ids(RING) for _ in range(4))
M5, M6 = _ids(RING), _ids(RING)
R1, R2, R5, R6 = (_ids(RING) for _ in range(4))
R3, R4 = _ids(), _ids(RING)
Q1, Q2, Q3, Q4, Q5, Q6, Q2B, Q4B, Q6B = (_ids() for _ in range(9))
VM, VS = _ids(RING), _ids(RING)
VP = _ids()
EY, ED, ES = _ids(), _ids(), _ids()
F1 = _ids(2 * RING)
F2 = _ids()
N_SEM = _next[0]


def gray(t):
    return t + (t // 2) * (5 - 2 * t)


def dot(a, b, dims=((1,), (0,))):
    return lax.dot_general(a, b, (dims, ((), ())), preferred_element_type=F32)


def pack(piece):
    u = piece.shape[0]
    cut, third = 3 * u // 4, u // 3
    beside = jnp.concatenate([piece[cut:, k * third:(k + 1) * third] for k in range(3)], axis=0)
    return jnp.concatenate([piece[:cut], beside], axis=1)


def unpack(packed):
    cut = packed.shape[0]
    u = 4 * cut // 3
    quarter = u - cut
    below = jnp.concatenate([packed[k * quarter:(k + 1) * quarter, u:] for k in range(3)], axis=1)
    return jnp.concatenate([packed[:, :u], below], axis=0)


def kernel(tile, x_hbm, sc_hbm, sh_hbm, w1_hbm, bu_hbm, w2_hbm, bd_hbm, g_hbm,
           y_ref, dx_ref, dw1_ref, dbu_ref, dw2_ref, dbd_ref, dsc_ref, dsh_ref,
           w1v, st1, l1, l2, xf, gf, lnv, wg, bi, bias_u, ab, gb, mean_s, inv_s,
           y_acc, da_acc, yr, dar, stat, statr, hs, dcs, hs2, dcs2, db_u, gw, opp, dirs, rel, s_opp, s_dir, s_rel,
           vv, vm, vs, vp, f1, f1l, f2, f2l, sc_ref, sh_ref, bu_ref, bd_ref, send, recv):
    r, c, e = lax.axis_index("row"), lax.axis_index("col"), lax.axis_index("dep")
    p = c + e * (r - c)
    q = r + e * (c - r)
    tokens, half = xf.shape[1], xf.shape[2]
    width = 2 * half
    unit = l2.shape[1]
    fb = RING * unit
    n_tiles = tokens // tile
    other = 1 - e

    def wrap(v):
        return lax.rem(v + 2 * RING, RING)

    def dev(pp, qq):
        return {"row": qq + e * (pp - qq), "col": pp + e * (qq - pp), "dep": e}

    m_right, m_left, m_opp = dev(wrap(p + 1), q), dev(wrap(p - 1), q), dev(wrap(p + 2), q)
    s_right, s_left, s_opp_dev = dev(p, wrap(q + 1)), dev(p, wrap(q - 1)), dev(p, wrap(q + 2))
    partner = {"row": r, "col": c, "dep": other}
    pr, pl_, po = wrap(p + 1), wrap(p - 1), wrap(p + 2)
    qr, ql, qo = wrap(q + 1), wrap(q - 1), wrap(q + 2)

    def rc(src, dst, ssem, device, rsem=None):
        return pltpu.make_async_remote_copy(
            src_ref=src, dst_ref=dst, send_sem=send.at[ssem], recv_sem=recv.at[ssem if rsem is None else rsem],
            device_id=device, device_id_type=MESH)

    def arrive(dst, rsem):
        rc(dst, dst, rsem, partner).wait_recv()

    def sent(src, ssem):
        rc(src, src, ssem, partner).wait_send()

    def go(ref, sem, device):
        rc(ref, ref, sem, device).start()

    load_w1 = pltpu.make_async_copy(w1_hbm, w1v, recv.at[IN_SEM])
    load_w2 = pltpu.make_async_copy(w2_hbm.at[pl.ds(pl.multiple_of(e * unit, 16), unit)], l2.at[e], recv.at[IN_SEM + 1])
    load_x = pltpu.make_async_copy(x_hbm, xf.at[e], recv.at[IN_SEM + 2])
    load_g = pltpu.make_async_copy(g_hbm, gf.at[e], recv.at[IN_SEM + 3])
    load_vectors = [pltpu.make_async_copy(src, dst, recv.at[IN_SEM + 4 + i]) for i, (src, dst) in enumerate(
        ((sc_hbm, sc_ref), (sh_hbm, sh_ref), (bu_hbm, bu_ref), (bd_hbm, bd_ref)))]
    load_w1.start()
    load_w2.start()
    for load in load_vectors:
        load.start()
    load_x.start()
    load_g.start()

    barrier = pltpu.get_barrier_semaphore()
    peers = [m_right, m_left, s_right, s_left, m_opp, s_opp_dev, partner]
    peers += [{"row": wrap(r + k), "col": c, "dep": other} for k in range(1, RING)]
    for d in peers:
        pl.semaphore_signal(barrier, inc=1, device_id=d, device_id_type=MESH)

    load_w1.wait()
    turned = w1v[...].astype(F32)
    turned = jnp.concatenate([turned, jnp.zeros((LANES - unit, 2 * fb), F32)], axis=0).T
    for k in range(RING):
        for h in range(2):
            st1[k, h] = pack(turned[(2 * k + h) * unit:(2 * k + h + 1) * unit, 0:unit]).astype(BF16)

    for load in load_vectors:
        load.wait()
    lnv[e, 0:1] = sc_ref[...].reshape(1, half)
    lnv[e, 1:2] = sh_ref[...].reshape(1, half)
    bi[c] = jnp.broadcast_to(bu_ref[...].astype(F32).reshape(1, 2 * fb), (8, 2 * fb))

    pl.semaphore_wait(barrier, len(peers))

    rc(w2_hbm.at[pl.ds(pl.multiple_of(other * unit, 16), unit)], l2.at[e], P2, partner).start()
    rc(st1.at[r, other], l1.at[r, e], P1 + other, partner, P1 + e).start()
    for k in (2, 1, 3):
        for h in range(2):
            rc(st1.at[wrap(r + k), h], l1.at[r, e], P1 + 2 * k + h,
               {"row": wrap(r + k), "col": c, "dep": h}, P1 + 2 * k + e).start()
    rc(lnv.at[e], lnv.at[e], DLN, partner).start()
    rc(x_hbm, xf.at[e], DX, partner).start()
    rc(g_hbm, gf.at[e], DG, partner).start()
    for k in range(1, RING):
        rc(bi.at[c], bi.at[c], BI + k, {"row": r, "col": wrap(c + k), "dep": e}).start()
    l1[r, e] = st1[r, e]

    def w1u(b, s):
        return wg.at[0, b, s]

    def w2u(b, s):
        return wg.at[1, b, s]

    load_w2.wait()
    arrive(l2.at[other], P2)
    wg[1, p, q, :, 0:half] = l2[0]
    wg[1, p, q, :, half:width] = l2[1]
    go(w2u(p, q), M2, m_right)
    go(w2u(p, q), S2, s_right)
    go(w2u(p, q), S4, s_left)
    go(w2u(p, q), M6, m_left)

    arrive(l1.at[r, other], P1 + other)
    for k in range(1, RING):
        for h in range(2):
            arrive(l1.at[wrap(r - k), h], P1 + 2 * k + h)
    wg[0, p, q] = jnp.concatenate([unpack(l1[k, h].astype(F32)) for h in range(2) for k in range(RING)], axis=1).astype(BF16)
    go(w1u(p, q), M1, m_left)
    go(w1u(p, q), S1, s_right)
    go(w1u(p, q), S3, s_left)
    go(w1u(p, q), M5, m_right)

    arrive(w2u(p, ql), S2)
    go(w2u(p, ql), S6, s_right)
    arrive(w2u(p, qr), S4)
    go(w2u(p, qr), M2 + 1, m_right)
    go(w2u(p, ql), M2 + 2, m_right)
    go(w2u(p, qr), M6 + 1, m_left)
    go(w2u(p, ql), M6 + 2, m_left)

    def nth(t):
        return wrap(q + gray(t))

    arrive(lnv.at[other], DLN)
    load_x.wait()
    arrive(xf.at[other], DX)
    load_g.wait()
    arrive(gf.at[other], DG)
    vv[...] = jnp.zeros_like(vv)
    def norm_tile(t, carry):
        rows = pl.ds(pl.multiple_of(t * tile, tile), tile)
        x0, x1 = xf[0, rows].astype(F32), xf[1, rows].astype(F32)
        total = jnp.sum(x0, axis=1, keepdims=True) + jnp.sum(x1, axis=1, keepdims=True)
        squares = jnp.sum(x0 * x0, axis=1, keepdims=True) + jnp.sum(x1 * x1, axis=1, keepdims=True)
        mean = total / width
        inv = lax.rsqrt(squares / width - mean * mean + LN_EPS)
        mean_s[rows] = mean
        inv_s[rows] = inv
        ab[rows, 0:half] = ((x0 - mean) * inv * lnv[0, 0:1] + lnv[0, 1:2]).astype(BF16)
        ab[rows, half:width] = ((x1 - mean) * inv * lnv[1, 0:1] + lnv[1, 1:2]).astype(BF16)
        gb[rows, 0:half] = gf[0, rows]
        gb[rows, half:width] = gf[1, rows]
        vv[RING:RING + 1] += jnp.sum(gf[e, rows].astype(F32), axis=0, keepdims=True)
        return carry

    lax.fori_loop(0, n_tiles // 2, norm_tile, 0)
    arrive(w1u(p, qr), S3)
    go(w1u(p, qr), S5, s_left)
    go(w1u(p, qr), M1 + 1, m_left)
    lax.fori_loop(n_tiles // 2, n_tiles, norm_tile, 0)

    def relay1(t):
        arrive(w1u(pr, nth(t)), M1 + t)
        go(w1u(pr, nth(t)), M3 + t, m_left)

    def relay2(t):
        arrive(w2u(pl_, nth(t)), M2 + t)
        go(w2u(pl_, nth(t)), M4 + t, m_right)

    arrive(w1u(p, ql), S1)
    go(w1u(p, ql), M1 + 2, m_left)
    relay2(0)
    for k in range(1, RING):
        arrive(bi.at[wrap(c - k)], BI + k)
    for b in range(RING):
        for k in range(RING):
            flat = bi[b, 0:1, 2 * k * unit:(2 * k + 1) * unit]
            across = bi[k, 0:1, (2 * b + 1) * unit:(2 * b + 2) * unit]
            bias_u[b, k, 0:1, 0:unit] = jnp.where(e == 0, flat, across)
    arrive(w2u(p, qo), S6)
    go(w2u(p, qo), M2 + 3, m_right)
    relay1(0)
    relay2(1)
    arrive(w1u(p, qo), S5)
    go(w1u(p, qo), M1 + 3, m_left)
    relay2(2)

    def block(slot, b, hook=None, send_part=None):
        bias = jnp.concatenate([bias_u[b, u, 0:1, 0:unit] for u in range(RING)], axis=1)

        def block_tile(t, carry):
            rows = pl.ds(pl.multiple_of(t * tile, tile), tile)
            pre = dot(ab[rows, :], wg[0, b].reshape(fb, width), ((1,), (1,))) + bias
            squared = pre * pre
            tanh_val = jnp.tanh(GELU_K * (pre + GELU_C * pre * squared))
            hs[slot, rows] = (0.5 * pre * (1.0 + tanh_val)).astype(BF16)
            slope = 0.5 * (1.0 + tanh_val) + 0.5 * pre * (1.0 - tanh_val * tanh_val) * GELU_K * (1.0 + 3.0 * GELU_C * squared)
            pre_grad = dot(gb[rows, :], wg[1, b].reshape(fb, width), ((1,), (1,))) * slope
            vv[pl.ds(b, 1)] += jnp.sum(pre_grad, axis=0, keepdims=True)
            dcs[slot, rows] = pre_grad.astype(BF16)
            if hook is not None:
                hook(t)
            return carry

        lax.fori_loop(0, n_tiles, block_tile, 0)
        for i, (rows_of, columns_of) in enumerate(((dcs, ab), (hs, gb))):
            gw[i, b] = dot(rows_of[slot], columns_of[...], ((0,), (0,))).reshape(RING, unit, width)
            if send_part is not None:
                send_part(i)

    def half_block(slot, b, part, units, send_part):
        bias = jnp.concatenate([bias_u[b, u, 0:1, 0:unit] for u in units], axis=1)
        columns = slice(2 * part * unit, 2 * (part + 1) * unit)

        def half_tile(t, carry):
            rows = pl.ds(pl.multiple_of(t * tile, tile), tile)
            w1, w2 = (jnp.concatenate([wg[i, b, u] for u in units], axis=0) for i in range(2))
            pre = dot(ab[rows, :], w1, ((1,), (1,))) + bias
            squared = pre * pre
            tanh_val = jnp.tanh(GELU_K * (pre + GELU_C * pre * squared))
            hidden = (0.5 * pre * (1.0 + tanh_val)).astype(BF16)
            hs2[rows, :] = hidden
            hs[slot, rows, columns] = hidden
            slope = 0.5 * (1.0 + tanh_val) + 0.5 * pre * (1.0 - tanh_val * tanh_val) * GELU_K * (1.0 + 3.0 * GELU_C * squared)
            pre_grad = dot(gb[rows, :], w2, ((1,), (1,))) * slope
            sums = jnp.sum(pre_grad, axis=0, keepdims=True)
            for j, u in enumerate(units):
                db_u[u, 0:1, 0:unit] += sums[:, j * unit:(j + 1) * unit]
            lowp = pre_grad.astype(BF16)
            dcs2[rows, :] = lowp
            dcs[slot, rows, columns] = lowp
            return carry

        lax.fori_loop(0, n_tiles, half_tile, 0)
        for i, (rows_of, columns_of) in enumerate(((dcs2, ab), (hs2, gb))):
            out = dot(rows_of[...], columns_of[...], ((0,), (0,)))
            for j, u in enumerate(units):
                gw[i, b, u] = out[j * unit:(j + 1) * unit]
            send_part(i)

    def relay_gather(t):
        @pl.when(t == 0)
        def _():
            relay1(1)

        @pl.when(t == 1)
        def _():
            relay1(2)
            relay2(3)

    assert n_tiles == RING
    block(0, p, hook=relay_gather)
    relay1(3)
    for t in range(1, RING):
        go(w1u(p, nth(t)), M5 + t, m_right)
    go(w2u(p, qo), M6 + 3, m_left)

    def back1(t):
        return wrap(q - gray(RING - 1 - t))

    def back2(t):
        return wrap(q + gray(RING - 1 - t))

    db_u[...] = jnp.zeros_like(db_u)
    for part in range(2):
        mine = (2 * part, 2 * part + 1)
        for t in mine:
            arrive(w2u(po, nth(t)), M4 + t)
            arrive(w1u(po, nth(t)), M3 + t)

        def send_opposite(i):
            for t in mine:
                u = nth(t)
                rc(gw.at[i, po, u], opp.at[i, u], (R2 if i else R1) + t, m_right if i else m_left).start()

        half_block(1, po, part, tuple(nth(t) for t in mine), send_opposite)
    vv[pl.ds(po, 1)] = jnp.concatenate([db_u[u, 0:1, 0:unit] for u in range(RING)], axis=1)

    for t in range(RING):
        arrive(w2u(pr, nth(t)), M6 + t)
    def send_right(i):
        if i == 0:
            rc(gw.at[0, pr], dirs.at[0], R3, m_right).start()

    block(2, pr, send_part=send_right)
    for t in range(RING):
        arrive(w1u(pl_, nth(t)), M5 + t)
    block(3, pl_)

    def direct2(t):
        u = back2(t)
        rc(gw.at[1, pl_, u], dirs.at[1, u], R4 + t, m_left).start()

    direct2(0)
    direct2(1)

    def product_tile(t, carry):
        rows = pl.ds(pl.multiple_of(t * tile, tile), tile)
        for i, (left, acc) in enumerate(((dcs, da_acc), (hs, y_acc))):
            weights = jnp.concatenate([wg[i, p].reshape(fb, width)] + [wg[i, po, nth(k)] for k in range(RING)]
                                      + [wg[i, b].reshape(fb, width) for b in (pr, pl_)], axis=0)
            out = dot(jnp.concatenate([left[slot, rows] for slot in range(RING)], axis=1), weights)
            acc[0, rows] = out[:, 0:half]
            acc[1, rows] = out[:, half:width]
        return carry

    lax.fori_loop(0, n_tiles, product_tile, 0)

    lane = lax.broadcasted_iota(jnp.int32, (tile, 128), 1)

    def stat_tile(t, carry):
        rows = pl.ds(pl.multiple_of(t * tile, tile), tile)
        mean, inv = mean_s[rows], inv_s[rows]
        v0 = da_acc[0, rows] * lnv[0, 0:1]
        v1 = da_acc[1, rows] * lnv[1, 0:1]
        h0 = (xf[0, rows].astype(F32) - mean) * inv
        h1 = (xf[1, rows].astype(F32) - mean) * inv
        one = jnp.sum(v0, axis=1, keepdims=True) + jnp.sum(v1, axis=1, keepdims=True)
        two = jnp.sum(v0 * h0, axis=1, keepdims=True) + jnp.sum(v1 * h1, axis=1, keepdims=True)
        stat[rows] = jnp.where(lane < 64, one, two)
        return carry

    rc(y_acc.at[other], yr, EY, partner).start()
    rc(da_acc.at[other], dar, ED, partner).start()
    lax.fori_loop(0, n_tiles, stat_tile, 0)
    rc(stat, statr, ES, partner).start()

    for t in range(RING):
        u1, u2 = back1(t), back2(t)
        arrive(opp.at[1, u2], R2 + (3, 2, 1, 0)[t])
        gw[1, pr, u2] += opp[1, u2]
        rc(gw.at[1, pr, u2], rel.at[1, u2], R6 + t, m_right).start()
        arrive(opp.at[0, u1], R1 + (3, 1, 2, 0)[t])
        gw[0, pl_, u1] += opp[0, u1]
        rc(gw.at[0, pl_, u1], rel.at[0, u1], R5 + t, m_left).start()
    direct2(2)
    direct2(3)

    arrive(yr, EY)
    arrive(dar, ED)
    arrive(statr, ES)
    b_down = bd_ref[...].astype(F32).reshape(1, half)

    def out_tile(t, carry):
        rows = pl.ds(pl.multiple_of(t * tile, tile), tile)
        x_own = xf[e, rows].astype(F32)
        y_ref[rows] = (x_own + (y_acc[e, rows] + yr[rows]) + b_down).astype(BF16)
        norm_grad = da_acc[e, rows] + dar[rows]
        sums = (stat[rows] + statr[rows]) / width
        inv = inv_s[rows]
        x_hat = (x_own - mean_s[rows]) * inv
        value = norm_grad * lnv[e, 0:1]
        dx_ref[rows] = (gf[e, rows].astype(F32) + inv * (value - sums[:, 0:1] - x_hat * sums[:, 64:65])).astype(BF16)
        vv[RING + 1:RING + 2] += jnp.sum(norm_grad * x_hat, axis=0, keepdims=True)
        vv[RING + 2:RING + 3] += jnp.sum(norm_grad, axis=0, keepdims=True)
        return carry

    lax.fori_loop(0, n_tiles, out_tile, 0)

    vs[q] = vv[...]
    for k, d in ((1, s_right), (2, s_opp_dev), (3, s_left)):
        go(vs.at[q], VS + k, d)
    for k in range(1, RING):
        arrive(vs.at[wrap(q - k)], VS + k)
    vm[p] = ((vs[0] + vs[1]) + vs[2]) + vs[3]
    for k, d in ((1, m_right), (2, m_opp), (3, m_left)):
        go(vm.at[p], VM + k, d)

    arrive(dirs.at[0], R3)

    def reduce1(t):
        u = back1(t)
        arrive(rel.at[0, u], R5 + t)
        gw[0, p, u] += dirs[0, u] + rel[0, u]
        if t == 0:
            rc(gw.at[0, p, u], s_opp.at[0], Q1, s_left).start()
        if t == 1:
            rc(gw.at[0, p, u], s_dir.at[0], Q3, s_right).start()
        if t == 2:
            arrive(s_opp.at[0], Q1)
            gw[0, p, u] += s_opp[0]
            rc(gw.at[0, p, u], s_rel.at[0], Q5, s_left).start()

    most, rest = pl.ds(0, 3 * unit // 4), pl.ds(3 * unit // 4, unit // 4)

    def reduce2(t):
        u = back2(t)
        arrive(dirs.at[1, u], R4 + t)
        arrive(rel.at[1, u], R6 + t)
        gw[1, p, u] += dirs[1, u] + rel[1, u]
        if t == 0:
            rc(gw.at[1, p, u, most], s_opp.at[1, most], Q2, s_right).start()
            rc(gw.at[1, p, u, rest], s_opp.at[1, rest], Q2B, s_left).start()
        if t == 1:
            rc(gw.at[1, p, u, most], s_dir.at[1, most], Q4, s_left).start()
        if t == 2:
            rc(gw.at[1, p, u, rest], s_dir.at[1, rest], Q4B, s_right).start()
            before = back2(1)
            arrive(s_opp.at[1, rest], Q2B)
            gw[1, p, before, rest] += s_opp[1, rest]
            rc(gw.at[1, p, before, rest], s_rel.at[1, rest], Q6B, s_left).start()
            arrive(s_opp.at[1, most], Q2)
            gw[1, p, u, most] += s_opp[1, most]
            rc(gw.at[1, p, u, most], s_rel.at[1, most], Q6, s_right).start()

    reduce1(0)
    reduce1(1)
    reduce2(0)
    reduce1(2)
    reduce2(1)
    reduce1(3)
    reduce2(2)

    arrive(s_dir.at[0], Q3)
    arrive(s_rel.at[0], Q5)
    done1 = gw[0, p, q] + s_dir[0] + s_rel[0]
    for k in range(RING):
        for h in range(2):
            start = (h * RING + k) * unit
            f1[k, h] = pack(done1[:, start:start + unit]).astype(BF16)
    for k in (2, 1, 3):
        for h in range(2):
            rc(f1.at[wrap(r + k), h], f1l.at[r, e], F1 + 2 * k + h,
               {"row": wrap(r + k), "col": c, "dep": h}, F1 + 2 * k + e).start()
    rc(f1.at[r, other], f1l.at[r, e], F1 + other, partner, F1 + e).start()
    f1l[r, e] = f1[r, e]
    reduce2(3)
    for k in range(1, RING):
        arrive(vm.at[wrap(p - k)], VM + k)
    vp[e] = ((vm[0] + vm[1]) + vm[2]) + vm[3]
    go(vp.at[e], VP, partner)
    arrive(s_dir.at[1, most], Q4)
    arrive(s_dir.at[1, rest], Q4B)
    arrive(s_rel.at[1, rest], Q6B)
    arrive(s_rel.at[1, most], Q6)
    done2 = (gw[1, p, q] + s_dir[1] + s_rel[1]).astype(BF16)
    f2[0] = done2[:, 0:half]
    f2[1] = done2[:, half:width]
    rc(f2.at[other], f2l.at[e], F2, partner).start()
    f2l[e] = f2[e]

    arrive(vp.at[other], VP)
    pieces = []
    for k in range(RING):
        pieces.append(vp[0, pl.ds(c, 1)][:, k * unit:(k + 1) * unit])
        row = vp[1, k:k + 1]
        piece = row[:, 0:unit]
        for j in range(1, RING):
            piece = jnp.where(c == j, row[:, j * unit:(j + 1) * unit], piece)
        pieces.append(piece)
    dbu_ref[...] = jnp.concatenate(pieces, axis=1).reshape(dbu_ref.shape)
    dbd_ref[...] = vp[e, RING:RING + 1].reshape(dbd_ref.shape)
    dsc_ref[...] = vp[e, RING + 1:RING + 2].reshape(dsc_ref.shape)
    dsh_ref[...] = vp[e, RING + 2:RING + 3].reshape(dsh_ref.shape)

    sent(l2.at[0], P2)
    sent(l1.at[0, 0], P1 + other)
    sent(l1.at[0, 0], F1 + other)
    for k in range(1, RING):
        for h in range(2):
            sent(l1.at[0, 0], P1 + 2 * k + h)
            sent(l1.at[0, 0], F1 + 2 * k + h)
        sent(bi.at[c], BI + k)
        sent(vm.at[p], VM + k)
        sent(vs.at[q], VS + k)
    sent(f2.at[0], F2)
    sent(lnv.at[0], DLN)
    sent(x_hbm, DX)
    sent(g_hbm, DG)
    for sem in (S1, S2, S3, S4, S5, S6):
        sent(w1u(p, q), sem)
    for t in range(RING):
        for sem in (M1, M2, M3, M4, M5, M6):
            sent(w1u(p, q), sem + t)
        for sem in (R1, R2, R4, R5, R6):
            sent(gw.at[0, p, q], sem + t)
    sent(gw.at[0, p], R3)
    for sem in (Q1, Q3, Q5):
        sent(gw.at[0, p, q], sem)
    for sem in (Q2, Q4, Q6):
        sent(gw.at[1, p, q, most], sem)
    for sem in (Q2B, Q4B, Q6B):
        sent(gw.at[1, p, q, rest], sem)
    sent(vp.at[e], VP)
    sent(yr, EY)
    sent(dar, ED)
    sent(stat, ES)

    arrive(f2l.at[other], F2)
    dw2_ref[0:unit] = f2l[0]
    dw2_ref[unit:2 * unit] = f2l[1]
    arrive(f1l.at[r, other], F1 + other)
    for k in range(1, RING):
        for h in range(2):
            arrive(f1l.at[wrap(r - k), h], F1 + 2 * k + h)
    turned = jnp.concatenate([unpack(f1l[k, h].astype(F32)) for k in range(RING) for h in range(2)], axis=0)
    turned = jnp.concatenate([turned, jnp.zeros((2 * fb, LANES - unit), F32)], axis=1)
    dw1_ref[...] = turned.T[0:unit].astype(BF16)


def copy_out(*refs):
    n = len(refs) // 2
    copies = [pltpu.make_async_copy(refs[i], refs[n + i], refs[2 * n].at[i]) for i in range(n)]
    for copy in copies:
        copy.start()
    for copy in copies:
        copy.wait()


def solution(mesh):
    assert mesh.shape["row"] == RING and mesh.shape["col"] == RING and mesh.shape["dep"] == 2
    tok_spec = P(("part", "row", "col"), "dep")
    vec_dep = P("dep")
    part_dep = P(("part", "dep"))
    in_specs = (tok_spec, vec_dep, vec_dep, P(("dep", "row"), "col"), P("col"), P(("col", "row"), "dep"), vec_dep, tok_spec)
    out_specs = (tok_spec, tok_spec, P(("part", "dep", "row"), "col"), P(("part", "col")), P(("part", "col", "row"), "dep"), part_dep, part_dep, part_dep)

    def local_step(x_in, ln_scale, ln_shift, w_up, b_up, w_down, b_down, y_grad):
        tokens, half = x_in.shape
        width = 2 * half
        unit = w_down.shape[0] // 2
        fb = RING * unit
        assert w_up.shape == (unit, 2 * fb) and half == RING * unit and fb == half
        tile = tokens // RING
        packed = (RING, 2, 3 * unit // 4, LANES)
        assert 3 * LANES == 4 * unit
        hbm_spec = pl.BlockSpec(memory_space=pltpu.HBM)
        vmem_spec = pl.BlockSpec(memory_space=pltpu.VMEM)
        vmem = pltpu.VMEM
        scratch = [
            vmem((unit, 2 * fb), BF16),
            vmem(packed, BF16), vmem(packed, BF16), vmem((2, unit, half), BF16),
            vmem((2, tokens, half), BF16), vmem((2, tokens, half), BF16),
            vmem((2, 8, half), F32),
            vmem((2, RING, RING, unit, width), BF16),
            vmem((RING, 8, 2 * fb), F32), vmem((RING, RING, 8, LANES), F32),
            vmem((tokens, width), BF16), vmem((tokens, width), BF16),
            vmem((tokens, 1), F32), vmem((tokens, 1), F32),
            vmem((2, tokens, half), F32), vmem((2, tokens, half), F32),
            vmem((tokens, half), F32), vmem((tokens, half), F32),
            vmem((tokens, 128), F32), vmem((tokens, 128), F32),
            vmem((RING, tokens, fb), BF16), vmem((RING, tokens, fb), BF16),
            vmem((tokens, 2 * unit), BF16), vmem((tokens, 2 * unit), BF16), vmem((RING, 8, LANES), F32),
            vmem((2, RING, RING, unit, width), F32),
            vmem((2, RING, unit, width), F32), vmem((2, RING, unit, width), F32), vmem((2, RING, unit, width), F32),
            vmem((2, unit, width), F32), vmem((2, unit, width), F32), vmem((2, unit, width), F32),
            vmem((8, half), F32), vmem((RING, 8, half), F32), vmem((RING, 8, half), F32), vmem((2, 8, half), F32),
            vmem(packed, BF16), vmem(packed, BF16),
            vmem((2, unit, half), BF16), vmem((2, unit, half), BF16),
            vmem((half,), F32), vmem((half,), F32), vmem((2 * fb,), BF16), vmem((half,), BF16),
            pltpu.SemaphoreType.DMA((N_SEM,)), pltpu.SemaphoreType.DMA((N_SEM,)),
        ]
        shapes = (
            jax.ShapeDtypeStruct((tokens, half), BF16), jax.ShapeDtypeStruct((tokens, half), BF16),
            jax.ShapeDtypeStruct(w_up.shape, BF16), jax.ShapeDtypeStruct(b_up.shape, F32),
            jax.ShapeDtypeStruct(w_down.shape, BF16), jax.ShapeDtypeStruct((half,), F32),
            jax.ShapeDtypeStruct((half,), F32), jax.ShapeDtypeStruct((half,), F32))
        outs = pl.pallas_call(
            functools.partial(kernel, tile),
            out_shape=shapes,
            in_specs=[hbm_spec] * 8,
            out_specs=(vmem_spec,) * 8,
            scratch_shapes=scratch,
            compiler_params=pltpu.CompilerParams(collective_id=0, has_side_effects=True, vmem_limit_bytes=51 * 1024 * 1024),
        )(*(pltpu.with_memory_space_constraint(v, pltpu.HBM) for v in (x_in, ln_scale, ln_shift, w_up, b_up, w_down, b_down, y_grad)))
        return pl.pallas_call(
            copy_out,
            out_shape=shapes,
            in_specs=[vmem_spec] * len(shapes),
            out_specs=(hbm_spec,) * len(shapes),
            scratch_shapes=[pltpu.SemaphoreType.DMA((len(shapes),))],
            compiler_params=pltpu.CompilerParams(vmem_limit_bytes=4 * 1024 * 1024),
        )(*outs)

    return jax.shard_map(local_step, mesh=mesh, in_specs=in_specs, out_specs=out_specs, check_vma=False)
```

```python
import functools

import jax
import jax.numpy as jnp
from jax import lax
from jax.experimental import pallas as pl
from jax.experimental.pallas import tpu as pltpu
from jax.sharding import PartitionSpec as P

LN_EPS = 1e-5
GELU_K = 0.7978845608028654
GELU_C = 0.044715
MESH = pl.DeviceIdType.MESH
F32 = jnp.float32
BF16 = jnp.bfloat16
RING = 4
LANES = 128

_next = [0]


def _ids(count=1):
    base = _next[0]
    _next[0] += count
    return base


IN_SEM = _ids(8)
P1 = _ids(2 * RING)
P2, DX, DG, DLN = _ids(), _ids(), _ids(), _ids()
BI = _ids(RING)
S1, S2, S3, S4, S5, S6 = (_ids() for _ in range(6))
M1, M2, M3, M4 = (_ids(RING) for _ in range(4))
M5, M6 = _ids(RING), _ids(RING)
R1, R2, R5, R6 = (_ids(RING) for _ in range(4))
R3, R4 = _ids(), _ids(RING)
Q1, Q2, Q3, Q4, Q5, Q6, Q1B, Q3B, Q5B = (_ids() for _ in range(9))
VM, VS = _ids(RING), _ids(RING)
VP = _ids()
EY, ED, ES = _ids(), _ids(), _ids()
F1 = _ids(2 * RING)
F2 = _ids()
N_SEM = _next[0]


def gray(t):
    return t + (t // 2) * (5 - 2 * t)


def dot(a, b, dims=((1,), (0,))):
    return lax.dot_general(a, b, (dims, ((), ())), preferred_element_type=F32)


def pack(piece):
    u = piece.shape[0]
    cut, third = 3 * u // 4, u // 3
    beside = jnp.concatenate([piece[cut:, k * third:(k + 1) * third] for k in range(3)], axis=0)
    return jnp.concatenate([piece[:cut], beside], axis=1)


def unpack(packed):
    cut = packed.shape[0]
    u = 4 * cut // 3
    quarter = u - cut
    below = jnp.concatenate([packed[k * quarter:(k + 1) * quarter, u:] for k in range(3)], axis=1)
    return jnp.concatenate([packed[:, :u], below], axis=0)


def kernel(tile, x_hbm, sc_hbm, sh_hbm, w1_hbm, bu_hbm, w2_hbm, bd_hbm, g_hbm,
           y_ref, dx_ref, dw1_ref, dbu_ref, dw2_ref, dbd_ref, dsc_ref, dsh_ref,
           w1v, st1, l1, l2, xf, gf, lnv, wg, bi, bias_u, ab, gb, mean_s, inv_s,
           y_acc, da_acc, yr, dar, stat, statr, hs, dcs, hs2, dcs2, db_u, gw, opp, dirs, rel, s_opp, s_dir, s_rel,
           vv, vm, vs, vp, f1, f1l, f2, f2l, sc_ref, sh_ref, bu_ref, bd_ref, send, recv):
    r, c, e = lax.axis_index("row"), lax.axis_index("col"), lax.axis_index("dep")
    p = c + e * (r - c)
    q = r + e * (c - r)
    tokens, half = xf.shape[1], xf.shape[2]
    width = 2 * half
    unit = l2.shape[1]
    fb = RING * unit
    n_tiles = tokens // tile
    other = 1 - e

    def wrap(v):
        return lax.rem(v + 2 * RING, RING)

    def dev(pp, qq):
        return {"row": qq + e * (pp - qq), "col": pp + e * (qq - pp), "dep": e}

    m_right, m_left, m_opp = dev(wrap(p + 1), q), dev(wrap(p - 1), q), dev(wrap(p + 2), q)
    s_right, s_left, s_opp_dev = dev(p, wrap(q + 1)), dev(p, wrap(q - 1)), dev(p, wrap(q + 2))
    partner = {"row": r, "col": c, "dep": other}
    pr, pl_, po = wrap(p + 1), wrap(p - 1), wrap(p + 2)
    qr, ql, qo = wrap(q + 1), wrap(q - 1), wrap(q + 2)

    def rc(src, dst, ssem, device, rsem=None):
        return pltpu.make_async_remote_copy(
            src_ref=src, dst_ref=dst, send_sem=send.at[ssem], recv_sem=recv.at[ssem if rsem is None else rsem],
            device_id=device, device_id_type=MESH)

    def arrive(dst, rsem):
        rc(dst, dst, rsem, partner).wait_recv()

    def sent(src, ssem):
        rc(src, src, ssem, partner).wait_send()

    def go(ref, sem, device):
        rc(ref, ref, sem, device).start()

    load_w1 = pltpu.make_async_copy(w1_hbm, w1v, recv.at[IN_SEM])
    load_w2 = pltpu.make_async_copy(w2_hbm.at[pl.ds(pl.multiple_of(e * unit, 16), unit)], l2.at[e], recv.at[IN_SEM + 1])
    load_x = pltpu.make_async_copy(x_hbm, xf.at[e], recv.at[IN_SEM + 2])
    load_g = pltpu.make_async_copy(g_hbm, gf.at[e], recv.at[IN_SEM + 3])
    load_vectors = [pltpu.make_async_copy(src, dst, recv.at[IN_SEM + 4 + i]) for i, (src, dst) in enumerate(
        ((sc_hbm, sc_ref), (sh_hbm, sh_ref), (bu_hbm, bu_ref), (bd_hbm, bd_ref)))]
    load_w1.start()
    load_w2.start()
    for load in load_vectors:
        load.start()
    load_x.start()
    load_g.start()

    barrier = pltpu.get_barrier_semaphore()
    peers = [m_right, m_left, s_right, s_left, m_opp, s_opp_dev, partner]
    peers += [{"row": wrap(r + k), "col": c, "dep": other} for k in range(1, RING)]
    for d in peers:
        pl.semaphore_signal(barrier, inc=1, device_id=d, device_id_type=MESH)

    load_w1.wait()
    turned = w1v[...].astype(F32)
    turned = jnp.concatenate([turned, jnp.zeros((LANES - unit, 2 * fb), F32)], axis=0).T
    for k in range(RING):
        for h in range(2):
            st1[k, h] = pack(turned[(2 * k + h) * unit:(2 * k + h + 1) * unit, 0:unit]).astype(BF16)

    for load in load_vectors:
        load.wait()
    lnv[e, 0:1] = sc_ref[...].reshape(1, half)
    lnv[e, 1:2] = sh_ref[...].reshape(1, half)
    bi[c] = jnp.broadcast_to(bu_ref[...].astype(F32).reshape(1, 2 * fb), (8, 2 * fb))

    pl.semaphore_wait(barrier, len(peers))

    rc(w2_hbm.at[pl.ds(pl.multiple_of(other * unit, 16), unit)], l2.at[e], P2, partner).start()
    rc(st1.at[r, other], l1.at[r, e], P1 + other, partner, P1 + e).start()
    for k in (2, 1, 3):
        for h in range(2):
            rc(st1.at[wrap(r + k), h], l1.at[r, e], P1 + 2 * k + h,
               {"row": wrap(r + k), "col": c, "dep": h}, P1 + 2 * k + e).start()
    rc(lnv.at[e], lnv.at[e], DLN, partner).start()
    rc(x_hbm, xf.at[e], DX, partner).start()
    rc(g_hbm, gf.at[e], DG, partner).start()
    for k in range(1, RING):
        rc(bi.at[c], bi.at[c], BI + k, {"row": r, "col": wrap(c + k), "dep": e}).start()
    l1[r, e] = st1[r, e]

    def w1u(b, s):
        return wg.at[0, b, s]

    def w2u(b, s):
        return wg.at[1, b, s]

    load_w2.wait()
    arrive(l2.at[other], P2)
    wg[1, p, q, :, 0:half] = l2[0]
    wg[1, p, q, :, half:width] = l2[1]
    go(w2u(p, q), M2, m_right)
    go(w2u(p, q), S2, s_right)
    go(w2u(p, q), S4, s_left)
    go(w2u(p, q), M6, m_left)

    arrive(l1.at[r, other], P1 + other)
    for k in range(1, RING):
        for h in range(2):
            arrive(l1.at[wrap(r - k), h], P1 + 2 * k + h)
    wg[0, p, q] = jnp.concatenate([unpack(l1[k, h].astype(F32)) for h in range(2) for k in range(RING)], axis=1).astype(BF16)
    go(w1u(p, q), M1, m_left)
    go(w1u(p, q), S1, s_right)
    go(w1u(p, q), S3, s_left)
    go(w1u(p, q), M5, m_right)

    arrive(w2u(p, ql), S2)
    go(w2u(p, ql), S6, s_right)
    arrive(w2u(p, qr), S4)
    go(w2u(p, qr), M2 + 1, m_right)
    go(w2u(p, ql), M2 + 2, m_right)
    go(w2u(p, qr), M6 + 1, m_left)
    go(w2u(p, ql), M6 + 2, m_left)

    def nth(t):
        return wrap(q + gray(t))

    arrive(lnv.at[other], DLN)
    load_x.wait()
    arrive(xf.at[other], DX)
    load_g.wait()
    arrive(gf.at[other], DG)
    vv[...] = jnp.zeros_like(vv)
    def norm_tile(t, carry):
        rows = pl.ds(pl.multiple_of(t * tile, tile), tile)
        x0, x1 = xf[0, rows].astype(F32), xf[1, rows].astype(F32)
        total = jnp.sum(x0, axis=1, keepdims=True) + jnp.sum(x1, axis=1, keepdims=True)
        squares = jnp.sum(x0 * x0, axis=1, keepdims=True) + jnp.sum(x1 * x1, axis=1, keepdims=True)
        mean = total / width
        inv = lax.rsqrt(squares / width - mean * mean + LN_EPS)
        mean_s[rows] = mean
        inv_s[rows] = inv
        ab[rows, 0:half] = ((x0 - mean) * inv * lnv[0, 0:1] + lnv[0, 1:2]).astype(BF16)
        ab[rows, half:width] = ((x1 - mean) * inv * lnv[1, 0:1] + lnv[1, 1:2]).astype(BF16)
        gb[rows, 0:half] = gf[0, rows]
        gb[rows, half:width] = gf[1, rows]
        vv[RING:RING + 1] += jnp.sum(gf[e, rows].astype(F32), axis=0, keepdims=True)
        return carry

    lax.fori_loop(0, n_tiles // 2, norm_tile, 0)
    arrive(w1u(p, qr), S3)
    go(w1u(p, qr), S5, s_left)
    go(w1u(p, qr), M1 + 1, m_left)
    lax.fori_loop(n_tiles // 2, n_tiles, norm_tile, 0)

    def relay1(t):
        arrive(w1u(pr, nth(t)), M1 + t)
        go(w1u(pr, nth(t)), M3 + t, m_left)

    def relay2(t):
        arrive(w2u(pl_, nth(t)), M2 + t)
        go(w2u(pl_, nth(t)), M4 + t, m_right)

    arrive(w1u(p, ql), S1)
    go(w1u(p, ql), M1 + 2, m_left)
    relay2(0)
    for k in range(1, RING):
        arrive(bi.at[wrap(c - k)], BI + k)
    for b in range(RING):
        for k in range(RING):
            flat = bi[b, 0:1, 2 * k * unit:(2 * k + 1) * unit]
            across = bi[k, 0:1, (2 * b + 1) * unit:(2 * b + 2) * unit]
            bias_u[b, k, 0:1, 0:unit] = jnp.where(e == 0, flat, across)
    arrive(w2u(p, qo), S6)
    go(w2u(p, qo), M2 + 3, m_right)
    relay1(0)
    relay2(1)
    arrive(w1u(p, qo), S5)
    go(w1u(p, qo), M1 + 3, m_left)
    relay2(2)

    def block(slot, b, hook=None, send_part=None):
        bias = jnp.concatenate([bias_u[b, u, 0:1, 0:unit] for u in range(RING)], axis=1)

        def block_tile(t, carry):
            rows = pl.ds(pl.multiple_of(t * tile, tile), tile)
            pre = dot(ab[rows, :], wg[0, b].reshape(fb, width), ((1,), (1,))) + bias
            squared = pre * pre
            tanh_val = jnp.tanh(GELU_K * (pre + GELU_C * pre * squared))
            hs[slot, rows] = (0.5 * pre * (1.0 + tanh_val)).astype(BF16)
            slope = 0.5 * (1.0 + tanh_val) + 0.5 * pre * (1.0 - tanh_val * tanh_val) * GELU_K * (1.0 + 3.0 * GELU_C * squared)
            pre_grad = dot(gb[rows, :], wg[1, b].reshape(fb, width), ((1,), (1,))) * slope
            vv[pl.ds(b, 1)] += jnp.sum(pre_grad, axis=0, keepdims=True)
            dcs[slot, rows] = pre_grad.astype(BF16)
            if hook is not None:
                hook(t)
            return carry

        lax.fori_loop(0, n_tiles, block_tile, 0)
        for i, (rows_of, columns_of) in enumerate(((dcs, ab), (hs, gb))):
            gw[i, b] = dot(rows_of[slot], columns_of[...], ((0,), (0,))).reshape(RING, unit, width)
            if send_part is not None:
                send_part(i)

    def half_block(slot, b, part, units, send_part):
        bias = jnp.concatenate([bias_u[b, u, 0:1, 0:unit] for u in units], axis=1)
        columns = slice(2 * part * unit, 2 * (part + 1) * unit)

        def half_tile(t, carry):
            rows = pl.ds(pl.multiple_of(t * tile, tile), tile)
            w1, w2 = (jnp.concatenate([wg[i, b, u] for u in units], axis=0) for i in range(2))
            pre = dot(ab[rows, :], w1, ((1,), (1,))) + bias
            squared = pre * pre
            tanh_val = jnp.tanh(GELU_K * (pre + GELU_C * pre * squared))
            hidden = (0.5 * pre * (1.0 + tanh_val)).astype(BF16)
            hs2[rows, :] = hidden
            hs[slot, rows, columns] = hidden
            slope = 0.5 * (1.0 + tanh_val) + 0.5 * pre * (1.0 - tanh_val * tanh_val) * GELU_K * (1.0 + 3.0 * GELU_C * squared)
            pre_grad = dot(gb[rows, :], w2, ((1,), (1,))) * slope
            sums = jnp.sum(pre_grad, axis=0, keepdims=True)
            for j, u in enumerate(units):
                db_u[u, 0:1, 0:unit] += sums[:, j * unit:(j + 1) * unit]
            lowp = pre_grad.astype(BF16)
            dcs2[rows, :] = lowp
            dcs[slot, rows, columns] = lowp
            return carry

        lax.fori_loop(0, n_tiles, half_tile, 0)
        for i, (rows_of, columns_of) in enumerate(((dcs2, ab), (hs2, gb))):
            out = dot(rows_of[...], columns_of[...], ((0,), (0,)))
            for j, u in enumerate(units):
                gw[i, b, u] = out[j * unit:(j + 1) * unit]
            send_part(i)

    def relay_gather(t):
        @pl.when(t == 0)
        def _():
            relay1(1)

        @pl.when(t == 1)
        def _():
            relay1(2)
            relay2(3)

    assert n_tiles == RING
    block(0, p, hook=relay_gather)
    relay1(3)
    for t in range(1, RING):
        go(w1u(p, nth(t)), M5 + t, m_right)
    go(w2u(p, qo), M6 + 3, m_left)

    def back1(t):
        return wrap(q - gray(RING - 1 - t))

    def back2(t):
        return wrap(q + gray(RING - 1 - t))

    db_u[...] = jnp.zeros_like(db_u)
    for part in range(2):
        mine = (2 * part, 2 * part + 1)
        for t in mine:
            arrive(w2u(po, nth(t)), M4 + t)
            arrive(w1u(po, nth(t)), M3 + t)

        def send_opposite(i):
            for t in mine:
                u = nth(t)
                rc(gw.at[i, po, u], opp.at[i, u], (R2 if i else R1) + t, m_right if i else m_left).start()

        half_block(1, po, part, tuple(nth(t) for t in mine), send_opposite)
    vv[pl.ds(po, 1)] = jnp.concatenate([db_u[u, 0:1, 0:unit] for u in range(RING)], axis=1)

    for t in range(RING):
        arrive(w2u(pr, nth(t)), M6 + t)
    def send_right(i):
        if i == 0:
            rc(gw.at[0, pr], dirs.at[0], R3, m_right).start()

    block(2, pr, send_part=send_right)
    for t in range(RING):
        arrive(w1u(pl_, nth(t)), M5 + t)
    block(3, pl_)

    def direct2(t):
        u = back2(t)
        rc(gw.at[1, pl_, u], dirs.at[1, u], R4 + t, m_left).start()

    direct2(0)
    direct2(1)

    def product_tile(t, carry):
        rows = pl.ds(pl.multiple_of(t * tile, tile), tile)
        for i, (left, acc) in enumerate(((dcs, da_acc), (hs, y_acc))):
            weights = jnp.concatenate([wg[i, p].reshape(fb, width)] + [wg[i, po, nth(k)] for k in range(RING)]
                                      + [wg[i, b].reshape(fb, width) for b in (pr, pl_)], axis=0)
            out = dot(jnp.concatenate([left[slot, rows] for slot in range(RING)], axis=1), weights)
            acc[0, rows] = out[:, 0:half]
            acc[1, rows] = out[:, half:width]
        return carry

    lax.fori_loop(0, n_tiles, product_tile, 0)

    lane = lax.broadcasted_iota(jnp.int32, (tile, 128), 1)

    def stat_tile(t, carry):
        rows = pl.ds(pl.multiple_of(t * tile, tile), tile)
        mean, inv = mean_s[rows], inv_s[rows]
        v0 = da_acc[0, rows] * lnv[0, 0:1]
        v1 = da_acc[1, rows] * lnv[1, 0:1]
        h0 = (xf[0, rows].astype(F32) - mean) * inv
        h1 = (xf[1, rows].astype(F32) - mean) * inv
        one = jnp.sum(v0, axis=1, keepdims=True) + jnp.sum(v1, axis=1, keepdims=True)
        two = jnp.sum(v0 * h0, axis=1, keepdims=True) + jnp.sum(v1 * h1, axis=1, keepdims=True)
        stat[rows] = jnp.where(lane < 64, one, two)
        return carry

    rc(y_acc.at[other], yr, EY, partner).start()
    rc(da_acc.at[other], dar, ED, partner).start()
    lax.fori_loop(0, n_tiles, stat_tile, 0)
    rc(stat, statr, ES, partner).start()

    for t in range(RING):
        u1, u2 = back1(t), back2(t)
        arrive(opp.at[1, u2], R2 + (3, 2, 1, 0)[t])
        gw[1, pr, u2] += opp[1, u2]
        rc(gw.at[1, pr, u2], rel.at[1, u2], R6 + t, m_right).start()
        arrive(opp.at[0, u1], R1 + (3, 1, 2, 0)[t])
        gw[0, pl_, u1] += opp[0, u1]
        rc(gw.at[0, pl_, u1], rel.at[0, u1], R5 + t, m_left).start()
    direct2(2)
    direct2(3)

    arrive(yr, EY)
    arrive(dar, ED)
    arrive(statr, ES)
    b_down = bd_ref[...].astype(F32).reshape(1, half)

    def out_tile(t, carry):
        rows = pl.ds(pl.multiple_of(t * tile, tile), tile)
        x_own = xf[e, rows].astype(F32)
        y_ref[rows] = (x_own + (y_acc[e, rows] + yr[rows]) + b_down).astype(BF16)
        norm_grad = da_acc[e, rows] + dar[rows]
        sums = (stat[rows] + statr[rows]) / width
        inv = inv_s[rows]
        x_hat = (x_own - mean_s[rows]) * inv
        value = norm_grad * lnv[e, 0:1]
        dx_ref[rows] = (gf[e, rows].astype(F32) + inv * (value - sums[:, 0:1] - x_hat * sums[:, 64:65])).astype(BF16)
        vv[RING + 1:RING + 2] += jnp.sum(norm_grad * x_hat, axis=0, keepdims=True)
        vv[RING + 2:RING + 3] += jnp.sum(norm_grad, axis=0, keepdims=True)
        return carry

    lax.fori_loop(0, n_tiles, out_tile, 0)

    vs[q] = vv[...]
    for k, d in ((1, s_right), (2, s_opp_dev), (3, s_left)):
        go(vs.at[q], VS + k, d)
    for k in range(1, RING):
        arrive(vs.at[wrap(q - k)], VS + k)
    vm[p] = ((vs[0] + vs[1]) + vs[2]) + vs[3]
    for k, d in ((1, m_right), (2, m_opp), (3, m_left)):
        go(vm.at[p], VM + k, d)

    arrive(dirs.at[0], R3)

    most, rest = pl.ds(0, 3 * unit // 4), pl.ds(3 * unit // 4, unit // 4)

    def reduce1(t):
        u = back1(t)
        arrive(rel.at[0, u], R5 + t)
        gw[0, p, u] += dirs[0, u] + rel[0, u]
        if t == 0:
            rc(gw.at[0, p, u, most], s_opp.at[0, most], Q1, s_left).start()
            rc(gw.at[0, p, u, rest], s_opp.at[0, rest], Q1B, s_right).start()
        if t == 1:
            rc(gw.at[0, p, u, most], s_dir.at[0, most], Q3, s_right).start()
        if t == 2:
            rc(gw.at[0, p, u, rest], s_dir.at[0, rest], Q3B, s_left).start()
            before = back1(1)
            arrive(s_opp.at[0, rest], Q1B)
            gw[0, p, before, rest] += s_opp[0, rest]
            rc(gw.at[0, p, before, rest], s_rel.at[0, rest], Q5B, s_right).start()
            arrive(s_opp.at[0, most], Q1)
            gw[0, p, u, most] += s_opp[0, most]
            rc(gw.at[0, p, u, most], s_rel.at[0, most], Q5, s_left).start()

    def reduce2(t):
        u = back2(t)
        arrive(dirs.at[1, u], R4 + t)
        arrive(rel.at[1, u], R6 + t)
        gw[1, p, u] += dirs[1, u] + rel[1, u]
        if t == 0:
            rc(gw.at[1, p, u], s_opp.at[1], Q2, s_right).start()
        if t == 1:
            rc(gw.at[1, p, u], s_dir.at[1], Q4, s_left).start()
        if t == 2:
            arrive(s_opp.at[1], Q2)
            gw[1, p, u] += s_opp[1]
            rc(gw.at[1, p, u], s_rel.at[1], Q6, s_right).start()

    reduce1(0)
    reduce1(1)
    reduce2(0)
    reduce1(2)
    reduce2(1)
    reduce1(3)
    reduce2(2)

    arrive(s_dir.at[0, most], Q3)
    arrive(s_dir.at[0, rest], Q3B)
    arrive(s_rel.at[0, rest], Q5B)
    arrive(s_rel.at[0, most], Q5)
    done1 = gw[0, p, q] + s_dir[0] + s_rel[0]
    for k in range(RING):
        for h in range(2):
            start = (h * RING + k) * unit
            f1[k, h] = pack(done1[:, start:start + unit]).astype(BF16)
    for k in (2, 1, 3):
        for h in range(2):
            rc(f1.at[wrap(r + k), h], f1l.at[r, e], F1 + 2 * k + h,
               {"row": wrap(r + k), "col": c, "dep": h}, F1 + 2 * k + e).start()
    rc(f1.at[r, other], f1l.at[r, e], F1 + other, partner, F1 + e).start()
    f1l[r, e] = f1[r, e]
    reduce2(3)
    for k in range(1, RING):
        arrive(vm.at[wrap(p - k)], VM + k)
    vp[e] = ((vm[0] + vm[1]) + vm[2]) + vm[3]
    go(vp.at[e], VP, partner)
    arrive(s_dir.at[1], Q4)
    arrive(s_rel.at[1], Q6)
    done2 = (gw[1, p, q] + s_dir[1] + s_rel[1]).astype(BF16)
    f2[0] = done2[:, 0:half]
    f2[1] = done2[:, half:width]
    rc(f2.at[other], f2l.at[e], F2, partner).start()
    f2l[e] = f2[e]

    arrive(vp.at[other], VP)
    pieces = []
    for k in range(RING):
        pieces.append(vp[0, pl.ds(c, 1)][:, k * unit:(k + 1) * unit])
        row = vp[1, k:k + 1]
        piece = row[:, 0:unit]
        for j in range(1, RING):
            piece = jnp.where(c == j, row[:, j * unit:(j + 1) * unit], piece)
        pieces.append(piece)
    dbu_ref[...] = jnp.concatenate(pieces, axis=1).reshape(dbu_ref.shape)
    dbd_ref[...] = vp[e, RING:RING + 1].reshape(dbd_ref.shape)
    dsc_ref[...] = vp[e, RING + 1:RING + 2].reshape(dsc_ref.shape)
    dsh_ref[...] = vp[e, RING + 2:RING + 3].reshape(dsh_ref.shape)

    sent(l2.at[0], P2)
    sent(l1.at[0, 0], P1 + other)
    sent(l1.at[0, 0], F1 + other)
    for k in range(1, RING):
        for h in range(2):
            sent(l1.at[0, 0], P1 + 2 * k + h)
            sent(l1.at[0, 0], F1 + 2 * k + h)
        sent(bi.at[c], BI + k)
        sent(vm.at[p], VM + k)
        sent(vs.at[q], VS + k)
    sent(f2.at[0], F2)
    sent(lnv.at[0], DLN)
    sent(x_hbm, DX)
    sent(g_hbm, DG)
    for sem in (S1, S2, S3, S4, S5, S6):
        sent(w1u(p, q), sem)
    for t in range(RING):
        for sem in (M1, M2, M3, M4, M5, M6):
            sent(w1u(p, q), sem + t)
        for sem in (R1, R2, R4, R5, R6):
            sent(gw.at[0, p, q], sem + t)
    sent(gw.at[0, p], R3)
    for sem in (Q2, Q4, Q6):
        sent(gw.at[1, p, q], sem)
    for sem in (Q1, Q3, Q5):
        sent(gw.at[0, p, q, most], sem)
    for sem in (Q1B, Q3B, Q5B):
        sent(gw.at[0, p, q, rest], sem)
    sent(vp.at[e], VP)
    sent(yr, EY)
    sent(dar, ED)
    sent(stat, ES)

    arrive(f2l.at[other], F2)
    dw2_ref[0:unit] = f2l[0]
    dw2_ref[unit:2 * unit] = f2l[1]
    arrive(f1l.at[r, other], F1 + other)
    for k in range(1, RING):
        for h in range(2):
            arrive(f1l.at[wrap(r - k), h], F1 + 2 * k + h)
    turned = jnp.concatenate([unpack(f1l[k, h].astype(F32)) for k in range(RING) for h in range(2)], axis=0)
    turned = jnp.concatenate([turned, jnp.zeros((2 * fb, LANES - unit), F32)], axis=1)
    dw1_ref[...] = turned.T[0:unit].astype(BF16)


def copy_out(*refs):
    n = len(refs) // 2
    copies = [pltpu.make_async_copy(refs[i], refs[n + i], refs[2 * n].at[i]) for i in range(n)]
    for copy in copies:
        copy.start()
    for copy in copies:
        copy.wait()


def solution(mesh):
    assert mesh.shape["row"] == RING and mesh.shape["col"] == RING and mesh.shape["dep"] == 2
    tok_spec = P(("part", "row", "col"), "dep")
    vec_dep = P("dep")
    part_dep = P(("part", "dep"))
    in_specs = (tok_spec, vec_dep, vec_dep, P(("dep", "row"), "col"), P("col"), P(("col", "row"), "dep"), vec_dep, tok_spec)
    out_specs = (tok_spec, tok_spec, P(("part", "dep", "row"), "col"), P(("part", "col")), P(("part", "col", "row"), "dep"), part_dep, part_dep, part_dep)

    def local_step(x_in, ln_scale, ln_shift, w_up, b_up, w_down, b_down, y_grad):
        tokens, half = x_in.shape
        width = 2 * half
        unit = w_down.shape[0] // 2
        fb = RING * unit
        assert w_up.shape == (unit, 2 * fb) and half == RING * unit and fb == half
        tile = tokens // RING
        packed = (RING, 2, 3 * unit // 4, LANES)
        assert 3 * LANES == 4 * unit
        hbm_spec = pl.BlockSpec(memory_space=pltpu.HBM)
        vmem_spec = pl.BlockSpec(memory_space=pltpu.VMEM)
        vmem = pltpu.VMEM
        scratch = [
            vmem((unit, 2 * fb), BF16),
            vmem(packed, BF16), vmem(packed, BF16), vmem((2, unit, half), BF16),
            vmem((2, tokens, half), BF16), vmem((2, tokens, half), BF16),
            vmem((2, 8, half), F32),
            vmem((2, RING, RING, unit, width), BF16),
            vmem((RING, 8, 2 * fb), F32), vmem((RING, RING, 8, LANES), F32),
            vmem((tokens, width), BF16), vmem((tokens, width), BF16),
            vmem((tokens, 1), F32), vmem((tokens, 1), F32),
            vmem((2, tokens, half), F32), vmem((2, tokens, half), F32),
            vmem((tokens, half), F32), vmem((tokens, half), F32),
            vmem((tokens, 128), F32), vmem((tokens, 128), F32),
            vmem((RING, tokens, fb), BF16), vmem((RING, tokens, fb), BF16),
            vmem((tokens, 2 * unit), BF16), vmem((tokens, 2 * unit), BF16), vmem((RING, 8, LANES), F32),
            vmem((2, RING, RING, unit, width), F32),
            vmem((2, RING, unit, width), F32), vmem((2, RING, unit, width), F32), vmem((2, RING, unit, width), F32),
            vmem((2, unit, width), F32), vmem((2, unit, width), F32), vmem((2, unit, width), F32),
            vmem((8, half), F32), vmem((RING, 8, half), F32), vmem((RING, 8, half), F32), vmem((2, 8, half), F32),
            vmem(packed, BF16), vmem(packed, BF16),
            vmem((2, unit, half), BF16), vmem((2, unit, half), BF16),
            vmem((half,), F32), vmem((half,), F32), vmem((2 * fb,), BF16), vmem((half,), BF16),
            pltpu.SemaphoreType.DMA((N_SEM,)), pltpu.SemaphoreType.DMA((N_SEM,)),
        ]
        shapes = (
            jax.ShapeDtypeStruct((tokens, half), BF16), jax.ShapeDtypeStruct((tokens, half), BF16),
            jax.ShapeDtypeStruct(w_up.shape, BF16), jax.ShapeDtypeStruct(b_up.shape, F32),
            jax.ShapeDtypeStruct(w_down.shape, BF16), jax.ShapeDtypeStruct((half,), F32),
            jax.ShapeDtypeStruct((half,), F32), jax.ShapeDtypeStruct((half,), F32))
        outs = pl.pallas_call(
            functools.partial(kernel, tile),
            out_shape=shapes,
            in_specs=[hbm_spec] * 8,
            out_specs=(vmem_spec,) * 8,
            scratch_shapes=scratch,
            compiler_params=pltpu.CompilerParams(collective_id=0, has_side_effects=True, vmem_limit_bytes=51 * 1024 * 1024),
        )(*(pltpu.with_memory_space_constraint(v, pltpu.HBM) for v in (x_in, ln_scale, ln_shift, w_up, b_up, w_down, b_down, y_grad)))
        return pl.pallas_call(
            copy_out,
            out_shape=shapes,
            in_specs=[vmem_spec] * len(shapes),
            out_specs=(hbm_spec,) * len(shapes),
            scratch_shapes=[pltpu.SemaphoreType.DMA((len(shapes),))],
            compiler_params=pltpu.CompilerParams(vmem_limit_bytes=4 * 1024 * 1024),
        )(*outs)

    return jax.shard_map(local_step, mesh=mesh, in_specs=in_specs, out_specs=out_specs, check_vma=False)
```

```python
import functools

import jax
import jax.numpy as jnp
from jax import lax
from jax.experimental import pallas as pl
from jax.experimental.pallas import tpu as pltpu
from jax.sharding import PartitionSpec as P

LN_EPS = 1e-5
GELU_K = 0.7978845608028654
GELU_C = 0.044715
MESH = pl.DeviceIdType.MESH
F32 = jnp.float32
BF16 = jnp.bfloat16
RING = 4
LANES = 128

_next = [0]


def _ids(count=1):
    base = _next[0]
    _next[0] += count
    return base


IN_SEM = _ids(8)
P1 = _ids(2 * RING)
P2, DX, DG, DLN = _ids(), _ids(), _ids(), _ids()
BI = _ids(RING)
S1, S2, S3, S4, S5, S6 = (_ids() for _ in range(6))
M1, M2, M3, M4 = (_ids(RING) for _ in range(4))
M5, M6 = _ids(RING), _ids(RING)
R1, R2, R5, R6 = (_ids(RING) for _ in range(4))
R3, R4 = _ids(), _ids(RING)
Q1, Q2, Q3, Q4, Q5, Q6 = (_ids() for _ in range(6))
VM, VS = _ids(RING), _ids(RING)
VP = _ids()
EY, ED, ES = _ids(), _ids(), _ids()
F1 = _ids(2 * RING)
F2 = _ids()
N_SEM = _next[0]


def gray(t):
    return t + (t // 2) * (5 - 2 * t)


def dot(a, b, dims=((1,), (0,))):
    return lax.dot_general(a, b, (dims, ((), ())), preferred_element_type=F32)


def pack(piece):
    u = piece.shape[0]
    cut, third = 3 * u // 4, u // 3
    beside = jnp.concatenate([piece[cut:, k * third:(k + 1) * third] for k in range(3)], axis=0)
    return jnp.concatenate([piece[:cut], beside], axis=1)


def unpack(packed):
    cut = packed.shape[0]
    u = 4 * cut // 3
    quarter = u - cut
    below = jnp.concatenate([packed[k * quarter:(k + 1) * quarter, u:] for k in range(3)], axis=1)
    return jnp.concatenate([packed[:, :u], below], axis=0)


def kernel(tile, x_hbm, sc_hbm, sh_hbm, w1_hbm, bu_hbm, w2_hbm, bd_hbm, g_hbm,
           y_ref, dx_ref, dw1_ref, dbu_ref, dw2_ref, dbd_ref, dsc_ref, dsh_ref,
           w1v, st1, l1, l2, xf, gf, lnv, wg, bi, bias_u, ab, gb, mean_s, inv_s,
           y_acc, da_acc, yr, dar, stat, statr, hs, dcs, hs2, dcs2, db_u, gw, opp, dirs, rel, s_opp, s_dir, s_rel,
           vv, vm, vs, vp, f1, f1l, f2, f2l, sc_ref, sh_ref, bu_ref, bd_ref, send, recv):
    r, c, e = lax.axis_index("row"), lax.axis_index("col"), lax.axis_index("dep")
    p = c + e * (r - c)
    q = r + e * (c - r)
    tokens, half = xf.shape[1], xf.shape[2]
    width = 2 * half
    unit = l2.shape[1]
    fb = RING * unit
    n_tiles = tokens // tile
    other = 1 - e

    def wrap(v):
        return lax.rem(v + 2 * RING, RING)

    def dev(pp, qq):
        return {"row": qq + e * (pp - qq), "col": pp + e * (qq - pp), "dep": e}

    m_right, m_left, m_opp = dev(wrap(p + 1), q), dev(wrap(p - 1), q), dev(wrap(p + 2), q)
    s_right, s_left, s_opp_dev = dev(p, wrap(q + 1)), dev(p, wrap(q - 1)), dev(p, wrap(q + 2))
    partner = {"row": r, "col": c, "dep": other}
    pr, pl_, po = wrap(p + 1), wrap(p - 1), wrap(p + 2)
    qr, ql, qo = wrap(q + 1), wrap(q - 1), wrap(q + 2)

    def rc(src, dst, ssem, device, rsem=None):
        return pltpu.make_async_remote_copy(
            src_ref=src, dst_ref=dst, send_sem=send.at[ssem], recv_sem=recv.at[ssem if rsem is None else rsem],
            device_id=device, device_id_type=MESH)

    def arrive(dst, rsem):
        rc(dst, dst, rsem, partner).wait_recv()

    def sent(src, ssem):
        rc(src, src, ssem, partner).wait_send()

    def go(ref, sem, device):
        rc(ref, ref, sem, device).start()

    load_w1 = pltpu.make_async_copy(w1_hbm, w1v, recv.at[IN_SEM])
    load_w2 = pltpu.make_async_copy(w2_hbm.at[pl.ds(pl.multiple_of(e * unit, 16), unit)], l2.at[e], recv.at[IN_SEM + 1])
    load_x = pltpu.make_async_copy(x_hbm, xf.at[e], recv.at[IN_SEM + 2])
    load_g = pltpu.make_async_copy(g_hbm, gf.at[e], recv.at[IN_SEM + 3])
    load_vectors = [pltpu.make_async_copy(src, dst, recv.at[IN_SEM + 4 + i]) for i, (src, dst) in enumerate(
        ((sc_hbm, sc_ref), (sh_hbm, sh_ref), (bu_hbm, bu_ref), (bd_hbm, bd_ref)))]
    load_w1.start()
    load_w2.start()
    for load in load_vectors:
        load.start()
    load_x.start()
    load_g.start()

    barrier = pltpu.get_barrier_semaphore()
    peers = [m_right, m_left, s_right, s_left, m_opp, s_opp_dev, partner]
    peers += [{"row": wrap(r + k), "col": c, "dep": other} for k in range(1, RING)]
    for d in peers:
        pl.semaphore_signal(barrier, inc=1, device_id=d, device_id_type=MESH)

    load_w1.wait()
    turned = w1v[...].astype(F32)
    turned = jnp.concatenate([turned, jnp.zeros((LANES - unit, 2 * fb), F32)], axis=0).T
    for k in range(RING):
        for h in range(2):
            st1[k, h] = pack(turned[(2 * k + h) * unit:(2 * k + h + 1) * unit, 0:unit]).astype(BF16)

    for load in load_vectors:
        load.wait()
    lnv[e, 0:1] = sc_ref[...].reshape(1, half)
    lnv[e, 1:2] = sh_ref[...].reshape(1, half)
    bi[c] = jnp.broadcast_to(bu_ref[...].astype(F32).reshape(1, 2 * fb), (8, 2 * fb))

    pl.semaphore_wait(barrier, len(peers))

    rc(w2_hbm.at[pl.ds(pl.multiple_of(other * unit, 16), unit)], l2.at[e], P2, partner).start()
    rc(st1.at[r, other], l1.at[r, e], P1 + other, partner, P1 + e).start()
    for k in (2, 1, 3):
        for h in range(2):
            rc(st1.at[wrap(r + k), h], l1.at[r, e], P1 + 2 * k + h,
               {"row": wrap(r + k), "col": c, "dep": h}, P1 + 2 * k + e).start()
    rc(lnv.at[e], lnv.at[e], DLN, partner).start()
    rc(x_hbm, xf.at[e], DX, partner).start()
    rc(g_hbm, gf.at[e], DG, partner).start()
    for k in range(1, RING):
        rc(bi.at[c], bi.at[c], BI + k, {"row": r, "col": wrap(c + k), "dep": e}).start()
    l1[r, e] = st1[r, e]

    def w1u(b, s):
        return wg.at[0, b, s]

    def w2u(b, s):
        return wg.at[1, b, s]

    load_w2.wait()
    arrive(l2.at[other], P2)
    wg[1, p, q, :, 0:half] = l2[0]
    wg[1, p, q, :, half:width] = l2[1]
    go(w2u(p, q), M2, m_right)
    go(w2u(p, q), S2, s_right)
    go(w2u(p, q), S4, s_left)
    go(w2u(p, q), M6, m_left)

    arrive(l1.at[r, other], P1 + other)
    for k in range(1, RING):
        for h in range(2):
            arrive(l1.at[wrap(r - k), h], P1 + 2 * k + h)
    wg[0, p, q] = jnp.concatenate([unpack(l1[k, h].astype(F32)) for h in range(2) for k in range(RING)], axis=1).astype(BF16)
    go(w1u(p, q), M1, m_left)
    go(w1u(p, q), S1, s_right)
    go(w1u(p, q), S3, s_left)
    go(w1u(p, q), M5, m_right)

    arrive(w2u(p, ql), S2)
    go(w2u(p, ql), S6, s_right)
    arrive(w2u(p, qr), S4)
    go(w2u(p, qr), M2 + 1, m_right)
    go(w2u(p, ql), M2 + 2, m_right)
    go(w2u(p, qr), M6 + 1, m_left)
    go(w2u(p, ql), M6 + 2, m_left)

    def nth(t):
        return wrap(q + gray(t))

    arrive(lnv.at[other], DLN)
    load_x.wait()
    arrive(xf.at[other], DX)
    load_g.wait()
    arrive(gf.at[other], DG)
    vv[...] = jnp.zeros_like(vv)
    def norm_tile(t, carry):
        rows = pl.ds(pl.multiple_of(t * tile, tile), tile)
        x0, x1 = xf[0, rows].astype(F32), xf[1, rows].astype(F32)
        total = jnp.sum(x0, axis=1, keepdims=True) + jnp.sum(x1, axis=1, keepdims=True)
        squares = jnp.sum(x0 * x0, axis=1, keepdims=True) + jnp.sum(x1 * x1, axis=1, keepdims=True)
        mean = total / width
        inv = lax.rsqrt(squares / width - mean * mean + LN_EPS)
        mean_s[rows] = mean
        inv_s[rows] = inv
        ab[rows, 0:half] = ((x0 - mean) * inv * lnv[0, 0:1] + lnv[0, 1:2]).astype(BF16)
        ab[rows, half:width] = ((x1 - mean) * inv * lnv[1, 0:1] + lnv[1, 1:2]).astype(BF16)
        gb[rows, 0:half] = gf[0, rows]
        gb[rows, half:width] = gf[1, rows]
        vv[RING:RING + 1] += jnp.sum(gf[e, rows].astype(F32), axis=0, keepdims=True)
        return carry

    lax.fori_loop(0, n_tiles // 2, norm_tile, 0)
    arrive(w1u(p, qr), S3)
    go(w1u(p, qr), S5, s_left)
    go(w1u(p, qr), M1 + 1, m_left)
    lax.fori_loop(n_tiles // 2, n_tiles, norm_tile, 0)

    def relay1(t):
        arrive(w1u(pr, nth(t)), M1 + t)
        go(w1u(pr, nth(t)), M3 + t, m_left)

    def relay2(t):
        arrive(w2u(pl_, nth(t)), M2 + t)
        go(w2u(pl_, nth(t)), M4 + t, m_right)

    arrive(w1u(p, ql), S1)
    go(w1u(p, ql), M1 + 2, m_left)
    relay2(0)
    for k in range(1, RING):
        arrive(bi.at[wrap(c - k)], BI + k)
    for b in range(RING):
        for k in range(RING):
            flat = bi[b, 0:1, 2 * k * unit:(2 * k + 1) * unit]
            across = bi[k, 0:1, (2 * b + 1) * unit:(2 * b + 2) * unit]
            bias_u[b, k, 0:1, 0:unit] = jnp.where(e == 0, flat, across)
    arrive(w2u(p, qo), S6)
    go(w2u(p, qo), M2 + 3, m_right)
    relay1(0)
    relay2(1)
    arrive(w1u(p, qo), S5)
    go(w1u(p, qo), M1 + 3, m_left)
    relay2(2)

    def block(slot, b, hook=None, send_part=None):
        bias = jnp.concatenate([bias_u[b, u, 0:1, 0:unit] for u in range(RING)], axis=1)

        def block_tile(t, carry):
            rows = pl.ds(pl.multiple_of(t * tile, tile), tile)
            pre = dot(ab[rows, :], wg[0, b].reshape(fb, width), ((1,), (1,))) + bias
            squared = pre * pre
            tanh_val = jnp.tanh(GELU_K * (pre + GELU_C * pre * squared))
            hs[slot, rows] = (0.5 * pre * (1.0 + tanh_val)).astype(BF16)
            slope = 0.5 * (1.0 + tanh_val) + 0.5 * pre * (1.0 - tanh_val * tanh_val) * GELU_K * (1.0 + 3.0 * GELU_C * squared)
            pre_grad = dot(gb[rows, :], wg[1, b].reshape(fb, width), ((1,), (1,))) * slope
            vv[pl.ds(b, 1)] += jnp.sum(pre_grad, axis=0, keepdims=True)
            dcs[slot, rows] = pre_grad.astype(BF16)
            if hook is not None:
                hook(t)
            return carry

        lax.fori_loop(0, n_tiles, block_tile, 0)
        for i, (rows_of, columns_of) in enumerate(((dcs, ab), (hs, gb))):
            gw[i, b] = dot(rows_of[slot], columns_of[...], ((0,), (0,))).reshape(RING, unit, width)
            if send_part is not None:
                send_part(i)

    def half_block(slot, b, part, units, send_part):
        bias = jnp.concatenate([bias_u[b, u, 0:1, 0:unit] for u in units], axis=1)
        columns = slice(2 * part * unit, 2 * (part + 1) * unit)

        def half_tile(t, carry):
            rows = pl.ds(pl.multiple_of(t * tile, tile), tile)
            w1, w2 = (jnp.concatenate([wg[i, b, u] for u in units], axis=0) for i in range(2))
            pre = dot(ab[rows, :], w1, ((1,), (1,))) + bias
            squared = pre * pre
            tanh_val = jnp.tanh(GELU_K * (pre + GELU_C * pre * squared))
            hidden = (0.5 * pre * (1.0 + tanh_val)).astype(BF16)
            hs2[rows, :] = hidden
            hs[slot, rows, columns] = hidden
            slope = 0.5 * (1.0 + tanh_val) + 0.5 * pre * (1.0 - tanh_val * tanh_val) * GELU_K * (1.0 + 3.0 * GELU_C * squared)
            pre_grad = dot(gb[rows, :], w2, ((1,), (1,))) * slope
            sums = jnp.sum(pre_grad, axis=0, keepdims=True)
            for j, u in enumerate(units):
                db_u[u, 0:1, 0:unit] += sums[:, j * unit:(j + 1) * unit]
            lowp = pre_grad.astype(BF16)
            dcs2[rows, :] = lowp
            dcs[slot, rows, columns] = lowp
            return carry

        lax.fori_loop(0, n_tiles, half_tile, 0)
        for i, (rows_of, columns_of) in enumerate(((dcs2, ab), (hs2, gb))):
            out = dot(rows_of[...], columns_of[...], ((0,), (0,)))
            for j, u in enumerate(units):
                gw[i, b, u] = out[j * unit:(j + 1) * unit]
            send_part(i)

    def relay_gather(t):
        @pl.when(t == 0)
        def _():
            relay1(1)

        @pl.when(t == 1)
        def _():
            relay1(2)
            relay2(3)

    assert n_tiles == RING
    block(0, p, hook=relay_gather)
    relay1(3)
    for t in range(1, RING):
        go(w1u(p, nth(t)), M5 + t, m_right)
    go(w2u(p, qo), M6 + 3, m_left)

    def back1(t):
        return wrap(q - gray(RING - 1 - t))

    def back2(t):
        return wrap(q + gray(RING - 1 - t))

    db_u[...] = jnp.zeros_like(db_u)
    for part in range(2):
        mine = (2 * part, 2 * part + 1)
        for t in mine:
            arrive(w2u(po, nth(t)), M4 + t)
            arrive(w1u(po, nth(t)), M3 + t)

        def send_opposite(i):
            for t in mine:
                u = nth(t)
                rc(gw.at[i, po, u], opp.at[i, u], (R2 if i else R1) + t, m_right if i else m_left).start()

        half_block(1, po, part, tuple(nth(t) for t in mine), send_opposite)
    vv[pl.ds(po, 1)] = jnp.concatenate([db_u[u, 0:1, 0:unit] for u in range(RING)], axis=1)

    for t in range(RING):
        arrive(w2u(pr, nth(t)), M6 + t)
    def send_right(i):
        if i == 0:
            rc(gw.at[0, pr], dirs.at[0], R3, m_right).start()

    block(2, pr, send_part=send_right)
    for t in range(RING):
        arrive(w1u(pl_, nth(t)), M5 + t)
    block(3, pl_)

    def direct2(t):
        u = back2(t)
        rc(gw.at[1, pl_, u], dirs.at[1, u], R4 + t, m_left).start()

    direct2(0)
    direct2(1)

    def product_tile(t, carry):
        rows = pl.ds(pl.multiple_of(t * tile, tile), tile)
        for i, (left, acc) in enumerate(((dcs, da_acc), (hs, y_acc))):
            weights = jnp.concatenate([wg[i, p].reshape(fb, width)] + [wg[i, po, nth(k)] for k in range(RING)]
                                      + [wg[i, b].reshape(fb, width) for b in (pr, pl_)], axis=0)
            out = dot(jnp.concatenate([left[slot, rows] for slot in range(RING)], axis=1), weights)
            acc[0, rows] = out[:, 0:half]
            acc[1, rows] = out[:, half:width]
        return carry

    lax.fori_loop(0, n_tiles, product_tile, 0)

    lane = lax.broadcasted_iota(jnp.int32, (tile, 128), 1)

    def stat_tile(t, carry):
        rows = pl.ds(pl.multiple_of(t * tile, tile), tile)
        mean, inv = mean_s[rows], inv_s[rows]
        v0 = da_acc[0, rows] * lnv[0, 0:1]
        v1 = da_acc[1, rows] * lnv[1, 0:1]
        h0 = (xf[0, rows].astype(F32) - mean) * inv
        h1 = (xf[1, rows].astype(F32) - mean) * inv
        one = jnp.sum(v0, axis=1, keepdims=True) + jnp.sum(v1, axis=1, keepdims=True)
        two = jnp.sum(v0 * h0, axis=1, keepdims=True) + jnp.sum(v1 * h1, axis=1, keepdims=True)
        stat[rows] = jnp.where(lane < 64, one, two)
        return carry

    rc(y_acc.at[other], yr, EY, partner).start()
    rc(da_acc.at[other], dar, ED, partner).start()
    lax.fori_loop(0, n_tiles, stat_tile, 0)
    rc(stat, statr, ES, partner).start()

    for t in range(RING):
        u1, u2 = back1(t), back2(t)
        arrive(opp.at[1, u2], R2 + (3, 2, 1, 0)[t])
        gw[1, pr, u2] += opp[1, u2]
        rc(gw.at[1, pr, u2], rel.at[1, u2], R6 + t, m_right).start()
        arrive(opp.at[0, u1], R1 + (3, 1, 2, 0)[t])
        gw[0, pl_, u1] += opp[0, u1]
        rc(gw.at[0, pl_, u1], rel.at[0, u1], R5 + t, m_left).start()
    direct2(2)
    direct2(3)

    arrive(yr, EY)
    arrive(dar, ED)
    arrive(statr, ES)
    b_down = bd_ref[...].astype(F32).reshape(1, half)

    def out_tile(t, carry):
        rows = pl.ds(pl.multiple_of(t * tile, tile), tile)
        x_own = xf[e, rows].astype(F32)
        y_ref[rows] = (x_own + (y_acc[e, rows] + yr[rows]) + b_down).astype(BF16)
        norm_grad = da_acc[e, rows] + dar[rows]
        sums = (stat[rows] + statr[rows]) / width
        inv = inv_s[rows]
        x_hat = (x_own - mean_s[rows]) * inv
        value = norm_grad * lnv[e, 0:1]
        dx_ref[rows] = (gf[e, rows].astype(F32) + inv * (value - sums[:, 0:1] - x_hat * sums[:, 64:65])).astype(BF16)
        vv[RING + 1:RING + 2] += jnp.sum(norm_grad * x_hat, axis=0, keepdims=True)
        vv[RING + 2:RING + 3] += jnp.sum(norm_grad, axis=0, keepdims=True)
        return carry

    lax.fori_loop(0, n_tiles, out_tile, 0)

    vs[q] = vv[...]
    for k, d in ((1, s_right), (2, s_opp_dev), (3, s_left)):
        go(vs.at[q], VS + k, d)
    for k in range(1, RING):
        arrive(vs.at[wrap(q - k)], VS + k)
    vm[p] = ((vs[0] + vs[1]) + vs[2]) + vs[3]
    for k, d in ((1, m_right), (2, m_opp), (3, m_left)):
        go(vm.at[p], VM + k, d)

    sent(l2.at[0], P2)
    sent(l1.at[0, 0], P1 + other)
    for k in range(1, RING):
        for h in range(2):
            sent(l1.at[0, 0], P1 + 2 * k + h)
        sent(bi.at[c], BI + k)
        sent(vs.at[q], VS + k)
    sent(lnv.at[0], DLN)
    sent(x_hbm, DX)
    sent(g_hbm, DG)
    for sem in (S1, S2, S3, S4, S5, S6):
        sent(w1u(p, q), sem)
    for t in range(RING):
        for sem in (M1, M2, M3, M4, M5, M6):
            sent(w1u(p, q), sem + t)
        for sem in (R1, R2):
            sent(gw.at[0, p, q], sem + t)
    sent(yr, EY)
    sent(dar, ED)
    sent(stat, ES)
    sent(gw.at[0, p, q], R4)
    sent(gw.at[0, p, q], R4 + 1)

    arrive(dirs.at[0], R3)

    def reduce1(t):
        u = back1(t)
        arrive(rel.at[0, u], R5 + t)
        gw[0, p, u] += dirs[0, u] + rel[0, u]
        if t == 0:
            rc(gw.at[0, p, u], s_opp.at[0], Q1, s_left).start()
        if t == 1:
            rc(gw.at[0, p, u], s_dir.at[0], Q3, s_right).start()
        if t == 2:
            arrive(s_opp.at[0], Q1)
            gw[0, p, u] += s_opp[0]
            rc(gw.at[0, p, u], s_rel.at[0], Q5, s_left).start()

    def reduce2(t):
        u = back2(t)
        arrive(dirs.at[1, u], R4 + t)
        arrive(rel.at[1, u], R6 + t)
        gw[1, p, u] += dirs[1, u] + rel[1, u]
        if t == 0:
            rc(gw.at[1, p, u], s_opp.at[1], Q2, s_right).start()
        if t == 1:
            rc(gw.at[1, p, u], s_dir.at[1], Q4, s_left).start()
        if t == 2:
            arrive(s_opp.at[1], Q2)
            gw[1, p, u] += s_opp[1]
            rc(gw.at[1, p, u], s_rel.at[1], Q6, s_right).start()

    reduce1(0)
    reduce1(1)
    reduce2(0)
    reduce1(2)
    reduce2(1)
    reduce1(3)
    reduce2(2)

    arrive(s_dir.at[0], Q3)
    arrive(s_rel.at[0], Q5)
    done1 = gw[0, p, q] + s_dir[0] + s_rel[0]
    for k in range(RING):
        for h in range(2):
            start = (h * RING + k) * unit
            f1[k, h] = pack(done1[:, start:start + unit]).astype(BF16)
    for k in (2, 1, 3):
        for h in range(2):
            rc(f1.at[wrap(r + k), h], f1l.at[r, e], F1 + 2 * k + h,
               {"row": wrap(r + k), "col": c, "dep": h}, F1 + 2 * k + e).start()
    rc(f1.at[r, other], f1l.at[r, e], F1 + other, partner, F1 + e).start()
    f1l[r, e] = f1[r, e]
    reduce2(3)
    for k in range(1, RING):
        arrive(vm.at[wrap(p - k)], VM + k)
    vp[e] = ((vm[0] + vm[1]) + vm[2]) + vm[3]
    go(vp.at[e], VP, partner)
    arrive(s_dir.at[1], Q4)
    arrive(s_rel.at[1], Q6)
    done2 = (gw[1, p, q] + s_dir[1] + s_rel[1]).astype(BF16)
    f2[0] = done2[:, 0:half]
    f2[1] = done2[:, half:width]
    rc(f2.at[other], f2l.at[e], F2, partner).start()
    f2l[e] = f2[e]

    arrive(vp.at[other], VP)
    pieces = []
    for k in range(RING):
        pieces.append(vp[0, pl.ds(c, 1)][:, k * unit:(k + 1) * unit])
        row = vp[1, k:k + 1]
        piece = row[:, 0:unit]
        for j in range(1, RING):
            piece = jnp.where(c == j, row[:, j * unit:(j + 1) * unit], piece)
        pieces.append(piece)
    dbu_ref[...] = jnp.concatenate(pieces, axis=1).reshape(dbu_ref.shape)
    dbd_ref[...] = vp[e, RING:RING + 1].reshape(dbd_ref.shape)
    dsc_ref[...] = vp[e, RING + 1:RING + 2].reshape(dsc_ref.shape)
    dsh_ref[...] = vp[e, RING + 2:RING + 3].reshape(dsh_ref.shape)

    sent(f1.at[0, 0], F1 + other)
    for k in range(1, RING):
        for h in range(2):
            sent(f1.at[0, 0], F1 + 2 * k + h)
        sent(vm.at[p], VM + k)
    sent(f2.at[0], F2)
    for sem in [R5 + t for t in range(RING)] + [R6 + t for t in range(RING)] + [R4 + 2, R4 + 3, Q1, Q2, Q3, Q4, Q5, Q6]:
        sent(gw.at[0, p, q], sem)
    sent(gw.at[0, p], R3)
    sent(vp.at[e], VP)

    arrive(f2l.at[other], F2)
    dw2_ref[0:unit] = f2l[0]
    dw2_ref[unit:2 * unit] = f2l[1]
    arrive(f1l.at[r, other], F1 + other)
    for k in range(1, RING):
        for h in range(2):
            arrive(f1l.at[wrap(r - k), h], F1 + 2 * k + h)
    turned = jnp.concatenate([unpack(f1l[k, h].astype(F32)) for k in range(RING) for h in range(2)], axis=0)
    turned = jnp.concatenate([turned, jnp.zeros((2 * fb, LANES - unit), F32)], axis=1)
    dw1_ref[...] = turned.T[0:unit].astype(BF16)


def copy_out(*refs):
    n = len(refs) // 2
    copies = [pltpu.make_async_copy(refs[i], refs[n + i], refs[2 * n].at[i]) for i in range(n)]
    for copy in copies:
        copy.start()
    for copy in copies:
        copy.wait()


def solution(mesh):
    assert mesh.shape["row"] == RING and mesh.shape["col"] == RING and mesh.shape["dep"] == 2
    tok_spec = P(("part", "row", "col"), "dep")
    vec_dep = P("dep")
    part_dep = P(("part", "dep"))
    in_specs = (tok_spec, vec_dep, vec_dep, P(("dep", "row"), "col"), P("col"), P(("col", "row"), "dep"), vec_dep, tok_spec)
    out_specs = (tok_spec, tok_spec, P(("part", "dep", "row"), "col"), P(("part", "col")), P(("part", "col", "row"), "dep"), part_dep, part_dep, part_dep)

    def local_step(x_in, ln_scale, ln_shift, w_up, b_up, w_down, b_down, y_grad):
        tokens, half = x_in.shape
        width = 2 * half
        unit = w_down.shape[0] // 2
        fb = RING * unit
        assert w_up.shape == (unit, 2 * fb) and half == RING * unit and fb == half
        tile = tokens // RING
        packed = (RING, 2, 3 * unit // 4, LANES)
        assert 3 * LANES == 4 * unit
        hbm_spec = pl.BlockSpec(memory_space=pltpu.HBM)
        vmem_spec = pl.BlockSpec(memory_space=pltpu.VMEM)
        vmem = pltpu.VMEM
        scratch = [
            vmem((unit, 2 * fb), BF16),
            vmem(packed, BF16), vmem(packed, BF16), vmem((2, unit, half), BF16),
            vmem((2, tokens, half), BF16), vmem((2, tokens, half), BF16),
            vmem((2, 8, half), F32),
            vmem((2, RING, RING, unit, width), BF16),
            vmem((RING, 8, 2 * fb), F32), vmem((RING, RING, 8, LANES), F32),
            vmem((tokens, width), BF16), vmem((tokens, width), BF16),
            vmem((tokens, 1), F32), vmem((tokens, 1), F32),
            vmem((2, tokens, half), F32), vmem((2, tokens, half), F32),
            vmem((tokens, half), F32), vmem((tokens, half), F32),
            vmem((tokens, 128), F32), vmem((tokens, 128), F32),
            vmem((RING, tokens, fb), BF16), vmem((RING, tokens, fb), BF16),
            vmem((tokens, 2 * unit), BF16), vmem((tokens, 2 * unit), BF16), vmem((RING, 8, LANES), F32),
            vmem((2, RING, RING, unit, width), F32),
            vmem((2, RING, unit, width), F32), vmem((2, RING, unit, width), F32), vmem((2, RING, unit, width), F32),
            vmem((2, unit, width), F32), vmem((2, unit, width), F32), vmem((2, unit, width), F32),
            vmem((8, half), F32), vmem((RING, 8, half), F32), vmem((RING, 8, half), F32), vmem((2, 8, half), F32),
            vmem(packed, BF16), vmem(packed, BF16),
            vmem((2, unit, half), BF16), vmem((2, unit, half), BF16),
            vmem((half,), F32), vmem((half,), F32), vmem((2 * fb,), BF16), vmem((half,), BF16),
            pltpu.SemaphoreType.DMA((N_SEM,)), pltpu.SemaphoreType.DMA((N_SEM,)),
        ]
        shapes = (
            jax.ShapeDtypeStruct((tokens, half), BF16), jax.ShapeDtypeStruct((tokens, half), BF16),
            jax.ShapeDtypeStruct(w_up.shape, BF16), jax.ShapeDtypeStruct(b_up.shape, F32),
            jax.ShapeDtypeStruct(w_down.shape, BF16), jax.ShapeDtypeStruct((half,), F32),
            jax.ShapeDtypeStruct((half,), F32), jax.ShapeDtypeStruct((half,), F32))
        outs = pl.pallas_call(
            functools.partial(kernel, tile),
            out_shape=shapes,
            in_specs=[hbm_spec] * 8,
            out_specs=(vmem_spec,) * 8,
            scratch_shapes=scratch,
            compiler_params=pltpu.CompilerParams(collective_id=0, has_side_effects=True, vmem_limit_bytes=51 * 1024 * 1024),
        )(*(pltpu.with_memory_space_constraint(v, pltpu.HBM) for v in (x_in, ln_scale, ln_shift, w_up, b_up, w_down, b_down, y_grad)))
        return pl.pallas_call(
            copy_out,
            out_shape=shapes,
            in_specs=[vmem_spec] * len(shapes),
            out_specs=(hbm_spec,) * len(shapes),
            scratch_shapes=[pltpu.SemaphoreType.DMA((len(shapes),))],
            compiler_params=pltpu.CompilerParams(vmem_limit_bytes=4 * 1024 * 1024),
        )(*outs)

    return jax.shard_map(local_step, mesh=mesh, in_specs=in_specs, out_specs=out_specs, check_vma=False)
```

```python
import functools

import jax
import jax.numpy as jnp
from jax import lax
from jax.experimental import pallas as pl
from jax.experimental.pallas import tpu as pltpu
from jax.sharding import PartitionSpec as P

LN_EPS = 1e-5
GELU_K = 0.7978845608028654
GELU_C = 0.044715
MESH = pl.DeviceIdType.MESH
F32 = jnp.float32
BF16 = jnp.bfloat16
RING = 4
LANES = 128

_next = [0]


def _ids(count=1):
    base = _next[0]
    _next[0] += count
    return base


IN_SEM = _ids(8)
P1 = _ids(2 * RING)
P2, DX, DG, DLN = _ids(), _ids(), _ids(), _ids()
BI = _ids(RING)
S1, S2, S3, S4, S5, S6 = (_ids() for _ in range(6))
M1, M2, M3, M4 = (_ids(RING) for _ in range(4))
M5, M6 = _ids(RING), _ids(RING)
R1, R2, R5, R6 = (_ids(RING) for _ in range(4))
R3, R4 = _ids(), _ids(RING)
Q1, Q2, Q3, Q4, Q5, Q6 = (_ids() for _ in range(6))
VM, VS = _ids(RING), _ids(RING)
VP = _ids()
EY, ED, ES = _ids(), _ids(), _ids()
F1 = _ids(2 * RING)
F2 = _ids()
N_SEM = _next[0]


def gray(t):
    return t + (t // 2) * (5 - 2 * t)


def dot(a, b, dims=((1,), (0,))):
    return lax.dot_general(a, b, (dims, ((), ())), preferred_element_type=F32)


def pack(piece):
    u = piece.shape[0]
    cut, third = 3 * u // 4, u // 3
    beside = jnp.concatenate([piece[cut:, k * third:(k + 1) * third] for k in range(3)], axis=0)
    return jnp.concatenate([piece[:cut], beside], axis=1)


def unpack(packed):
    cut = packed.shape[0]
    u = 4 * cut // 3
    quarter = u - cut
    below = jnp.concatenate([packed[k * quarter:(k + 1) * quarter, u:] for k in range(3)], axis=1)
    return jnp.concatenate([packed[:, :u], below], axis=0)


def kernel(tile, x_hbm, sc_hbm, sh_hbm, w1_hbm, bu_hbm, w2_hbm, bd_hbm, g_hbm,
           y_ref, dx_ref, dw1_ref, dbu_ref, dw2_ref, dbd_ref, dsc_ref, dsh_ref,
           w1v, st1, l1, l2, xf, gf, lnv, wg, bi, bias_u, ab, gb, mean_s, inv_s,
           y_acc, da_acc, yr, dar, stat, statr, hs, dcs, hs2, dcs2, db_u, gw, opp, dirs, rel, s_opp, s_dir, s_rel,
           vv, vm, vs, vp, f1, f1l, f2, f2l, sc_ref, sh_ref, bu_ref, bd_ref, send, recv):
    r, c, e = lax.axis_index("row"), lax.axis_index("col"), lax.axis_index("dep")
    p = c + e * (r - c)
    q = r + e * (c - r)
    tokens, half = xf.shape[1], xf.shape[2]
    width = 2 * half
    unit = l2.shape[1]
    fb = RING * unit
    n_tiles = tokens // tile
    other = 1 - e

    def wrap(v):
        return lax.rem(v + 2 * RING, RING)

    def dev(pp, qq):
        return {"row": qq + e * (pp - qq), "col": pp + e * (qq - pp), "dep": e}

    m_right, m_left, m_opp = dev(wrap(p + 1), q), dev(wrap(p - 1), q), dev(wrap(p + 2), q)
    s_right, s_left, s_opp_dev = dev(p, wrap(q + 1)), dev(p, wrap(q - 1)), dev(p, wrap(q + 2))
    partner = {"row": r, "col": c, "dep": other}
    pr, pl_, po = wrap(p + 1), wrap(p - 1), wrap(p + 2)
    qr, ql, qo = wrap(q + 1), wrap(q - 1), wrap(q + 2)

    def rc(src, dst, ssem, device, rsem=None):
        return pltpu.make_async_remote_copy(
            src_ref=src, dst_ref=dst, send_sem=send.at[ssem], recv_sem=recv.at[ssem if rsem is None else rsem],
            device_id=device, device_id_type=MESH)

    def arrive(dst, rsem):
        rc(dst, dst, rsem, partner).wait_recv()

    def sent(src, ssem):
        rc(src, src, ssem, partner).wait_send()

    def go(ref, sem, device):
        rc(ref, ref, sem, device).start()

    load_w1 = pltpu.make_async_copy(w1_hbm, w1v, recv.at[IN_SEM])
    load_w2 = pltpu.make_async_copy(w2_hbm.at[pl.ds(pl.multiple_of(e * unit, 16), unit)], l2.at[e], recv.at[IN_SEM + 1])
    load_x = pltpu.make_async_copy(x_hbm, xf.at[e], recv.at[IN_SEM + 2])
    load_g = pltpu.make_async_copy(g_hbm, gf.at[e], recv.at[IN_SEM + 3])
    load_vectors = [pltpu.make_async_copy(src, dst, recv.at[IN_SEM + 4 + i]) for i, (src, dst) in enumerate(
        ((sc_hbm, sc_ref), (sh_hbm, sh_ref), (bu_hbm, bu_ref), (bd_hbm, bd_ref)))]
    load_w1.start()
    load_w2.start()
    for load in load_vectors:
        load.start()
    load_x.start()
    load_g.start()

    barrier = pltpu.get_barrier_semaphore()
    peers = [m_right, m_left, s_right, s_left, m_opp, s_opp_dev, partner]
    peers += [{"row": wrap(r + k), "col": c, "dep": other} for k in range(1, RING)]
    for d in peers:
        pl.semaphore_signal(barrier, inc=1, device_id=d, device_id_type=MESH)

    load_w1.wait()
    turned = w1v[...].astype(F32)
    turned = jnp.concatenate([turned, jnp.zeros((LANES - unit, 2 * fb), F32)], axis=0).T
    for k in range(RING):
        for h in range(2):
            st1[k, h] = pack(turned[(2 * k + h) * unit:(2 * k + h + 1) * unit, 0:unit]).astype(BF16)

    for load in load_vectors:
        load.wait()
    lnv[e, 0:1] = sc_ref[...].reshape(1, half)
    lnv[e, 1:2] = sh_ref[...].reshape(1, half)
    bi[c] = bu_ref[...].astype(F32).reshape(1, 2 * fb)

    pl.semaphore_wait(barrier, len(peers))

    rc(w2_hbm.at[pl.ds(pl.multiple_of(other * unit, 16), unit)], l2.at[e], P2, partner).start()
    rc(st1.at[r, other], l1.at[r, e], P1 + other, partner, P1 + e).start()
    for k in (2, 1, 3):
        for h in range(2):
            rc(st1.at[wrap(r + k), h], l1.at[r, e], P1 + 2 * k + h,
               {"row": wrap(r + k), "col": c, "dep": h}, P1 + 2 * k + e).start()
    rc(lnv.at[e], lnv.at[e], DLN, partner).start()
    rc(x_hbm, xf.at[e], DX, partner).start()
    rc(g_hbm, gf.at[e], DG, partner).start()
    for k in range(1, RING):
        rc(bi.at[c], bi.at[c], BI + k, {"row": r, "col": wrap(c + k), "dep": e}).start()
    l1[r, e] = st1[r, e]

    def w1u(b, s):
        return wg.at[0, b, s]

    def w2u(b, s):
        return wg.at[1, b, s]

    load_w2.wait()
    arrive(l2.at[other], P2)
    wg[1, p, q, :, 0:half] = l2[0]
    wg[1, p, q, :, half:width] = l2[1]
    go(w2u(p, q), M2, m_right)
    go(w2u(p, q), S2, s_right)
    go(w2u(p, q), S4, s_left)
    go(w2u(p, q), M6, m_left)

    arrive(l1.at[r, other], P1 + other)
    for k in range(1, RING):
        for h in range(2):
            arrive(l1.at[wrap(r - k), h], P1 + 2 * k + h)
    wg[0, p, q] = jnp.concatenate([unpack(l1[k, h].astype(F32)) for h in range(2) for k in range(RING)], axis=1).astype(BF16)
    go(w1u(p, q), M1, m_left)
    go(w1u(p, q), S1, s_right)
    go(w1u(p, q), S3, s_left)
    go(w1u(p, q), M5, m_right)

    arrive(w2u(p, ql), S2)
    go(w2u(p, ql), S6, s_right)
    arrive(w2u(p, qr), S4)
    go(w2u(p, qr), M2 + 1, m_right)
    go(w2u(p, ql), M2 + 2, m_right)
    go(w2u(p, qr), M6 + 1, m_left)
    go(w2u(p, ql), M6 + 2, m_left)

    def nth(t):
        return wrap(q + gray(t))

    arrive(lnv.at[other], DLN)
    load_x.wait()
    arrive(xf.at[other], DX)
    load_g.wait()
    arrive(gf.at[other], DG)
    vv[...] = jnp.zeros_like(vv)
    def norm_tile(t, carry):
        rows = pl.ds(pl.multiple_of(t * tile, tile), tile)
        x0, x1 = xf[0, rows].astype(F32), xf[1, rows].astype(F32)
        total = jnp.sum(x0, axis=1, keepdims=True) + jnp.sum(x1, axis=1, keepdims=True)
        squares = jnp.sum(x0 * x0, axis=1, keepdims=True) + jnp.sum(x1 * x1, axis=1, keepdims=True)
        mean = total / width
        inv = lax.rsqrt(squares / width - mean * mean + LN_EPS)
        mean_s[rows] = mean
        inv_s[rows] = inv
        ab[rows, 0:half] = ((x0 - mean) * inv * lnv[0, 0:1] + lnv[0, 1:2]).astype(BF16)
        ab[rows, half:width] = ((x1 - mean) * inv * lnv[1, 0:1] + lnv[1, 1:2]).astype(BF16)
        gb[rows, 0:half] = gf[0, rows]
        gb[rows, half:width] = gf[1, rows]
        vv[RING:RING + 1] += jnp.sum(gf[e, rows].astype(F32), axis=0, keepdims=True)
        return carry

    lax.fori_loop(0, n_tiles // 2, norm_tile, 0)
    arrive(w1u(p, qr), S3)
    go(w1u(p, qr), S5, s_left)
    go(w1u(p, qr), M1 + 1, m_left)
    lax.fori_loop(n_tiles // 2, n_tiles, norm_tile, 0)

    def relay1(t):
        arrive(w1u(pr, nth(t)), M1 + t)
        go(w1u(pr, nth(t)), M3 + t, m_left)

    def relay2(t):
        arrive(w2u(pl_, nth(t)), M2 + t)
        go(w2u(pl_, nth(t)), M4 + t, m_right)

    arrive(w1u(p, ql), S1)
    go(w1u(p, ql), M1 + 2, m_left)
    relay2(0)
    for k in range(1, RING):
        arrive(bi.at[wrap(c - k)], BI + k)
    for b in range(RING):
        for k in range(RING):
            flat = bi[b, 0:1, 2 * k * unit:(2 * k + 1) * unit]
            across = bi[k, 0:1, (2 * b + 1) * unit:(2 * b + 2) * unit]
            bias_u[b, k, 0:1, 0:unit] = jnp.where(e == 0, flat, across)
    arrive(w2u(p, qo), S6)
    go(w2u(p, qo), M2 + 3, m_right)
    relay1(0)
    relay2(1)
    arrive(w1u(p, qo), S5)
    go(w1u(p, qo), M1 + 3, m_left)
    relay2(2)

    def block(slot, b, hook=None, send_part=None):
        bias = jnp.concatenate([bias_u[b, u, 0:1, 0:unit] for u in range(RING)], axis=1)

        def block_tile(t, carry):
            rows = pl.ds(pl.multiple_of(t * tile, tile), tile)
            pre = dot(ab[rows, :], wg[0, b].reshape(fb, width), ((1,), (1,))) + bias
            squared = pre * pre
            tanh_val = jnp.tanh(GELU_K * (pre + GELU_C * pre * squared))
            hs[slot, rows] = (0.5 * pre * (1.0 + tanh_val)).astype(BF16)
            slope = 0.5 * (1.0 + tanh_val) + 0.5 * pre * (1.0 - tanh_val * tanh_val) * GELU_K * (1.0 + 3.0 * GELU_C * squared)
            pre_grad = dot(gb[rows, :], wg[1, b].reshape(fb, width), ((1,), (1,))) * slope
            vv[pl.ds(b, 1)] += jnp.sum(pre_grad, axis=0, keepdims=True)
            dcs[slot, rows] = pre_grad.astype(BF16)
            if hook is not None:
                hook(t)
            return carry

        lax.fori_loop(0, n_tiles, block_tile, 0)
        for i, (rows_of, columns_of) in enumerate(((dcs, ab), (hs, gb))):
            gw[i, b] = dot(rows_of[slot], columns_of[...], ((0,), (0,))).reshape(RING, unit, width)
            if send_part is not None:
                send_part(i)

    def half_block(slot, b, part, units, send_part):
        bias = jnp.concatenate([bias_u[b, u, 0:1, 0:unit] for u in units], axis=1)
        columns = slice(2 * part * unit, 2 * (part + 1) * unit)

        def half_tile(t, carry):
            rows = pl.ds(pl.multiple_of(t * tile, tile), tile)
            w1, w2 = (jnp.concatenate([wg[i, b, u] for u in units], axis=0) for i in range(2))
            pre = dot(ab[rows, :], w1, ((1,), (1,))) + bias
            squared = pre * pre
            tanh_val = jnp.tanh(GELU_K * (pre + GELU_C * pre * squared))
            hidden = (0.5 * pre * (1.0 + tanh_val)).astype(BF16)
            hs2[rows, :] = hidden
            hs[slot, rows, columns] = hidden
            slope = 0.5 * (1.0 + tanh_val) + 0.5 * pre * (1.0 - tanh_val * tanh_val) * GELU_K * (1.0 + 3.0 * GELU_C * squared)
            pre_grad = dot(gb[rows, :], w2, ((1,), (1,))) * slope
            sums = jnp.sum(pre_grad, axis=0, keepdims=True)
            for j, u in enumerate(units):
                db_u[u, 0:1, 0:unit] += sums[:, j * unit:(j + 1) * unit]
            lowp = pre_grad.astype(BF16)
            dcs2[rows, :] = lowp
            dcs[slot, rows, columns] = lowp
            return carry

        lax.fori_loop(0, n_tiles, half_tile, 0)
        for i, (rows_of, columns_of) in enumerate(((dcs2, ab), (hs2, gb))):
            out = dot(rows_of[...], columns_of[...], ((0,), (0,)))
            for j, u in enumerate(units):
                gw[i, b, u] = out[j * unit:(j + 1) * unit]
            send_part(i)

    def relay_gather(t):
        @pl.when(t == 0)
        def _():
            relay1(1)

        @pl.when(t == 1)
        def _():
            relay1(2)
            relay2(3)

    assert n_tiles == RING
    block(0, p, hook=relay_gather)
    relay1(3)
    for t in range(1, RING):
        go(w1u(p, nth(t)), M5 + t, m_right)
    go(w2u(p, qo), M6 + 3, m_left)

    def back1(t):
        return wrap(q - gray(RING - 1 - t))

    def back2(t):
        return wrap(q + gray(RING - 1 - t))

    db_u[...] = jnp.zeros_like(db_u)
    for part in range(2):
        mine = (2 * part, 2 * part + 1)
        for t in mine:
            arrive(w2u(po, nth(t)), M4 + t)
            arrive(w1u(po, nth(t)), M3 + t)

        def send_opposite(i):
            for t in mine:
                u = nth(t)
                rc(gw.at[i, po, u], opp.at[i, u], (R2 if i else R1) + t, m_right if i else m_left).start()

        half_block(1, po, part, tuple(nth(t) for t in mine), send_opposite)
    vv[pl.ds(po, 1)] = jnp.concatenate([db_u[u, 0:1, 0:unit] for u in range(RING)], axis=1)

    for t in range(RING):
        arrive(w2u(pr, nth(t)), M6 + t)
    def send_right(i):
        if i == 0:
            rc(gw.at[0, pr], dirs.at[0], R3, m_right).start()

    block(2, pr, send_part=send_right)
    for t in range(RING):
        arrive(w1u(pl_, nth(t)), M5 + t)
    block(3, pl_)

    def direct2(t):
        u = back2(t)
        rc(gw.at[1, pl_, u], dirs.at[1, u], R4 + t, m_left).start()

    direct2(0)
    direct2(1)

    def product_tile(t, carry):
        rows = pl.ds(pl.multiple_of(t * tile, tile), tile)
        for i, (left, acc) in enumerate(((dcs, da_acc), (hs, y_acc))):
            weights = jnp.concatenate([wg[i, p].reshape(fb, width)] + [wg[i, po, nth(k)] for k in range(RING)]
                                      + [wg[i, b].reshape(fb, width) for b in (pr, pl_)], axis=0)
            out = dot(jnp.concatenate([left[slot, rows] for slot in range(RING)], axis=1), weights)
            acc[0, rows] = out[:, 0:half]
            acc[1, rows] = out[:, half:width]
        return carry

    lax.fori_loop(0, n_tiles, product_tile, 0)

    rc(y_acc.at[other], yr, EY, partner).start()
    rc(da_acc.at[other], dar, ED, partner).start()

    for t in range(RING):
        u1, u2 = back1(t), back2(t)
        arrive(opp.at[1, u2], R2 + (3, 2, 1, 0)[t])
        gw[1, pr, u2] += opp[1, u2]
        rc(gw.at[1, pr, u2], rel.at[1, u2], R6 + t, m_right).start()
        arrive(opp.at[0, u1], R1 + (3, 1, 2, 0)[t])
        gw[0, pl_, u1] += opp[0, u1]
        rc(gw.at[0, pl_, u1], rel.at[0, u1], R5 + t, m_left).start()
    direct2(2)
    direct2(3)

    lane = lax.broadcasted_iota(jnp.int32, (tile, 128), 1)

    def stat_tile(t, carry):
        rows = pl.ds(pl.multiple_of(t * tile, tile), tile)
        mean, inv = mean_s[rows], inv_s[rows]
        v0 = da_acc[0, rows] * lnv[0, 0:1]
        v1 = da_acc[1, rows] * lnv[1, 0:1]
        h0 = (xf[0, rows].astype(F32) - mean) * inv
        h1 = (xf[1, rows].astype(F32) - mean) * inv
        one = jnp.sum(v0, axis=1, keepdims=True) + jnp.sum(v1, axis=1, keepdims=True)
        two = jnp.sum(v0 * h0, axis=1, keepdims=True) + jnp.sum(v1 * h1, axis=1, keepdims=True)
        stat[rows] = jnp.where(lane < 64, one, two)
        return carry

    lax.fori_loop(0, n_tiles, stat_tile, 0)
    rc(stat, statr, ES, partner).start()

    arrive(yr, EY)
    arrive(dar, ED)
    arrive(statr, ES)
    b_down = bd_ref[...].astype(F32).reshape(1, half)

    def out_tile(t, carry):
        rows = pl.ds(pl.multiple_of(t * tile, tile), tile)
        x_own = xf[e, rows].astype(F32)
        y_ref[rows] = (x_own + (y_acc[e, rows] + yr[rows]) + b_down).astype(BF16)
        norm_grad = da_acc[e, rows] + dar[rows]
        sums = (stat[rows] + statr[rows]) / width
        inv = inv_s[rows]
        x_hat = (x_own - mean_s[rows]) * inv
        value = norm_grad * lnv[e, 0:1]
        dx_ref[rows] = (gf[e, rows].astype(F32) + inv * (value - sums[:, 0:1] - x_hat * sums[:, 64:65])).astype(BF16)
        vv[RING + 1:RING + 2] += jnp.sum(norm_grad * x_hat, axis=0, keepdims=True)
        vv[RING + 2:RING + 3] += jnp.sum(norm_grad, axis=0, keepdims=True)
        return carry

    lax.fori_loop(0, n_tiles, out_tile, 0)

    vs[q] = vv[...]
    for k, d in ((1, s_right), (2, s_opp_dev), (3, s_left)):
        go(vs.at[q], VS + k, d)
    for k in range(1, RING):
        arrive(vs.at[wrap(q - k)], VS + k)
    vm[p] = ((vs[0] + vs[1]) + vs[2]) + vs[3]
    for k, d in ((1, m_right), (2, m_opp), (3, m_left)):
        go(vm.at[p], VM + k, d)

    sent(l2.at[0], P2)
    sent(l1.at[0, 0], P1 + other)
    for k in range(1, RING):
        for h in range(2):
            sent(l1.at[0, 0], P1 + 2 * k + h)
        sent(bi.at[c], BI + k)
        sent(vs.at[q], VS + k)
    sent(lnv.at[0], DLN)
    sent(x_hbm, DX)
    sent(g_hbm, DG)
    for sem in (S1, S2, S3, S4, S5, S6):
        sent(w1u(p, q), sem)
    for t in range(RING):
        for sem in (M1, M2, M3, M4, M5, M6):
            sent(w1u(p, q), sem + t)
        for sem in (R1, R2):
            sent(gw.at[0, p, q], sem + t)
    sent(yr, EY)
    sent(dar, ED)
    sent(stat, ES)
    sent(gw.at[0, p, q], R4)
    sent(gw.at[0, p, q], R4 + 1)

    arrive(dirs.at[0], R3)

    def reduce1(t):
        u = back1(t)
        arrive(rel.at[0, u], R5 + t)
        gw[0, p, u] += dirs[0, u] + rel[0, u]
        if t == 0:
            rc(gw.at[0, p, u], s_opp.at[0], Q1, s_left).start()
        if t == 1:
            rc(gw.at[0, p, u], s_dir.at[0], Q3, s_right).start()
        if t == 2:
            arrive(s_opp.at[0], Q1)
            gw[0, p, u] += s_opp[0]
            rc(gw.at[0, p, u], s_rel.at[0], Q5, s_left).start()

    def reduce2(t):
        u = back2(t)
        arrive(dirs.at[1, u], R4 + t)
        arrive(rel.at[1, u], R6 + t)
        gw[1, p, u] += dirs[1, u] + rel[1, u]
        if t == 0:
            rc(gw.at[1, p, u], s_opp.at[1], Q2, s_right).start()
        if t == 1:
            rc(gw.at[1, p, u], s_dir.at[1], Q4, s_left).start()
        if t == 2:
            arrive(s_opp.at[1], Q2)
            gw[1, p, u] += s_opp[1]
            rc(gw.at[1, p, u], s_rel.at[1], Q6, s_right).start()

    reduce1(0)
    reduce1(1)
    reduce2(0)
    reduce1(2)
    reduce2(1)
    reduce1(3)
    reduce2(2)

    arrive(s_dir.at[0], Q3)
    arrive(s_rel.at[0], Q5)
    done1 = gw[0, p, q] + s_dir[0] + s_rel[0]
    for k in range(RING):
        for h in range(2):
            start = (h * RING + k) * unit
            f1[k, h] = pack(done1[:, start:start + unit]).astype(BF16)
    for k in (2, 1, 3):
        for h in range(2):
            rc(f1.at[wrap(r + k), h], f1l.at[r, e], F1 + 2 * k + h,
               {"row": wrap(r + k), "col": c, "dep": h}, F1 + 2 * k + e).start()
    rc(f1.at[r, other], f1l.at[r, e], F1 + other, partner, F1 + e).start()
    f1l[r, e] = f1[r, e]
    reduce2(3)
    for k in range(1, RING):
        arrive(vm.at[wrap(p - k)], VM + k)
    vp[e] = ((vm[0] + vm[1]) + vm[2]) + vm[3]
    go(vp.at[e], VP, partner)
    arrive(s_dir.at[1], Q4)
    arrive(s_rel.at[1], Q6)
    done2 = (gw[1, p, q] + s_dir[1] + s_rel[1]).astype(BF16)
    f2[0] = done2[:, 0:half]
    f2[1] = done2[:, half:width]
    rc(f2.at[other], f2l.at[e], F2, partner).start()
    f2l[e] = f2[e]

    arrive(vp.at[other], VP)
    pieces = []
    for k in range(RING):
        pieces.append(vp[0, pl.ds(c, 1)][:, k * unit:(k + 1) * unit])
        row = vp[1, k:k + 1]
        piece = row[:, 0:unit]
        for j in range(1, RING):
            piece = jnp.where(c == j, row[:, j * unit:(j + 1) * unit], piece)
        pieces.append(piece)
    dbu_ref[...] = jnp.concatenate(pieces, axis=1).reshape(dbu_ref.shape)
    dbd_ref[...] = vp[e, RING:RING + 1].reshape(dbd_ref.shape)
    dsc_ref[...] = vp[e, RING + 1:RING + 2].reshape(dsc_ref.shape)
    dsh_ref[...] = vp[e, RING + 2:RING + 3].reshape(dsh_ref.shape)

    sent(f1.at[0, 0], F1 + other)
    for k in range(1, RING):
        for h in range(2):
            sent(f1.at[0, 0], F1 + 2 * k + h)
        sent(vm.at[p], VM + k)
    sent(f2.at[0], F2)
    for sem in [R5 + t for t in range(RING)] + [R6 + t for t in range(RING)] + [R4 + 2, R4 + 3, Q1, Q2, Q3, Q4, Q5, Q6]:
        sent(gw.at[0, p, q], sem)
    sent(gw.at[0, p], R3)
    sent(vp.at[e], VP)

    arrive(f2l.at[other], F2)
    dw2_ref[0:unit] = f2l[0]
    dw2_ref[unit:2 * unit] = f2l[1]
    arrive(f1l.at[r, other], F1 + other)
    for k in range(1, RING):
        for h in range(2):
            arrive(f1l.at[wrap(r - k), h], F1 + 2 * k + h)
    turned = jnp.concatenate([unpack(f1l[k, h].astype(F32)) for k in range(RING) for h in range(2)], axis=0)
    turned = jnp.concatenate([turned, jnp.zeros((2 * fb, LANES - unit), F32)], axis=1)
    dw1_ref[...] = turned.T[0:unit].astype(BF16)


def copy_out(*refs):
    n = len(refs) // 2
    copies = [pltpu.make_async_copy(refs[i], refs[n + i], refs[2 * n].at[i]) for i in range(n)]
    for copy in copies:
        copy.start()
    for copy in copies:
        copy.wait()


def solution(mesh):
    assert mesh.shape["row"] == RING and mesh.shape["col"] == RING and mesh.shape["dep"] == 2
    tok_spec = P(("part", "row", "col"), "dep")
    vec_dep = P("dep")
    part_dep = P(("part", "dep"))
    in_specs = (tok_spec, vec_dep, vec_dep, P(("dep", "row"), "col"), P("col"), P(("col", "row"), "dep"), vec_dep, tok_spec)
    out_specs = (tok_spec, tok_spec, P(("part", "dep", "row"), "col"), P(("part", "col")), P(("part", "col", "row"), "dep"), part_dep, part_dep, part_dep)

    def local_step(x_in, ln_scale, ln_shift, w_up, b_up, w_down, b_down, y_grad):
        tokens, half = x_in.shape
        width = 2 * half
        unit = w_down.shape[0] // 2
        fb = RING * unit
        assert w_up.shape == (unit, 2 * fb) and half == RING * unit and fb == half
        tile = tokens // RING
        packed = (RING, 2, 3 * unit // 4, LANES)
        assert 3 * LANES == 4 * unit
        hbm_spec = pl.BlockSpec(memory_space=pltpu.HBM)
        vmem_spec = pl.BlockSpec(memory_space=pltpu.VMEM)
        vmem = pltpu.VMEM
        scratch = [
            vmem((unit, 2 * fb), BF16),
            vmem(packed, BF16), vmem(packed, BF16), vmem((2, unit, half), BF16),
            vmem((2, tokens, half), BF16), vmem((2, tokens, half), BF16),
            vmem((2, 8, half), F32),
            vmem((2, RING, RING, unit, width), BF16),
            vmem((RING, 1, 2 * fb), F32), vmem((RING, RING, 8, LANES), F32),
            vmem((tokens, width), BF16), vmem((tokens, width), BF16),
            vmem((tokens, 1), F32), vmem((tokens, 1), F32),
            vmem((2, tokens, half), F32), vmem((2, tokens, half), F32),
            vmem((tokens, half), F32), vmem((tokens, half), F32),
            vmem((tokens, 128), F32), vmem((tokens, 128), F32),
            vmem((RING, tokens, fb), BF16), vmem((RING, tokens, fb), BF16),
            vmem((tokens, 2 * unit), BF16), vmem((tokens, 2 * unit), BF16), vmem((RING, 8, LANES), F32),
            vmem((2, RING, RING, unit, width), F32),
            vmem((2, RING, unit, width), F32), vmem((2, RING, unit, width), F32), vmem((2, RING, unit, width), F32),
            vmem((2, unit, width), F32), vmem((2, unit, width), F32), vmem((2, unit, width), F32),
            vmem((8, half), F32), vmem((RING, 8, half), F32), vmem((RING, 8, half), F32), vmem((2, 8, half), F32),
            vmem(packed, BF16), vmem(packed, BF16),
            vmem((2, unit, half), BF16), vmem((2, unit, half), BF16),
            vmem((half,), F32), vmem((half,), F32), vmem((2 * fb,), BF16), vmem((half,), BF16),
            pltpu.SemaphoreType.DMA((N_SEM,)), pltpu.SemaphoreType.DMA((N_SEM,)),
        ]
        shapes = (
            jax.ShapeDtypeStruct((tokens, half), BF16), jax.ShapeDtypeStruct((tokens, half), BF16),
            jax.ShapeDtypeStruct(w_up.shape, BF16), jax.ShapeDtypeStruct(b_up.shape, F32),
            jax.ShapeDtypeStruct(w_down.shape, BF16), jax.ShapeDtypeStruct((half,), F32),
            jax.ShapeDtypeStruct((half,), F32), jax.ShapeDtypeStruct((half,), F32))
        outs = pl.pallas_call(
            functools.partial(kernel, tile),
            out_shape=shapes,
            in_specs=[hbm_spec] * 8,
            out_specs=(vmem_spec,) * 8,
            scratch_shapes=scratch,
            compiler_params=pltpu.CompilerParams(collective_id=0, has_side_effects=True, vmem_limit_bytes=51 * 1024 * 1024),
        )(*(pltpu.with_memory_space_constraint(v, pltpu.HBM) for v in (x_in, ln_scale, ln_shift, w_up, b_up, w_down, b_down, y_grad)))
        return pl.pallas_call(
            copy_out,
            out_shape=shapes,
            in_specs=[vmem_spec] * len(shapes),
            out_specs=(hbm_spec,) * len(shapes),
            scratch_shapes=[pltpu.SemaphoreType.DMA((len(shapes),))],
            compiler_params=pltpu.CompilerParams(vmem_limit_bytes=4 * 1024 * 1024),
        )(*outs)

    return jax.shard_map(local_step, mesh=mesh, in_specs=in_specs, out_specs=out_specs, check_vma=False)
```

```python
import functools

import jax
import jax.numpy as jnp
from jax import lax
from jax.experimental import pallas as pl
from jax.experimental.pallas import tpu as pltpu
from jax.sharding import PartitionSpec as P

LN_EPS = 1e-5
GELU_K = 0.7978845608028654
GELU_C = 0.044715
MESH = pl.DeviceIdType.MESH
F32 = jnp.float32
BF16 = jnp.bfloat16
RING = 4
LANES = 128

_next = [0]


def _ids(count=1):
    base = _next[0]
    _next[0] += count
    return base


IN_SEM = _ids(8)
P1 = _ids(2 * RING)
P2, DX, DG, DLN = _ids(), _ids(), _ids(), _ids()
BI = _ids(RING)
S1, S2, S3, S4, S5, S6 = (_ids() for _ in range(6))
M1, M2, M3, M4 = (_ids(RING) for _ in range(4))
M5, M6 = _ids(RING), _ids(RING)
R1, R2, R5, R6 = (_ids(RING) for _ in range(4))
R3, R4 = _ids(), _ids(RING)
Q1, Q2, Q3, Q4, Q5, Q6 = (_ids() for _ in range(6))
VM, VS = _ids(RING), _ids(RING)
VP = _ids()
EY, ED, ES = _ids(), _ids(), _ids()
F1 = _ids(2 * RING)
F2 = _ids()
N_SEM = _next[0]


def gray(t):
    return t + (t // 2) * (5 - 2 * t)


def dot(a, b, dims=((1,), (0,))):
    return lax.dot_general(a, b, (dims, ((), ())), preferred_element_type=F32)


def pack(piece):
    u = piece.shape[0]
    cut, third = 3 * u // 4, u // 3
    beside = jnp.concatenate([piece[cut:, k * third:(k + 1) * third] for k in range(3)], axis=0)
    return jnp.concatenate([piece[:cut], beside], axis=1)


def unpack(packed):
    cut = packed.shape[0]
    u = 4 * cut // 3
    quarter = u - cut
    below = jnp.concatenate([packed[k * quarter:(k + 1) * quarter, u:] for k in range(3)], axis=1)
    return jnp.concatenate([packed[:, :u], below], axis=0)


def kernel(tile, x_hbm, sc_hbm, sh_hbm, w1_hbm, bu_hbm, w2_hbm, bd_hbm, g_hbm,
           y_ref, dx_ref, dw1_ref, dbu_ref, dw2_ref, dbd_ref, dsc_ref, dsh_ref,
           w1v, st1, l1, l2, xf, gf, lnv, wg, bi, bias_u, ab, gb, mean_s, inv_s,
           y_acc, da_acc, yr, dar, stat, statr, hs, dcs, hs2, dcs2, db_u, gw, opp, dirs, rel, s_opp, s_dir, s_rel,
           vv, vm, vs, vp, f1, f1l, f2, f2l, sc_ref, sh_ref, bu_ref, bd_ref, send, recv):
    r, c, e = lax.axis_index("row"), lax.axis_index("col"), lax.axis_index("dep")
    p = c + e * (r - c)
    q = r + e * (c - r)
    tokens, half = xf.shape[1], xf.shape[2]
    width = 2 * half
    unit = l2.shape[1]
    fb = RING * unit
    n_tiles = tokens // tile
    other = 1 - e

    def wrap(v):
        return lax.rem(v + 2 * RING, RING)

    def dev(pp, qq):
        return {"row": qq + e * (pp - qq), "col": pp + e * (qq - pp), "dep": e}

    m_right, m_left, m_opp = dev(wrap(p + 1), q), dev(wrap(p - 1), q), dev(wrap(p + 2), q)
    s_right, s_left, s_opp_dev = dev(p, wrap(q + 1)), dev(p, wrap(q - 1)), dev(p, wrap(q + 2))
    partner = {"row": r, "col": c, "dep": other}
    pr, pl_, po = wrap(p + 1), wrap(p - 1), wrap(p + 2)
    qr, ql, qo = wrap(q + 1), wrap(q - 1), wrap(q + 2)

    def rc(src, dst, ssem, device, rsem=None):
        return pltpu.make_async_remote_copy(
            src_ref=src, dst_ref=dst, send_sem=send.at[ssem], recv_sem=recv.at[ssem if rsem is None else rsem],
            device_id=device, device_id_type=MESH)

    def arrive(dst, rsem):
        rc(dst, dst, rsem, partner).wait_recv()

    def sent(src, ssem):
        rc(src, src, ssem, partner).wait_send()

    def go(ref, sem, device):
        rc(ref, ref, sem, device).start()

    barrier = pltpu.get_barrier_semaphore()
    peers = [m_opp, s_opp_dev]
    peers += [{"row": wrap(r + k), "col": c, "dep": other} for k in (2, 1, 3)]
    peers += [m_right, m_left, s_right, s_left, partner]
    for d in peers:
        pl.semaphore_signal(barrier, inc=1, device_id=d, device_id_type=MESH)

    load_w1 = pltpu.make_async_copy(w1_hbm, w1v, recv.at[IN_SEM])
    load_w2 = pltpu.make_async_copy(w2_hbm.at[pl.ds(pl.multiple_of(e * unit, 16), unit)], l2.at[e], recv.at[IN_SEM + 1])
    load_x = pltpu.make_async_copy(x_hbm, xf.at[e], recv.at[IN_SEM + 2])
    load_g = pltpu.make_async_copy(g_hbm, gf.at[e], recv.at[IN_SEM + 3])
    load_vectors = [pltpu.make_async_copy(src, dst, recv.at[IN_SEM + 4 + i]) for i, (src, dst) in enumerate(
        ((sc_hbm, sc_ref), (sh_hbm, sh_ref), (bu_hbm, bu_ref), (bd_hbm, bd_ref)))]
    load_w1.start()
    load_w2.start()
    for load in load_vectors:
        load.start()
    load_x.start()
    load_g.start()

    load_w1.wait()
    turned = w1v[...].astype(F32)
    turned = jnp.concatenate([turned, jnp.zeros((LANES - unit, 2 * fb), F32)], axis=0).T
    for k in range(RING):
        for h in range(2):
            st1[k, h] = pack(turned[(2 * k + h) * unit:(2 * k + h + 1) * unit, 0:unit]).astype(BF16)

    for load in load_vectors:
        load.wait()
    lnv[e, 0:1] = sc_ref[...].reshape(1, half)
    lnv[e, 1:2] = sh_ref[...].reshape(1, half)
    bi[c] = bu_ref[...].astype(F32).reshape(1, 2 * fb)

    pl.semaphore_wait(barrier, len(peers))

    rc(w2_hbm.at[pl.ds(pl.multiple_of(other * unit, 16), unit)], l2.at[e], P2, partner).start()
    rc(st1.at[r, other], l1.at[r, e], P1 + other, partner, P1 + e).start()
    for k in (2, 1, 3):
        for h in range(2):
            rc(st1.at[wrap(r + k), h], l1.at[r, e], P1 + 2 * k + h,
               {"row": wrap(r + k), "col": c, "dep": h}, P1 + 2 * k + e).start()
    rc(lnv.at[e], lnv.at[e], DLN, partner).start()
    rc(x_hbm, xf.at[e], DX, partner).start()
    rc(g_hbm, gf.at[e], DG, partner).start()
    for k in range(1, RING):
        rc(bi.at[c], bi.at[c], BI + k, {"row": r, "col": wrap(c + k), "dep": e}).start()
    l1[r, e] = st1[r, e]

    def w1u(b, s):
        return wg.at[0, b, s]

    def w2u(b, s):
        return wg.at[1, b, s]

    load_w2.wait()
    arrive(l2.at[other], P2)
    wg[1, p, q, :, 0:half] = l2[0]
    wg[1, p, q, :, half:width] = l2[1]
    go(w2u(p, q), M2, m_right)
    go(w2u(p, q), S2, s_right)
    go(w2u(p, q), S4, s_left)
    go(w2u(p, q), M6, m_left)

    arrive(l1.at[r, other], P1 + other)
    for k in range(1, RING):
        for h in range(2):
            arrive(l1.at[wrap(r - k), h], P1 + 2 * k + h)
    wg[0, p, q] = jnp.concatenate([unpack(l1[k, h].astype(F32)) for h in range(2) for k in range(RING)], axis=1).astype(BF16)
    go(w1u(p, q), M1, m_left)
    go(w1u(p, q), S1, s_right)
    go(w1u(p, q), S3, s_left)
    go(w1u(p, q), M5, m_right)

    arrive(w2u(p, ql), S2)
    go(w2u(p, ql), S6, s_right)
    arrive(w2u(p, qr), S4)
    go(w2u(p, qr), M2 + 1, m_right)
    go(w2u(p, ql), M2 + 2, m_right)
    go(w2u(p, qr), M6 + 1, m_left)
    go(w2u(p, ql), M6 + 2, m_left)

    def nth(t):
        return wrap(q + gray(t))

    arrive(lnv.at[other], DLN)
    load_x.wait()
    arrive(xf.at[other], DX)
    load_g.wait()
    arrive(gf.at[other], DG)
    vv[...] = jnp.zeros_like(vv)
    def norm_tile(t, carry):
        rows = pl.ds(pl.multiple_of(t * tile, tile), tile)
        x0, x1 = xf[0, rows].astype(F32), xf[1, rows].astype(F32)
        total = jnp.sum(x0, axis=1, keepdims=True) + jnp.sum(x1, axis=1, keepdims=True)
        squares = jnp.sum(x0 * x0, axis=1, keepdims=True) + jnp.sum(x1 * x1, axis=1, keepdims=True)
        mean = total / width
        inv = lax.rsqrt(squares / width - mean * mean + LN_EPS)
        mean_s[rows] = mean
        inv_s[rows] = inv
        ab[rows, 0:half] = ((x0 - mean) * inv * lnv[0, 0:1] + lnv[0, 1:2]).astype(BF16)
        ab[rows, half:width] = ((x1 - mean) * inv * lnv[1, 0:1] + lnv[1, 1:2]).astype(BF16)
        gb[rows, 0:half] = gf[0, rows]
        gb[rows, half:width] = gf[1, rows]
        vv[RING:RING + 1] += jnp.sum(gf[e, rows].astype(F32), axis=0, keepdims=True)
        return carry

    lax.fori_loop(0, n_tiles // 2, norm_tile, 0)
    arrive(w1u(p, qr), S3)
    go(w1u(p, qr), S5, s_left)
    go(w1u(p, qr), M1 + 1, m_left)
    lax.fori_loop(n_tiles // 2, n_tiles, norm_tile, 0)

    def relay1(t):
        arrive(w1u(pr, nth(t)), M1 + t)
        go(w1u(pr, nth(t)), M3 + t, m_left)

    def relay2(t):
        arrive(w2u(pl_, nth(t)), M2 + t)
        go(w2u(pl_, nth(t)), M4 + t, m_right)

    arrive(w1u(p, ql), S1)
    go(w1u(p, ql), M1 + 2, m_left)
    relay2(0)
    for k in range(1, RING):
        arrive(bi.at[wrap(c - k)], BI + k)
    for b in range(RING):
        for k in range(RING):
            flat = bi[b, 0:1, 2 * k * unit:(2 * k + 1) * unit]
            across = bi[k, 0:1, (2 * b + 1) * unit:(2 * b + 2) * unit]
            bias_u[b, k, 0:1, 0:unit] = jnp.where(e == 0, flat, across)
    arrive(w2u(p, qo), S6)
    go(w2u(p, qo), M2 + 3, m_right)
    relay1(0)
    relay2(1)
    arrive(w1u(p, qo), S5)
    go(w1u(p, qo), M1 + 3, m_left)
    relay2(2)

    def block(slot, b, hook=None, send_part=None):
        bias = jnp.concatenate([bias_u[b, u, 0:1, 0:unit] for u in range(RING)], axis=1)

        def block_tile(t, carry):
            rows = pl.ds(pl.multiple_of(t * tile, tile), tile)
            pre = dot(ab[rows, :], wg[0, b].reshape(fb, width), ((1,), (1,))) + bias
            squared = pre * pre
            tanh_val = jnp.tanh(GELU_K * (pre + GELU_C * pre * squared))
            hs[slot, rows] = (0.5 * pre * (1.0 + tanh_val)).astype(BF16)
            slope = 0.5 * (1.0 + tanh_val) + 0.5 * pre * (1.0 - tanh_val * tanh_val) * GELU_K * (1.0 + 3.0 * GELU_C * squared)
            pre_grad = dot(gb[rows, :], wg[1, b].reshape(fb, width), ((1,), (1,))) * slope
            vv[pl.ds(b, 1)] += jnp.sum(pre_grad, axis=0, keepdims=True)
            dcs[slot, rows] = pre_grad.astype(BF16)
            if hook is not None:
                hook(t)
            return carry

        lax.fori_loop(0, n_tiles, block_tile, 0)
        for i, (rows_of, columns_of) in enumerate(((dcs, ab), (hs, gb))):
            gw[i, b] = dot(rows_of[slot], columns_of[...], ((0,), (0,))).reshape(RING, unit, width)
            if send_part is not None:
                send_part(i)

    def half_block(slot, b, part, units, send_part):
        bias = jnp.concatenate([bias_u[b, u, 0:1, 0:unit] for u in units], axis=1)
        columns = slice(2 * part * unit, 2 * (part + 1) * unit)

        def half_tile(t, carry):
            rows = pl.ds(pl.multiple_of(t * tile, tile), tile)
            w1, w2 = (jnp.concatenate([wg[i, b, u] for u in units], axis=0) for i in range(2))
            pre = dot(ab[rows, :], w1, ((1,), (1,))) + bias
            squared = pre * pre
            tanh_val = jnp.tanh(GELU_K * (pre + GELU_C * pre * squared))
            hidden = (0.5 * pre * (1.0 + tanh_val)).astype(BF16)
            hs2[rows, :] = hidden
            hs[slot, rows, columns] = hidden
            slope = 0.5 * (1.0 + tanh_val) + 0.5 * pre * (1.0 - tanh_val * tanh_val) * GELU_K * (1.0 + 3.0 * GELU_C * squared)
            pre_grad = dot(gb[rows, :], w2, ((1,), (1,))) * slope
            sums = jnp.sum(pre_grad, axis=0, keepdims=True)
            for j, u in enumerate(units):
                db_u[u, 0:1, 0:unit] += sums[:, j * unit:(j + 1) * unit]
            lowp = pre_grad.astype(BF16)
            dcs2[rows, :] = lowp
            dcs[slot, rows, columns] = lowp
            return carry

        lax.fori_loop(0, n_tiles, half_tile, 0)
        for i, (rows_of, columns_of) in enumerate(((dcs2, ab), (hs2, gb))):
            out = dot(rows_of[...], columns_of[...], ((0,), (0,)))
            for j, u in enumerate(units):
                gw[i, b, u] = out[j * unit:(j + 1) * unit]
            send_part(i)

    def relay_gather(t):
        @pl.when(t == 0)
        def _():
            relay1(1)

        @pl.when(t == 1)
        def _():
            relay1(2)
            relay2(3)

    assert n_tiles == RING
    block(0, p, hook=relay_gather)
    relay1(3)
    for t in range(1, RING):
        go(w1u(p, nth(t)), M5 + t, m_right)
    go(w2u(p, qo), M6 + 3, m_left)

    def back1(t):
        return wrap(q - gray(RING - 1 - t))

    def back2(t):
        return wrap(q + gray(RING - 1 - t))

    db_u[...] = jnp.zeros_like(db_u)
    for part in range(2):
        mine = (2 * part, 2 * part + 1)
        for t in mine:
            arrive(w2u(po, nth(t)), M4 + t)
            arrive(w1u(po, nth(t)), M3 + t)

        def send_opposite(i):
            for t in mine:
                u = nth(t)
                rc(gw.at[i, po, u], opp.at[i, u], (R2 if i else R1) + t, m_right if i else m_left).start()

        half_block(1, po, part, tuple(nth(t) for t in mine), send_opposite)
    vv[pl.ds(po, 1)] = jnp.concatenate([db_u[u, 0:1, 0:unit] for u in range(RING)], axis=1)

    for t in range(RING):
        arrive(w2u(pr, nth(t)), M6 + t)
    def send_right(i):
        if i == 0:
            rc(gw.at[0, pr], dirs.at[0], R3, m_right).start()

    block(2, pr, send_part=send_right)
    for t in range(RING):
        arrive(w1u(pl_, nth(t)), M5 + t)
    block(3, pl_)

    def direct2(t):
        u = back2(t)
        rc(gw.at[1, pl_, u], dirs.at[1, u], R4 + t, m_left).start()

    direct2(0)
    direct2(1)

    def product_tile(t, carry):
        rows = pl.ds(pl.multiple_of(t * tile, tile), tile)
        for i, (left, acc) in enumerate(((dcs, da_acc), (hs, y_acc))):
            weights = jnp.concatenate([wg[i, p].reshape(fb, width)] + [wg[i, po, nth(k)] for k in range(RING)]
                                      + [wg[i, b].reshape(fb, width) for b in (pr, pl_)], axis=0)
            out = dot(jnp.concatenate([left[slot, rows] for slot in range(RING)], axis=1), weights)
            acc[0, rows] = out[:, 0:half]
            acc[1, rows] = out[:, half:width]
        return carry

    lax.fori_loop(0, n_tiles, product_tile, 0)

    rc(y_acc.at[other], yr, EY, partner).start()
    rc(da_acc.at[other], dar, ED, partner).start()

    for t in range(RING):
        u1, u2 = back1(t), back2(t)
        arrive(opp.at[1, u2], R2 + (3, 2, 1, 0)[t])
        gw[1, pr, u2] += opp[1, u2]
        rc(gw.at[1, pr, u2], rel.at[1, u2], R6 + t, m_right).start()
        arrive(opp.at[0, u1], R1 + (3, 1, 2, 0)[t])
        gw[0, pl_, u1] += opp[0, u1]
        rc(gw.at[0, pl_, u1], rel.at[0, u1], R5 + t, m_left).start()
    direct2(2)
    direct2(3)

    lane = lax.broadcasted_iota(jnp.int32, (tile, 128), 1)

    def stat_tile(t, carry):
        rows = pl.ds(pl.multiple_of(t * tile, tile), tile)
        mean, inv = mean_s[rows], inv_s[rows]
        v0 = da_acc[0, rows] * lnv[0, 0:1]
        v1 = da_acc[1, rows] * lnv[1, 0:1]
        h0 = (xf[0, rows].astype(F32) - mean) * inv
        h1 = (xf[1, rows].astype(F32) - mean) * inv
        one = jnp.sum(v0, axis=1, keepdims=True) + jnp.sum(v1, axis=1, keepdims=True)
        two = jnp.sum(v0 * h0, axis=1, keepdims=True) + jnp.sum(v1 * h1, axis=1, keepdims=True)
        stat[rows] = jnp.where(lane < 64, one, two)
        return carry

    lax.fori_loop(0, n_tiles, stat_tile, 0)
    rc(stat, statr, ES, partner).start()

    arrive(yr, EY)
    arrive(dar, ED)
    arrive(statr, ES)
    b_down = bd_ref[...].astype(F32).reshape(1, half)

    def out_tile(t, carry):
        rows = pl.ds(pl.multiple_of(t * tile, tile), tile)
        x_own = xf[e, rows].astype(F32)
        y_ref[rows] = (x_own + (y_acc[e, rows] + yr[rows]) + b_down).astype(BF16)
        norm_grad = da_acc[e, rows] + dar[rows]
        sums = (stat[rows] + statr[rows]) / width
        inv = inv_s[rows]
        x_hat = (x_own - mean_s[rows]) * inv
        value = norm_grad * lnv[e, 0:1]
        dx_ref[rows] = (gf[e, rows].astype(F32) + inv * (value - sums[:, 0:1] - x_hat * sums[:, 64:65])).astype(BF16)
        vv[RING + 1:RING + 2] += jnp.sum(norm_grad * x_hat, axis=0, keepdims=True)
        vv[RING + 2:RING + 3] += jnp.sum(norm_grad, axis=0, keepdims=True)
        return carry

    lax.fori_loop(0, n_tiles, out_tile, 0)

    vs[q] = vv[...]
    for k, d in ((1, s_right), (2, s_opp_dev), (3, s_left)):
        go(vs.at[q], VS + k, d)
    for k in range(1, RING):
        arrive(vs.at[wrap(q - k)], VS + k)
    vm[p] = ((vs[0] + vs[1]) + vs[2]) + vs[3]
    for k, d in ((1, m_right), (2, m_opp), (3, m_left)):
        go(vm.at[p], VM + k, d)

    sent(l2.at[0], P2)
    sent(l1.at[0, 0], P1 + other)
    for k in range(1, RING):
        for h in range(2):
            sent(l1.at[0, 0], P1 + 2 * k + h)
        sent(bi.at[c], BI + k)
        sent(vs.at[q], VS + k)
    sent(lnv.at[0], DLN)
    sent(x_hbm, DX)
    sent(g_hbm, DG)
    for sem in (S1, S2, S3, S4, S5, S6):
        sent(w1u(p, q), sem)
    for t in range(RING):
        for sem in (M1, M2, M3, M4, M5, M6):
            sent(w1u(p, q), sem + t)
        for sem in (R1, R2):
            sent(gw.at[0, p, q], sem + t)
    sent(yr, EY)
    sent(dar, ED)
    sent(stat, ES)
    sent(gw.at[0, p, q], R4)
    sent(gw.at[0, p, q], R4 + 1)

    arrive(dirs.at[0], R3)

    def reduce1(t):
        u = back1(t)
        arrive(rel.at[0, u], R5 + t)
        gw[0, p, u] += dirs[0, u] + rel[0, u]
        if t == 0:
            rc(gw.at[0, p, u], s_opp.at[0], Q1, s_left).start()
        if t == 1:
            rc(gw.at[0, p, u], s_dir.at[0], Q3, s_right).start()
        if t == 2:
            arrive(s_opp.at[0], Q1)
            gw[0, p, u] += s_opp[0]
            rc(gw.at[0, p, u], s_rel.at[0], Q5, s_left).start()

    def reduce2(t):
        u = back2(t)
        arrive(dirs.at[1, u], R4 + t)
        arrive(rel.at[1, u], R6 + t)
        gw[1, p, u] += dirs[1, u] + rel[1, u]
        if t == 0:
            rc(gw.at[1, p, u], s_opp.at[1], Q2, s_right).start()
        if t == 1:
            rc(gw.at[1, p, u], s_dir.at[1], Q4, s_left).start()
        if t == 2:
            arrive(s_opp.at[1], Q2)
            gw[1, p, u] += s_opp[1]
            rc(gw.at[1, p, u], s_rel.at[1], Q6, s_right).start()

    reduce1(0)
    reduce1(1)
    reduce2(0)
    reduce1(2)
    reduce2(1)
    reduce1(3)
    reduce2(2)

    reduce2(3)

    arrive(s_dir.at[0], Q3)
    arrive(s_rel.at[0], Q5)
    done1 = gw[0, p, q] + s_dir[0] + s_rel[0]
    for k in range(RING):
        for h in range(2):
            start = (h * RING + k) * unit
            f1[k, h] = pack(done1[:, start:start + unit]).astype(BF16)
    for k in (2, 1, 3):
        for h in range(2):
            rc(f1.at[wrap(r + k), h], f1l.at[r, e], F1 + 2 * k + h,
               {"row": wrap(r + k), "col": c, "dep": h}, F1 + 2 * k + e).start()
    rc(f1.at[r, other], f1l.at[r, e], F1 + other, partner, F1 + e).start()
    f1l[r, e] = f1[r, e]

    for k in range(1, RING):
        arrive(vm.at[wrap(p - k)], VM + k)
    vp[e] = ((vm[0] + vm[1]) + vm[2]) + vm[3]
    go(vp.at[e], VP, partner)
    arrive(s_dir.at[1], Q4)
    arrive(s_rel.at[1], Q6)
    done2 = (gw[1, p, q] + s_dir[1] + s_rel[1]).astype(BF16)
    f2[0] = done2[:, 0:half]
    f2[1] = done2[:, half:width]
    rc(f2.at[other], f2l.at[e], F2, partner).start()
    f2l[e] = f2[e]

    arrive(vp.at[other], VP)
    pieces = []
    for k in range(RING):
        pieces.append(vp[0, pl.ds(c, 1)][:, k * unit:(k + 1) * unit])
        row = vp[1, k:k + 1]
        piece = row[:, 0:unit]
        for j in range(1, RING):
            piece = jnp.where(c == j, row[:, j * unit:(j + 1) * unit], piece)
        pieces.append(piece)
    dbu_ref[...] = jnp.concatenate(pieces, axis=1).reshape(dbu_ref.shape)
    dbd_ref[...] = vp[e, RING:RING + 1].reshape(dbd_ref.shape)
    dsc_ref[...] = vp[e, RING + 1:RING + 2].reshape(dsc_ref.shape)
    dsh_ref[...] = vp[e, RING + 2:RING + 3].reshape(dsh_ref.shape)

    sent(f1.at[0, 0], F1 + other)
    for k in range(1, RING):
        for h in range(2):
            sent(f1.at[0, 0], F1 + 2 * k + h)
        sent(vm.at[p], VM + k)
    sent(f2.at[0], F2)
    for sem in [R5 + t for t in range(RING)] + [R6 + t for t in range(RING)] + [R4 + 2, R4 + 3, Q1, Q2, Q3, Q4, Q5, Q6]:
        sent(gw.at[0, p, q], sem)
    sent(gw.at[0, p], R3)
    sent(vp.at[e], VP)

    arrive(f2l.at[other], F2)
    dw2_ref[0:unit] = f2l[0]
    dw2_ref[unit:2 * unit] = f2l[1]
    arrive(f1l.at[r, other], F1 + other)
    for k in range(1, RING):
        for h in range(2):
            arrive(f1l.at[wrap(r - k), h], F1 + 2 * k + h)
    turned = jnp.concatenate([unpack(f1l[k, h].astype(F32)) for k in range(RING) for h in range(2)], axis=0)
    turned = jnp.concatenate([turned, jnp.zeros((2 * fb, LANES - unit), F32)], axis=1)
    dw1_ref[...] = turned.T[0:unit].astype(BF16)


def copy_out(*refs):
    n = len(refs) // 2
    copies = [pltpu.make_async_copy(refs[i], refs[n + i], refs[2 * n].at[i]) for i in range(n)]
    for copy in copies:
        copy.start()
    for copy in copies:
        copy.wait()


def solution(mesh):
    assert mesh.shape["row"] == RING and mesh.shape["col"] == RING and mesh.shape["dep"] == 2
    tok_spec = P(("part", "row", "col"), "dep")
    vec_dep = P("dep")
    part_dep = P(("part", "dep"))
    in_specs = (tok_spec, vec_dep, vec_dep, P(("dep", "row"), "col"), P("col"), P(("col", "row"), "dep"), vec_dep, tok_spec)
    out_specs = (tok_spec, tok_spec, P(("part", "dep", "row"), "col"), P(("part", "col")), P(("part", "col", "row"), "dep"), part_dep, part_dep, part_dep)

    def local_step(x_in, ln_scale, ln_shift, w_up, b_up, w_down, b_down, y_grad):
        tokens, half = x_in.shape
        width = 2 * half
        unit = w_down.shape[0] // 2
        fb = RING * unit
        assert w_up.shape == (unit, 2 * fb) and half == RING * unit and fb == half
        tile = tokens // RING
        packed = (RING, 2, 3 * unit // 4, LANES)
        assert 3 * LANES == 4 * unit
        hbm_spec = pl.BlockSpec(memory_space=pltpu.HBM)
        vmem_spec = pl.BlockSpec(memory_space=pltpu.VMEM)
        vmem = pltpu.VMEM
        scratch = [
            vmem((unit, 2 * fb), BF16),
            vmem(packed, BF16), vmem(packed, BF16), vmem((2, unit, half), BF16),
            vmem((2, tokens, half), BF16), vmem((2, tokens, half), BF16),
            vmem((2, 8, half), F32),
            vmem((2, RING, RING, unit, width), BF16),
            vmem((RING, 1, 2 * fb), F32), vmem((RING, RING, 8, LANES), F32),
            vmem((tokens, width), BF16), vmem((tokens, width), BF16),
            vmem((tokens, 1), F32), vmem((tokens, 1), F32),
            vmem((2, tokens, half), F32), vmem((2, tokens, half), F32),
            vmem((tokens, half), F32), vmem((tokens, half), F32),
            vmem((tokens, 128), F32), vmem((tokens, 128), F32),
            vmem((RING, tokens, fb), BF16), vmem((RING, tokens, fb), BF16),
            vmem((tokens, 2 * unit), BF16), vmem((tokens, 2 * unit), BF16), vmem((RING, 8, LANES), F32),
            vmem((2, RING, RING, unit, width), F32),
            vmem((2, RING, unit, width), F32), vmem((2, RING, unit, width), F32), vmem((2, RING, unit, width), F32),
            vmem((2, unit, width), F32), vmem((2, unit, width), F32), vmem((2, unit, width), F32),
            vmem((8, half), F32), vmem((RING, 8, half), F32), vmem((RING, 8, half), F32), vmem((2, 8, half), F32),
            vmem(packed, BF16), vmem(packed, BF16),
            vmem((2, unit, half), BF16), vmem((2, unit, half), BF16),
            vmem((half,), F32), vmem((half,), F32), vmem((2 * fb,), BF16), vmem((half,), BF16),
            pltpu.SemaphoreType.DMA((N_SEM,)), pltpu.SemaphoreType.DMA((N_SEM,)),
        ]
        shapes = (
            jax.ShapeDtypeStruct((tokens, half), BF16), jax.ShapeDtypeStruct((tokens, half), BF16),
            jax.ShapeDtypeStruct(w_up.shape, BF16), jax.ShapeDtypeStruct(b_up.shape, F32),
            jax.ShapeDtypeStruct(w_down.shape, BF16), jax.ShapeDtypeStruct((half,), F32),
            jax.ShapeDtypeStruct((half,), F32), jax.ShapeDtypeStruct((half,), F32))
        outs = pl.pallas_call(
            functools.partial(kernel, tile),
            out_shape=shapes,
            in_specs=[hbm_spec] * 8,
            out_specs=(vmem_spec,) * 8,
            scratch_shapes=scratch,
            compiler_params=pltpu.CompilerParams(collective_id=0, has_side_effects=True, vmem_limit_bytes=51 * 1024 * 1024),
        )(*(pltpu.with_memory_space_constraint(v, pltpu.HBM) for v in (x_in, ln_scale, ln_shift, w_up, b_up, w_down, b_down, y_grad)))
        return pl.pallas_call(
            copy_out,
            out_shape=shapes,
            in_specs=[vmem_spec] * len(shapes),
            out_specs=(hbm_spec,) * len(shapes),
            scratch_shapes=[pltpu.SemaphoreType.DMA((len(shapes),))],
            compiler_params=pltpu.CompilerParams(vmem_limit_bytes=4 * 1024 * 1024),
        )(*outs)

    return jax.shard_map(local_step, mesh=mesh, in_specs=in_specs, out_specs=out_specs, check_vma=False)
```

```python
import functools

import jax
import jax.numpy as jnp
from jax import lax
from jax.experimental import pallas as pl
from jax.experimental.pallas import tpu as pltpu
from jax.sharding import PartitionSpec as P

LN_EPS = 1e-5
GELU_K = 0.7978845608028654
GELU_C = 0.044715
MESH = pl.DeviceIdType.MESH
F32 = jnp.float32
BF16 = jnp.bfloat16
RING = 4
LANES = 128

_next = [0]


def _ids(count=1):
    base = _next[0]
    _next[0] += count
    return base


IN_SEM = _ids(8)
P1 = _ids(2 * RING)
P2, DX, DG, DLN = _ids(), _ids(), _ids(), _ids()
BI = _ids(RING)
S1, S2, S3, S4, S5, S6 = (_ids() for _ in range(6))
M1, M2, M3, M4 = (_ids(RING) for _ in range(4))
M5, M6 = _ids(RING), _ids(RING)
R1, R2, R5, R6 = (_ids(RING) for _ in range(4))
R3, R4 = _ids(), _ids(RING)
Q1, Q2, Q3, Q4, Q5, Q6 = (_ids() for _ in range(6))
VM, VS = _ids(RING), _ids(RING)
VP = _ids()
EY, ED, ES = _ids(), _ids(), _ids()
F1 = _ids(2 * RING)
F2 = _ids()
N_SEM = _next[0]


def gray(t):
    return t + (t // 2) * (5 - 2 * t)


def dot(a, b, dims=((1,), (0,))):
    return lax.dot_general(a, b, (dims, ((), ())), preferred_element_type=F32)


def pack(piece):
    u = piece.shape[0]
    cut, third = 3 * u // 4, u // 3
    beside = jnp.concatenate([piece[cut:, k * third:(k + 1) * third] for k in range(3)], axis=0)
    return jnp.concatenate([piece[:cut], beside], axis=1)


def unpack(packed):
    cut = packed.shape[0]
    u = 4 * cut // 3
    quarter = u - cut
    below = jnp.concatenate([packed[k * quarter:(k + 1) * quarter, u:] for k in range(3)], axis=1)
    return jnp.concatenate([packed[:, :u], below], axis=0)


def kernel(tile, x_hbm, sc_hbm, sh_hbm, w1_hbm, bu_hbm, w2_hbm, bd_hbm, g_hbm,
           y_ref, dx_ref, dw1_ref, dbu_ref, dw2_ref, dbd_ref, dsc_ref, dsh_ref,
           w1v, st1, l1, l2, xf, gf, lnv, wg, bi, bias_u, ab, gb, mean_s, inv_s,
           y_acc, da_acc, yr, dar, stat, statr, hs, dcs, hs2, dcs2, db_u, gw, opp, dirs, rel, s_opp, s_dir, s_rel,
           vv, vm, vs, vp, f1, f1l, f2, f2l, sc_ref, sh_ref, bu_ref, bd_ref, send, recv):
    r, c, e = lax.axis_index("row"), lax.axis_index("col"), lax.axis_index("dep")
    p = c + e * (r - c)
    q = r + e * (c - r)
    tokens, half = xf.shape[1], xf.shape[2]
    width = 2 * half
    unit = l2.shape[1]
    fb = RING * unit
    n_tiles = tokens // tile
    other = 1 - e

    def wrap(v):
        return lax.rem(v + 2 * RING, RING)

    def dev(pp, qq):
        return {"row": qq + e * (pp - qq), "col": pp + e * (qq - pp), "dep": e}

    m_right, m_left, m_opp = dev(wrap(p + 1), q), dev(wrap(p - 1), q), dev(wrap(p + 2), q)
    s_right, s_left, s_opp_dev = dev(p, wrap(q + 1)), dev(p, wrap(q - 1)), dev(p, wrap(q + 2))
    partner = {"row": r, "col": c, "dep": other}
    pr, pl_, po = wrap(p + 1), wrap(p - 1), wrap(p + 2)
    qr, ql, qo = wrap(q + 1), wrap(q - 1), wrap(q + 2)

    def rc(src, dst, ssem, device, rsem=None):
        return pltpu.make_async_remote_copy(
            src_ref=src, dst_ref=dst, send_sem=send.at[ssem], recv_sem=recv.at[ssem if rsem is None else rsem],
            device_id=device, device_id_type=MESH)

    def arrive(dst, rsem):
        rc(dst, dst, rsem, partner).wait_recv()

    def sent(src, ssem):
        rc(src, src, ssem, partner).wait_send()

    def go(ref, sem, device):
        rc(ref, ref, sem, device).start()

    barrier = pltpu.get_barrier_semaphore()
    peers = [m_opp, s_opp_dev]
    peers += [{"row": wrap(r + k), "col": c, "dep": other} for k in (2, 1, 3)]
    peers += [m_right, m_left, s_right, s_left, partner]
    for d in peers:
        pl.semaphore_signal(barrier, inc=1, device_id=d, device_id_type=MESH)

    load_w1 = pltpu.make_async_copy(w1_hbm, w1v, recv.at[IN_SEM])
    load_w2 = pltpu.make_async_copy(w2_hbm.at[pl.ds(pl.multiple_of(e * unit, 16), unit)], l2.at[e], recv.at[IN_SEM + 1])
    load_x = pltpu.make_async_copy(x_hbm, xf.at[e], recv.at[IN_SEM + 2])
    load_g = pltpu.make_async_copy(g_hbm, gf.at[e], recv.at[IN_SEM + 3])
    load_vectors = [pltpu.make_async_copy(src, dst, recv.at[IN_SEM + 4 + i]) for i, (src, dst) in enumerate(
        ((sc_hbm, sc_ref), (sh_hbm, sh_ref), (bu_hbm, bu_ref), (bd_hbm, bd_ref)))]
    load_w1.start()
    load_w2.start()
    for load in load_vectors:
        load.start()
    load_x.start()
    load_g.start()

    load_w1.wait()
    turned = w1v[...].astype(F32)
    turned = jnp.concatenate([turned, jnp.zeros((LANES - unit, 2 * fb), F32)], axis=0).T
    for k in range(RING):
        for h in range(2):
            st1[k, h] = pack(turned[(2 * k + h) * unit:(2 * k + h + 1) * unit, 0:unit]).astype(BF16)

    for load in load_vectors:
        load.wait()
    lnv[e, 0:1] = sc_ref[...].reshape(1, half)
    lnv[e, 1:2] = sh_ref[...].reshape(1, half)
    bi[c] = bu_ref[...].astype(F32).reshape(1, 2 * fb)

    pl.semaphore_wait(barrier, len(peers))

    rc(w2_hbm.at[pl.ds(pl.multiple_of(other * unit, 16), unit)], l2.at[e], P2, partner).start()
    rc(st1.at[r, other], l1.at[r, e], P1 + other, partner, P1 + e).start()
    for k in (2, 1, 3):
        for h in range(2):
            rc(st1.at[wrap(r + k), h], l1.at[r, e], P1 + 2 * k + h,
               {"row": wrap(r + k), "col": c, "dep": h}, P1 + 2 * k + e).start()
    rc(lnv.at[e], lnv.at[e], DLN, partner).start()
    rc(x_hbm, xf.at[e], DX, partner).start()
    rc(g_hbm, gf.at[e], DG, partner).start()
    for k in range(1, RING):
        rc(bi.at[c], bi.at[c], BI + k, {"row": r, "col": wrap(c + k), "dep": e}).start()
    l1[r, e] = st1[r, e]

    def w1u(b, s):
        return wg.at[0, b, s]

    def w2u(b, s):
        return wg.at[1, b, s]

    load_w2.wait()
    arrive(l2.at[other], P2)
    wg[1, p, q, :, 0:half] = l2[0]
    wg[1, p, q, :, half:width] = l2[1]
    go(w2u(p, q), M2, m_right)
    go(w2u(p, q), S2, s_right)
    go(w2u(p, q), S4, s_left)
    go(w2u(p, q), M6, m_left)

    arrive(l1.at[r, other], P1 + other)
    for k in range(1, RING):
        for h in range(2):
            arrive(l1.at[wrap(r - k), h], P1 + 2 * k + h)
    wg[0, p, q] = jnp.concatenate([unpack(l1[k, h].astype(F32)) for h in range(2) for k in range(RING)], axis=1).astype(BF16)
    go(w1u(p, q), M1, m_left)
    go(w1u(p, q), S1, s_right)
    go(w1u(p, q), S3, s_left)
    go(w1u(p, q), M5, m_right)

    arrive(w2u(p, ql), S2)
    go(w2u(p, ql), S6, s_right)
    arrive(w2u(p, qr), S4)
    go(w2u(p, qr), M2 + 1, m_right)
    go(w2u(p, ql), M2 + 2, m_right)
    go(w2u(p, qr), M6 + 1, m_left)
    go(w2u(p, ql), M6 + 2, m_left)

    def nth(t):
        return wrap(q + gray(t))

    arrive(lnv.at[other], DLN)
    load_x.wait()
    arrive(xf.at[other], DX)
    load_g.wait()
    arrive(gf.at[other], DG)
    vv[...] = jnp.zeros_like(vv)
    def norm_tile(t, carry):
        rows = pl.ds(pl.multiple_of(t * tile, tile), tile)
        x0, x1 = xf[0, rows].astype(F32), xf[1, rows].astype(F32)
        total = jnp.sum(x0, axis=1, keepdims=True) + jnp.sum(x1, axis=1, keepdims=True)
        squares = jnp.sum(x0 * x0, axis=1, keepdims=True) + jnp.sum(x1 * x1, axis=1, keepdims=True)
        mean = total / width
        inv = lax.rsqrt(squares / width - mean * mean + LN_EPS)
        mean_s[rows] = mean
        inv_s[rows] = inv
        ab[rows, 0:half] = ((x0 - mean) * inv * lnv[0, 0:1] + lnv[0, 1:2]).astype(BF16)
        ab[rows, half:width] = ((x1 - mean) * inv * lnv[1, 0:1] + lnv[1, 1:2]).astype(BF16)
        gb[rows, 0:half] = gf[0, rows]
        gb[rows, half:width] = gf[1, rows]
        vv[RING:RING + 1] += jnp.sum(gf[e, rows].astype(F32), axis=0, keepdims=True)
        return carry

    lax.fori_loop(0, n_tiles // 2, norm_tile, 0)
    arrive(w1u(p, qr), S3)
    go(w1u(p, qr), S5, s_left)
    go(w1u(p, qr), M1 + 1, m_left)
    lax.fori_loop(n_tiles // 2, n_tiles, norm_tile, 0)

    def relay1(t):
        arrive(w1u(pr, nth(t)), M1 + t)
        go(w1u(pr, nth(t)), M3 + t, m_left)

    def relay2(t):
        arrive(w2u(pl_, nth(t)), M2 + t)
        go(w2u(pl_, nth(t)), M4 + t, m_right)

    arrive(w1u(p, ql), S1)
    go(w1u(p, ql), M1 + 2, m_left)
    relay2(0)
    for k in range(1, RING):
        arrive(bi.at[wrap(c - k)], BI + k)
    for b in range(RING):
        for k in range(RING):
            flat = bi[b, 0:1, 2 * k * unit:(2 * k + 1) * unit]
            across = bi[k, 0:1, (2 * b + 1) * unit:(2 * b + 2) * unit]
            bias_u[b, k, 0:1, 0:unit] = jnp.where(e == 0, flat, across)
    arrive(w2u(p, qo), S6)
    go(w2u(p, qo), M2 + 3, m_right)
    relay1(0)
    relay2(1)
    arrive(w1u(p, qo), S5)
    go(w1u(p, qo), M1 + 3, m_left)
    relay2(2)

    def block(slot, b, hook=None, send_part=None):
        bias = jnp.concatenate([bias_u[b, u, 0:1, 0:unit] for u in range(RING)], axis=1)

        def block_tile(t, carry):
            rows = pl.ds(pl.multiple_of(t * tile, tile), tile)
            pre = dot(ab[rows, :], wg[0, b].reshape(fb, width), ((1,), (1,))) + bias
            squared = pre * pre
            tanh_val = jnp.tanh(GELU_K * (pre + GELU_C * pre * squared))
            hs[slot, rows] = (0.5 * pre * (1.0 + tanh_val)).astype(BF16)
            slope = 0.5 * (1.0 + tanh_val) + 0.5 * pre * (1.0 - tanh_val * tanh_val) * GELU_K * (1.0 + 3.0 * GELU_C * squared)
            pre_grad = dot(gb[rows, :], wg[1, b].reshape(fb, width), ((1,), (1,))) * slope
            vv[pl.ds(b, 1)] += jnp.sum(pre_grad, axis=0, keepdims=True)
            dcs[slot, rows] = pre_grad.astype(BF16)
            if hook is not None:
                hook(t)
            return carry

        lax.fori_loop(0, n_tiles, block_tile, 0)
        for i, (rows_of, columns_of) in enumerate(((dcs, ab), (hs, gb))):
            gw[i, b] = dot(rows_of[slot], columns_of[...], ((0,), (0,))).reshape(RING, unit, width)
            if send_part is not None:
                send_part(i)

    def half_block(slot, b, part, units, send_part):
        bias = jnp.concatenate([bias_u[b, u, 0:1, 0:unit] for u in units], axis=1)
        columns = slice(2 * part * unit, 2 * (part + 1) * unit)

        def half_tile(t, carry):
            rows = pl.ds(pl.multiple_of(t * tile, tile), tile)
            w1, w2 = (jnp.concatenate([wg[i, b, u] for u in units], axis=0) for i in range(2))
            pre = dot(ab[rows, :], w1, ((1,), (1,))) + bias
            squared = pre * pre
            tanh_val = jnp.tanh(GELU_K * (pre + GELU_C * pre * squared))
            hidden = (0.5 * pre * (1.0 + tanh_val)).astype(BF16)
            hs2[rows, :] = hidden
            hs[slot, rows, columns] = hidden
            slope = 0.5 * (1.0 + tanh_val) + 0.5 * pre * (1.0 - tanh_val * tanh_val) * GELU_K * (1.0 + 3.0 * GELU_C * squared)
            pre_grad = dot(gb[rows, :], w2, ((1,), (1,))) * slope
            sums = jnp.sum(pre_grad, axis=0, keepdims=True)
            for j, u in enumerate(units):
                db_u[u, 0:1, 0:unit] += sums[:, j * unit:(j + 1) * unit]
            lowp = pre_grad.astype(BF16)
            dcs2[rows, :] = lowp
            dcs[slot, rows, columns] = lowp
            return carry

        lax.fori_loop(0, n_tiles, half_tile, 0)
        for i, (rows_of, columns_of) in enumerate(((dcs2, ab), (hs2, gb))):
            out = dot(rows_of[...], columns_of[...], ((0,), (0,)))
            for j, u in enumerate(units):
                gw[i, b, u] = out[j * unit:(j + 1) * unit]
            send_part(i)

    def relay_gather(t):
        @pl.when(t == 0)
        def _():
            relay1(1)

        @pl.when(t == 1)
        def _():
            relay1(2)
            relay2(3)

    assert n_tiles == RING
    block(0, p, hook=relay_gather)
    relay1(3)
    for t in range(1, RING):
        go(w1u(p, nth(t)), M5 + t, m_right)
    go(w2u(p, qo), M6 + 3, m_left)

    def back1(t):
        return wrap(q - gray(RING - 1 - t))

    def back2(t):
        return wrap(q + gray(RING - 1 - t))

    db_u[...] = jnp.zeros_like(db_u)
    for part in range(2):
        mine = (2 * part, 2 * part + 1)
        for t in mine:
            arrive(w2u(po, nth(t)), M4 + t)
            arrive(w1u(po, nth(t)), M3 + t)

        def send_opposite(i):
            for t in mine:
                u = nth(t)
                rc(gw.at[i, po, u], opp.at[i, u], (R2 if i else R1) + t, m_right if i else m_left).start()

        half_block(1, po, part, tuple(nth(t) for t in mine), send_opposite)
    vv[pl.ds(po, 1)] = jnp.concatenate([db_u[u, 0:1, 0:unit] for u in range(RING)], axis=1)

    for t in range(RING):
        arrive(w2u(pr, nth(t)), M6 + t)
    def send_right(i):
        if i == 0:
            rc(gw.at[0, pr], dirs.at[0], R3, m_right).start()

    block(2, pr, send_part=send_right)
    for t in range(RING):
        arrive(w1u(pl_, nth(t)), M5 + t)
    block(3, pl_)

    def direct2(t):
        u = back2(t)
        rc(gw.at[1, pl_, u], dirs.at[1, u], R4 + t, m_left).start()

    direct2(0)
    direct2(1)

    def product_tile(t, carry):
        rows = pl.ds(pl.multiple_of(t * tile, tile), tile)
        for i, (left, acc) in enumerate(((dcs, da_acc), (hs, y_acc))):
            weights = jnp.concatenate([wg[i, p].reshape(fb, width)] + [wg[i, po, nth(k)] for k in range(RING)]
                                      + [wg[i, b].reshape(fb, width) for b in (pr, pl_)], axis=0)
            out = dot(jnp.concatenate([left[slot, rows] for slot in range(RING)], axis=1), weights)
            acc[0, rows] = out[:, 0:half]
            acc[1, rows] = out[:, half:width]
        return carry

    lax.fori_loop(0, n_tiles, product_tile, 0)

    rc(y_acc.at[other], yr, EY, partner).start()
    rc(da_acc.at[other], dar, ED, partner).start()

    for t in range(RING):
        u1, u2 = back1(t), back2(t)
        arrive(opp.at[1, u2], R2 + (3, 2, 1, 0)[t])
        gw[1, pr, u2] += opp[1, u2]
        rc(gw.at[1, pr, u2], rel.at[1, u2], R6 + t, m_right).start()
        arrive(opp.at[0, u1], R1 + (3, 1, 2, 0)[t])
        gw[0, pl_, u1] += opp[0, u1]
        rc(gw.at[0, pl_, u1], rel.at[0, u1], R5 + t, m_left).start()
    direct2(2)
    direct2(3)

    lane = lax.broadcasted_iota(jnp.int32, (tile, 128), 1)

    def stat_tile(t, carry):
        rows = pl.ds(pl.multiple_of(t * tile, tile), tile)
        mean, inv = mean_s[rows], inv_s[rows]
        v0 = da_acc[0, rows] * lnv[0, 0:1]
        v1 = da_acc[1, rows] * lnv[1, 0:1]
        h0 = (xf[0, rows].astype(F32) - mean) * inv
        h1 = (xf[1, rows].astype(F32) - mean) * inv
        one = jnp.sum(v0, axis=1, keepdims=True) + jnp.sum(v1, axis=1, keepdims=True)
        two = jnp.sum(v0 * h0, axis=1, keepdims=True) + jnp.sum(v1 * h1, axis=1, keepdims=True)
        stat[rows] = jnp.where(lane < 64, one, two)
        return carry

    lax.fori_loop(0, n_tiles, stat_tile, 0)
    rc(stat, statr, ES, partner).start()

    arrive(yr, EY)
    arrive(dar, ED)
    arrive(statr, ES)
    b_down = bd_ref[...].astype(F32).reshape(1, half)

    def out_tile(t, carry):
        rows = pl.ds(pl.multiple_of(t * tile, tile), tile)
        x_own = xf[e, rows].astype(F32)
        y_ref[rows] = (x_own + (y_acc[e, rows] + yr[rows]) + b_down).astype(BF16)
        norm_grad = da_acc[e, rows] + dar[rows]
        sums = (stat[rows] + statr[rows]) / width
        inv = inv_s[rows]
        x_hat = (x_own - mean_s[rows]) * inv
        value = norm_grad * lnv[e, 0:1]
        dx_ref[rows] = (gf[e, rows].astype(F32) + inv * (value - sums[:, 0:1] - x_hat * sums[:, 64:65])).astype(BF16)
        vv[RING + 1:RING + 2] += jnp.sum(norm_grad * x_hat, axis=0, keepdims=True)
        vv[RING + 2:RING + 3] += jnp.sum(norm_grad, axis=0, keepdims=True)
        return carry

    lax.fori_loop(0, n_tiles, out_tile, 0)

    vs[q] = vv[...]
    for k, d in ((1, s_right), (2, s_opp_dev), (3, s_left)):
        go(vs.at[q], VS + k, d)
    for k in range(1, RING):
        arrive(vs.at[wrap(q - k)], VS + k)
    vm[p] = ((vs[0] + vs[1]) + vs[2]) + vs[3]
    for k, d in ((1, m_right), (2, m_opp), (3, m_left)):
        go(vm.at[p], VM + k, d)

    sent(l2.at[0], P2)
    sent(l1.at[0, 0], P1 + other)
    for k in range(1, RING):
        for h in range(2):
            sent(l1.at[0, 0], P1 + 2 * k + h)
        sent(bi.at[c], BI + k)
        sent(vs.at[q], VS + k)
    sent(lnv.at[0], DLN)
    sent(x_hbm, DX)
    sent(g_hbm, DG)
    for sem in (S1, S2, S3, S4, S5, S6):
        sent(w1u(p, q), sem)
    for t in range(RING):
        for sem in (M1, M2, M3, M4, M5, M6):
            sent(w1u(p, q), sem + t)
        for sem in (R1, R2):
            sent(gw.at[0, p, q], sem + t)
    sent(yr, EY)
    sent(dar, ED)
    sent(stat, ES)
    sent(gw.at[0, p, q], R4)
    sent(gw.at[0, p, q], R4 + 1)

    arrive(dirs.at[0], R3)

    def reduce1(t):
        u = back1(t)
        arrive(rel.at[0, u], R5 + t)
        gw[0, p, u] += dirs[0, u] + rel[0, u]
        if t == 0:
            rc(gw.at[0, p, u], s_opp.at[0], Q1, s_left).start()
        if t == 1:
            rc(gw.at[0, p, u], s_dir.at[0], Q3, s_right).start()
        if t == 2:
            arrive(s_opp.at[0], Q1)
            gw[0, p, u] += s_opp[0]
            rc(gw.at[0, p, u], s_rel.at[0], Q5, s_left).start()

    def reduce2(t):
        u = back2(t)
        arrive(dirs.at[1, u], R4 + t)
        arrive(rel.at[1, u], R6 + t)
        gw[1, p, u] += dirs[1, u] + rel[1, u]
        if t == 0:
            rc(gw.at[1, p, u], s_opp.at[1], Q2, s_right).start()
        if t == 1:
            rc(gw.at[1, p, u], s_dir.at[1], Q4, s_left).start()
        if t == 2:
            arrive(s_opp.at[1], Q2)
            gw[1, p, u] += s_opp[1]
            rc(gw.at[1, p, u], s_rel.at[1], Q6, s_right).start()

    reduce1(0)
    reduce1(1)
    reduce2(0)
    reduce1(2)
    reduce2(1)
    reduce1(3)
    reduce2(2)

    arrive(s_dir.at[0], Q3)
    arrive(s_rel.at[0], Q5)
    done1 = gw[0, p, q] + s_dir[0] + s_rel[0]
    for k in range(RING):
        for h in range(2):
            start = (h * RING + k) * unit
            f1[k, h] = pack(done1[:, start:start + unit]).astype(BF16)
    for k in (2, 1, 3):
        for h in range(2):
            rc(f1.at[wrap(r + k), h], f1l.at[r, e], F1 + 2 * k + h,
               {"row": wrap(r + k), "col": c, "dep": h}, F1 + 2 * k + e).start()
    rc(f1.at[r, other], f1l.at[r, e], F1 + other, partner, F1 + e).start()
    f1l[r, e] = f1[r, e]
    reduce2(3)
    for k in range(1, RING):
        arrive(vm.at[wrap(p - k)], VM + k)
    vp[e] = ((vm[0] + vm[1]) + vm[2]) + vm[3]
    go(vp.at[e], VP, partner)
    arrive(s_dir.at[1], Q4)
    arrive(s_rel.at[1], Q6)
    done2 = (gw[1, p, q] + s_dir[1] + s_rel[1]).astype(BF16)
    f2[0] = done2[:, 0:half]
    f2[1] = done2[:, half:width]
    rc(f2.at[other], f2l.at[e], F2, partner).start()
    f2l[e] = f2[e]

    arrive(vp.at[other], VP)
    pieces = []
    for k in range(RING):
        pieces.append(vp[0, pl.ds(c, 1)][:, k * unit:(k + 1) * unit])
        row = vp[1, k:k + 1]
        piece = row[:, 0:unit]
        for j in range(1, RING):
            piece = jnp.where(c == j, row[:, j * unit:(j + 1) * unit], piece)
        pieces.append(piece)
    dbu_ref[...] = jnp.concatenate(pieces, axis=1).reshape(dbu_ref.shape)
    dbd_ref[...] = vp[e, RING:RING + 1].reshape(dbd_ref.shape)
    dsc_ref[...] = vp[e, RING + 1:RING + 2].reshape(dsc_ref.shape)
    dsh_ref[...] = vp[e, RING + 2:RING + 3].reshape(dsh_ref.shape)

    sent(f1.at[0, 0], F1 + other)
    for k in range(1, RING):
        for h in range(2):
            sent(f1.at[0, 0], F1 + 2 * k + h)
        sent(vm.at[p], VM + k)
    sent(f2.at[0], F2)
    for sem in [R5 + t for t in range(RING)] + [R6 + t for t in range(RING)] + [R4 + 2, R4 + 3, Q1, Q2, Q3, Q4, Q5, Q6]:
        sent(gw.at[0, p, q], sem)
    sent(gw.at[0, p], R3)
    sent(vp.at[e], VP)

    arrive(f2l.at[other], F2)
    dw2_ref[0:unit] = f2l[0]
    dw2_ref[unit:2 * unit] = f2l[1]
    arrive(f1l.at[r, other], F1 + other)
    for k in range(1, RING):
        for h in range(2):
            arrive(f1l.at[wrap(r - k), h], F1 + 2 * k + h)
    turned = jnp.concatenate([unpack(f1l[k, h].astype(F32)) for k in range(RING) for h in range(2)], axis=0)
    turned = jnp.concatenate([turned, jnp.zeros((2 * fb, LANES - unit), F32)], axis=1)
    dw1_ref[...] = turned.T[0:unit].astype(BF16)


def copy_out(*refs):
    n = len(refs) // 2
    copies = [pltpu.make_async_copy(refs[i], refs[n + i], refs[2 * n].at[i]) for i in range(n)]
    for copy in copies:
        copy.start()
    for copy in copies:
        copy.wait()


def solution(mesh):
    assert mesh.shape["row"] == RING and mesh.shape["col"] == RING and mesh.shape["dep"] == 2
    tok_spec = P(("part", "row", "col"), "dep")
    vec_dep = P("dep")
    part_dep = P(("part", "dep"))
    in_specs = (tok_spec, vec_dep, vec_dep, P(("dep", "row"), "col"), P("col"), P(("col", "row"), "dep"), vec_dep, tok_spec)
    out_specs = (tok_spec, tok_spec, P(("part", "dep", "row"), "col"), P(("part", "col")), P(("part", "col", "row"), "dep"), part_dep, part_dep, part_dep)

    def local_step(x_in, ln_scale, ln_shift, w_up, b_up, w_down, b_down, y_grad):
        tokens, half = x_in.shape
        width = 2 * half
        unit = w_down.shape[0] // 2
        fb = RING * unit
        assert w_up.shape == (unit, 2 * fb) and half == RING * unit and fb == half
        tile = tokens // RING
        packed = (RING, 2, 3 * unit // 4, LANES)
        assert 3 * LANES == 4 * unit
        hbm_spec = pl.BlockSpec(memory_space=pltpu.HBM)
        vmem_spec = pl.BlockSpec(memory_space=pltpu.VMEM)
        vmem = pltpu.VMEM
        scratch = [
            vmem((unit, 2 * fb), BF16),
            vmem(packed, BF16), vmem(packed, BF16), vmem((2, unit, half), BF16),
            vmem((2, tokens, half), BF16), vmem((2, tokens, half), BF16),
            vmem((2, 8, half), F32),
            vmem((2, RING, RING, unit, width), BF16),
            vmem((RING, 1, 2 * fb), F32), vmem((RING, RING, 8, LANES), F32),
            vmem((tokens, width), BF16), vmem((tokens, width), BF16),
            vmem((tokens, 1), F32), vmem((tokens, 1), F32),
            vmem((2, tokens, half), F32), vmem((2, tokens, half), F32),
            vmem((tokens, half), F32), vmem((tokens, half), F32),
            vmem((tokens, 128), F32), vmem((tokens, 128), F32),
            vmem((RING, tokens, fb), BF16), vmem((RING, tokens, fb), BF16),
            vmem((tokens, 2 * unit), BF16), vmem((tokens, 2 * unit), BF16), vmem((RING, 8, LANES), F32),
            vmem((2, RING, RING, unit, width), F32),
            vmem((2, RING, unit, width), F32), vmem((2, RING, unit, width), F32), vmem((2, RING, unit, width), F32),
            vmem((2, unit, width), F32), vmem((2, unit, width), F32), vmem((2, unit, width), F32),
            vmem((8, half), F32), vmem((RING, 8, half), F32), vmem((RING, 8, half), F32), vmem((2, 8, half), F32),
            vmem(packed, BF16), vmem(packed, BF16),
            vmem((2, unit, half), BF16), vmem((2, unit, half), BF16),
            vmem((half,), F32), vmem((half,), F32), vmem((2 * fb,), BF16), vmem((half,), BF16),
            pltpu.SemaphoreType.DMA((N_SEM,)), pltpu.SemaphoreType.DMA((N_SEM,)),
        ]
        shapes = (
            jax.ShapeDtypeStruct((tokens, half), BF16), jax.ShapeDtypeStruct((tokens, half), BF16),
            jax.ShapeDtypeStruct(w_up.shape, BF16), jax.ShapeDtypeStruct(b_up.shape, F32),
            jax.ShapeDtypeStruct(w_down.shape, BF16), jax.ShapeDtypeStruct((half,), F32),
            jax.ShapeDtypeStruct((half,), F32), jax.ShapeDtypeStruct((half,), F32))
        outs = pl.pallas_call(
            functools.partial(kernel, tile),
            out_shape=shapes,
            in_specs=[hbm_spec] * 8,
            out_specs=(vmem_spec,) * 8,
            scratch_shapes=scratch,
            compiler_params=pltpu.CompilerParams(collective_id=0, has_side_effects=True, vmem_limit_bytes=51 * 1024 * 1024),
        )(*(pltpu.with_memory_space_constraint(v, pltpu.HBM) for v in (x_in, ln_scale, ln_shift, w_up, b_up, w_down, b_down, y_grad)))
        return pl.pallas_call(
            copy_out,
            out_shape=shapes,
            in_specs=[vmem_spec] * len(shapes),
            out_specs=(hbm_spec,) * len(shapes),
            scratch_shapes=[pltpu.SemaphoreType.DMA((len(shapes),))],
            compiler_params=pltpu.CompilerParams(vmem_limit_bytes=4 * 1024 * 1024),
        )(*outs)

    return jax.shard_map(local_step, mesh=mesh, in_specs=in_specs, out_specs=out_specs, check_vma=False)
```

```python
import functools

import jax
import jax.numpy as jnp
from jax import lax
from jax.experimental import pallas as pl
from jax.experimental.pallas import tpu as pltpu
from jax.sharding import PartitionSpec as P

LN_EPS = 1e-5
GELU_K = 0.7978845608028654
GELU_C = 0.044715
MESH = pl.DeviceIdType.MESH
F32 = jnp.float32
BF16 = jnp.bfloat16
RING = 4
LANES = 128

_next = [0]


def _ids(count=1):
    base = _next[0]
    _next[0] += count
    return base


IN_SEM = _ids(8)
P1 = _ids(2 * RING)
P2, DX, DG, DLN = _ids(), _ids(), _ids(), _ids()
BI = _ids(RING)
S1, S2, S3, S4, S5, S6 = (_ids() for _ in range(6))
M1, M2, M3, M4 = (_ids(RING) for _ in range(4))
M5, M6 = _ids(RING), _ids(RING)
R1, R2, R5, R6 = (_ids(RING) for _ in range(4))
R3, R4 = _ids(), _ids(RING)
Q1, Q2, Q3, Q4, Q5, Q6 = (_ids() for _ in range(6))
VM, VS = _ids(RING), _ids(RING)
VP = _ids()
EY, ED, ES = _ids(), _ids(), _ids()
F1 = _ids(2 * RING)
F2 = _ids()
N_SEM = _next[0]


def gray(t):
    return t + (t // 2) * (5 - 2 * t)


def dot(a, b, dims=((1,), (0,))):
    return lax.dot_general(a, b, (dims, ((), ())), preferred_element_type=F32)


def pack(piece):
    u = piece.shape[0]
    cut, third = 3 * u // 4, u // 3
    beside = jnp.concatenate([piece[cut:, k * third:(k + 1) * third] for k in range(3)], axis=0)
    return jnp.concatenate([piece[:cut], beside], axis=1)


def unpack(packed):
    cut = packed.shape[0]
    u = 4 * cut // 3
    quarter = u - cut
    below = jnp.concatenate([packed[k * quarter:(k + 1) * quarter, u:] for k in range(3)], axis=1)
    return jnp.concatenate([packed[:, :u], below], axis=0)


def kernel(tile, x_hbm, sc_hbm, sh_hbm, w1_hbm, bu_hbm, w2_hbm, bd_hbm, g_hbm,
           y_ref, dx_ref, dw1_ref, dbu_ref, dw2_ref, dbd_ref, dsc_ref, dsh_ref,
           w1v, st1, l1, l2, xf, gf, lnv, wg, bi, bias_u, ab, gb, mean_s, inv_s,
           y_acc, da_acc, yr, dar, stat, statr, hs, dcs, hs2, dcs2, db_u, gw, opp, dirs, rel, s_opp, s_dir, s_rel,
           vv, vm, vs, vp, f1, f1l, f2, f2l, sc_ref, sh_ref, bu_ref, bd_ref, send, recv):
    r, c, e = lax.axis_index("row"), lax.axis_index("col"), lax.axis_index("dep")
    p = c + e * (r - c)
    q = r + e * (c - r)
    tokens, half = xf.shape[1], xf.shape[2]
    width = 2 * half
    unit = l2.shape[1]
    fb = RING * unit
    n_tiles = tokens // tile
    other = 1 - e

    def wrap(v):
        return lax.rem(v + 2 * RING, RING)

    def dev(pp, qq):
        return {"row": qq + e * (pp - qq), "col": pp + e * (qq - pp), "dep": e}

    m_right, m_left, m_opp = dev(wrap(p + 1), q), dev(wrap(p - 1), q), dev(wrap(p + 2), q)
    s_right, s_left, s_opp_dev = dev(p, wrap(q + 1)), dev(p, wrap(q - 1)), dev(p, wrap(q + 2))
    partner = {"row": r, "col": c, "dep": other}
    pr, pl_, po = wrap(p + 1), wrap(p - 1), wrap(p + 2)
    qr, ql, qo = wrap(q + 1), wrap(q - 1), wrap(q + 2)

    def rc(src, dst, ssem, device, rsem=None):
        return pltpu.make_async_remote_copy(
            src_ref=src, dst_ref=dst, send_sem=send.at[ssem], recv_sem=recv.at[ssem if rsem is None else rsem],
            device_id=device, device_id_type=MESH)

    def arrive(dst, rsem):
        rc(dst, dst, rsem, partner).wait_recv()

    def sent(src, ssem):
        rc(src, src, ssem, partner).wait_send()

    def go(ref, sem, device):
        rc(ref, ref, sem, device).start()

    barrier = pltpu.get_barrier_semaphore()
    peers = [m_opp, s_opp_dev]
    peers += [{"row": wrap(r + k), "col": c, "dep": other} for k in (2, 1, 3)]
    peers += [m_right, m_left, s_right, s_left, partner]
    for d in peers:
        pl.semaphore_signal(barrier, inc=1, device_id=d, device_id_type=MESH)

    load_w1 = pltpu.make_async_copy(w1_hbm, w1v, recv.at[IN_SEM])
    load_w2 = pltpu.make_async_copy(w2_hbm.at[pl.ds(pl.multiple_of(e * unit, 16), unit)], l2.at[e], recv.at[IN_SEM + 1])
    load_x = pltpu.make_async_copy(x_hbm, xf.at[e], recv.at[IN_SEM + 2])
    load_g = pltpu.make_async_copy(g_hbm, gf.at[e], recv.at[IN_SEM + 3])
    load_vectors = [pltpu.make_async_copy(src, dst, recv.at[IN_SEM + 4 + i]) for i, (src, dst) in enumerate(
        ((sc_hbm, sc_ref), (sh_hbm, sh_ref), (bu_hbm, bu_ref), (bd_hbm, bd_ref)))]
    load_w1.start()
    load_w2.start()
    for load in load_vectors:
        load.start()
    load_x.start()
    load_g.start()

    load_w1.wait()
    turned = w1v[...].astype(F32)
    turned = jnp.concatenate([turned, jnp.zeros((LANES - unit, 2 * fb), F32)], axis=0).T
    for k in range(RING):
        for h in range(2):
            st1[k, h] = pack(turned[(2 * k + h) * unit:(2 * k + h + 1) * unit, 0:unit]).astype(BF16)

    for load in load_vectors:
        load.wait()
    lnv[e, 0:1] = sc_ref[...].reshape(1, half)
    lnv[e, 1:2] = sh_ref[...].reshape(1, half)
    bi[c] = bu_ref[...].astype(F32).reshape(1, 2 * fb)

    pl.semaphore_wait(barrier, len(peers))

    rc(w2_hbm.at[pl.ds(pl.multiple_of(other * unit, 16), unit)], l2.at[e], P2, partner).start()
    rc(st1.at[r, other], l1.at[r, e], P1 + other, partner, P1 + e).start()
    for k in (2, 1, 3):
        for h in range(2):
            rc(st1.at[wrap(r + k), h], l1.at[r, e], P1 + 2 * k + h,
               {"row": wrap(r + k), "col": c, "dep": h}, P1 + 2 * k + e).start()
    rc(lnv.at[e], lnv.at[e], DLN, partner).start()
    rc(x_hbm, xf.at[e], DX, partner).start()
    rc(g_hbm, gf.at[e], DG, partner).start()
    for k in range(1, RING):
        rc(bi.at[c], bi.at[c], BI + k, {"row": r, "col": wrap(c + k), "dep": e}).start()
    l1[r, e] = st1[r, e]

    def w1u(b, s):
        return wg.at[0, b, s]

    def w2u(b, s):
        return wg.at[1, b, s]

    load_w2.wait()
    arrive(l2.at[other], P2)
    wg[1, p, q, :, 0:half] = l2[0]
    wg[1, p, q, :, half:width] = l2[1]
    go(w2u(p, q), M2, m_right)
    go(w2u(p, q), S2, s_right)
    go(w2u(p, q), S4, s_left)
    go(w2u(p, q), M6, m_left)

    arrive(l1.at[r, other], P1 + other)
    for k in range(1, RING):
        for h in range(2):
            arrive(l1.at[wrap(r - k), h], P1 + 2 * k + h)
    wg[0, p, q] = jnp.concatenate([unpack(l1[k, h].astype(F32)) for h in range(2) for k in range(RING)], axis=1).astype(BF16)
    go(w1u(p, q), M1, m_left)
    go(w1u(p, q), S1, s_right)
    go(w1u(p, q), S3, s_left)
    go(w1u(p, q), M5, m_right)

    arrive(w2u(p, ql), S2)
    go(w2u(p, ql), S6, s_right)
    arrive(w2u(p, qr), S4)
    go(w2u(p, qr), M2 + 1, m_right)
    go(w2u(p, ql), M2 + 2, m_right)
    go(w2u(p, qr), M6 + 1, m_left)
    go(w2u(p, ql), M6 + 2, m_left)

    def nth(t):
        return wrap(q + gray(t))

    arrive(lnv.at[other], DLN)
    load_x.wait()
    arrive(xf.at[other], DX)
    load_g.wait()
    arrive(gf.at[other], DG)
    vv[...] = jnp.zeros_like(vv)
    def norm_tile(t, carry):
        rows = pl.ds(pl.multiple_of(t * tile, tile), tile)
        x0, x1 = xf[0, rows].astype(F32), xf[1, rows].astype(F32)
        total = jnp.sum(x0, axis=1, keepdims=True) + jnp.sum(x1, axis=1, keepdims=True)
        squares = jnp.sum(x0 * x0, axis=1, keepdims=True) + jnp.sum(x1 * x1, axis=1, keepdims=True)
        mean = total / width
        inv = lax.rsqrt(squares / width - mean * mean + LN_EPS)
        mean_s[rows] = mean
        inv_s[rows] = inv
        ab[rows, 0:half] = ((x0 - mean) * inv * lnv[0, 0:1] + lnv[0, 1:2]).astype(BF16)
        ab[rows, half:width] = ((x1 - mean) * inv * lnv[1, 0:1] + lnv[1, 1:2]).astype(BF16)
        gb[rows, 0:half] = gf[0, rows]
        gb[rows, half:width] = gf[1, rows]
        vv[RING:RING + 1] += jnp.sum(gf[e, rows].astype(F32), axis=0, keepdims=True)
        return carry

    lax.fori_loop(0, n_tiles // 2, norm_tile, 0)
    arrive(w1u(p, qr), S3)
    go(w1u(p, qr), S5, s_left)
    go(w1u(p, qr), M1 + 1, m_left)
    lax.fori_loop(n_tiles // 2, n_tiles, norm_tile, 0)

    def relay1(t):
        arrive(w1u(pr, nth(t)), M1 + t)
        go(w1u(pr, nth(t)), M3 + t, m_left)

    def relay2(t):
        arrive(w2u(pl_, nth(t)), M2 + t)
        go(w2u(pl_, nth(t)), M4 + t, m_right)

    arrive(w1u(p, ql), S1)
    go(w1u(p, ql), M1 + 2, m_left)
    relay2(0)
    for k in range(1, RING):
        arrive(bi.at[wrap(c - k)], BI + k)
    for b in range(RING):
        for k in range(RING):
            flat = bi[b, 0:1, 2 * k * unit:(2 * k + 1) * unit]
            across = bi[k, 0:1, (2 * b + 1) * unit:(2 * b + 2) * unit]
            bias_u[b, k, 0:1, 0:unit] = jnp.where(e == 0, flat, across)
    arrive(w2u(p, qo), S6)
    go(w2u(p, qo), M2 + 3, m_right)
    relay1(0)
    relay2(1)
    arrive(w1u(p, qo), S5)
    go(w1u(p, qo), M1 + 3, m_left)
    relay2(2)

    def block(slot, b, hook=None, send_part=None):
        bias = jnp.concatenate([bias_u[b, u, 0:1, 0:unit] for u in range(RING)], axis=1)

        def block_tile(t, carry):
            rows = pl.ds(pl.multiple_of(t * tile, tile), tile)
            pre = dot(ab[rows, :], wg[0, b].reshape(fb, width), ((1,), (1,))) + bias
            squared = pre * pre
            tanh_val = jnp.tanh(GELU_K * (pre + GELU_C * pre * squared))
            hs[slot, rows] = (0.5 * pre * (1.0 + tanh_val)).astype(BF16)
            slope = 0.5 * (1.0 + tanh_val) + 0.5 * pre * (1.0 - tanh_val * tanh_val) * GELU_K * (1.0 + 3.0 * GELU_C * squared)
            pre_grad = dot(gb[rows, :], wg[1, b].reshape(fb, width), ((1,), (1,))) * slope
            vv[pl.ds(b, 1)] += jnp.sum(pre_grad, axis=0, keepdims=True)
            dcs[slot, rows] = pre_grad.astype(BF16)
            if hook is not None:
                hook(t)
            return carry

        lax.fori_loop(0, n_tiles, block_tile, 0)
        for i, (rows_of, columns_of) in enumerate(((dcs, ab), (hs, gb))):
            gw[i, b] = dot(rows_of[slot], columns_of[...], ((0,), (0,))).reshape(RING, unit, width)
            if send_part is not None:
                send_part(i)

    def half_block(slot, b, part, units, send_part):
        bias = jnp.concatenate([bias_u[b, u, 0:1, 0:unit] for u in units], axis=1)
        columns = slice(2 * part * unit, 2 * (part + 1) * unit)

        def half_tile(t, carry):
            rows = pl.ds(pl.multiple_of(t * tile, tile), tile)
            w1, w2 = (jnp.concatenate([wg[i, b, u] for u in units], axis=0) for i in range(2))
            pre = dot(ab[rows, :], w1, ((1,), (1,))) + bias
            squared = pre * pre
            tanh_val = jnp.tanh(GELU_K * (pre + GELU_C * pre * squared))
            hidden = (0.5 * pre * (1.0 + tanh_val)).astype(BF16)
            hs2[rows, :] = hidden
            hs[slot, rows, columns] = hidden
            slope = 0.5 * (1.0 + tanh_val) + 0.5 * pre * (1.0 - tanh_val * tanh_val) * GELU_K * (1.0 + 3.0 * GELU_C * squared)
            pre_grad = dot(gb[rows, :], w2, ((1,), (1,))) * slope
            sums = jnp.sum(pre_grad, axis=0, keepdims=True)
            for j, u in enumerate(units):
                db_u[u, 0:1, 0:unit] += sums[:, j * unit:(j + 1) * unit]
            lowp = pre_grad.astype(BF16)
            dcs2[rows, :] = lowp
            dcs[slot, rows, columns] = lowp
            return carry

        lax.fori_loop(0, n_tiles, half_tile, 0)
        for i, (rows_of, columns_of) in enumerate(((dcs2, ab), (hs2, gb))):
            out = dot(rows_of[...], columns_of[...], ((0,), (0,)))
            for j, u in enumerate(units):
                gw[i, b, u] = out[j * unit:(j + 1) * unit]
            send_part(i)

    def relay_gather(t):
        @pl.when(t == 0)
        def _():
            relay1(1)

        @pl.when(t == 1)
        def _():
            relay1(2)
            relay2(3)

    assert n_tiles == RING
    block(0, p, hook=relay_gather)
    relay1(3)
    for t in range(1, RING):
        go(w1u(p, nth(t)), M5 + t, m_right)
    go(w2u(p, qo), M6 + 3, m_left)

    def back1(t):
        return wrap(q - gray(RING - 1 - t))

    def back2(t):
        return wrap(q + gray(RING - 1 - t))

    db_u[...] = jnp.zeros_like(db_u)
    for part in range(2):
        mine = (2 * part, 2 * part + 1)
        for t in mine:
            arrive(w2u(po, nth(t)), M4 + t)
            arrive(w1u(po, nth(t)), M3 + t)

        def send_opposite(i):
            for t in mine:
                u = nth(t)
                rc(gw.at[i, po, u], opp.at[i, u], (R2 if i else R1) + t, m_right if i else m_left).start()

        half_block(1, po, part, tuple(nth(t) for t in mine), send_opposite)
    vv[pl.ds(po, 1)] = jnp.concatenate([db_u[u, 0:1, 0:unit] for u in range(RING)], axis=1)

    for t in range(RING):
        arrive(w2u(pr, nth(t)), M6 + t)
    def send_right(i):
        if i == 0:
            rc(gw.at[0, pr], dirs.at[0], R3, m_right).start()

    block(2, pr, send_part=send_right)
    for t in range(RING):
        arrive(w1u(pl_, nth(t)), M5 + t)
    block(3, pl_)

    def direct2(t):
        u = back2(t)
        rc(gw.at[1, pl_, u], dirs.at[1, u], R4 + t, m_left).start()

    direct2(0)
    direct2(1)

    def product_tile(t, carry):
        rows = pl.ds(pl.multiple_of(t * tile, tile), tile)
        for i, (left, acc) in enumerate(((dcs, da_acc), (hs, y_acc))):
            weights = jnp.concatenate([wg[i, p].reshape(fb, width)] + [wg[i, po, nth(k)] for k in range(RING)]
                                      + [wg[i, b].reshape(fb, width) for b in (pr, pl_)], axis=0)
            out = dot(jnp.concatenate([left[slot, rows] for slot in range(RING)], axis=1), weights)
            acc[0, rows] = out[:, 0:half]
            acc[1, rows] = out[:, half:width]
        return carry

    lax.fori_loop(0, n_tiles, product_tile, 0)

    rc(y_acc.at[other], yr, EY, partner).start()
    rc(da_acc.at[other], dar, ED, partner).start()

    for t in range(RING):
        u1, u2 = back1(t), back2(t)
        arrive(opp.at[1, u2], R2 + (3, 2, 1, 0)[t])
        gw[1, pr, u2] += opp[1, u2]
        rc(gw.at[1, pr, u2], rel.at[1, u2], R6 + t, m_right).start()
        arrive(opp.at[0, u1], R1 + (3, 1, 2, 0)[t])
        gw[0, pl_, u1] += opp[0, u1]
        rc(gw.at[0, pl_, u1], rel.at[0, u1], R5 + t, m_left).start()
    direct2(2)
    direct2(3)

    lane = lax.broadcasted_iota(jnp.int32, (tile, 128), 1)

    def stat_tile(t, carry):
        rows = pl.ds(pl.multiple_of(t * tile, tile), tile)
        mean, inv = mean_s[rows], inv_s[rows]
        v0 = da_acc[0, rows] * lnv[0, 0:1]
        v1 = da_acc[1, rows] * lnv[1, 0:1]
        h0 = (xf[0, rows].astype(F32) - mean) * inv
        h1 = (xf[1, rows].astype(F32) - mean) * inv
        one = jnp.sum(v0, axis=1, keepdims=True) + jnp.sum(v1, axis=1, keepdims=True)
        two = jnp.sum(v0 * h0, axis=1, keepdims=True) + jnp.sum(v1 * h1, axis=1, keepdims=True)
        stat[rows] = jnp.where(lane < 64, one, two)
        return carry

    lax.fori_loop(0, n_tiles, stat_tile, 0)
    rc(stat, statr, ES, partner).start()

    arrive(yr, EY)
    arrive(dar, ED)
    arrive(statr, ES)
    b_down = bd_ref[...].astype(F32).reshape(1, half)

    def out_tile(t, carry):
        rows = pl.ds(pl.multiple_of(t * tile, tile), tile)
        x_own = xf[e, rows].astype(F32)
        y_ref[rows] = (x_own + (y_acc[e, rows] + yr[rows]) + b_down).astype(BF16)
        norm_grad = da_acc[e, rows] + dar[rows]
        sums = (stat[rows] + statr[rows]) / width
        inv = inv_s[rows]
        x_hat = (x_own - mean_s[rows]) * inv
        value = norm_grad * lnv[e, 0:1]
        dx_ref[rows] = (gf[e, rows].astype(F32) + inv * (value - sums[:, 0:1] - x_hat * sums[:, 64:65])).astype(BF16)
        vv[RING + 1:RING + 2] += jnp.sum(norm_grad * x_hat, axis=0, keepdims=True)
        vv[RING + 2:RING + 3] += jnp.sum(norm_grad, axis=0, keepdims=True)
        return carry

    lax.fori_loop(0, n_tiles, out_tile, 0)

    vs[q] = vv[...]
    for k, d in ((1, s_right), (2, s_opp_dev), (3, s_left)):
        go(vs.at[q], VS + k, d)
    for k in range(1, RING):
        arrive(vs.at[wrap(q - k)], VS + k)
    vm[p] = ((vs[0] + vs[1]) + vs[2]) + vs[3]
    for k, d in ((1, m_right), (2, m_opp), (3, m_left)):
        go(vm.at[p], VM + k, d)

    sent(l2.at[0], P2)
    sent(l1.at[0, 0], P1 + other)
    for k in range(1, RING):
        for h in range(2):
            sent(l1.at[0, 0], P1 + 2 * k + h)
        sent(bi.at[c], BI + k)
        sent(vs.at[q], VS + k)
    sent(lnv.at[0], DLN)
    sent(x_hbm, DX)
    sent(g_hbm, DG)
    for sem in (S1, S2, S3, S4, S5, S6):
        sent(w1u(p, q), sem)
    for t in range(RING):
        for sem in (M1, M2, M3, M4, M5, M6):
            sent(w1u(p, q), sem + t)
        for sem in (R1, R2):
            sent(gw.at[0, p, q], sem + t)
    sent(yr, EY)
    sent(dar, ED)
    sent(stat, ES)
    sent(gw.at[0, p, q], R4)
    sent(gw.at[0, p, q], R4 + 1)

    arrive(dirs.at[0], R3)

    def reduce1(t):
        u = back1(t)
        arrive(rel.at[0, u], R5 + t)
        gw[0, p, u] += dirs[0, u] + rel[0, u]
        if t == 0:
            rc(gw.at[0, p, u], s_opp.at[0], Q1, s_left).start()
        if t == 1:
            rc(gw.at[0, p, u], s_dir.at[0], Q3, s_right).start()
        if t == 2:
            arrive(s_opp.at[0], Q1)
            gw[0, p, u] += s_opp[0]
            rc(gw.at[0, p, u], s_rel.at[0], Q5, s_left).start()

    def reduce2(t):
        u = back2(t)
        arrive(dirs.at[1, u], R4 + t)
        arrive(rel.at[1, u], R6 + t)
        gw[1, p, u] += dirs[1, u] + rel[1, u]
        if t == 0:
            rc(gw.at[1, p, u], s_opp.at[1], Q2, s_right).start()
        if t == 1:
            rc(gw.at[1, p, u], s_dir.at[1], Q4, s_left).start()
        if t == 2:
            arrive(s_opp.at[1], Q2)
            gw[1, p, u] += s_opp[1]
            rc(gw.at[1, p, u], s_rel.at[1], Q6, s_right).start()

    reduce1(0)
    reduce1(1)
    reduce2(0)
    reduce1(2)
    reduce2(1)
    reduce1(3)
    reduce2(2)

    arrive(s_dir.at[0], Q3)
    arrive(s_rel.at[0], Q5)
    done1 = gw[0, p, q] + s_dir[0] + s_rel[0]
    for k in range(RING):
        for h in range(2):
            start = (h * RING + k) * unit
            f1[k, h] = pack(done1[:, start:start + unit]).astype(BF16)
    for k in (2, 1, 3):
        for h in range(2):
            rc(f1.at[wrap(r + k), h], f1l.at[r, e], F1 + 2 * k + h,
               {"row": wrap(r + k), "col": c, "dep": h}, F1 + 2 * k + e).start()
    rc(f1.at[r, other], f1l.at[r, e], F1 + other, partner, F1 + e).start()
    f1l[r, e] = f1[r, e]
    reduce2(3)
    arrive(s_dir.at[1], Q4)
    arrive(s_rel.at[1], Q6)
    done2 = (gw[1, p, q] + s_dir[1] + s_rel[1]).astype(BF16)
    f2[0] = done2[:, 0:half]
    f2[1] = done2[:, half:width]
    rc(f2.at[other], f2l.at[e], F2, partner).start()
    f2l[e] = f2[e]
    for k in range(1, RING):
        arrive(vm.at[wrap(p - k)], VM + k)
    vp[e] = ((vm[0] + vm[1]) + vm[2]) + vm[3]
    go(vp.at[e], VP, partner)

    arrive(vp.at[other], VP)
    pieces = []
    for k in range(RING):
        pieces.append(vp[0, pl.ds(c, 1)][:, k * unit:(k + 1) * unit])
        row = vp[1, k:k + 1]
        piece = row[:, 0:unit]
        for j in range(1, RING):
            piece = jnp.where(c == j, row[:, j * unit:(j + 1) * unit], piece)
        pieces.append(piece)
    dbu_ref[...] = jnp.concatenate(pieces, axis=1).reshape(dbu_ref.shape)
    dbd_ref[...] = vp[e, RING:RING + 1].reshape(dbd_ref.shape)
    dsc_ref[...] = vp[e, RING + 1:RING + 2].reshape(dsc_ref.shape)
    dsh_ref[...] = vp[e, RING + 2:RING + 3].reshape(dsh_ref.shape)

    sent(f1.at[0, 0], F1 + other)
    for k in range(1, RING):
        for h in range(2):
            sent(f1.at[0, 0], F1 + 2 * k + h)
        sent(vm.at[p], VM + k)
    sent(f2.at[0], F2)
    for sem in [R5 + t for t in range(RING)] + [R6 + t for t in range(RING)] + [R4 + 2, R4 + 3, Q1, Q2, Q3, Q4, Q5, Q6]:
        sent(gw.at[0, p, q], sem)
    sent(gw.at[0, p], R3)
    sent(vp.at[e], VP)

    arrive(f2l.at[other], F2)
    dw2_ref[0:unit] = f2l[0]
    dw2_ref[unit:2 * unit] = f2l[1]
    arrive(f1l.at[r, other], F1 + other)
    for k in range(1, RING):
        for h in range(2):
            arrive(f1l.at[wrap(r - k), h], F1 + 2 * k + h)
    turned = jnp.concatenate([unpack(f1l[k, h].astype(F32)) for k in range(RING) for h in range(2)], axis=0)
    turned = jnp.concatenate([turned, jnp.zeros((2 * fb, LANES - unit), F32)], axis=1)
    dw1_ref[...] = turned.T[0:unit].astype(BF16)


def copy_out(*refs):
    n = len(refs) // 2
    copies = [pltpu.make_async_copy(refs[i], refs[n + i], refs[2 * n].at[i]) for i in range(n)]
    for copy in copies:
        copy.start()
    for copy in copies:
        copy.wait()


def solution(mesh):
    assert mesh.shape["row"] == RING and mesh.shape["col"] == RING and mesh.shape["dep"] == 2
    tok_spec = P(("part", "row", "col"), "dep")
    vec_dep = P("dep")
    part_dep = P(("part", "dep"))
    in_specs = (tok_spec, vec_dep, vec_dep, P(("dep", "row"), "col"), P("col"), P(("col", "row"), "dep"), vec_dep, tok_spec)
    out_specs = (tok_spec, tok_spec, P(("part", "dep", "row"), "col"), P(("part", "col")), P(("part", "col", "row"), "dep"), part_dep, part_dep, part_dep)

    def local_step(x_in, ln_scale, ln_shift, w_up, b_up, w_down, b_down, y_grad):
        tokens, half = x_in.shape
        width = 2 * half
        unit = w_down.shape[0] // 2
        fb = RING * unit
        assert w_up.shape == (unit, 2 * fb) and half == RING * unit and fb == half
        tile = tokens // RING
        packed = (RING, 2, 3 * unit // 4, LANES)
        assert 3 * LANES == 4 * unit
        hbm_spec = pl.BlockSpec(memory_space=pltpu.HBM)
        vmem_spec = pl.BlockSpec(memory_space=pltpu.VMEM)
        vmem = pltpu.VMEM
        scratch = [
            vmem((unit, 2 * fb), BF16),
            vmem(packed, BF16), vmem(packed, BF16), vmem((2, unit, half), BF16),
            vmem((2, tokens, half), BF16), vmem((2, tokens, half), BF16),
            vmem((2, 8, half), F32),
            vmem((2, RING, RING, unit, width), BF16),
            vmem((RING, 1, 2 * fb), F32), vmem((RING, RING, 8, LANES), F32),
            vmem((tokens, width), BF16), vmem((tokens, width), BF16),
            vmem((tokens, 1), F32), vmem((tokens, 1), F32),
            vmem((2, tokens, half), F32), vmem((2, tokens, half), F32),
            vmem((tokens, half), F32), vmem((tokens, half), F32),
            vmem((tokens, 128), F32), vmem((tokens, 128), F32),
            vmem((RING, tokens, fb), BF16), vmem((RING, tokens, fb), BF16),
            vmem((tokens, 2 * unit), BF16), vmem((tokens, 2 * unit), BF16), vmem((RING, 8, LANES), F32),
            vmem((2, RING, RING, unit, width), F32),
            vmem((2, RING, unit, width), F32), vmem((2, RING, unit, width), F32), vmem((2, RING, unit, width), F32),
            vmem((2, unit, width), F32), vmem((2, unit, width), F32), vmem((2, unit, width), F32),
            vmem((8, half), F32), vmem((RING, 8, half), F32), vmem((RING, 8, half), F32), vmem((2, 8, half), F32),
            vmem(packed, BF16), vmem(packed, BF16),
            vmem((2, unit, half), BF16), vmem((2, unit, half), BF16),
            vmem((half,), F32), vmem((half,), F32), vmem((2 * fb,), BF16), vmem((half,), BF16),
            pltpu.SemaphoreType.DMA((N_SEM,)), pltpu.SemaphoreType.DMA((N_SEM,)),
        ]
        shapes = (
            jax.ShapeDtypeStruct((tokens, half), BF16), jax.ShapeDtypeStruct((tokens, half), BF16),
            jax.ShapeDtypeStruct(w_up.shape, BF16), jax.ShapeDtypeStruct(b_up.shape, F32),
            jax.ShapeDtypeStruct(w_down.shape, BF16), jax.ShapeDtypeStruct((half,), F32),
            jax.ShapeDtypeStruct((half,), F32), jax.ShapeDtypeStruct((half,), F32))
        outs = pl.pallas_call(
            functools.partial(kernel, tile),
            out_shape=shapes,
            in_specs=[hbm_spec] * 8,
            out_specs=(vmem_spec,) * 8,
            scratch_shapes=scratch,
            compiler_params=pltpu.CompilerParams(collective_id=0, has_side_effects=True, vmem_limit_bytes=51 * 1024 * 1024),
        )(*(pltpu.with_memory_space_constraint(v, pltpu.HBM) for v in (x_in, ln_scale, ln_shift, w_up, b_up, w_down, b_down, y_grad)))
        return pl.pallas_call(
            copy_out,
            out_shape=shapes,
            in_specs=[vmem_spec] * len(shapes),
            out_specs=(hbm_spec,) * len(shapes),
            scratch_shapes=[pltpu.SemaphoreType.DMA((len(shapes),))],
            compiler_params=pltpu.CompilerParams(vmem_limit_bytes=4 * 1024 * 1024),
        )(*outs)

    return jax.shard_map(local_step, mesh=mesh, in_specs=in_specs, out_specs=out_specs, check_vma=False)
```
